32 devices in a mesh: fsdp: 4 (over x, core), rep: 8 (over z, y).
Axes of the slice: x: 2, y: 2, z: 4, core: 2. Of those that a mesh axis runs over, the one named last changes fastest.
Arguments:
- tokens: bfloat16 [12288, 1024], P(('fsdp', 'rep')), may hold values from -6 to 6
- out_grad: bfloat16 [12288, 1024], P(('fsdp', 'rep')), may hold values from -6 to 6
- norm1_gain: bfloat16 [1024], P('fsdp'), may hold values from 0.5 to 1.5
- norm1_bias: bfloat16 [1024], P('fsdp'), may hold values from -1.5 to 1.5
- w_qkv: bfloat16 [1024, 3072], P('fsdp'), may hold values from -0.1875 to 0.1875
- q_bias: bfloat16 [1024], P('fsdp'), may hold values from -2.5 to 2.5
- v_bias: bfloat16 [1024], P('fsdp'), may hold values from -2.5 to 2.5
- w_out: bfloat16 [1024, 1024], P('fsdp'), may hold values from -2 to 2
- out_bias: bfloat16 [1024], P('fsdp'), may hold values from -1.5 to 1.5
- attn_scale: bfloat16 [1024], P('fsdp'), may hold values from 0.5 to 1.5
- norm2_gain: bfloat16 [1024], P('fsdp'), may hold values from 0.5 to 1.5
- norm2_bias: bfloat16 [1024], P('fsdp'), may hold values from -1.5 to 1.5
- w_up: bfloat16 [1024, 4096], P('fsdp'), may hold values from -0.1875 to 0.1875
- up_bias: bfloat16 [4096], P('fsdp'), may hold values from -2.5 to 2.5
- w_down: bfloat16 [4096, 1024], P('fsdp'), may hold values from -0.09375 to 0.09375
- down_bias: bfloat16 [1024], P('fsdp'), may hold values from -1.5 to 1.5
- mlp_scale: bfloat16 [1024], P('fsdp'), may hold values from 0.5 to 1.5
- image_ids: int32 [12288], P(('fsdp', 'rep')), may hold values from 0 to 7, as said below
- pad_mask: int32 [12288], P(('fsdp', 'rep')), may hold values from 0 to 1, as said below
Outputs:
- layer_out: bfloat16 [12288, 1024], P(('fsdp', 'rep'))
- tokens_grad: bfloat16 [12288, 1024], P(('fsdp', 'rep'))
- norm1_gain_grad: float32 [1024], P('fsdp')
- norm1_bias_grad: float32 [1024], P('fsdp')
- w_qkv_grad: float32 [1024, 3072], P('fsdp')
- q_bias_grad: float32 [1024], P('fsdp')
- v_bias_grad: float32 [1024], P('fsdp')
- w_out_grad: float32 [1024, 1024], P('fsdp')
- out_bias_grad: float32 [1024], P('fsdp')
- attn_scale_grad: float32 [1024], P('fsdp')
- norm2_gain_grad: float32 [1024], P('fsdp')
- norm2_bias_grad: float32 [1024], P('fsdp')
- w_up_grad: float32 [1024, 4096], P('fsdp')
- up_bias_grad: float32 [4096], P('fsdp')
- w_down_grad: float32 [4096, 1024], P('fsdp')
- down_bias_grad: float32 [1024], P('fsdp')
- mlp_scale_grad: float32 [1024], P('fsdp')
The draws below stay inside these ranges and needn't reach their ends.
Inputs may be any that keep to these rules, and one draw needn't show every extreme that they name: `image_ids`: nondecreasing along the tokens. The tokens with pad_mask 1 and one image number are 1370 consecutive tokens, and every number from 0 to 7 has such a run. A pad token carries the number of the image before it, or 0 before the first image. `pad_mask`: pad tokens lie only before, between or after the images' runs.
All inputs are finite; a program needn't handle non-finite values.
Results may differ from the reference program's by a relative error of at most 0.01.
Values may be sent and summed in bfloat16 or wider, within the bound.
A program may use at most 192 MiB of HBM per device.

```python
import jax
import jax.numpy as jnp
from jax import lax

D = 1024
HEADS = 16
HEAD_DIM = 64
FF = 4096
IMG = 1370
TOK_DEV = 384
TOKENS = 12288
IMAGES = 8
REACH = 4


def packed_layout(seed_key):
    spare = TOKENS - IMAGES * IMG
    offsets = jnp.sort(jax.random.randint(seed_key, (IMAGES,), 0, spare + 1))
    starts = jnp.arange(IMAGES, dtype=jnp.int32) * IMG + offsets.astype(jnp.int32)
    position = jnp.arange(TOKENS, dtype=jnp.int32)
    counted = jnp.searchsorted(starts, position, side='right').astype(jnp.int32)
    number = jnp.maximum(counted - 1, 0)
    inside = (counted > 0) & (position < jnp.take(starts, number) + IMG)
    return (number, inside.astype(jnp.int32))


def draw_image_ids(key, part):
    return packed_layout(jax.random.fold_in(key, 11))[0]


def draw_pad_mask(key, part):
    return packed_layout(jax.random.fold_in(key, 11))[1]


def level_of(key, shape, cuts, least, top_value):
    def one(axis_at, shards_of):
        heights = jax.random.uniform(jax.random.fold_in(jax.random.fold_in(key, 6), axis_at), (shards_of,), jnp.float32, least / len(cuts), top_value / len(cuts))
        return jnp.repeat(jnp.exp(heights), shape[axis_at] // shards_of).reshape((-1,) + (1,) * (len(shape) - axis_at - 1))

    level = one(*cuts[0])
    for cut in cuts[1:]:
        level = level * one(*cut)
    return level


def bell_draw(rng, extent, scale, limit, shards=(), kind=jnp.bfloat16):
    entries = jax.random.normal(rng, extent, jnp.float32) * scale
    if len(shards) > 0:
        entries = level_of(rng, extent, shards, -0.22, 0.18) * entries
    return jnp.clip(entries, min=-limit, max=limit).astype(kind)


def setup_inputs(seed: int = 0) -> dict:
    key_list = jax.random.split(jax.random.key(seed), 20)
    tokens = bell_draw(key_list[0], (TOKENS, D), 1.0, 6.0, ((0, 32),))
    out_grad = bell_draw(key_list[1], (TOKENS, D), 1.0, 6.0, ((0, 32),))
    norm1_gain = jnp.clip(1.0 + 0.1 * jax.random.normal(key_list[2], (D,), jnp.float32), 0.5, 1.5).astype(jnp.bfloat16)
    norm1_bias = bell_draw(key_list[3], (D,), 0.3, 1.5, ((0, 4),))
    w_qkv = bell_draw(key_list[4], (D, 3 * D), D ** -0.5, 0.1875, ((0, 4),))
    q_bias = bell_draw(key_list[5], (D,), 0.5, 2.5, ((0, 4),))
    v_bias = bell_draw(key_list[6], (D,), 0.5, 2.5, ((0, 4),))
    w_out = bell_draw(key_list[7], (D, D), (max(D // 128, 1)) ** -0.5, 2.0, ((0, 4),))
    out_bias = bell_draw(key_list[8], (D,), 0.3, 1.5, ((0, 4),))
    attn_scale = jnp.clip(0.5 + 1.0 * jax.random.uniform(key_list[9], (D,), jnp.float32) ** level_of(key_list[9], (D,), ((0, 4),), -0.2, 0.2), 0.5, 1.5).astype(jnp.bfloat16)
    norm2_gain = jnp.clip(1.0 + 0.1 * jax.random.normal(key_list[10], (D,), jnp.float32), 0.5, 1.5).astype(jnp.bfloat16)
    norm2_bias = bell_draw(key_list[11], (D,), 0.3, 1.5, ((0, 4),))
    w_up = bell_draw(key_list[12], (D, FF), D ** -0.5, 0.1875, ((0, 4),))
    up_bias = bell_draw(key_list[13], (FF,), 0.5, 2.5, ((0, 4),))
    w_down = bell_draw(key_list[14], (FF, D), FF ** -0.5, 0.09375, ((0, 4),))
    down_bias = bell_draw(key_list[15], (D,), 0.3, 1.5, ((0, 4),))
    mlp_scale = jnp.clip(0.5 + 1.0 * jax.random.uniform(key_list[16], (D,), jnp.float32) ** level_of(key_list[16], (D,), ((0, 4),), -0.2, 0.2), 0.5, 1.5).astype(jnp.bfloat16)
    image_ids = draw_image_ids(jax.random.fold_in(key_list[19], 71), 0)
    pad_mask = draw_pad_mask(jax.random.fold_in(key_list[19], 71), 0)
    return {"tokens": tokens, "out_grad": out_grad, "norm1_gain": norm1_gain, "norm1_bias": norm1_bias, "w_qkv": w_qkv, "q_bias": q_bias, "v_bias": v_bias, "w_out": w_out, "out_bias": out_bias, "attn_scale": attn_scale, "norm2_gain": norm2_gain, "norm2_bias": norm2_bias, "w_up": w_up, "up_bias": up_bias, "w_down": w_down, "down_bias": down_bias, "mlp_scale": mlp_scale, "image_ids": image_ids, "pad_mask": pad_mask}


@jax.custom_vjp
def low(v):
    return lax.optimization_barrier(v.astype(jnp.bfloat16)).astype(jnp.float32)

@jax.custom_vjp
def low_back(v):
    return v

def low_keep(v):
    return (low(v), None)

def low_pass(kept, grad):
    return (grad,)

def back_keep(v):
    return (v, None)

def back_low(kept, grad):
    return (low(grad),)
low.defvjp(low_keep, low_pass)
low_back.defvjp(back_keep, back_low)
EPSILON = 1e-06
NEG_BIG = -1e+30

def layer_norm(values, gain, shift):
    center = lax.optimization_barrier(jnp.mean(values, axis=-1, keepdims=True))
    centered = values - center
    spread = lax.optimization_barrier(jnp.mean(centered * centered, axis=-1, keepdims=True))
    return centered * lax.rsqrt(spread + EPSILON) * gain + shift

def product(left, right):
    return jnp.dot(left, right, precision=lax.Precision.HIGHEST, preferred_element_type=jnp.float32)

def reference(tokens, out_grad, norm1_gain, norm1_bias, w_qkv, q_bias, v_bias, w_out, out_bias, attn_scale, norm2_gain, norm2_bias, w_up, up_bias, w_down, down_bias, mlp_scale, image_ids, pad_mask):
    blocks = TOKENS // TOK_DEV
    window = 2 * REACH + 1
    factor = HEAD_DIM ** (-0.5)
    ids_block = image_ids.reshape(blocks, TOK_DEV)
    mask_block = pad_mask.reshape(blocks, TOK_DEV)
    edge_ids = jnp.full((REACH, TOK_DEV), -1, jnp.int32)
    edge_mask = jnp.zeros((REACH, TOK_DEV), jnp.int32)
    ids_padded = jnp.concatenate([edge_ids, ids_block, edge_ids], axis=0)
    mask_padded = jnp.concatenate([edge_mask, mask_block, edge_mask], axis=0)

    def layer(inputs, gain_first, shift_first, wide_qkv, query_bias, value_bias, wide_out, proj_bias, attn_gamma, gain_second, shift_second, wide_up, hidden_bias, wide_down, final_bias, mlp_gamma):
        rows_block = inputs.reshape(blocks, TOK_DEV, D)

        def project(rows):
            act_one = low(layer_norm(rows, gain_first, shift_first))
            qkv_rows = product(act_one, wide_qkv)
            query = low((low_back(qkv_rows[:, :D]) + query_bias) * factor)
            keys = low(low_back(qkv_rows[:, D:2 * D]))
            values = low(low_back(qkv_rows[:, 2 * D:]) + value_bias)
            return (query, keys, values)
        query, keys, values = lax.map(jax.checkpoint(project), rows_block)
        zero_rows = jnp.zeros((REACH, TOK_DEV, D), jnp.float32)
        keys_padded = jnp.concatenate([zero_rows, keys, zero_rows], axis=0)
        values_padded = jnp.concatenate([zero_rows, values, zero_rows], axis=0)

        def attend(packed):
            block_index, query_rows = packed
            key_win = lax.dynamic_slice_in_dim(keys_padded, block_index, window, 0).reshape(window * TOK_DEV, HEADS, HEAD_DIM)
            value_win = lax.dynamic_slice_in_dim(values_padded, block_index, window, 0).reshape(window * TOK_DEV, HEADS, HEAD_DIM)
            ids_win = lax.dynamic_slice_in_dim(ids_padded, block_index, window, 0).reshape(-1)
            mask_win = lax.dynamic_slice_in_dim(mask_padded, block_index, window, 0).reshape(-1)
            ids_query = lax.dynamic_slice_in_dim(ids_padded, block_index + REACH, 1, 0).reshape(-1)
            mask_query = lax.dynamic_slice_in_dim(mask_padded, block_index + REACH, 1, 0).reshape(-1)
            allowed = (ids_query[:, None] == ids_win[None, :]) & (mask_query[:, None] > 0) & (mask_win[None, :] > 0)
            query_heads = query_rows.reshape(TOK_DEV, HEADS, HEAD_DIM)
            scores = low_back(jnp.einsum('qhd,khd->hqk', query_heads, key_win, precision=lax.Precision.HIGHEST))
            masked = jnp.where(allowed[None], scores, NEG_BIG)
            row_top = lax.optimization_barrier(jnp.max(masked, axis=2, keepdims=True))
            weights_raw = jnp.where(allowed[None], jnp.exp(masked - row_top), 0.0)
            totals = lax.optimization_barrier(jnp.sum(weights_raw, axis=2, keepdims=True))
            totals = jnp.where(totals > 0, totals, 1.0)
            weights_low = low(weights_raw / totals)
            mixed = jnp.einsum('hqk,khd->qhd', weights_low, value_win, precision=lax.Precision.HIGHEST).reshape(TOK_DEV, D)
            return low(low_back(mixed))
        attn = lax.map(jax.checkpoint(attend), (jnp.arange(blocks, dtype=jnp.int32), query))

        def finish(packed):
            rows, attn_rows = packed
            proj = low_back(product(attn_rows, wide_out)) + proj_bias
            residual = rows + attn_gamma * proj
            act_two = low(layer_norm(residual, gain_second, shift_second))
            pre_act = low_back(product(act_two, wide_up)) + hidden_bias
            hidden = low(jax.nn.gelu(pre_act, approximate=False))
            branch = low_back(product(hidden, wide_down)) + final_bias
            return residual + mlp_gamma * branch
        result = lax.map(jax.checkpoint(finish), (rows_block, attn))
        return result.reshape(TOKENS, D)
    floats = [member.astype(jnp.float32) for member in (tokens, norm1_gain, norm1_bias, w_qkv, q_bias, v_bias, w_out, out_bias, attn_scale, norm2_gain, norm2_bias, w_up, up_bias, w_down, down_bias, mlp_scale)]
    layer_value, pullback = jax.vjp(layer, *floats)
    grads = pullback(out_grad.astype(jnp.float32))
    return (layer_value.astype(jnp.bfloat16), grads[0].astype(jnp.bfloat16), grads[1], grads[2], grads[3], grads[4], grads[5], grads[6], grads[7], grads[8], grads[9], grads[10], grads[11], grads[12], grads[13], grads[14], grads[15])
```

```python
import functools

import jax
import jax.numpy as jnp
from jax import lax
from jax.experimental import pallas as pl
from jax.experimental.pallas import tpu as pltpu
from jax.sharding import PartitionSpec as P

D = 1024
HEADS = 16
HEAD_DIM = 64
IMG = 1370

PAIR = 2 * HEAD_DIM
GROUP = HEADS // 2
BLOCK = 256
HALO = 1408
SLOTS = 63

EPSILON = 1e-06
NEG_BIG = -1e30
NEG_EDGE = -1e29

NT = (((1,), (1,)), ((), ()))


def from_behind(block, axis, distance):
    devices = range(lax.axis_size(axis))
    route = [(i - distance, i) for i in devices if i - distance in devices]
    return lax.ppermute(block, axis, route)


def normalize(values):
    center = jnp.mean(values, axis=-1, keepdims=True)
    centered = values - center
    spread = jnp.mean(centered * centered, axis=-1, keepdims=True)
    scale = lax.rsqrt(spread + EPSILON)
    return centered * scale, scale


def norm_back(cotangent, unit, scale, gain):
    scaled = cotangent * gain
    along = jnp.mean(scaled, axis=-1, keepdims=True)
    across = jnp.mean(scaled * unit, axis=-1, keepdims=True)
    return scale * (scaled - along - unit * across)


def matmul(left, right):
    return jnp.dot(left, right, preferred_element_type=jnp.float32)


def matmul_nt(left, right):
    return jnp.einsum("te,de->td", left, right, preferred_element_type=jnp.float32)


def matmul_tn(left, right):
    return jnp.einsum("td,te->de", left, right, preferred_element_type=jnp.float32)


def fold_rows(values, op):
    return op(values.reshape(values.shape[0] // 8, 8, values.shape[1]), axis=0)


def attend_kernel(meta, q_ref, k_ref, v_ref, o_ref, ot_ref, lse_ref, vt, scores):
    tiles = o_ref.shape[0] // BLOCK
    window = k_ref.shape[1]

    @pl.loop(0, window // BLOCK)
    def _(i):
        at = pl.ds(pl.multiple_of(i * BLOCK, BLOCK), BLOCK)
        vt[:, at] = v_ref[at, :].T

    @pl.loop(0, tiles)
    def _(t):
        start = meta[2 * t]
        count = meta[2 * t + 1]
        rows = pl.ds(pl.multiple_of(t * BLOCK, BLOCK), BLOCK)
        query = [q_ref[h, rows, :] for h in range(2)]

        def score(i, tops):
            at = pl.ds(pl.multiple_of(start + i * BLOCK, 128), BLOCK)
            keep = pl.ds(pl.multiple_of(i * BLOCK, BLOCK), BLOCK)
            new = []
            for h in range(2):
                part = lax.dot_general(
                    k_ref[h, at, :], query[h], NT, preferred_element_type=jnp.float32
                )
                scores[h, keep, :] = part
                new.append(jnp.maximum(tops[h], fold_rows(part, jnp.max)))
            return tuple(new)

        low = jnp.full((8, BLOCK), NEG_BIG, jnp.float32)
        tops = lax.fori_loop(0, count, score, (low, low))
        tops = [jnp.max(top, axis=0, keepdims=True) for top in tops]
        tops = [jnp.where(top < NEG_EDGE, 0.0, top) for top in tops]

        def mix(i, carry):
            at = pl.ds(pl.multiple_of(start + i * BLOCK, 128), BLOCK)
            keep = pl.ds(pl.multiple_of(i * BLOCK, BLOCK), BLOCK)
            new = []
            for h in range(2):
                total, mixed = carry[h]
                weights = jnp.exp(scores[h, keep, :] - tops[h])
                total = total + fold_rows(weights, jnp.sum)
                mixed = mixed + matmul(
                    vt[h * HEAD_DIM : (h + 1) * HEAD_DIM, at], weights.astype(jnp.bfloat16)
                )
                new.append((total, mixed))
            return tuple(new)

        zero = (jnp.zeros((8, BLOCK), jnp.float32), jnp.zeros((HEAD_DIM, BLOCK), jnp.float32))
        done = lax.fori_loop(0, count, mix, (zero, zero))
        outs = []
        for h in range(2):
            total = jnp.sum(done[h][0], axis=0, keepdims=True)
            total = jnp.where(total > 0, total, 1.0)
            lse_ref[h : h + 1, rows] = tops[h] + jnp.log(total)
            outs.append(done[h][1] / total)
        out = jnp.concatenate(outs, axis=0)
        ot_ref[:, rows] = out
        o_ref[rows, :] = out.T.astype(jnp.bfloat16)


def attend(meta, q_aug, k_aug, values):
    rows = q_aug.shape[1]
    window = k_aug.shape[1]
    deepest = (2 * IMG + 3 * BLOCK) // BLOCK * BLOCK
    vmem = pl.BlockSpec(memory_space=pltpu.VMEM)
    return pl.pallas_call(
        attend_kernel,
        out_shape=(
            jax.ShapeDtypeStruct((rows, PAIR), jnp.bfloat16),
            jax.ShapeDtypeStruct((PAIR, rows), jnp.float32),
            jax.ShapeDtypeStruct((8, rows), jnp.float32),
        ),
        in_specs=[pl.BlockSpec(memory_space=pltpu.SMEM), vmem, vmem, vmem],
        out_specs=(vmem, vmem, vmem),
        scratch_shapes=[
            pltpu.VMEM((PAIR, window), jnp.bfloat16),
            pltpu.VMEM((2, deepest, BLOCK), jnp.float32),
        ],
        cost_estimate=pl.CostEstimate(
            flops=4 * rows * 2 * IMG * PAIR, transcendentals=2 * rows * IMG, bytes_accessed=9 << 20
        ),
        name="attend",
    )(meta, q_aug, k_aug, values)


def attend_back_kernel(
    meta, q_ref, k_ref, v_ref, g_ref, ot_ref, lse_ref, dq_ref, dk_ref, dv_ref, kt
):
    tiles = dq_ref.shape[0] // BLOCK
    window = k_ref.shape[1]
    half = lax.broadcasted_iota(jnp.int32, (BLOCK, PAIR), 1) // HEAD_DIM

    @pl.loop(0, window // BLOCK)
    def _(i):
        at = pl.ds(pl.multiple_of(i * BLOCK, BLOCK), BLOCK)
        kt[:, at] = jnp.where(half == 0, k_ref[0, at, :], k_ref[1, at, :]).T
        dk_ref[at, :] = jnp.zeros((BLOCK, PAIR), jnp.float32)
        dv_ref[at, :] = jnp.zeros((BLOCK, PAIR), jnp.float32)

    @pl.loop(0, tiles)
    def _(t):
        start = meta[2 * t]
        count = meta[2 * t + 1]
        rows = pl.ds(pl.multiple_of(t * BLOCK, BLOCK), BLOCK)
        grad = g_ref[rows, :]
        blank = jnp.zeros_like(grad)
        query = [q_ref[h, rows, :] for h in range(2)]
        query_only = jnp.concatenate(
            [jnp.where(half == h, query[h], blank) for h in range(2)], axis=0
        )
        grads = [jnp.where(half == h, grad, blank) for h in range(2)]
        grads_both = jnp.concatenate(grads, axis=0)
        product = grad.astype(jnp.float32).T * ot_ref[:, rows]
        delta = [
            jnp.sum(product[h * HEAD_DIM : (h + 1) * HEAD_DIM], axis=0, keepdims=True)
            for h in range(2)
        ]
        lse = [lse_ref[h : h + 1, rows] for h in range(2)]

        def step(i, carry):
            at = pl.ds(pl.multiple_of(start + i * BLOCK, 128), BLOCK)
            value = v_ref[at, :]
            probs, slopes, new = [], [], []
            for h in range(2):
                part = lax.dot_general(
                    k_ref[h, at, :], query[h], NT, preferred_element_type=jnp.float32
                )
                weights = jnp.exp(part - lse[h])
                pull = lax.dot_general(value, grads[h], NT, preferred_element_type=jnp.float32)
                slope = (weights * (pull - delta[h])).astype(jnp.bfloat16)
                probs.append(weights.astype(jnp.bfloat16))
                slopes.append(slope)
                new.append(carry[h] + matmul(kt[h * HEAD_DIM : (h + 1) * HEAD_DIM, at], slope))
            dv_ref[at, :] += matmul(jnp.concatenate(probs, axis=1), grads_both)
            dk_ref[at, :] += matmul(jnp.concatenate(slopes, axis=1), query_only)
            return tuple(new)

        zero = jnp.zeros((HEAD_DIM, BLOCK), jnp.float32)
        done = lax.fori_loop(0, count, step, (zero, zero))
        dq = jnp.concatenate(done, axis=0) * (HEAD_DIM**-0.5)
        dq_ref[rows, :] = dq.T.astype(jnp.bfloat16)


def attend_back(meta, q_aug, k_aug, values, grad, out_t, lse):
    rows = q_aug.shape[1]
    window = k_aug.shape[1]
    vmem = pl.BlockSpec(memory_space=pltpu.VMEM)
    return pl.pallas_call(
        attend_back_kernel,
        out_shape=(
            jax.ShapeDtypeStruct((rows, PAIR), jnp.bfloat16),
            jax.ShapeDtypeStruct((window, PAIR), jnp.float32),
            jax.ShapeDtypeStruct((window, PAIR), jnp.float32),
        ),
        in_specs=[pl.BlockSpec(memory_space=pltpu.SMEM)] + [vmem] * 6,
        out_specs=(vmem, vmem, vmem),
        scratch_shapes=[pltpu.VMEM((PAIR, window), jnp.bfloat16)],
        cost_estimate=pl.CostEstimate(
            flops=10 * rows * 2 * IMG * PAIR, transcendentals=2 * rows * IMG, bytes_accessed=16 << 20
        ),
        name="attend_back",
    )(meta, q_aug, k_aug, values, grad, out_t, lse)


def shards(
    tokens,
    out_grad,
    norm1_gain,
    norm1_bias,
    w_qkv,
    q_bias,
    v_bias,
    w_out,
    out_bias,
    attn_scale,
    norm2_gain,
    norm2_bias,
    w_up,
    up_bias,
    w_down,
    down_bias,
    mlp_scale,
    image_ids,
    pad_mask,
):
    both = ("fsdp", "rep")
    owners = lax.axis_size("fsdp")
    replicas = lax.axis_size("rep")
    me = lax.axis_index("fsdp") * replicas + lax.axis_index("rep")
    tok_rows = tokens.shape[0]
    rows = GROUP * tok_rows
    groups = [list(range(g, g + GROUP)) for g in range(0, replicas, GROUP)]
    factor = HEAD_DIM ** (-0.5)

    small = (
        norm1_gain,
        norm1_bias,
        q_bias,
        v_bias,
        out_bias,
        attn_scale,
        norm2_gain,
        norm2_bias,
        down_bias,
        mlp_scale,
        up_bias,
    )
    vectors = lax.all_gather(jnp.concatenate(small), "fsdp", axis=0, tiled=False).astype(
        jnp.float32
    )
    parts = []
    place = 0
    for member in small:
        parts.append(vectors[:, place : place + member.shape[0]].reshape(-1))
        place += member.shape[0]
    (
        gain_first,
        shift_first,
        query_bias,
        value_bias,
        proj_bias,
        attn_gamma,
        gain_second,
        shift_second,
        final_bias,
        mlp_gamma,
        hidden_bias,
    ) = parts

    codes = lax.all_gather(
        jnp.where(pad_mask > 0, image_ids + 1, 0), both, axis=0, tiled=True
    )
    wide_qkv = lax.all_gather(w_qkv, "fsdp", axis=0, tiled=True)
    wide_out = lax.all_gather(w_out, "fsdp", axis=0, tiled=True)
    wide_up = lax.all_gather(w_up, "fsdp", axis=0, tiled=True)
    wide_down = lax.all_gather(w_down, "fsdp", axis=0, tiled=True)

    window = HALO + rows + HALO + BLOCK
    padded = jnp.concatenate(
        [jnp.zeros((HALO,), jnp.int32), codes, jnp.zeros((HALO + BLOCK,), jnp.int32)]
    )
    seen = lax.dynamic_slice_in_dim(padded, (me // GROUP) * rows, window, 0)
    spot = jnp.arange(window, dtype=jnp.int32)
    seen = jnp.where(spot < window - BLOCK, seen, 0)
    asked = seen[HALO : HALO + rows]
    tile_codes = asked.reshape(rows // BLOCK, BLOCK)
    first_code = jnp.min(jnp.where(tile_codes > 0, tile_codes, 1 << 30), axis=1)
    last_code = jnp.max(tile_codes, axis=1)
    begin = jnp.min(jnp.where(seen[None] == first_code[:, None], spot[None], window), axis=1)
    finish = jnp.max(jnp.where(seen[None] == last_code[:, None], spot[None] + 1, 0), axis=1)
    begin = begin // 128 * 128
    count = jnp.where(last_code > 0, (finish - begin + BLOCK - 1) // BLOCK, 0)
    meta = jnp.stack([begin, count], axis=1).reshape(-1)

    lane = jnp.arange(PAIR, dtype=jnp.int32)
    lane_half = lane // HEAD_DIM
    lane_slot = lane % HEAD_DIM
    key_slot = jnp.where(seen > 0, 1 + (seen - 1) % SLOTS, 0)
    ask_slot = key_slot[HALO : HALO + rows]
    key_marks = (key_slot[:, None] == lane_slot[None]).astype(jnp.bfloat16)
    ask_marks = jnp.where(
        (ask_slot[:, None] == lane_slot[None]) & (ask_slot[:, None] > 0), 0.0, NEG_BIG
    ).astype(jnp.bfloat16)

    inputs = tokens.astype(jnp.float32)
    unit_one, scale_one = normalize(inputs)
    act_one = (unit_one * gain_first + shift_first).astype(jnp.bfloat16)
    qkv_rows = matmul(act_one, wide_qkv)
    query = ((qkv_rows[:, :D] + query_bias) * factor).astype(jnp.bfloat16)
    keys = qkv_rows[:, D : 2 * D].astype(jnp.bfloat16)
    values = (qkv_rows[:, 2 * D :] + value_bias).astype(jnp.bfloat16)
    sent = jnp.stack(
        [member.reshape(tok_rows, GROUP, PAIR) for member in (query, keys, values)], axis=2
    )
    sent = sent.transpose(1, 0, 2, 3).reshape(GROUP, tok_rows, 3 * PAIR)

    def exchange(block):
        return lax.all_to_all(
            block, "rep", split_axis=0, concat_axis=0, tiled=True, axis_index_groups=groups
        )

    mine = exchange(sent).reshape(rows, 3 * PAIR)
    before = from_behind(mine[rows - HALO :, PAIR:], both, GROUP)
    after = from_behind(mine[:HALO, PAIR:], both, -GROUP)
    pad = jnp.zeros((BLOCK, 2 * PAIR), jnp.bfloat16)
    key_value = jnp.concatenate([before, mine[:, PAIR:], after, pad], axis=0)
    value_window = key_value[:, PAIR:]
    k_aug = jnp.stack(
        [jnp.where(lane_half[None] == h, key_value[:, :PAIR], key_marks) for h in range(2)]
    )
    q_aug = jnp.stack(
        [jnp.where(lane_half[None] == h, mine[:, :PAIR], ask_marks) for h in range(2)]
    )
    attn_mine, attn_t, lse = attend(meta, q_aug, k_aug, value_window)

    def to_tokens(block):
        back = exchange(block.reshape(GROUP, tok_rows, block.shape[-1]))
        return back.transpose(1, 0, 2)

    attn_low = to_tokens(attn_mine).reshape(tok_rows, D)
    proj = matmul(attn_low, wide_out) + proj_bias
    residual = inputs + attn_gamma * proj
    unit_two, scale_two = normalize(residual)
    act_two = (unit_two * gain_second + shift_second).astype(jnp.bfloat16)
    pre_act = matmul(act_two, wide_up) + hidden_bias
    phi_cdf = 0.5 * (1.0 + lax.erf(pre_act * (0.5**0.5)))
    hidden = (pre_act * phi_cdf).astype(jnp.bfloat16)
    slope = phi_cdf + pre_act * (jnp.exp(-0.5 * pre_act * pre_act) * 0.3989422804014327)
    branch = matmul(hidden, wide_down) + final_bias
    layer_out = (residual + mlp_gamma * branch).astype(jnp.bfloat16)

    upstream = out_grad.astype(jnp.float32)
    mlp_gamma_grad = jnp.sum(upstream * branch, axis=0)
    branch_grad = mlp_gamma * upstream
    final_bias_grad = jnp.sum(branch_grad, axis=0)
    branch_low = branch_grad.astype(jnp.bfloat16)
    down_grad = matmul_tn(hidden, branch_low).astype(jnp.bfloat16)
    pre_grad = matmul_nt(branch_low, wide_down) * slope
    hidden_bias_grad = jnp.sum(pre_grad, axis=0)
    pre_low = pre_grad.astype(jnp.bfloat16)
    up_grad = matmul_tn(act_two, pre_low).astype(jnp.bfloat16)
    act_two_grad = matmul_nt(pre_low, wide_up)
    gain_second_grad = jnp.sum(act_two_grad * unit_two, axis=0)
    shift_second_grad = jnp.sum(act_two_grad, axis=0)
    residual_grad = upstream + norm_back(act_two_grad, unit_two, scale_two, gain_second)
    attn_gamma_grad = jnp.sum(residual_grad * proj, axis=0)
    proj_grad = attn_gamma * residual_grad
    proj_bias_grad = jnp.sum(proj_grad, axis=0)
    proj_low = proj_grad.astype(jnp.bfloat16)
    out_weight_grad = matmul_tn(attn_low, proj_low).astype(jnp.bfloat16)
    attn_grad_low = matmul_nt(proj_low, wide_out).astype(jnp.bfloat16)

    grad_sent = attn_grad_low.reshape(tok_rows, GROUP, PAIR).transpose(1, 0, 2)
    grad_mine = exchange(grad_sent).reshape(rows, PAIR)
    dq, dk, dv = attend_back(meta, q_aug, k_aug, value_window, grad_mine, attn_t, lse)
    dkv = jnp.concatenate([dk, dv], axis=1)
    tail = dkv[:HALO].astype(jnp.bfloat16)
    head = dkv[HALO + rows : HALO + rows + HALO].astype(jnp.bfloat16)
    from_after = from_behind(tail, both, -GROUP).astype(jnp.float32)
    from_before = from_behind(head, both, GROUP).astype(jnp.float32)
    own = dkv[HALO : HALO + rows]
    gap = jnp.zeros((rows - HALO, 2 * PAIR), jnp.float32)
    own = (
        own
        + jnp.concatenate([from_before, gap], axis=0)
        + jnp.concatenate([gap, from_after], axis=0)
    )
    dqkv_mine = jnp.concatenate([dq, own.astype(jnp.bfloat16)], axis=1)
    dqkv = to_tokens(dqkv_mine).reshape(tok_rows, GROUP, 3, PAIR)
    dqkv = dqkv.transpose(0, 2, 1, 3).reshape(tok_rows, 3 * D)
    query_bias_grad = jnp.sum(dqkv[:, :D].astype(jnp.float32), axis=0)
    value_bias_grad = jnp.sum(dqkv[:, 2 * D :].astype(jnp.float32), axis=0)
    qkv_weight_grad = matmul_tn(act_one, dqkv).astype(jnp.bfloat16)
    act_one_grad = matmul_nt(dqkv, wide_qkv)
    gain_first_grad = jnp.sum(act_one_grad * unit_one, axis=0)
    shift_first_grad = jnp.sum(act_one_grad, axis=0)
    input_part = norm_back(act_one_grad, unit_one, scale_one, gain_first)
    tokens_grad = (residual_grad + input_part).astype(jnp.bfloat16)

    small_grads = (
        gain_first_grad,
        shift_first_grad,
        query_bias_grad,
        value_bias_grad,
        proj_bias_grad,
        attn_gamma_grad,
        gain_second_grad,
        shift_second_grad,
        final_bias_grad,
        mlp_gamma_grad,
        hidden_bias_grad,
    )
    packed = jnp.concatenate([member.reshape(owners, -1) for member in small_grads], axis=1)
    packed = lax.psum(packed, both)
    packed = lax.dynamic_slice_in_dim(packed, lax.axis_index("fsdp"), 1, 0)[0]
    small_out = []
    place = 0
    for member in small_grads:
        size = member.shape[0] // owners
        small_out.append(packed[place : place + size])
        place += size

    def reduced(partial):
        owned = lax.psum_scatter(partial, "fsdp", scatter_dimension=0, tiled=True)
        return lax.psum(owned, "rep").astype(jnp.float32)

    down_out = reduced(down_grad)
    up_out = reduced(up_grad)
    out_out = reduced(out_weight_grad)
    qkv_out = reduced(qkv_weight_grad)
    return (
        layer_out,
        tokens_grad,
        small_out[0],
        small_out[1],
        qkv_out,
        small_out[2],
        small_out[3],
        out_out,
        small_out[4],
        small_out[5],
        small_out[6],
        small_out[7],
        up_out,
        small_out[10],
        down_out,
        small_out[8],
        small_out[9],
    )


def solution(mesh):
    spread = P(("fsdp", "rep"), None)
    line = P("fsdp")
    plane = P("fsdp", None)
    return jax.shard_map(
        shards,
        mesh=mesh,
        in_specs=(
            spread,
            spread,
            line,
            line,
            plane,
            line,
            line,
            plane,
            line,
            line,
            line,
            line,
            plane,
            line,
            plane,
            line,
            line,
            P(("fsdp", "rep")),
            P(("fsdp", "rep")),
        ),
        out_specs=(
            spread,
            spread,
            line,
            line,
            plane,
            line,
            line,
            plane,
            line,
            line,
            line,
            line,
            plane,
            line,
            plane,
            line,
            line,
        ),
        check_vma=False,
    )
```

```python
import functools

import jax
import jax.numpy as jnp
from jax import lax
from jax.experimental import pallas as pl
from jax.experimental.pallas import tpu as pltpu
from jax.sharding import PartitionSpec as P

D = 1024
HEADS = 16
HEAD_DIM = 64
IMG = 1370

PAIR = 2 * HEAD_DIM
GROUP = HEADS // 2
BLOCK = 256
HALO = 1408
SLOTS = 63

EPSILON = 1e-06
NEG_BIG = -1e30
NEG_EDGE = -1e29

NT = (((1,), (1,)), ((), ()))


def from_behind(block, axis, distance):
    devices = range(lax.axis_size(axis))
    route = [(i - distance, i) for i in devices if i - distance in devices]
    return lax.ppermute(block, axis, route)


def normalize(values):
    center = jnp.mean(values, axis=-1, keepdims=True)
    centered = values - center
    spread = jnp.mean(centered * centered, axis=-1, keepdims=True)
    scale = lax.rsqrt(spread + EPSILON)
    return centered * scale, scale


def norm_back(cotangent, unit, scale, gain):
    scaled = cotangent * gain
    along = jnp.mean(scaled, axis=-1, keepdims=True)
    across = jnp.mean(scaled * unit, axis=-1, keepdims=True)
    return scale * (scaled - along - unit * across)


def matmul(left, right):
    return jnp.dot(left, right, preferred_element_type=jnp.float32)


def matmul_nt(left, right):
    return jnp.einsum("te,de->td", left, right, preferred_element_type=jnp.float32)


def matmul_tn(left, right):
    return jnp.einsum("td,te->de", left, right, preferred_element_type=jnp.float32)


def fold_rows(values, op):
    return op(values.reshape(values.shape[0] // 8, 8, values.shape[1]), axis=0)


def attend_kernel(meta, q_ref, k_ref, v_ref, o_ref, ot_ref, lse_ref, vt, scores):
    tiles = o_ref.shape[0] // BLOCK
    window = k_ref.shape[1]

    @pl.loop(0, window // BLOCK)
    def _(i):
        at = pl.ds(pl.multiple_of(i * BLOCK, BLOCK), BLOCK)
        vt[:, at] = v_ref[at, :].T

    @pl.loop(0, tiles)
    def _(t):
        start = meta[2 * t]
        count = meta[2 * t + 1]
        rows = pl.ds(pl.multiple_of(t * BLOCK, BLOCK), BLOCK)
        query = [q_ref[h, rows, :] for h in range(2)]

        def score(i, tops):
            at = pl.ds(pl.multiple_of(start + i * BLOCK, 128), BLOCK)
            keep = pl.ds(pl.multiple_of(i * BLOCK, BLOCK), BLOCK)
            new = []
            for h in range(2):
                part = lax.dot_general(
                    k_ref[h, at, :], query[h], NT, preferred_element_type=jnp.float32
                )
                scores[h, keep, :] = part
                new.append(jnp.maximum(tops[h], fold_rows(part, jnp.max)))
            return tuple(new)

        low = jnp.full((8, BLOCK), NEG_BIG, jnp.float32)
        tops = lax.fori_loop(0, count, score, (low, low))
        tops = [jnp.max(top, axis=0, keepdims=True) for top in tops]
        tops = [jnp.where(top < NEG_EDGE, 0.0, top) for top in tops]

        def mix(i, carry):
            at = pl.ds(pl.multiple_of(start + i * BLOCK, 128), BLOCK)
            keep = pl.ds(pl.multiple_of(i * BLOCK, BLOCK), BLOCK)
            new = []
            for h in range(2):
                total, mixed = carry[h]
                weights = jnp.exp(scores[h, keep, :] - tops[h])
                total = total + fold_rows(weights, jnp.sum)
                mixed = mixed + matmul(
                    vt[h * HEAD_DIM : (h + 1) * HEAD_DIM, at], weights.astype(jnp.bfloat16)
                )
                new.append((total, mixed))
            return tuple(new)

        zero = (jnp.zeros((8, BLOCK), jnp.float32), jnp.zeros((HEAD_DIM, BLOCK), jnp.float32))
        done = lax.fori_loop(0, count, mix, (zero, zero))
        outs = []
        for h in range(2):
            total = jnp.sum(done[h][0], axis=0, keepdims=True)
            total = jnp.where(total > 0, total, 1.0)
            lse_ref[h : h + 1, rows] = tops[h] + jnp.log(total)
            outs.append(done[h][1] / total)
        out = jnp.concatenate(outs, axis=0)
        ot_ref[:, rows] = out
        o_ref[rows, :] = out.T.astype(jnp.bfloat16)


def attend(meta, q_aug, k_aug, values):
    rows = q_aug.shape[1]
    window = k_aug.shape[1]
    deepest = (2 * IMG + 3 * BLOCK) // BLOCK * BLOCK
    vmem = pl.BlockSpec(memory_space=pltpu.VMEM)
    return pl.pallas_call(
        attend_kernel,
        out_shape=(
            jax.ShapeDtypeStruct((rows, PAIR), jnp.bfloat16),
            jax.ShapeDtypeStruct((PAIR, rows), jnp.float32),
            jax.ShapeDtypeStruct((8, rows), jnp.float32),
        ),
        in_specs=[pl.BlockSpec(memory_space=pltpu.SMEM), vmem, vmem, vmem],
        out_specs=(vmem, vmem, vmem),
        scratch_shapes=[
            pltpu.VMEM((PAIR, window), jnp.bfloat16),
            pltpu.VMEM((2, deepest, BLOCK), jnp.float32),
        ],
        cost_estimate=pl.CostEstimate(
            flops=4 * rows * 2 * IMG * PAIR, transcendentals=2 * rows * IMG, bytes_accessed=9 << 20
        ),
        name="attend",
    )(meta, q_aug, k_aug, values)


def attend_back_kernel(
    meta, q_ref, k_ref, v_ref, g_ref, ot_ref, lse_ref, dq_ref, dk_ref, dv_ref, kt
):
    tiles = dq_ref.shape[0] // BLOCK
    window = k_ref.shape[1]
    half = lax.broadcasted_iota(jnp.int32, (BLOCK, PAIR), 1) // HEAD_DIM

    @pl.loop(0, window // BLOCK)
    def _(i):
        at = pl.ds(pl.multiple_of(i * BLOCK, BLOCK), BLOCK)
        kt[:, at] = jnp.where(half == 0, k_ref[0, at, :], k_ref[1, at, :]).T
        dk_ref[at, :] = jnp.zeros((BLOCK, PAIR), jnp.float32)
        dv_ref[at, :] = jnp.zeros((BLOCK, PAIR), jnp.float32)

    @pl.loop(0, tiles)
    def _(t):
        start = meta[2 * t]
        count = meta[2 * t + 1]
        rows = pl.ds(pl.multiple_of(t * BLOCK, BLOCK), BLOCK)
        grad = g_ref[rows, :]
        blank = jnp.zeros_like(grad)
        query = [q_ref[h, rows, :] for h in range(2)]
        query_only = jnp.concatenate(
            [jnp.where(half == h, query[h], blank) for h in range(2)], axis=0
        )
        grads = [jnp.where(half == h, grad, blank) for h in range(2)]
        grads_both = jnp.concatenate(grads, axis=0)
        product = grad.astype(jnp.float32).T * ot_ref[:, rows]
        delta = [
            jnp.sum(product[h * HEAD_DIM : (h + 1) * HEAD_DIM], axis=0, keepdims=True)
            for h in range(2)
        ]
        lse = [lse_ref[h : h + 1, rows] for h in range(2)]

        def step(i, carry):
            at = pl.ds(pl.multiple_of(start + i * BLOCK, 128), BLOCK)
            value = v_ref[at, :]
            probs, slopes, new = [], [], []
            for h in range(2):
                part = lax.dot_general(
                    k_ref[h, at, :], query[h], NT, preferred_element_type=jnp.float32
                )
                weights = jnp.exp(part - lse[h])
                pull = lax.dot_general(value, grads[h], NT, preferred_element_type=jnp.float32)
                slope = (weights * (pull - delta[h])).astype(jnp.bfloat16)
                probs.append(weights.astype(jnp.bfloat16))
                slopes.append(slope)
                new.append(carry[h] + matmul(kt[h * HEAD_DIM : (h + 1) * HEAD_DIM, at], slope))
            dv_ref[at, :] += matmul(jnp.concatenate(probs, axis=1), grads_both)
            dk_ref[at, :] += matmul(jnp.concatenate(slopes, axis=1), query_only)
            return tuple(new)

        zero = jnp.zeros((HEAD_DIM, BLOCK), jnp.float32)
        done = lax.fori_loop(0, count, step, (zero, zero))
        dq = jnp.concatenate(done, axis=0) * (HEAD_DIM**-0.5)
        dq_ref[rows, :] = dq.T.astype(jnp.bfloat16)


def attend_back(meta, q_aug, k_aug, values, grad, out_t, lse):
    rows = q_aug.shape[1]
    window = k_aug.shape[1]
    vmem = pl.BlockSpec(memory_space=pltpu.VMEM)
    return pl.pallas_call(
        attend_back_kernel,
        out_shape=(
            jax.ShapeDtypeStruct((rows, PAIR), jnp.bfloat16),
            jax.ShapeDtypeStruct((window, PAIR), jnp.float32),
            jax.ShapeDtypeStruct((window, PAIR), jnp.float32),
        ),
        in_specs=[pl.BlockSpec(memory_space=pltpu.SMEM)] + [vmem] * 6,
        out_specs=(vmem, vmem, vmem),
        scratch_shapes=[pltpu.VMEM((PAIR, window), jnp.bfloat16)],
        cost_estimate=pl.CostEstimate(
            flops=10 * rows * 2 * IMG * PAIR, transcendentals=2 * rows * IMG, bytes_accessed=16 << 20
        ),
        name="attend_back",
    )(meta, q_aug, k_aug, values, grad, out_t, lse)


CHUNK = 64
LAG = 2
MESH = pl.DeviceIdType.MESH
STAGES = 6


def reduce_kernel(
    down_ref,
    up_ref,
    out_ref,
    qkv_ref,
    small_ref,
    final,
    small_final,
    own,
    from_core,
    from_x,
    from_y,
    from_z,
    small_own,
    small_core,
    small_x,
    small_all,
    load_sem,
    core_sem,
    x_sem,
    y_sem,
    z_sem,
    zz_sem,
    yy_sem,
    small_sem,
):
    f = lax.axis_index("fsdp")
    r = lax.axis_index("rep")
    x, c = f // 2, f % 2
    z, y = (r % GROUP) // 2, r % 2
    base = r - r % GROUP
    core_peer = (x * 2 + 1 - c, r)
    x_peer = ((1 - x) * 2 + c, r)
    y_peer = (f, base + z * 2 + 1 - y)
    z_spots = [(z + step) % 4 for step in range(1, 4)]
    z_peers = [(f, base + spot * 2 + y) for spot in z_spots]
    plane = [(f, base + (r % GROUP + step) % GROUP) for step in range(1, GROUP)]
    total = final.shape[0]

    barrier = pltpu.get_barrier_semaphore()
    for peer in [core_peer, x_peer] + plane:
        pl.semaphore_signal(barrier, inc=1, device_id=peer, device_id_type=MESH)
    pl.semaphore_wait(barrier, 2 + len(plane))

    def remote(source, target, send, recv, peer):
        return pltpu.make_async_remote_copy(
            src_ref=source,
            dst_ref=target,
            send_sem=send,
            recv_sem=recv,
            device_id=peer,
            device_id_type=MESH,
        )

    refs = (down_ref, up_ref, out_ref, qkv_ref)
    spans = []
    first = 0
    for ref in refs:
        height = ref.shape[0] // 4 // CHUNK
        amount = height * (ref.shape[1] // D)
        spans.append((ref, first, first + amount, height))
        first += amount

    def piece(ref, low, height, k, owner):
        at = k - low
        top = owner * (height * CHUNK) + (at % height) * CHUNK
        left = (at // height) * D
        return ref.at[pl.ds(pl.multiple_of(top, CHUNK), CHUNK), pl.ds(pl.multiple_of(left, D), D)]

    def enter_copies(ref, low, height, k):
        copies = []
        for side in range(2):
            copies.append(
                remote(
                    piece(ref, low, height, k, side * 2 + 1 - c),
                    from_core.at[k, side],
                    core_sem.at[0, k, side],
                    core_sem.at[1, k, side],
                    core_peer,
                )
            )
            copies.append(
                pltpu.make_async_copy(
                    piece(ref, low, height, k, side * 2 + c), own.at[k, side], load_sem.at[k, side]
                )
            )
        return copies

    def enter(k):
        for ref, low, high, height in spans:

            @pl.when((k >= low) & (k < high))
            def _():
                for copy in enter_copies(ref, low, height, k):
                    copy.start()

    x_copy = lambda k: remote(
        own.at[k, 1 - x], from_x.at[k], x_sem.at[0, k], x_sem.at[1, k], x_peer
    )
    half = CHUNK // 2
    quarter = D // 4

    def y_copy(k):
        rows = pl.ds(pl.multiple_of((1 - y) * half, half), half)
        return remote(
            own.at[k, x, rows], from_y.at[k], y_sem.at[0, k], y_sem.at[1, k], y_peer
        )

    my_rows = pl.ds(pl.multiple_of(y * half, half), half)
    my_lanes = pl.ds(pl.multiple_of(z * quarter, quarter), quarter)

    def z_copies(k):
        copies = []
        for step in range(3):
            lanes = pl.ds(pl.multiple_of(z_spots[step] * quarter, quarter), quarter)
            copies.append(
                remote(
                    own.at[k, x, my_rows, lanes],
                    from_z.at[k, step],
                    z_sem.at[0, k, step],
                    z_sem.at[1, k, step],
                    z_peers[step],
                )
            )
        return copies

    def zz_copies(k):
        here = final.at[k, my_rows, my_lanes]
        return [
            remote(here, here, zz_sem.at[0, k, step], zz_sem.at[1, k, step], z_peers[step])
            for step in range(3)
        ]

    def yy_copy(k):
        here = final.at[k, my_rows]
        return remote(here, here, yy_sem.at[0, k], yy_sem.at[1, k], y_peer)

    def core_sum(k):
        for side in range(2):
            target = own.at[k, side]
            pltpu.make_async_copy(target, target, load_sem.at[k, side]).wait()
            remote(
                target,
                from_core.at[k, side],
                core_sem.at[0, k, side],
                core_sem.at[1, k, side],
                core_peer,
            ).wait()
        for side in range(2):
            own[k, side] = (
                own[k, side].astype(jnp.float32) + from_core[k, side].astype(jnp.float32)
            ).astype(jnp.bfloat16)
        x_copy(k).start()

    def x_sum(k):
        x_copy(k).wait()
        own[k, x] = (own[k, x].astype(jnp.float32) + from_x[k].astype(jnp.float32)).astype(
            jnp.bfloat16
        )
        y_copy(k).start()

    def y_sum(k):
        y_copy(k).wait()
        own[k, x, my_rows] = (
            own[k, x, my_rows].astype(jnp.float32) + from_y[k].astype(jnp.float32)
        ).astype(jnp.bfloat16)
        for copy in z_copies(k):
            copy.start()

    def z_sum(k):
        for copy in z_copies(k):
            copy.wait()
        value = own[k, x, my_rows, my_lanes].astype(jnp.float32)
        for step in range(3):
            value = value + from_z[k, step].astype(jnp.float32)
        final[k, my_rows, my_lanes] = value.astype(jnp.bfloat16)
        for copy in zz_copies(k):
            copy.start()

    def z_join(k):
        for copy in zz_copies(k):
            copy.wait()
        yy_copy(k).start()

    def small_enter(side):
        return remote(
            small_ref.at[side * 2 + 1 - c],
            small_core.at[side],
            small_sem.at[0, side],
            small_sem.at[1, side],
            core_peer,
        )

    small_cross = remote(
        small_own.at[1 - x], small_x, small_sem.at[0, 2], small_sem.at[1, 2], x_peer
    )

    def small_spread(step):
        return remote(
            small_own.at[2],
            small_all.at[step - 1],
            small_sem.at[0, 2 + step],
            small_sem.at[1, 2 + step],
            plane[step - 1],
        )

    for side in range(2):
        small_enter(side).start()

    steps = (enter, core_sum, x_sum, y_sum, z_sum, z_join, lambda k: yy_copy(k).wait())

    @pl.loop(0, total + LAG * (len(steps) - 1))
    def _(now):
        @pl.when(now == 4)
        def _():
            for side in range(2):
                small_enter(side).wait()
            for side in range(2):
                small_own[side] = small_ref[side * 2 + c] + small_core[side]
            small_cross.start()

        @pl.when(now == 8)
        def _():
            small_cross.wait()
            small_own[2] = small_own[x] + small_x[...]
            for step in range(1, GROUP):
                small_spread(step).start()

        for order, step in enumerate(steps):
            k = now - order * LAG

            @pl.when((k >= 0) & (k < total))
            def _():
                step(k)

    for step in range(1, GROUP):
        small_spread(step).wait()
    value = small_own[2]
    for step in range(1, GROUP):
        value = value + small_all[step - 1]
    small_final[...] = value


def reduce_grads(weights, small):
    chunks = sum(weight.size for weight in weights) // (4 * CHUNK * D)
    tall = small.shape[1]
    anywhere = pl.BlockSpec(memory_space=pl.ANY)
    vmem = pl.BlockSpec(memory_space=pltpu.VMEM)
    dma = pltpu.SemaphoreType.DMA
    low = jnp.bfloat16
    return pl.pallas_call(
        reduce_kernel,
        out_shape=(
            jax.ShapeDtypeStruct((chunks, CHUNK, D), low),
            jax.ShapeDtypeStruct((tall, 128), jnp.float32),
        ),
        in_specs=[anywhere] * 4 + [vmem],
        out_specs=(vmem, vmem),
        scratch_shapes=[
            pltpu.VMEM((chunks, 2, CHUNK, D), low),
            pltpu.VMEM((chunks, 2, CHUNK, D), low),
            pltpu.VMEM((chunks, CHUNK, D), low),
            pltpu.VMEM((chunks, CHUNK // 2, D), low),
            pltpu.VMEM((chunks, 3, CHUNK // 2, D // 4), low),
            pltpu.VMEM((3, tall, 128), jnp.float32),
            pltpu.VMEM((2, tall, 128), jnp.float32),
            pltpu.VMEM((tall, 128), jnp.float32),
            pltpu.VMEM((GROUP - 1, tall, 128), jnp.float32),
            dma((chunks, 2)),
            dma((2, chunks, 2)),
            dma((2, chunks)),
            dma((2, chunks)),
            dma((2, chunks, 3)),
            dma((2, chunks, 3)),
            dma((2, chunks)),
            dma((2, GROUP + 2)),
        ],
        compiler_params=pltpu.CompilerParams(
            collective_id=1, has_side_effects=True, vmem_limit_bytes=60 << 20
        ),
        cost_estimate=pl.CostEstimate(flops=0, transcendentals=0, bytes_accessed=200 << 20),
        name="reduce_grads",
    )(*weights, small)


def shards(
    tokens,
    out_grad,
    norm1_gain,
    norm1_bias,
    w_qkv,
    q_bias,
    v_bias,
    w_out,
    out_bias,
    attn_scale,
    norm2_gain,
    norm2_bias,
    w_up,
    up_bias,
    w_down,
    down_bias,
    mlp_scale,
    image_ids,
    pad_mask,
):
    both = ("fsdp", "rep")
    owners = lax.axis_size("fsdp")
    replicas = lax.axis_size("rep")
    tok_rows = tokens.shape[0]
    rows = GROUP * tok_rows
    groups = [list(range(g, g + GROUP)) for g in range(0, replicas, GROUP)]
    factor = HEAD_DIM ** (-0.5)

    small = (
        norm1_gain,
        norm1_bias,
        q_bias,
        v_bias,
        out_bias,
        attn_scale,
        norm2_gain,
        norm2_bias,
        down_bias,
        mlp_scale,
        up_bias,
    )
    vectors = lax.all_gather(jnp.concatenate(small), "fsdp", axis=0, tiled=False).astype(
        jnp.float32
    )
    parts = []
    place = 0
    for member in small:
        parts.append(vectors[:, place : place + member.shape[0]].reshape(-1))
        place += member.shape[0]
    (
        gain_first,
        shift_first,
        query_bias,
        value_bias,
        proj_bias,
        attn_gamma,
        gain_second,
        shift_second,
        final_bias,
        mlp_gamma,
        hidden_bias,
    ) = parts

    codes = jnp.where(pad_mask > 0, image_ids + 1, 0)
    codes = lax.all_gather(codes, "rep", axis=0, tiled=True, axis_index_groups=groups)
    codes = [
        from_behind(codes[rows - HALO :], both, GROUP),
        codes,
        from_behind(codes[:HALO], both, -GROUP),
        jnp.zeros((BLOCK,), jnp.int32),
    ]
    wide_qkv = lax.all_gather(w_qkv, "fsdp", axis=0, tiled=True)
    wide_out = lax.all_gather(w_out, "fsdp", axis=0, tiled=True)
    wide_up = lax.all_gather(w_up, "fsdp", axis=0, tiled=True)
    wide_down = lax.all_gather(w_down, "fsdp", axis=0, tiled=True)

    window = HALO + rows + HALO + BLOCK
    seen = jnp.concatenate(codes)
    spot = jnp.arange(window, dtype=jnp.int32)
    asked = seen[HALO : HALO + rows]
    tile_codes = asked.reshape(rows // BLOCK, BLOCK)
    first_code = jnp.min(jnp.where(tile_codes > 0, tile_codes, 1 << 30), axis=1)
    last_code = jnp.max(tile_codes, axis=1)
    begin = jnp.min(jnp.where(seen[None] == first_code[:, None], spot[None], window), axis=1)
    finish = jnp.max(jnp.where(seen[None] == last_code[:, None], spot[None] + 1, 0), axis=1)
    begin = begin // 128 * 128
    count = jnp.where(last_code > 0, (finish - begin + BLOCK - 1) // BLOCK, 0)
    meta = jnp.stack([begin, count], axis=1).reshape(-1)

    lane = jnp.arange(PAIR, dtype=jnp.int32)
    lane_half = lane // HEAD_DIM
    lane_slot = lane % HEAD_DIM
    key_slot = jnp.where(seen > 0, 1 + (seen - 1) % SLOTS, 0)
    ask_slot = key_slot[HALO : HALO + rows]
    key_marks = (key_slot[:, None] == lane_slot[None]).astype(jnp.bfloat16)
    ask_marks = jnp.where(
        (ask_slot[:, None] == lane_slot[None]) & (ask_slot[:, None] > 0), 0.0, NEG_BIG
    ).astype(jnp.bfloat16)

    inputs = tokens.astype(jnp.float32)
    unit_one, scale_one = normalize(inputs)
    act_one = (unit_one * gain_first + shift_first).astype(jnp.bfloat16)
    qkv_rows = matmul(act_one, wide_qkv)
    query = ((qkv_rows[:, :D] + query_bias) * factor).astype(jnp.bfloat16)
    keys = qkv_rows[:, D : 2 * D].astype(jnp.bfloat16)
    values = (qkv_rows[:, 2 * D :] + value_bias).astype(jnp.bfloat16)
    sent = jnp.stack(
        [member.reshape(tok_rows, GROUP, PAIR) for member in (query, keys, values)], axis=2
    )
    sent = sent.transpose(1, 0, 2, 3).reshape(GROUP, tok_rows, 3 * PAIR)

    def exchange(block):
        return lax.all_to_all(
            block, "rep", split_axis=0, concat_axis=0, tiled=True, axis_index_groups=groups
        )

    mine = exchange(sent).reshape(rows, 3 * PAIR)
    before = from_behind(mine[rows - HALO :, PAIR:], both, GROUP)
    after = from_behind(mine[:HALO, PAIR:], both, -GROUP)
    pad = jnp.zeros((BLOCK, 2 * PAIR), jnp.bfloat16)
    key_value = jnp.concatenate([before, mine[:, PAIR:], after, pad], axis=0)
    value_window = key_value[:, PAIR:]
    k_aug = jnp.stack(
        [jnp.where(lane_half[None] == h, key_value[:, :PAIR], key_marks) for h in range(2)]
    )
    q_aug = jnp.stack(
        [jnp.where(lane_half[None] == h, mine[:, :PAIR], ask_marks) for h in range(2)]
    )
    attn_mine, attn_t, lse = attend(meta, q_aug, k_aug, value_window)

    def to_tokens(block):
        back = exchange(block.reshape(GROUP, tok_rows, block.shape[-1]))
        return back.transpose(1, 0, 2)

    attn_low = to_tokens(attn_mine).reshape(tok_rows, D)
    proj = matmul(attn_low, wide_out) + proj_bias
    residual = inputs + attn_gamma * proj
    unit_two, scale_two = normalize(residual)
    act_two = (unit_two * gain_second + shift_second).astype(jnp.bfloat16)
    pre_act = matmul(act_two, wide_up) + hidden_bias
    phi_cdf = 0.5 * (1.0 + lax.erf(pre_act * (0.5**0.5)))
    hidden = (pre_act * phi_cdf).astype(jnp.bfloat16)
    slope = phi_cdf + pre_act * (jnp.exp(-0.5 * pre_act * pre_act) * 0.3989422804014327)
    branch = matmul(hidden, wide_down) + final_bias
    layer_out = (residual + mlp_gamma * branch).astype(jnp.bfloat16)

    upstream = out_grad.astype(jnp.float32)
    mlp_gamma_grad = jnp.sum(upstream * branch, axis=0)
    branch_grad = mlp_gamma * upstream
    final_bias_grad = jnp.sum(branch_grad, axis=0)
    branch_low = branch_grad.astype(jnp.bfloat16)
    down_grad = matmul_tn(hidden, branch_low).astype(jnp.bfloat16)
    pre_grad = matmul_nt(branch_low, wide_down) * slope
    hidden_bias_grad = jnp.sum(pre_grad, axis=0)
    pre_low = pre_grad.astype(jnp.bfloat16)
    up_grad = matmul_tn(act_two, pre_low).astype(jnp.bfloat16)
    act_two_grad = matmul_nt(pre_low, wide_up)
    gain_second_grad = jnp.sum(act_two_grad * unit_two, axis=0)
    shift_second_grad = jnp.sum(act_two_grad, axis=0)
    residual_grad = upstream + norm_back(act_two_grad, unit_two, scale_two, gain_second)
    attn_gamma_grad = jnp.sum(residual_grad * proj, axis=0)
    proj_grad = attn_gamma * residual_grad
    proj_bias_grad = jnp.sum(proj_grad, axis=0)
    proj_low = proj_grad.astype(jnp.bfloat16)
    out_weight_grad = matmul_tn(attn_low, proj_low).astype(jnp.bfloat16)
    attn_grad_low = matmul_nt(proj_low, wide_out).astype(jnp.bfloat16)

    grad_sent = attn_grad_low.reshape(tok_rows, GROUP, PAIR).transpose(1, 0, 2)
    grad_mine = exchange(grad_sent).reshape(rows, PAIR)
    dq, dk, dv = attend_back(meta, q_aug, k_aug, value_window, grad_mine, attn_t, lse)
    dkv = jnp.concatenate([dk, dv], axis=1)
    tail = dkv[:HALO].astype(jnp.bfloat16)
    head = dkv[HALO + rows : HALO + rows + HALO].astype(jnp.bfloat16)
    from_after = from_behind(tail, both, -GROUP).astype(jnp.float32)
    from_before = from_behind(head, both, GROUP).astype(jnp.float32)
    own = dkv[HALO : HALO + rows]
    gap = jnp.zeros((rows - HALO, 2 * PAIR), jnp.float32)
    own = (
        own
        + jnp.concatenate([from_before, gap], axis=0)
        + jnp.concatenate([gap, from_after], axis=0)
    )
    dqkv_mine = jnp.concatenate([dq, own.astype(jnp.bfloat16)], axis=1)
    dqkv = to_tokens(dqkv_mine).reshape(tok_rows, GROUP, 3, PAIR)
    dqkv = dqkv.transpose(0, 2, 1, 3).reshape(tok_rows, 3 * D)
    query_bias_grad = jnp.sum(dqkv[:, :D].astype(jnp.float32), axis=0)
    value_bias_grad = jnp.sum(dqkv[:, 2 * D :].astype(jnp.float32), axis=0)
    qkv_weight_grad = matmul_tn(act_one, dqkv).astype(jnp.bfloat16)
    act_one_grad = matmul_nt(dqkv, wide_qkv)
    gain_first_grad = jnp.sum(act_one_grad * unit_one, axis=0)
    shift_first_grad = jnp.sum(act_one_grad, axis=0)
    input_part = norm_back(act_one_grad, unit_one, scale_one, gain_first)
    tokens_grad = (residual_grad + input_part).astype(jnp.bfloat16)

    small_grads = (
        gain_first_grad,
        shift_first_grad,
        query_bias_grad,
        value_bias_grad,
        proj_bias_grad,
        attn_gamma_grad,
        gain_second_grad,
        shift_second_grad,
        final_bias_grad,
        mlp_gamma_grad,
        hidden_bias_grad,
    )
    packed = jnp.concatenate([member.reshape(owners, -1) for member in small_grads], axis=1)
    packed = packed.reshape(owners, -1, 128)
    grads, packed = reduce_grads((down_grad, up_grad, out_weight_grad, qkv_weight_grad), packed)
    grads = grads.astype(jnp.float32)
    if replicas > GROUP:
        apart = [list(range(low, replicas, GROUP)) for low in range(GROUP)]
        grads = lax.psum(grads, "rep", axis_index_groups=apart)
        packed = lax.psum(packed, "rep", axis_index_groups=apart)
    packed = packed.reshape(-1)
    small_out = []
    place = 0
    for member in small_grads:
        size = member.shape[0] // owners
        small_out.append(packed[place : place + size])
        place += size

    def joined(start, height, width):
        deep, across = height // CHUNK, width // D
        part = grads[start : start + deep * across]
        part = part.reshape(across, deep, CHUNK, D).transpose(1, 2, 0, 3)
        return part.reshape(height, width), start + deep * across

    down_out, place = joined(0, *w_down.shape)
    up_out, place = joined(place, *w_up.shape)
    out_out, place = joined(place, *w_out.shape)
    qkv_out, place = joined(place, *w_qkv.shape)
    return (
        layer_out,
        tokens_grad,
        small_out[0],
        small_out[1],
        qkv_out,
        small_out[2],
        small_out[3],
        out_out,
        small_out[4],
        small_out[5],
        small_out[6],
        small_out[7],
        up_out,
        small_out[10],
        down_out,
        small_out[8],
        small_out[9],
    )


def solution(mesh):
    spread = P(("fsdp", "rep"), None)
    line = P("fsdp")
    plane = P("fsdp", None)
    return jax.shard_map(
        shards,
        mesh=mesh,
        in_specs=(
            spread,
            spread,
            line,
            line,
            plane,
            line,
            line,
            plane,
            line,
            line,
            line,
            line,
            plane,
            line,
            plane,
            line,
            line,
            P(("fsdp", "rep")),
            P(("fsdp", "rep")),
        ),
        out_specs=(
            spread,
            spread,
            line,
            line,
            plane,
            line,
            line,
            plane,
            line,
            line,
            line,
            line,
            plane,
            line,
            plane,
            line,
            line,
        ),
        check_vma=False,
    )
```

```python
import functools

import jax
import jax.numpy as jnp
from jax import lax
from jax.experimental import pallas as pl
from jax.experimental.pallas import tpu as pltpu
from jax.sharding import PartitionSpec as P

D = 1024
HEADS = 16
HEAD_DIM = 64
IMG = 1370

PAIR = 2 * HEAD_DIM
GROUP = HEADS // 2
BLOCK = 256
SLOTS = 63

EPSILON = 1e-06
NEG_BIG = -1e30
NEG_EDGE = -1e29

NT = (((1,), (1,)), ((), ()))


def from_behind(block, axis, distance):
    devices = range(lax.axis_size(axis))
    route = [(i - distance, i) for i in devices if i - distance in devices]
    return lax.ppermute(block, axis, route)


def normalize(values):
    center = jnp.mean(values, axis=-1, keepdims=True)
    centered = values - center
    spread = jnp.mean(centered * centered, axis=-1, keepdims=True)
    scale = lax.rsqrt(spread + EPSILON)
    return centered * scale, scale


def norm_back(cotangent, unit, scale, gain):
    scaled = cotangent * gain
    along = jnp.mean(scaled, axis=-1, keepdims=True)
    across = jnp.mean(scaled * unit, axis=-1, keepdims=True)
    return scale * (scaled - along - unit * across)


def matmul(left, right):
    return jnp.dot(left, right, preferred_element_type=jnp.float32)


def matmul_nt(left, right):
    return jnp.einsum("te,de->td", left, right, preferred_element_type=jnp.float32)


def matmul_tn(left, right):
    return jnp.einsum("td,te->de", left, right, preferred_element_type=jnp.float32)


def fold_rows(values, op):
    return op(values.reshape(values.shape[0] // 8, 8, values.shape[1]), axis=0)


def lane_marks():
    lane = lax.broadcasted_iota(jnp.int32, (BLOCK, PAIR), 1)
    return lane // HEAD_DIM, lane % HEAD_DIM > 0


def asking(query, marks, half, usable):
    wanted = jnp.where((marks.astype(jnp.float32) > 0) & usable, 0.0, NEG_BIG).astype(jnp.bfloat16)
    return [jnp.where(half == h, query, wanted) for h in range(2)]


def attend_kernel(meta, q_ref, k_ref, v_ref, m_ref, o_ref, ot_ref, lse_ref, vt, k_aug, scores):
    rows_all = o_ref.shape[0]
    tiles = rows_all // BLOCK
    window = k_ref.shape[0]
    halo = (window - BLOCK - rows_all) // 2
    half, usable = lane_marks()

    @pl.loop(0, window // BLOCK)
    def _(i):
        at = pl.ds(pl.multiple_of(i * BLOCK, BLOCK), BLOCK)
        vt[:, at] = v_ref[at, :].T
        for h in range(2):
            k_aug[h, at, :] = jnp.where(half == h, k_ref[at, :], m_ref[at, :])

    @pl.loop(0, tiles)
    def _(t):
        start = meta[2 * t]
        count = meta[2 * t + 1]
        rows = pl.ds(pl.multiple_of(t * BLOCK, BLOCK), BLOCK)
        spots = pl.ds(pl.multiple_of(halo + t * BLOCK, BLOCK), BLOCK)
        query = asking(q_ref[rows, :], m_ref[spots, :], half, usable)

        def score(i, tops):
            at = pl.ds(pl.multiple_of(start + i * BLOCK, 128), BLOCK)
            keep = pl.ds(pl.multiple_of(i * BLOCK, BLOCK), BLOCK)
            new = []
            for h in range(2):
                part = lax.dot_general(
                    k_aug[h, at, :], query[h], NT, preferred_element_type=jnp.float32
                )
                scores[h, keep, :] = part
                new.append(jnp.maximum(tops[h], fold_rows(part, jnp.max)))
            return tuple(new)

        low = jnp.full((8, BLOCK), NEG_BIG, jnp.float32)
        tops = lax.fori_loop(0, count, score, (low, low))
        tops = [jnp.max(top, axis=0, keepdims=True) for top in tops]
        tops = [jnp.where(top < NEG_EDGE, 0.0, top) for top in tops]

        def mix(i, carry):
            at = pl.ds(pl.multiple_of(start + i * BLOCK, 128), BLOCK)
            keep = pl.ds(pl.multiple_of(i * BLOCK, BLOCK), BLOCK)
            new = []
            for h in range(2):
                total, mixed = carry[h]
                weights = jnp.exp(scores[h, keep, :] - tops[h])
                total = total + fold_rows(weights, jnp.sum)
                mixed = mixed + matmul(
                    vt[h * HEAD_DIM : (h + 1) * HEAD_DIM, at], weights.astype(jnp.bfloat16)
                )
                new.append((total, mixed))
            return tuple(new)

        zero = (jnp.zeros((8, BLOCK), jnp.float32), jnp.zeros((HEAD_DIM, BLOCK), jnp.float32))
        done = lax.fori_loop(0, count, mix, (zero, zero))
        outs = []
        for h in range(2):
            total = jnp.sum(done[h][0], axis=0, keepdims=True)
            total = jnp.where(total > 0, total, 1.0)
            lse_ref[h : h + 1, rows] = tops[h] + jnp.log(total)
            outs.append(done[h][1] / total)
        out = jnp.concatenate(outs, axis=0)
        ot_ref[:, rows] = out
        o_ref[rows, :] = out.T.astype(jnp.bfloat16)


def attend(meta, query, keys, values, marks):
    rows = query.shape[0]
    window = keys.shape[0]
    deepest = (2 * IMG + 3 * BLOCK) // BLOCK * BLOCK
    vmem = pl.BlockSpec(memory_space=pltpu.VMEM)
    return pl.pallas_call(
        attend_kernel,
        out_shape=(
            jax.ShapeDtypeStruct((rows, PAIR), jnp.bfloat16),
            jax.ShapeDtypeStruct((PAIR, rows), jnp.float32),
            jax.ShapeDtypeStruct((8, rows), jnp.float32),
        ),
        in_specs=[pl.BlockSpec(memory_space=pltpu.SMEM), vmem, vmem, vmem, vmem],
        out_specs=(vmem, vmem, vmem),
        scratch_shapes=[
            pltpu.VMEM((PAIR, window), jnp.bfloat16),
            pltpu.VMEM((2, window, PAIR), jnp.bfloat16),
            pltpu.VMEM((2, deepest, BLOCK), jnp.float32),
        ],
        cost_estimate=pl.CostEstimate(
            flops=4 * rows * 2 * IMG * PAIR, transcendentals=2 * rows * IMG, bytes_accessed=9 << 20
        ),
        name="attend",
    )(meta, query, keys, values, marks)


def attend_back_kernel(
    meta, q_ref, k_ref, v_ref, m_ref, g_ref, ot_ref, lse_ref, dq_ref, dk_ref, dv_ref, kt, k_aug
):
    rows_all = dq_ref.shape[0]
    tiles = rows_all // BLOCK
    window = k_ref.shape[0]
    halo = (window - BLOCK - rows_all) // 2
    half, usable = lane_marks()

    @pl.loop(0, window // BLOCK)
    def _(i):
        at = pl.ds(pl.multiple_of(i * BLOCK, BLOCK), BLOCK)
        kt[:, at] = k_ref[at, :].T
        for h in range(2):
            k_aug[h, at, :] = jnp.where(half == h, k_ref[at, :], m_ref[at, :])
        dk_ref[at, :] = jnp.zeros((BLOCK, PAIR), jnp.float32)
        dv_ref[at, :] = jnp.zeros((BLOCK, PAIR), jnp.float32)

    @pl.loop(0, tiles)
    def _(t):
        start = meta[2 * t]
        count = meta[2 * t + 1]
        rows = pl.ds(pl.multiple_of(t * BLOCK, BLOCK), BLOCK)
        grad = g_ref[rows, :]
        blank = jnp.zeros_like(grad)
        spots = pl.ds(pl.multiple_of(halo + t * BLOCK, BLOCK), BLOCK)
        query = asking(q_ref[rows, :], m_ref[spots, :], half, usable)
        query_only = jnp.concatenate(
            [jnp.where(half == h, query[h], blank) for h in range(2)], axis=0
        )
        grads = [jnp.where(half == h, grad, blank) for h in range(2)]
        grads_both = jnp.concatenate(grads, axis=0)
        product = grad.astype(jnp.float32).T * ot_ref[:, rows]
        delta = [
            jnp.sum(product[h * HEAD_DIM : (h + 1) * HEAD_DIM], axis=0, keepdims=True)
            for h in range(2)
        ]
        lse = [lse_ref[h : h + 1, rows] for h in range(2)]

        def step(i, carry):
            at = pl.ds(pl.multiple_of(start + i * BLOCK, 128), BLOCK)
            value = v_ref[at, :]
            probs, slopes, new = [], [], []
            for h in range(2):
                part = lax.dot_general(
                    k_aug[h, at, :], query[h], NT, preferred_element_type=jnp.float32
                )
                weights = jnp.exp(part - lse[h])
                pull = lax.dot_general(value, grads[h], NT, preferred_element_type=jnp.float32)
                slope = (weights * (pull - delta[h])).astype(jnp.bfloat16)
                probs.append(weights.astype(jnp.bfloat16))
                slopes.append(slope)
                new.append(carry[h] + matmul(kt[h * HEAD_DIM : (h + 1) * HEAD_DIM, at], slope))
            dv_ref[at, :] += matmul(jnp.concatenate(probs, axis=1), grads_both)
            dk_ref[at, :] += matmul(jnp.concatenate(slopes, axis=1), query_only)
            return tuple(new)

        zero = jnp.zeros((HEAD_DIM, BLOCK), jnp.float32)
        done = lax.fori_loop(0, count, step, (zero, zero))
        dq = jnp.concatenate(done, axis=0) * (HEAD_DIM**-0.5)
        dq_ref[rows, :] = dq.T.astype(jnp.bfloat16)


def attend_back(meta, query, keys, values, marks, grad, out_t, lse):
    rows = query.shape[0]
    window = keys.shape[0]
    vmem = pl.BlockSpec(memory_space=pltpu.VMEM)
    return pl.pallas_call(
        attend_back_kernel,
        out_shape=(
            jax.ShapeDtypeStruct((rows, PAIR), jnp.bfloat16),
            jax.ShapeDtypeStruct((window, PAIR), jnp.float32),
            jax.ShapeDtypeStruct((window, PAIR), jnp.float32),
        ),
        in_specs=[pl.BlockSpec(memory_space=pltpu.SMEM)] + [vmem] * 7,
        out_specs=(vmem, vmem, vmem),
        scratch_shapes=[
            pltpu.VMEM((PAIR, window), jnp.bfloat16),
            pltpu.VMEM((2, window, PAIR), jnp.bfloat16),
        ],
        cost_estimate=pl.CostEstimate(
            flops=10 * rows * 2 * IMG * PAIR, transcendentals=2 * rows * IMG, bytes_accessed=16 << 20
        ),
        name="attend_back",
    )(meta, query, keys, values, marks, grad, out_t, lse)


CHUNK = 64
LAG = 2
MESH = pl.DeviceIdType.MESH


def split_index(f, r):
    return f // 2, f % 2, (r % GROUP) // 2, r % 2


def mixed_bits(left, right):
    value = 0
    for weight in (4, 2, 1):
        value = value + weight * ((left // weight + right // weight) % 2)
    return value


def remote(source, target, send, recv, peer):
    return pltpu.make_async_remote_copy(
        src_ref=source,
        dst_ref=target,
        send_sem=send,
        recv_sem=recv,
        device_id=peer,
        device_id_type=MESH,
    )


def greet(peers, optional=()):
    barrier = pltpu.get_barrier_semaphore()
    expected = len(peers)
    for peer in peers:
        pl.semaphore_signal(barrier, inc=1, device_id=peer, device_id_type=MESH)
    for there, peer in optional:

        @pl.when(there)
        def _():
            pl.semaphore_signal(barrier, inc=1, device_id=peer, device_id_type=MESH)

        expected = expected + there.astype(jnp.int32)
    pl.semaphore_wait(barrier, expected)


def qkv_kernel(
    replicas,
    tokens_ref,
    small_ref,
    codes_ref,
    w_ref,
    act_ref,
    q_out,
    k_out,
    v_out,
    codes_out,
    small_out,
    w_buf,
    stage,
    bias,
    own_sem,
    x_sem,
    core_sem,
    relay_sem,
    block_sem,
    halo_sem,
    code_sem,
    edge_sem,
    small_sem,
):
    f = lax.axis_index("fsdp")
    r = lax.axis_index("rep")
    x, c, z, y = split_index(f, r)
    lo = r % GROUP
    base = r - lo
    tok_rows = tokens_ref.shape[0]
    rows = GROUP * tok_rows
    halo = (k_out.shape[0] - BLOCK - rows) // 2
    half = GROUP // 2
    share = w_ref.shape[0]
    core_peer = (x * 2 + 1 - c, r)
    x_peer = ((1 - x) * 2 + c, r)
    fsdp_peers = [((f + step) % 4, r) for step in range(1, 4)]
    plane = [(f, base + (lo + step) % GROUP) for step in range(1, GROUP)]
    spot = f * replicas + r
    has_next = spot + GROUP < 4 * replicas
    has_prev = spot >= GROUP
    after = lax.rem(spot + GROUP, 4 * replicas)
    before = lax.rem(spot + 3 * replicas + (replicas - GROUP), 4 * replicas)
    next_peer = (after // replicas, lax.rem(after, replicas))
    prev_peer = (before // replicas, lax.rem(before, replicas))
    greet(fsdp_peers + plane, [(has_next, next_peer), (has_prev, prev_peer)])

    def small_copy(step):
        return remote(
            small_ref,
            small_out.at[f],
            small_sem.at[0, step - 1],
            small_sem.at[1, step - 1],
            fsdp_peers[step - 1],
        )

    def lanes(part):
        return pl.ds(part * PAIR, PAIR)

    def shard_rows(owner):
        return pl.ds(pl.multiple_of(owner * share, share), share)

    def columns(part, pair):
        return w_ref.at[:, pl.ds(pl.multiple_of(part * D + pair * PAIR, PAIR), PAIR)]

    def slot(e, owner, part):
        return w_buf.at[e, shard_rows(owner), lanes(part)]

    def x_copy(e, part):
        pair = mixed_bits(lo, e)
        return remote(
            columns(part, pair), slot(e, f, part), x_sem.at[0, e, part], x_sem.at[1, e, part], x_peer
        )

    def core_copy(e, part):
        pair = mixed_bits(lo, e)
        return remote(
            columns(part, pair),
            slot(e, f, part),
            core_sem.at[0, e, part],
            core_sem.at[1, e, part],
            core_peer,
        )

    def own_copy(e, part):
        pair = mixed_bits(lo, e)
        return pltpu.make_async_copy(columns(part, pair), slot(e, f, part), own_sem.at[e, part])

    def relay_copy(e, part):
        here = slot(e, (1 - x) * 2 + c, part)
        return remote(here, here, relay_sem.at[0, e, part], relay_sem.at[1, e, part], core_peer)

    def code_copy(step):
        return remote(
            codes_ref,
            codes_out.at[half + lo],
            code_sem.at[0, step - 1],
            code_sem.at[1, step - 1],
            plane[step - 1],
        )

    order = (4, 5, 6, 7, 2, 3, 1, 0)
    for step in range(1, 4):
        small_copy(step).start()
    for e in order:
        for part in range(3):
            x_copy(e, part).start()
            core_copy(e, part).start()
            own_copy(e, part).start()
    for step in range(1, GROUP):
        code_copy(step).start()
    codes_out[half + lo] = codes_ref[...]

    k_out[2 * halo + rows :, :] = jnp.zeros((BLOCK, PAIR), jnp.bfloat16)
    v_out[2 * halo + rows :, :] = jnp.zeros((BLOCK, PAIR), jnp.bfloat16)
    for there, low, edge in ((has_prev, 0, 0), (has_next, halo + rows, half + GROUP)):

        @pl.when(jnp.logical_not(there))
        def _():
            k_out[low : low + halo, :] = jnp.zeros((halo, PAIR), jnp.bfloat16)
            v_out[low : low + halo, :] = jnp.zeros((halo, PAIR), jnp.bfloat16)
            codes_out[edge : edge + half] = jnp.zeros((half, 8, PAIR), jnp.float32)

    unit, scale = normalize(tokens_ref[...].astype(jnp.float32))
    small_out[f] = small_ref[...]
    for step in range(1, 4):
        small_copy(step).wait()
    table = [small_out[owner].astype(jnp.float32) for owner in range(4)]

    def vector(line):
        return jnp.concatenate(
            [table[owner][line + row : line + row + 1] for owner in range(4) for row in range(2)],
            axis=1,
        )

    for which, line in ((0, 4), (1, 6)):
        bias[which] = jnp.concatenate(
            [table[owner][line : line + 2] for owner in range(4)], axis=0
        )
    act_ref[...] = (unit * vector(0) + vector(2)).astype(jnp.bfloat16)

    def block_copy(e, part):
        pair = mixed_bits(lo, e)
        into = (q_out, k_out, v_out)[part]
        lead = lo * tok_rows + (0 if part == 0 else halo)
        return remote(
            stage.at[e, part],
            into.at[pl.ds(pl.multiple_of(lead, 128), tok_rows), :],
            block_sem.at[0, e, part],
            block_sem.at[1, e, part],
            (f, base + pair),
        )

    @pl.loop(0, GROUP)
    def _(s):
        e = jnp.where(s < 4, s + 4, jnp.where(s < 6, s - 2, 7 - s))
        pair = mixed_bits(lo, e)
        for part in range(3):
            x_copy(e, part).wait_recv()
            relay_copy(e, part).start()
        for part in range(3):
            own_copy(e, part).wait()
            core_copy(e, part).wait_recv()
            relay_copy(e, part).wait_recv()
        result = matmul(act_ref[...], w_buf[e])
        outs = (
            (result[:, :PAIR] + bias[0, pl.ds(pair, 1), :]) * (HEAD_DIM**-0.5),
            result[:, PAIR : 2 * PAIR],
            result[:, 2 * PAIR :] + bias[1, pl.ds(pair, 1), :],
        )
        for part in range(3):
            stage[e, part] = outs[part].astype(jnp.bfloat16)

        @pl.when(s < GROUP - 1)
        def _():
            for part in range(3):
                block_copy(e, part).start()

        @pl.when(s == GROUP - 1)
        def _():
            for part, into in enumerate((q_out, k_out, v_out)):
                lead = lo * tok_rows + (0 if part == 0 else halo)
                into[pl.ds(pl.multiple_of(lead, 128), tok_rows), :] = outs[part].astype(
                    jnp.bfloat16
                )

    def halo_copy(source, part, forward):
        into = (k_out, v_out)[part]
        lead = source * tok_rows
        put = lead + halo - rows if forward else lead + halo + rows
        return remote(
            into.at[pl.ds(pl.multiple_of(halo + lead, 128), tok_rows), :],
            into.at[pl.ds(pl.multiple_of(put, 128), tok_rows), :],
            halo_sem.at[0, source, part],
            halo_sem.at[1, source, part],
            next_peer if forward else prev_peer,
        )

    def pass_on(source):
        for there, forward, fits in (
            (has_next, True, source >= half),
            (has_prev, False, source < half),
        ):

            @pl.when(there & fits)
            def _():
                for part in range(2):
                    halo_copy(source, part, forward).start()

    pass_on(lo)
    for e in (1, 2, 3, 4, 5, 6, 7):
        for part in range(3):
            block_copy(e, part).wait_recv()
        pass_on(mixed_bits(lo, e))

    for step in range(1, GROUP):
        code_copy(step).wait()

    def edge_copy(forward):
        low, put = (GROUP, 0) if forward else (half, half + GROUP)
        return remote(
            codes_out.at[pl.ds(low, half)],
            codes_out.at[pl.ds(put, half)],
            edge_sem.at[0, int(forward)],
            edge_sem.at[1, int(forward)],
            next_peer if forward else prev_peer,
        )

    sides = ((has_next, has_prev, True), (has_prev, has_next, False))
    for there, here, forward in sides:

        @pl.when(there)
        def _():
            edge_copy(forward).start()

    for e in range(GROUP):
        for part in range(3):
            x_copy(e, part).wait_send()
            core_copy(e, part).wait_send()
            relay_copy(e, part).wait_send()
            if e > 0:
                block_copy(e, part).wait_send()
    for there, here, forward in sides:
        sources = range(half, GROUP) if forward else range(half)

        @pl.when(there)
        def _():
            edge_copy(forward).wait_send()
            for source in sources:
                for part in range(2):
                    halo_copy(source, part, forward).wait_send()

        @pl.when(here)
        def _():
            edge_copy(forward).wait_recv()
            for source in sources:
                for part in range(2):
                    halo_copy(source, part, forward).wait_recv()


def project(replicas, tokens, small, codes, w_qkv):
    tok_rows = tokens.shape[0]
    rows = GROUP * tok_rows
    window = 2 * rows + BLOCK
    low = jnp.bfloat16
    vmem = pl.BlockSpec(memory_space=pltpu.VMEM)
    dma = pltpu.SemaphoreType.DMA
    shape = jax.ShapeDtypeStruct
    return pl.pallas_call(
        functools.partial(qkv_kernel, replicas),
        out_shape=(
            shape((tok_rows, D), low),
            shape((rows, PAIR), low),
            shape((window, PAIR), low),
            shape((window, PAIR), low),
            shape((2 * GROUP, 8, PAIR), jnp.float32),
            shape((4,) + small.shape, low),
        ),
        in_specs=[vmem, vmem, vmem, pl.BlockSpec(memory_space=pl.ANY)],
        out_specs=(vmem,) * 6,
        scratch_shapes=[
            pltpu.VMEM((GROUP, D, 3 * PAIR), low),
            pltpu.VMEM((GROUP, 3, tok_rows, PAIR), low),
            pltpu.VMEM((2, GROUP, PAIR), jnp.float32),
            dma((GROUP, 3)),
            dma((2, GROUP, 3)),
            dma((2, GROUP, 3)),
            dma((2, GROUP, 3)),
            dma((2, GROUP, 3)),
            dma((2, GROUP, 2)),
            dma((2, GROUP - 1)),
            dma((2, 2)),
            dma((2, 3)),
        ],
        compiler_params=pltpu.CompilerParams(
            collective_id=2, has_side_effects=True, vmem_limit_bytes=40 << 20
        ),
        cost_estimate=pl.CostEstimate(
            flops=2 * tok_rows * D * 3 * D, transcendentals=0, bytes_accessed=60 << 20
        ),
        name="project",
    )(tokens, small, codes, w_qkv)


def reduce_kernel(
    down_ref,
    up_ref,
    out_ref,
    qkv_ref,
    small_ref,
    down_final,
    up_final,
    out_final,
    qkv_final,
    small_final,
    own,
    from_core,
    from_x,
    from_y,
    from_z,
    small_own,
    small_core,
    small_x,
    small_all,
    load_sem,
    core_sem,
    x_sem,
    y_sem,
    z_sem,
    zz_sem,
    yy_sem,
    small_sem,
):
    f = lax.axis_index("fsdp")
    r = lax.axis_index("rep")
    x, c, z, y = split_index(f, r)
    base = r - r % GROUP
    core_peer = (x * 2 + 1 - c, r)
    x_peer = ((1 - x) * 2 + c, r)
    y_peer = (f, base + z * 2 + 1 - y)
    z_spots = [(z + step) % 4 for step in range(1, 4)]
    z_peers = [(f, base + spot * 2 + y) for spot in z_spots]
    plane = [(f, base + (r % GROUP + step) % GROUP) for step in range(1, GROUP)]
    total = own.shape[0]

    greet([core_peer, x_peer] + plane)

    refs = (down_ref, up_ref, out_ref, qkv_ref)
    finals = (down_final, up_final, out_final, qkv_final)
    spans = []
    first = 0
    for ref, final in zip(refs, finals):
        height = final.shape[0] // CHUNK
        amount = height * (final.shape[1] // D)
        spans.append((ref, first, first + amount, height, final))
        first += amount

    def piece(ref, low, height, k, owner):
        at = k - low
        top = owner * (height * CHUNK) + (at % height) * CHUNK
        left = (at // height) * D
        return ref.at[pl.ds(pl.multiple_of(top, CHUNK), CHUNK), pl.ds(pl.multiple_of(left, D), D)]

    def enter_copies(ref, low, height, k):
        copies = []
        for side in range(2):
            copies.append(
                remote(
                    piece(ref, low, height, k, side * 2 + 1 - c),
                    from_core.at[k, side],
                    core_sem.at[0, k, side],
                    core_sem.at[1, k, side],
                    core_peer,
                )
            )
            copies.append(
                pltpu.make_async_copy(
                    piece(ref, low, height, k, side * 2 + c), own.at[k, side], load_sem.at[k, side]
                )
            )
        return copies

    def enter(k):
        for ref, low, high, height, final in spans:

            @pl.when((k >= low) & (k < high))
            def _():
                for copy in enter_copies(ref, low, height, k):
                    copy.start()

    x_copy = lambda k: remote(
        own.at[k, 1 - x], from_x.at[k], x_sem.at[0, k], x_sem.at[1, k], x_peer
    )
    half = CHUNK // 2
    quarter = D // 4

    def y_copy(k):
        rows = pl.ds(pl.multiple_of((1 - y) * half, half), half)
        return remote(
            own.at[k, x, rows], from_y.at[k], y_sem.at[0, k], y_sem.at[1, k], y_peer
        )

    my_rows = pl.ds(pl.multiple_of(y * half, half), half)
    my_lanes = pl.ds(pl.multiple_of(z * quarter, quarter), quarter)

    def z_copies(k):
        copies = []
        for step in range(3):
            lanes = pl.ds(pl.multiple_of(z_spots[step] * quarter, quarter), quarter)
            copies.append(
                remote(
                    own.at[k, x, my_rows, lanes],
                    from_z.at[k, step],
                    z_sem.at[0, k, step],
                    z_sem.at[1, k, step],
                    z_peers[step],
                )
            )
        return copies

    def place(low, height, k, shift, tall, across, wide):
        at = k - low
        top = (at % height) * CHUNK + shift
        left = (at // height) * D + across
        return (
            pl.ds(pl.multiple_of(top, tall), tall),
            pl.ds(pl.multiple_of(left, wide), wide),
        )

    def zz_copy(k, step, here):
        return remote(here, here, zz_sem.at[0, k, step], zz_sem.at[1, k, step], z_peers[step])

    def yy_copy(k, here):
        return remote(here, here, yy_sem.at[0, k], yy_sem.at[1, k], y_peer)

    def core_sum(k):
        for side in range(2):
            target = own.at[k, side]
            pltpu.make_async_copy(target, target, load_sem.at[k, side]).wait()
            remote(
                target,
                from_core.at[k, side],
                core_sem.at[0, k, side],
                core_sem.at[1, k, side],
                core_peer,
            ).wait()
        for side in range(2):
            own[k, side] = (
                own[k, side].astype(jnp.float32) + from_core[k, side].astype(jnp.float32)
            ).astype(jnp.bfloat16)
        x_copy(k).start()

    def x_sum(k):
        x_copy(k).wait()
        own[k, x] = (own[k, x].astype(jnp.float32) + from_x[k].astype(jnp.float32)).astype(
            jnp.bfloat16
        )
        y_copy(k).start()

    def y_sum(k):
        y_copy(k).wait()
        own[k, x, my_rows] = (
            own[k, x, my_rows].astype(jnp.float32) + from_y[k].astype(jnp.float32)
        ).astype(jnp.bfloat16)
        for copy in z_copies(k):
            copy.start()

    def z_sum(k):
        for copy in z_copies(k):
            copy.wait()
        value = own[k, x, my_rows, my_lanes].astype(jnp.float32)
        for step in range(3):
            value = value + from_z[k, step].astype(jnp.float32)
        value = value.astype(jnp.bfloat16)
        for ref, low, high, height, final in spans:

            @pl.when((k >= low) & (k < high))
            def _():
                at = place(low, height, k, y * half, half, z * quarter, quarter)
                final[at] = value
                for step in range(3):
                    zz_copy(k, step, final.at[at]).start()

    def z_join(k):
        for step in range(3):
            zz_copy(k, step, from_z.at[k, step]).wait()
        for ref, low, high, height, final in spans:

            @pl.when((k >= low) & (k < high))
            def _():
                at = place(low, height, k, y * half, half, 0, D)
                yy_copy(k, final.at[at]).start()

    def y_join(k):
        yy_copy(k, from_y.at[k]).wait()

    def small_enter(side):
        return remote(
            small_ref.at[side * 2 + 1 - c],
            small_core.at[side],
            small_sem.at[0, side],
            small_sem.at[1, side],
            core_peer,
        )

    small_cross = remote(
        small_own.at[1 - x], small_x, small_sem.at[0, 2], small_sem.at[1, 2], x_peer
    )

    def small_spread(step):
        return remote(
            small_own.at[2],
            small_all.at[step - 1],
            small_sem.at[0, 2 + step],
            small_sem.at[1, 2 + step],
            plane[step - 1],
        )

    for side in range(2):
        small_enter(side).start()

    steps = (enter, core_sum, x_sum, y_sum, z_sum, z_join, y_join)

    @pl.loop(0, total + LAG * (len(steps) - 1))
    def _(now):
        @pl.when(now == 4)
        def _():
            for side in range(2):
                small_enter(side).wait()
            for side in range(2):
                small_own[side] = small_ref[side * 2 + c] + small_core[side]
            small_cross.start()

        @pl.when(now == 8)
        def _():
            small_cross.wait()
            small_own[2] = small_own[x] + small_x[...]
            for step in range(1, GROUP):
                small_spread(step).start()

        for order, step in enumerate(steps):
            k = now - order * LAG

            @pl.when((k >= 0) & (k < total))
            def _():
                step(k)

    for step in range(1, GROUP):
        small_spread(step).wait()
    value = small_own[2]
    for step in range(1, GROUP):
        value = value + small_all[step - 1]
    small_final[...] = value


def reduce_grads(weights, small):
    chunks = sum(weight.size for weight in weights) // (4 * CHUNK * D)
    tall = small.shape[1]
    anywhere = pl.BlockSpec(memory_space=pl.ANY)
    vmem = pl.BlockSpec(memory_space=pltpu.VMEM)
    dma = pltpu.SemaphoreType.DMA
    low = jnp.bfloat16
    return pl.pallas_call(
        reduce_kernel,
        out_shape=tuple(
            jax.ShapeDtypeStruct((weight.shape[0] // 4, weight.shape[1]), low) for weight in weights
        )
        + (jax.ShapeDtypeStruct((tall, 128), jnp.float32),),
        in_specs=[anywhere] * 4 + [vmem],
        out_specs=(vmem,) * 5,
        scratch_shapes=[
            pltpu.VMEM((chunks, 2, CHUNK, D), low),
            pltpu.VMEM((chunks, 2, CHUNK, D), low),
            pltpu.VMEM((chunks, CHUNK, D), low),
            pltpu.VMEM((chunks, CHUNK // 2, D), low),
            pltpu.VMEM((chunks, 3, CHUNK // 2, D // 4), low),
            pltpu.VMEM((3, tall, 128), jnp.float32),
            pltpu.VMEM((2, tall, 128), jnp.float32),
            pltpu.VMEM((tall, 128), jnp.float32),
            pltpu.VMEM((GROUP - 1, tall, 128), jnp.float32),
            dma((chunks, 2)),
            dma((2, chunks, 2)),
            dma((2, chunks)),
            dma((2, chunks)),
            dma((2, chunks, 3)),
            dma((2, chunks, 3)),
            dma((2, chunks)),
            dma((2, GROUP + 2)),
        ],
        compiler_params=pltpu.CompilerParams(
            collective_id=1, has_side_effects=True, vmem_limit_bytes=60 << 20
        ),
        cost_estimate=pl.CostEstimate(flops=0, transcendentals=0, bytes_accessed=200 << 20),
        name="reduce_grads",
    )(*weights, small)


def shards(
    tokens,
    out_grad,
    norm1_gain,
    norm1_bias,
    w_qkv,
    q_bias,
    v_bias,
    w_out,
    out_bias,
    attn_scale,
    norm2_gain,
    norm2_bias,
    w_up,
    up_bias,
    w_down,
    down_bias,
    mlp_scale,
    image_ids,
    pad_mask,
):
    both = ("fsdp", "rep")
    owners = lax.axis_size("fsdp")
    replicas = lax.axis_size("rep")
    tok_rows = tokens.shape[0]
    rows = GROUP * tok_rows
    groups = [list(range(g, g + GROUP)) for g in range(0, replicas, GROUP)]
    factor = HEAD_DIM ** (-0.5)

    small = (
        norm1_gain,
        norm1_bias,
        q_bias,
        v_bias,
        out_bias,
        attn_scale,
        norm2_gain,
        norm2_bias,
        down_bias,
        mlp_scale,
        up_bias,
    )
    sizes = [member.shape[0] for member in small]
    packed = jnp.concatenate(small + (jnp.zeros((-sum(sizes) % 2048,), jnp.bfloat16),))
    codes = jnp.where(pad_mask > 0, image_ids + 1, 0).astype(jnp.float32).reshape(-1, PAIR)
    code_rows = codes.shape[0]
    codes = jnp.concatenate([codes, jnp.zeros((8 - code_rows, PAIR), jnp.float32)], axis=0)
    act_one, query, key_window, value_window, codes, vectors = project(
        replicas, tokens, packed.reshape(-1, PAIR), codes, w_qkv
    )
    vectors = vectors.reshape(4, -1).astype(jnp.float32)
    parts = []
    place = 0
    for member in small:
        parts.append(vectors[:, place : place + member.shape[0]].reshape(-1))
        place += member.shape[0]
    (
        gain_first,
        shift_first,
        query_bias,
        value_bias,
        proj_bias,
        attn_gamma,
        gain_second,
        shift_second,
        final_bias,
        mlp_gamma,
        hidden_bias,
    ) = parts

    wide_qkv = lax.all_gather(w_qkv, "fsdp", axis=0, tiled=True)
    wide_out = lax.all_gather(w_out, "fsdp", axis=0, tiled=True)
    wide_up = lax.all_gather(w_up, "fsdp", axis=0, tiled=True)
    wide_down = lax.all_gather(w_down, "fsdp", axis=0, tiled=True)

    window = key_window.shape[0]
    halo = rows // 2
    seen = codes[:, :code_rows].reshape(-1).astype(jnp.int32)
    seen = jnp.concatenate([seen, jnp.zeros((BLOCK,), jnp.int32)])
    spot = jnp.arange(window, dtype=jnp.int32)
    asked = seen[halo : halo + rows]
    tile_codes = asked.reshape(rows // BLOCK, BLOCK)
    first_code = jnp.min(jnp.where(tile_codes > 0, tile_codes, 1 << 30), axis=1)
    last_code = jnp.max(tile_codes, axis=1)
    begin = jnp.min(jnp.where(seen[None] == first_code[:, None], spot[None], window), axis=1)
    finish = jnp.max(jnp.where(seen[None] == last_code[:, None], spot[None] + 1, 0), axis=1)
    begin = begin // 128 * 128
    count = jnp.where(last_code > 0, (finish - begin + BLOCK - 1) // BLOCK, 0)
    meta = jnp.stack([begin, count], axis=1).reshape(-1)

    lane_slot = jnp.arange(PAIR, dtype=jnp.int32) % HEAD_DIM
    key_slot = jnp.where(seen > 0, 1 + (seen - 1) % SLOTS, 0)
    marks = (key_slot[:, None] == lane_slot[None]).astype(jnp.bfloat16)

    inputs = tokens.astype(jnp.float32)
    unit_one, scale_one = normalize(inputs)

    def exchange(block):
        return lax.all_to_all(
            block, "rep", split_axis=0, concat_axis=0, tiled=True, axis_index_groups=groups
        )

    attn_mine, attn_t, lse = attend(meta, query, key_window, value_window, marks)

    def to_tokens(block):
        back = exchange(block.reshape(GROUP, tok_rows, block.shape[-1]))
        return back.transpose(1, 0, 2)

    attn_low = to_tokens(attn_mine).reshape(tok_rows, D)
    proj = matmul(attn_low, wide_out) + proj_bias
    residual = inputs + attn_gamma * proj
    unit_two, scale_two = normalize(residual)
    act_two = (unit_two * gain_second + shift_second).astype(jnp.bfloat16)
    pre_act = matmul(act_two, wide_up) + hidden_bias
    phi_cdf = 0.5 * (1.0 + lax.erf(pre_act * (0.5**0.5)))
    hidden = (pre_act * phi_cdf).astype(jnp.bfloat16)
    slope = phi_cdf + pre_act * (jnp.exp(-0.5 * pre_act * pre_act) * 0.3989422804014327)
    branch = matmul(hidden, wide_down) + final_bias
    layer_out = (residual + mlp_gamma * branch).astype(jnp.bfloat16)

    upstream = out_grad.astype(jnp.float32)
    mlp_gamma_grad = jnp.sum(upstream * branch, axis=0)
    branch_grad = mlp_gamma * upstream
    final_bias_grad = jnp.sum(branch_grad, axis=0)
    branch_low = branch_grad.astype(jnp.bfloat16)
    down_grad = matmul_tn(hidden, branch_low).astype(jnp.bfloat16)
    pre_grad = matmul_nt(branch_low, wide_down) * slope
    hidden_bias_grad = jnp.sum(pre_grad, axis=0)
    pre_low = pre_grad.astype(jnp.bfloat16)
    up_grad = matmul_tn(act_two, pre_low).astype(jnp.bfloat16)
    act_two_grad = matmul_nt(pre_low, wide_up)
    gain_second_grad = jnp.sum(act_two_grad * unit_two, axis=0)
    shift_second_grad = jnp.sum(act_two_grad, axis=0)
    residual_grad = upstream + norm_back(act_two_grad, unit_two, scale_two, gain_second)
    attn_gamma_grad = jnp.sum(residual_grad * proj, axis=0)
    proj_grad = attn_gamma * residual_grad
    proj_bias_grad = jnp.sum(proj_grad, axis=0)
    proj_low = proj_grad.astype(jnp.bfloat16)
    out_weight_grad = matmul_tn(attn_low, proj_low).astype(jnp.bfloat16)
    attn_grad_low = matmul_nt(proj_low, wide_out).astype(jnp.bfloat16)

    grad_sent = attn_grad_low.reshape(tok_rows, GROUP, PAIR).transpose(1, 0, 2)
    grad_mine = exchange(grad_sent).reshape(rows, PAIR)
    dq, dk, dv = attend_back(
        meta, query, key_window, value_window, marks, grad_mine, attn_t, lse
    )
    dkv = jnp.concatenate([dk, dv], axis=1)
    tail = dkv[:halo].astype(jnp.bfloat16)
    head = dkv[halo + rows : halo + rows + halo].astype(jnp.bfloat16)
    from_after = from_behind(tail, both, -GROUP)
    from_before = from_behind(head, both, GROUP)
    own = dkv[halo : halo + rows] + jnp.concatenate([from_before, from_after], axis=0)
    dqkv_mine = jnp.concatenate([dq, own.astype(jnp.bfloat16)], axis=1)
    dqkv = to_tokens(dqkv_mine).reshape(tok_rows, GROUP, 3, PAIR)
    dqkv = dqkv.transpose(0, 2, 1, 3).reshape(tok_rows, 3 * D)
    query_bias_grad = jnp.sum(dqkv[:, :D].astype(jnp.float32), axis=0)
    value_bias_grad = jnp.sum(dqkv[:, 2 * D :].astype(jnp.float32), axis=0)
    qkv_weight_grad = matmul_tn(act_one, dqkv).astype(jnp.bfloat16)
    act_one_grad = matmul_nt(dqkv, wide_qkv)
    gain_first_grad = jnp.sum(act_one_grad * unit_one, axis=0)
    shift_first_grad = jnp.sum(act_one_grad, axis=0)
    input_part = norm_back(act_one_grad, unit_one, scale_one, gain_first)
    tokens_grad = (residual_grad + input_part).astype(jnp.bfloat16)

    small_grads = (
        gain_first_grad,
        shift_first_grad,
        query_bias_grad,
        value_bias_grad,
        proj_bias_grad,
        attn_gamma_grad,
        gain_second_grad,
        shift_second_grad,
        final_bias_grad,
        mlp_gamma_grad,
        hidden_bias_grad,
    )
    packed = jnp.concatenate([member.reshape(owners, -1) for member in small_grads], axis=1)
    packed = packed.reshape(owners, -1, 128)
    *grads, packed = reduce_grads((down_grad, up_grad, out_weight_grad, qkv_weight_grad), packed)
    grads = [grad.astype(jnp.float32) for grad in grads]
    if replicas > GROUP:
        apart = [list(range(low, replicas, GROUP)) for low in range(GROUP)]
        grads = lax.psum(grads, "rep", axis_index_groups=apart)
        packed = lax.psum(packed, "rep", axis_index_groups=apart)
    packed = packed.reshape(-1)
    small_out = []
    place = 0
    for member in small_grads:
        size = member.shape[0] // owners
        small_out.append(packed[place : place + size])
        place += size

    down_out, up_out, out_out, qkv_out = grads
    return (
        layer_out,
        tokens_grad,
        small_out[0],
        small_out[1],
        qkv_out,
        small_out[2],
        small_out[3],
        out_out,
        small_out[4],
        small_out[5],
        small_out[6],
        small_out[7],
        up_out,
        small_out[10],
        down_out,
        small_out[8],
        small_out[9],
    )


def solution(mesh):
    spread = P(("fsdp", "rep"), None)
    line = P("fsdp")
    plane = P("fsdp", None)
    return jax.shard_map(
        shards,
        mesh=mesh,
        in_specs=(
            spread,
            spread,
            line,
            line,
            plane,
            line,
            line,
            plane,
            line,
            line,
            line,
            line,
            plane,
            line,
            plane,
            line,
            line,
            P(("fsdp", "rep")),
            P(("fsdp", "rep")),
        ),
        out_specs=(
            spread,
            spread,
            line,
            line,
            plane,
            line,
            line,
            plane,
            line,
            line,
            line,
            line,
            plane,
            line,
            plane,
            line,
            line,
        ),
        check_vma=False,
    )
```

```python
import functools

import jax
import jax.numpy as jnp
from jax import lax
from jax.experimental import pallas as pl
from jax.experimental.pallas import tpu as pltpu
from jax.sharding import PartitionSpec as P

D = 1024
HEADS = 16
HEAD_DIM = 64
IMG = 1370

PAIR = 2 * HEAD_DIM
GROUP = HEADS // 2
BLOCK = 256
KEYS = 1536
SLOTS = 63

EPSILON = 1e-06
NEG_BIG = -1e30
NEG_EDGE = -1e29

NT = (((1,), (1,)), ((), ()))


def from_behind(block, axis, distance):
    devices = range(lax.axis_size(axis))
    route = [(i - distance, i) for i in devices if i - distance in devices]
    return lax.ppermute(block, axis, route)


def normalize(values):
    center = jnp.mean(values, axis=-1, keepdims=True)
    centered = values - center
    spread = jnp.mean(centered * centered, axis=-1, keepdims=True)
    scale = lax.rsqrt(spread + EPSILON)
    return centered * scale, scale


def norm_back(cotangent, unit, scale, gain):
    scaled = cotangent * gain
    along = jnp.mean(scaled, axis=-1, keepdims=True)
    across = jnp.mean(scaled * unit, axis=-1, keepdims=True)
    return scale * (scaled - along - unit * across)


def matmul(left, right):
    return jnp.dot(left, right, preferred_element_type=jnp.float32)


def fold_rows(values, op):
    return op(values.reshape(values.shape[0] // 8, 8, values.shape[1]), axis=0)


def lane_marks():
    lane = lax.broadcasted_iota(jnp.int32, (BLOCK, PAIR), 1)
    return lane // HEAD_DIM, lane % HEAD_DIM > 0


def asking(query, marks, half, usable):
    wanted = jnp.where((marks.astype(jnp.float32) > 0) & usable, 0.0, NEG_BIG).astype(jnp.bfloat16)
    return [jnp.where(half == h, query, wanted) for h in range(2)]


def attend_kernel(meta, q_ref, k_ref, v_ref, m_ref, o_ref, ot_ref, lse_ref, vt, k_aug, scores):
    rows_all = o_ref.shape[0]
    tiles = rows_all // BLOCK
    window = k_ref.shape[0]
    halo = (window - KEYS - rows_all) // 2
    half, usable = lane_marks()

    @pl.loop(0, window // BLOCK)
    def _(i):
        at = pl.ds(pl.multiple_of(i * BLOCK, BLOCK), BLOCK)
        vt[:, at] = v_ref[at, :].T
        for h in range(2):
            k_aug[h, at, :] = jnp.where(half == h, k_ref[at, :], m_ref[at, :])

    @pl.loop(0, tiles)
    def _(t):
        start = meta[2 * t]
        count = meta[2 * t + 1]
        rows = pl.ds(pl.multiple_of(t * BLOCK, BLOCK), BLOCK)
        spots = pl.ds(pl.multiple_of(halo + t * BLOCK, BLOCK), BLOCK)
        query = asking(q_ref[rows, :], m_ref[spots, :], half, usable)

        def score(i, tops):
            at = pl.ds(pl.multiple_of(start + i * KEYS, 128), KEYS)
            keep = pl.ds(pl.multiple_of(i * KEYS, KEYS), KEYS)
            new = []
            for h in range(2):
                part = lax.dot_general(
                    k_aug[h, at, :], query[h], NT, preferred_element_type=jnp.float32
                )
                scores[h, keep, :] = part
                new.append(jnp.maximum(tops[h], fold_rows(part, jnp.max)))
            return tuple(new)

        low = jnp.full((8, BLOCK), NEG_BIG, jnp.float32)
        tops = lax.fori_loop(0, count, score, (low, low))
        tops = [jnp.max(top, axis=0, keepdims=True) for top in tops]
        tops = [jnp.where(top < NEG_EDGE, 0.0, top) for top in tops]

        def mix(i, carry):
            at = pl.ds(pl.multiple_of(start + i * KEYS, 128), KEYS)
            keep = pl.ds(pl.multiple_of(i * KEYS, KEYS), KEYS)
            new = []
            for h in range(2):
                total, mixed = carry[h]
                weights = jnp.exp(scores[h, keep, :] - tops[h])
                total = total + fold_rows(weights, jnp.sum)
                mixed = mixed + matmul(
                    vt[h * HEAD_DIM : (h + 1) * HEAD_DIM, at], weights.astype(jnp.bfloat16)
                )
                new.append((total, mixed))
            return tuple(new)

        zero = (jnp.zeros((8, BLOCK), jnp.float32), jnp.zeros((HEAD_DIM, BLOCK), jnp.float32))
        done = lax.fori_loop(0, count, mix, (zero, zero))
        outs = []
        for h in range(2):
            total = jnp.sum(done[h][0], axis=0, keepdims=True)
            total = jnp.where(total > 0, total, 1.0)
            lse_ref[h : h + 1, rows] = tops[h] + jnp.log(total)
            outs.append(done[h][1] / total)
        out = jnp.concatenate(outs, axis=0)
        ot_ref[:, rows] = out
        o_ref[rows, :] = out.T.astype(jnp.bfloat16)


def attend(meta, query, keys, values, marks):
    rows = query.shape[0]
    window = keys.shape[0]
    deepest = (2 * IMG + 2 * BLOCK + KEYS) // KEYS * KEYS
    vmem = pl.BlockSpec(memory_space=pltpu.VMEM)
    return pl.pallas_call(
        attend_kernel,
        out_shape=(
            jax.ShapeDtypeStruct((rows, PAIR), jnp.bfloat16),
            jax.ShapeDtypeStruct((PAIR, rows), jnp.float32),
            jax.ShapeDtypeStruct((8, rows), jnp.float32),
        ),
        in_specs=[pl.BlockSpec(memory_space=pltpu.SMEM), vmem, vmem, vmem, vmem],
        out_specs=(vmem, vmem, vmem),
        scratch_shapes=[
            pltpu.VMEM((PAIR, window), jnp.bfloat16),
            pltpu.VMEM((2, window, PAIR), jnp.bfloat16),
            pltpu.VMEM((2, deepest, BLOCK), jnp.float32),
        ],
        cost_estimate=pl.CostEstimate(
            flops=4 * rows * 2 * IMG * PAIR, transcendentals=2 * rows * IMG, bytes_accessed=9 << 20
        ),
        name="attend",
    )(meta, query, keys, values, marks)


def attend_back_kernel(
    meta, q_ref, k_ref, v_ref, m_ref, g_ref, ot_ref, lse_ref, dq_ref, dk_out, dv_out, kt, k_aug, dk_ref, dv_ref
):
    rows_all = dq_ref.shape[0]
    tiles = rows_all // BLOCK
    window = k_ref.shape[0]
    halo = (window - KEYS - rows_all) // 2
    half, usable = lane_marks()

    @pl.loop(0, window // BLOCK)
    def _(i):
        at = pl.ds(pl.multiple_of(i * BLOCK, BLOCK), BLOCK)
        kt[:, at] = k_ref[at, :].T
        for h in range(2):
            k_aug[h, at, :] = jnp.where(half == h, k_ref[at, :], m_ref[at, :])
        dk_ref[at, :] = jnp.zeros((BLOCK, PAIR), jnp.float32)
        dv_ref[at, :] = jnp.zeros((BLOCK, PAIR), jnp.float32)

    @pl.loop(0, tiles)
    def _(t):
        start = meta[2 * t]
        count = meta[2 * t + 1]
        rows = pl.ds(pl.multiple_of(t * BLOCK, BLOCK), BLOCK)
        grad = g_ref[rows, :]
        blank = jnp.zeros_like(grad)
        spots = pl.ds(pl.multiple_of(halo + t * BLOCK, BLOCK), BLOCK)
        query = asking(q_ref[rows, :], m_ref[spots, :], half, usable)
        query_only = jnp.concatenate(
            [jnp.where(half == h, query[h], blank) for h in range(2)], axis=0
        )
        grads = [jnp.where(half == h, grad, blank) for h in range(2)]
        grads_both = jnp.concatenate(grads, axis=0)
        product = grad.astype(jnp.float32).T * ot_ref[:, rows]
        delta = [
            jnp.sum(product[h * HEAD_DIM : (h + 1) * HEAD_DIM], axis=0, keepdims=True)
            for h in range(2)
        ]
        lse = [lse_ref[h : h + 1, rows] for h in range(2)]

        def step(i, carry):
            at = pl.ds(pl.multiple_of(start + i * KEYS, 128), KEYS)
            value = v_ref[at, :]
            probs, slopes, new = [], [], []
            for h in range(2):
                part = lax.dot_general(
                    k_aug[h, at, :], query[h], NT, preferred_element_type=jnp.float32
                )
                weights = jnp.exp(part - lse[h])
                pull = lax.dot_general(value, grads[h], NT, preferred_element_type=jnp.float32)
                slope = (weights * (pull - delta[h])).astype(jnp.bfloat16)
                probs.append(weights.astype(jnp.bfloat16))
                slopes.append(slope)
                new.append(carry[h] + matmul(kt[h * HEAD_DIM : (h + 1) * HEAD_DIM, at], slope))
            dv_ref[at, :] += matmul(jnp.concatenate(probs, axis=1), grads_both)
            dk_ref[at, :] += matmul(jnp.concatenate(slopes, axis=1), query_only)
            return tuple(new)

        zero = jnp.zeros((HEAD_DIM, BLOCK), jnp.float32)
        done = lax.fori_loop(0, count, step, (zero, zero))
        dq = jnp.concatenate(done, axis=0) * (HEAD_DIM**-0.5)
        dq_ref[rows, :] = dq.T.astype(jnp.bfloat16)

    @pl.loop(0, window // BLOCK)
    def _(i):
        at = pl.ds(pl.multiple_of(i * BLOCK, BLOCK), BLOCK)
        dk_out[at, :] = dk_ref[at, :].astype(jnp.bfloat16)
        dv_out[at, :] = dv_ref[at, :].astype(jnp.bfloat16)


def attend_back(meta, query, keys, values, marks, grad, out_t, lse):
    rows = query.shape[0]
    window = keys.shape[0]
    vmem = pl.BlockSpec(memory_space=pltpu.VMEM)
    return pl.pallas_call(
        attend_back_kernel,
        out_shape=(
            jax.ShapeDtypeStruct((rows, PAIR), jnp.bfloat16),
            jax.ShapeDtypeStruct((window, PAIR), jnp.bfloat16),
            jax.ShapeDtypeStruct((window, PAIR), jnp.bfloat16),
        ),
        in_specs=[pl.BlockSpec(memory_space=pltpu.SMEM)] + [vmem] * 7,
        out_specs=(vmem, vmem, vmem),
        scratch_shapes=[
            pltpu.VMEM((PAIR, window), jnp.bfloat16),
            pltpu.VMEM((2, window, PAIR), jnp.bfloat16),
            pltpu.VMEM((window, PAIR), jnp.float32),
            pltpu.VMEM((window, PAIR), jnp.float32),
        ],
        cost_estimate=pl.CostEstimate(
            flops=10 * rows * 2 * IMG * PAIR, transcendentals=2 * rows * IMG, bytes_accessed=16 << 20
        ),
        name="attend_back",
    )(meta, query, keys, values, marks, grad, out_t, lse)


CHUNK = 64
LAG = 2
GIVE_AT = 3
TAKE_AT = 16
TAKE_BY = 1
LAST_TAKE = TAKE_AT + (GROUP - 1) * TAKE_BY
PAIR_BY = 2
WIDE_AT = 3
SHARED = (1, 2)
MESH = pl.DeviceIdType.MESH


def split_index(f, r):
    return f // 2, f % 2, (r % GROUP) // 2, r % 2


def mixed_bits(left, right):
    value = 0
    for weight in (4, 2, 1):
        value = value + weight * ((left // weight + right // weight) % 2)
    return value


def remote(source, target, send, recv, peer):
    return pltpu.make_async_remote_copy(
        src_ref=source,
        dst_ref=target,
        send_sem=send,
        recv_sem=recv,
        device_id=peer,
        device_id_type=MESH,
    )


def greet(peers, optional=()):
    barrier = pltpu.get_barrier_semaphore()
    expected = len(peers)
    for peer in peers:
        pl.semaphore_signal(barrier, inc=1, device_id=peer, device_id_type=MESH)
    for there, peer in optional:

        @pl.when(there)
        def _():
            pl.semaphore_signal(barrier, inc=1, device_id=peer, device_id_type=MESH)

        expected = expected + there.astype(jnp.int32)
    pl.semaphore_wait(barrier, expected)


def group_neighbours(f, r, replicas):
    spot = f * replicas + r
    after = lax.rem(spot + GROUP, 4 * replicas)
    before = lax.rem(spot + 3 * replicas + (replicas - GROUP), 4 * replicas)
    next_peer = (after // replicas, lax.rem(after, replicas))
    prev_peer = (before // replicas, lax.rem(before, replicas))
    return spot + GROUP < 4 * replicas, next_peer, spot >= GROUP, prev_peer


def qkv_kernel(
    replicas,
    tokens_ref,
    small_ref,
    codes_ref,
    w_ref,
    out_ref,
    up_ref,
    act_ref,
    q_out,
    k_out,
    v_out,
    codes_out,
    small_out,
    w_buf,
    out_full,
    up_full,
    stage,
    bias,
    own_sem,
    x_sem,
    y_sem,
    core_sem,
    relay_sem,
    block_sem,
    halo_sem,
    code_sem,
    edge_sem,
    small_sem,
    wide_sem,
):
    f = lax.axis_index("fsdp")
    r = lax.axis_index("rep")
    x, c, z, y = split_index(f, r)
    lo = r % GROUP
    base = r - lo
    tok_rows = tokens_ref.shape[0]
    rows = GROUP * tok_rows
    halo = (k_out.shape[0] - KEYS - rows) // 2
    half = GROUP // 2
    share = w_ref.shape[0]
    core_peer = (x * 2 + 1 - c, r)
    x_peer = ((1 - x) * 2 + c, r)
    y_peer = (f, base + z * 2 + 1 - y)
    fsdp_peers = [((f + step) % 4, r) for step in range(1, 4)]
    plane = [(f, base + (lo + step) % GROUP) for step in range(1, GROUP)]
    has_next, next_peer, has_prev, prev_peer = group_neighbours(f, r, replicas)
    greet(fsdp_peers + plane, [(has_next, next_peer), (has_prev, prev_peer)])

    def small_copy(step):
        return remote(
            small_ref,
            small_out.at[f],
            small_sem.at[0, step - 1],
            small_sem.at[1, step - 1],
            fsdp_peers[step - 1],
        )

    def lanes(part):
        return pl.ds(part * PAIR, PAIR)

    def shard_rows(owner):
        return pl.ds(pl.multiple_of(owner * share, share), share)

    def columns(part, pair):
        return w_ref.at[:, pl.ds(pl.multiple_of(part * D + pair * PAIR, PAIR), PAIR)]

    def slot(e, owner, part):
        return w_buf.at[e, shard_rows(owner), lanes(part)]

    across = (1 - x) * 2 + c
    wide_sets = 1 + up_ref.shape[0] // 64

    def wide_chunk(m, side, owner, mine):
        if m == 0:
            size, lead = out_ref.shape[0], 0
            own, full = out_ref, out_full
        else:
            size, lead = 64, 64 * (m - 1)
            own, full = up_ref, up_full
        if side is not None:
            size //= 2
            lead = lead + size * side
        if mine:
            return own.at[pl.ds(pl.multiple_of(lead, 32), size)]
        return full.at[pl.ds(pl.multiple_of(owner * own.shape[0] + lead, 32), size)]

    def wide_link(which, m, here, there, peer):
        return remote(here, there, wide_sem.at[0, which, m], wide_sem.at[1, which, m], peer)

    def wide_x(m):
        side = y if m in SHARED else None
        return wide_link(0, m, wide_chunk(m, side, f, True), wide_chunk(m, side, f, False), x_peer)

    def wide_y(m, side):
        here = wide_chunk(m, side, across, False)
        return wide_link(1, m, here, here, y_peer)

    def wide_core(m):
        return wide_link(
            2, m, wide_chunk(m, None, f, True), wide_chunk(m, None, f, False), core_peer
        )

    def wide_relay(m, side, which):
        here = wide_chunk(m, side, across, False)
        return wide_link(which, m, here, here, core_peer)

    def wide_pass(m):
        wide_x(m).wait_recv()
        if m in SHARED:
            wide_y(m, y).start()
        wide_relay(m, y if m in SHARED else None, 3).start()

    def wide_finish(m):
        wide_y(m, 1 - y).wait_recv()
        wide_relay(m, 1 - y, 4).start()

    def x_copy(e, part):
        pair = mixed_bits(lo, e)
        return remote(
            columns(part, pair), slot(e, f, part), x_sem.at[0, e, part], x_sem.at[1, e, part], x_peer
        )

    def y_copy(e, part):
        return remote(
            slot(e, across, part),
            slot(e + 1, across, part),
            y_sem.at[e, part],
            x_sem.at[1, e + 1, part],
            y_peer,
        )

    def arrival(e, part):
        here = slot(e, across, part)
        return remote(here, here, x_sem.at[0, e, part], x_sem.at[1, e, part], x_peer)

    def core_copy(e, part):
        pair = mixed_bits(lo, e)
        return remote(
            columns(part, pair),
            slot(e, f, part),
            core_sem.at[0, e, part],
            core_sem.at[1, e, part],
            core_peer,
        )

    def own_copy(e, part):
        pair = mixed_bits(lo, e)
        return pltpu.make_async_copy(columns(part, pair), slot(e, f, part), own_sem.at[e, part])

    def relay_copy(e, part):
        here = slot(e, across, part)
        return remote(here, here, relay_sem.at[0, e, part], relay_sem.at[1, e, part], core_peer)

    def code_copy(step):
        return remote(
            codes_ref,
            codes_out.at[half + lo],
            code_sem.at[0, step - 1],
            code_sem.at[1, step - 1],
            plane[step - 1],
        )

    order = (4, 5, 2, 3, 6, 7, 0, 1)
    for step in range(1, 4):
        small_copy(step).start()
    for e in order:
        for part in range(3):
            if e % 2 == 0:
                x_copy(e, part).start()
            core_copy(e, part).start()
            own_copy(e, part).start()
    for m in range(wide_sets):
        wide_x(m).start()
    for m in range(wide_sets):
        wide_core(m).start()
    for step in range(1, GROUP):
        code_copy(step).start()
    codes_out[half + lo] = codes_ref[...]

    k_out[2 * halo + rows :, :] = jnp.zeros((KEYS, PAIR), jnp.bfloat16)
    v_out[2 * halo + rows :, :] = jnp.zeros((KEYS, PAIR), jnp.bfloat16)
    for there, low, edge in ((has_prev, 0, 0), (has_next, halo + rows, half + GROUP)):

        @pl.when(jnp.logical_not(there))
        def _():
            k_out[low : low + halo, :] = jnp.zeros((halo, PAIR), jnp.bfloat16)
            v_out[low : low + halo, :] = jnp.zeros((halo, PAIR), jnp.bfloat16)
            codes_out[edge : edge + half] = jnp.zeros((half, 8, PAIR), jnp.float32)

    unit, scale = normalize(tokens_ref[...].astype(jnp.float32))
    small_out[f] = small_ref[...]
    for step in range(1, 4):
        small_copy(step).wait()
    table = [small_out[owner].astype(jnp.float32) for owner in range(4)]

    def vector(line):
        return jnp.concatenate(
            [table[owner][line + row : line + row + 1] for owner in range(4) for row in range(2)],
            axis=1,
        )

    for which, line in ((0, 4), (1, 6)):
        bias[which] = jnp.concatenate(
            [table[owner][line : line + 2] for owner in range(4)], axis=0
        )
    act_ref[...] = (unit * vector(0) + vector(2)).astype(jnp.bfloat16)

    def block_copy(e, part):
        pair = mixed_bits(lo, e)
        into = (q_out, k_out, v_out)[part]
        lead = lo * tok_rows + (0 if part == 0 else halo)
        return remote(
            stage.at[e, part],
            into.at[pl.ds(pl.multiple_of(lead, 128), tok_rows), :],
            block_sem.at[0, e, part],
            block_sem.at[1, e, part],
            (f, base + pair),
        )

    def nth(s):
        return jnp.where(s < 2, s + 4, jnp.where(s < 4, s, jnp.where(s < 6, s + 2, s - 6)))

    def halo_copy(source, part, forward):
        into = (k_out, v_out)[part]
        lead = source * tok_rows
        put = lead + halo - rows if forward else lead + halo + rows
        return remote(
            into.at[pl.ds(pl.multiple_of(halo + lead, 128), tok_rows), :],
            into.at[pl.ds(pl.multiple_of(put, 128), tok_rows), :],
            halo_sem.at[0, source, part],
            halo_sem.at[1, source, part],
            next_peer if forward else prev_peer,
        )

    def pass_on(source):
        for there, forward, fits in (
            (has_next, True, source >= half),
            (has_prev, False, source < half),
        ):

            @pl.when(there & fits)
            def _():
                for part in range(2):
                    halo_copy(source, part, forward).start()

    def pass_arrived(e):
        for part in range(3):
            block_copy(e, part).wait_recv()
        pass_on(mixed_bits(lo, e))

    @pl.loop(0, GROUP)
    def _(s):
        e = nth(s)
        pair = mixed_bits(lo, e)
        for part in range(3):
            arrival(e, part).wait_recv()
            relay_copy(e, part).start()

        @pl.when(e % 2 == 0)
        def _():
            for part in range(3):
                y_copy(e, part).start()

        for part in range(3):
            own_copy(e, part).wait()
            core_copy(e, part).wait_recv()
            relay_copy(e, part).wait_recv()
        result = matmul(act_ref[...], w_buf[e])
        outs = (
            (result[:, :PAIR] + bias[0, pl.ds(pair, 1), :]) * (HEAD_DIM**-0.5),
            result[:, PAIR : 2 * PAIR],
            result[:, 2 * PAIR :] + bias[1, pl.ds(pair, 1), :],
        )
        for part in range(3):
            stage[e, part] = outs[part].astype(jnp.bfloat16)

        @pl.when(e > 0)
        def _():
            for part in range(3):
                block_copy(e, part).start()

        @pl.when(e == 0)
        def _():
            for part, into in enumerate((q_out, k_out, v_out)):
                lead = lo * tok_rows + (0 if part == 0 else halo)
                into[pl.ds(pl.multiple_of(lead, 128), tok_rows), :] = outs[part].astype(
                    jnp.bfloat16
                )
            pass_on(lo)

        @pl.when(s >= GROUP // 2)
        def _():
            pass_arrived(nth(s - GROUP // 2))

        for m in range(wide_sets):
            if WIDE_AT + m < GROUP:
                pl.when(s == WIDE_AT + m)(functools.partial(wide_pass, m))


    for m in range(wide_sets):
        if WIDE_AT + m >= GROUP:
            wide_pass(m)
    pass_arrived(1)
    for m in SHARED:
        wide_finish(m)
    pass_arrived(6)
    pass_arrived(7)

    for step in range(1, GROUP):
        code_copy(step).wait()

    def edge_copy(forward):
        low, put = (GROUP, 0) if forward else (half, half + GROUP)
        return remote(
            codes_out.at[pl.ds(low, half)],
            codes_out.at[pl.ds(put, half)],
            edge_sem.at[0, int(forward)],
            edge_sem.at[1, int(forward)],
            next_peer if forward else prev_peer,
        )

    sides = ((has_next, has_prev, True), (has_prev, has_next, False))
    for there, here, forward in sides:

        @pl.when(there)
        def _():
            edge_copy(forward).start()

    for m in range(wide_sets):
        wide_x(m).wait_send()
        wide_core(m).wait()
        wide_relay(m, y if m in SHARED else None, 3).wait()
        if m in SHARED:
            wide_y(m, y).wait_send()
            wide_relay(m, 1 - y, 4).wait()
    for e in range(GROUP):
        for part in range(3):
            if e % 2 == 0:
                x_copy(e, part).wait_send()
                y_copy(e, part).wait_send()
            core_copy(e, part).wait_send()
            relay_copy(e, part).wait_send()
            if e > 0:
                block_copy(e, part).wait_send()
    for there, here, forward in sides:
        sources = range(half, GROUP) if forward else range(half)

        @pl.when(there)
        def _():
            edge_copy(forward).wait_send()
            for source in sources:
                for part in range(2):
                    halo_copy(source, part, forward).wait_send()

        @pl.when(here)
        def _():
            edge_copy(forward).wait_recv()
            for source in sources:
                for part in range(2):
                    halo_copy(source, part, forward).wait_recv()


def project(replicas, tokens, small, codes, w_qkv, w_out, w_up):
    tok_rows = tokens.shape[0]
    rows = GROUP * tok_rows
    window = 2 * rows + KEYS
    low = jnp.bfloat16
    vmem = pl.BlockSpec(memory_space=pltpu.VMEM)
    anywhere = pl.BlockSpec(memory_space=pl.ANY)
    dma = pltpu.SemaphoreType.DMA
    shape = jax.ShapeDtypeStruct
    return pl.pallas_call(
        functools.partial(qkv_kernel, replicas),
        out_shape=(
            shape((tok_rows, D), low),
            shape((rows, PAIR), low),
            shape((window, PAIR), low),
            shape((window, PAIR), low),
            shape((2 * GROUP, 8, PAIR), jnp.float32),
            shape((4,) + small.shape, low),
            shape((GROUP, D, 3 * PAIR), low),
            shape((4 * w_out.shape[0], w_out.shape[1]), low),
            shape((4 * w_up.shape[0], w_up.shape[1]), low),
        ),
        in_specs=[vmem] * 3 + [anywhere] * 3,
        out_specs=(vmem,) * 7 + (anywhere,) * 2,
        scratch_shapes=[
            pltpu.VMEM((GROUP, 3, tok_rows, PAIR), low),
            pltpu.VMEM((2, GROUP, PAIR), jnp.float32),
            dma((GROUP, 3)),
            dma((2, GROUP, 3)),
            dma((GROUP, 3)),
            dma((2, GROUP, 3)),
            dma((2, GROUP, 3)),
            dma((2, GROUP, 3)),
            dma((2, GROUP, 2)),
            dma((2, GROUP - 1)),
            dma((2, 2)),
            dma((2, 3)),
            dma((2, 5, 1 + w_up.shape[0] // 64)),
        ],
        compiler_params=pltpu.CompilerParams(
            collective_id=2, has_side_effects=True, vmem_limit_bytes=40 << 20
        ),
        cost_estimate=pl.CostEstimate(
            flops=2 * tok_rows * D * 3 * D, transcendentals=0, bytes_accessed=60 << 20
        ),
        name="project",
    )(tokens, small, codes, w_qkv, w_out, w_up)


def low(value):
    return value.astype(jnp.bfloat16)


def high(value):
    return value.astype(jnp.float32)


def span(start, size):
    return pl.ds(pl.multiple_of(start, size), size)


def make_pipe(place, own, source, load, from_core, from_x, from_y, from_near, from_far, final, sem):
    x, c, y, z_near, z_far = place["x"], place["c"], place["y"], place["z_near"], place["z_far"]
    depth = final.shape[1]
    half, mid, short = depth // 2, depth // 4, depth // 8
    my_half = span(y * half, half)
    my_mid = span(y * half + z_near * mid, mid)
    my_short = span(y * half + z_near * mid + z_far * short, short)

    def spot(side):
        return side if own.shape[1] == 2 else side * 2 + c

    def link(k, which, here, there, peer):
        return remote(here, there, sem.at[0, k, which], sem.at[1, k, which], place[peer])

    def core_copy(k, side):
        owner = side * 2 + 1 - c
        here = own.at[k, owner] if source is None else source(k, owner)
        return link(k, side, here, from_core.at[k, side], "core")

    def load_copy(k, side):
        return pltpu.make_async_copy(
            source(k, side * 2 + c), own.at[k, side], load.at[k, side]
        )

    def x_copy(k):
        return link(k, 2, own.at[k, spot(1 - x)], from_x.at[k], "x_peer")

    def y_copy(k):
        return link(k, 3, own.at[k, spot(x), span((1 - y) * half, half)], from_y.at[k], "y_peer")

    def near_copy(k):
        away = span(y * half + (1 - z_near) * mid, mid)
        return link(k, 4, own.at[k, spot(x), away], from_near.at[k], "near")

    def far_copy(k):
        away = span(y * half + z_near * mid + (1 - z_far) * short, short)
        return link(k, 5, own.at[k, spot(x), away], from_far.at[k], "far")

    def far_join_copy(k):
        here = final.at[k, my_short]
        return link(k, 6, here, here, "far")

    def near_join_copy(k):
        here = final.at[k, my_mid]
        return link(k, 7, here, here, "near")

    def y_join_copy(k):
        here = final.at[k, my_half]
        return link(k, 8, here, here, "y_peer")

    def enter(k):
        for side in range(2):
            core_copy(k, side).start()
            if source is not None:
                load_copy(k, side).start()

    def core_sum(k):
        for side in range(2):
            if source is not None:
                load_copy(k, side).wait()
            core_copy(k, side).wait()
            own[k, spot(side)] = low(high(own[k, spot(side)]) + high(from_core[k, side]))
        x_copy(k).start()

    def x_sum(k):
        x_copy(k).wait()
        own[k, spot(x)] = low(high(own[k, spot(x)]) + high(from_x[k]))
        y_copy(k).start()

    def y_sum(k):
        y_copy(k).wait()
        own[k, spot(x), my_half] = low(high(own[k, spot(x), my_half]) + high(from_y[k]))
        near_copy(k).start()

    def near_sum(k):
        near_copy(k).wait()
        own[k, spot(x), my_mid] = low(high(own[k, spot(x), my_mid]) + high(from_near[k]))
        far_copy(k).start()

    def far_sum(k):
        far_copy(k).wait()
        final[k, my_short] = low(high(own[k, spot(x), my_short]) + high(from_far[k]))
        far_join_copy(k).start()

    def far_join(k):
        far_join_copy(k).wait()
        near_join_copy(k).start()

    def near_join(k):
        near_join_copy(k).wait()
        y_join_copy(k).start()

    def y_join(k):
        y_join_copy(k).wait()

    return [enter, core_sum, x_sum, y_sum, near_sum, far_sum, far_join, near_join, y_join]


def run_pipe(steps, count, now):
    for where, step in enumerate(steps):
        k = now - where * LAG

        @pl.when((k >= 0) & (k < count))
        def _():
            step(k)


def pipe_shapes(count, held, depth, width, loads):
    low_type = jnp.bfloat16
    return [
        pltpu.VMEM((count, held, depth, width), low_type),
        pltpu.VMEM((count, 2, depth, width), low_type),
        pltpu.VMEM((count, depth, width), low_type),
        pltpu.VMEM((count, depth // 2, width), low_type),
        pltpu.VMEM((count, depth // 4, width), low_type),
        pltpu.VMEM((count, depth // 8, width), low_type),
        pltpu.VMEM((count, depth, width), low_type),
        pltpu.SemaphoreType.DMA((2, count, 9)),
    ] + ([pltpu.SemaphoreType.DMA((count, 2))] if loads else [])


def find_place():
    f = lax.axis_index("fsdp")
    r = lax.axis_index("rep")
    x, c, z, y = split_index(f, r)
    lo = r % GROUP
    base = r - lo
    z_near, z_far = z % 2, z // 2
    return {
        "f": f,
        "r": r,
        "x": x,
        "c": c,
        "y": y,
        "z_near": z_near,
        "z_far": z_far,
        "lo": lo,
        "base": base,
        "core": (x * 2 + 1 - c, r),
        "x_peer": ((1 - x) * 2 + c, r),
        "y_peer": (f, base + z * 2 + 1 - y),
        "near": (f, base + (z_far * 2 + 1 - z_near) * 2 + y),
        "far": (f, base + ((1 - z_far) * 2 + z_near) * 2 + y),
        "plane": [(f, base + (lo + step) % GROUP) for step in range(1, GROUP)],
    }


def erf(value):
    return lax.erf(value)


def middle_kernel(
    o_ref,
    tokens_ref,
    grad_ref,
    lines_ref,
    bias_ref,
    wo_ref,
    wo_own,
    wu_ref,
    wu_own,
    wd_own,
    half_ref,
    layer_out,
    residual_out,
    grad_out,
    small_out,
    up_final,
    rest,
    wo,
    wu,
    wd,
    attn,
    act,
    act_t,
    slim,
    x1,
    proj,
    branch,
    act_grad,
    pre,
    hidden,
    slope,
    pre_grad,
    attn_grad,
    proj_grad,
    sums,
    stage,
    own,
    from_core,
    from_x,
    from_y,
    from_near,
    from_far,
    final,
    sem,
    load_sem,
    attn_sem,
    grad_sem,
    down_x_sem,
    down_y_sem,
    down_core_sem,
    down_relay_sem,
    stage_sem,
):
    place = find_place()
    f, x, c, y, lo, base = (place[name] for name in ("f", "x", "c", "y", "lo", "base"))
    across = (1 - x) * 2 + c
    tok_rows = tokens_ref.shape[0]
    share = wo_own.shape[0]
    deep = wd_own.shape[0]
    sets = bias_ref.shape[0]
    tall = 128
    greet([place["core"], place["x_peer"]] + place["plane"])

    def shard_rows(owner, size):
        return span(owner * size, size)

    def attn_copy(e):
        pair = mixed_bits(lo, e)
        return remote(
            o_ref.at[span(pair * tok_rows, tok_rows), :],
            attn.at[:, span(lo * PAIR, PAIR)],
            attn_sem.at[0, e],
            attn_sem.at[1, e],
            (f, base + pair),
        )

    def grad_copy(e):
        pair = mixed_bits(lo, e)
        return remote(
            attn_grad.at[:, span(pair * PAIR, PAIR)],
            grad_out.at[span(lo * tok_rows, tok_rows), :],
            grad_sem.at[0, e],
            grad_sem.at[1, e],
            (f, base + pair),
        )

    def down_at(owner, i):
        return wd.at[span(owner * deep + i * tall, tall), :]

    def down_mine(i):
        return wd_own.at[span(i * tall, tall), :]

    def down_y(m, i):
        return remote(
            half_ref.at[m],
            down_at(across, i),
            down_y_sem.at[0, m],
            down_y_sem.at[1, m],
            place["y_peer"],
        )

    def down_core(i):
        return remote(
            down_mine(i),
            down_at(f, i),
            down_core_sem.at[0, i],
            down_core_sem.at[1, i],
            place["core"],
        )

    def down_relay(i, here):
        return remote(
            here,
            down_at(across, i),
            down_relay_sem.at[0, i],
            down_relay_sem.at[1, i],
            place["core"],
        )

    order = (4, 5, 6, 7, 2, 3, 1)
    for e in order:
        attn_copy(e).start()
    for m in range(sets // 2):
        i = 2 * m + y
        down_y(m, i).start()
        down_relay(i, half_ref.at[m]).start()
        pltpu.make_async_copy(half_ref.at[m], down_at(across, i), down_x_sem.at[m]).start()
    for i in range(sets):
        down_core(i).start()
    loads = [pltpu.make_async_copy(wd_own, wd.at[shard_rows(f, deep)], load_sem.at[0])]
    for owner in range(4):
        rows = pl.ds(owner * share, share)
        for which, (full, mine, into) in enumerate(((wo_ref, wo_own, wo), (wu_ref, wu_own, wu))):
            at = load_sem.at[1 + owner * 2 + which]
            loads.append((f == owner, full.at[rows], mine, into.at[rows], at))

    loads[0].start()
    for same, full, mine, into, at in loads[1:]:

        @pl.when(same)
        def _():
            pltpu.make_async_copy(mine, into, at).start()

        @pl.when(jnp.logical_not(same))
        def _():
            pltpu.make_async_copy(full, into, at).start()

    attn[:, span(lo * PAIR, PAIR)] = o_ref[span(lo * tok_rows, tok_rows), :]
    small_out[...] = jnp.zeros_like(small_out)
    sums[...] = jnp.zeros_like(sums)
    branch[...] = jnp.zeros_like(branch)
    act_grad[...] = jnp.zeros_like(act_grad)

    def line(which):
        return lines_ref[which : which + 1, :]

    def by_rows(step, body):
        @pl.loop(0, tok_rows // step)
        def _(b):
            body(span(b * step, step))

    def scale_grad(at):
        slim[at, :] = low(line(5) * high(grad_ref[at, :]))

    by_rows(64, scale_grad)

    for e in order:
        attn_copy(e).wait_recv()
    for same, full, mine, into, at in loads[1:]:
        pltpu.make_async_copy(full, into, at).wait()
    proj[...] = matmul(attn[...], wo[...])

    def enter_mlp(at):
        value = proj[at, :] + line(0)
        proj[at, :] = value
        value = high(tokens_ref[at, :]) + line(1) * value
        x1[at, :] = value
        unit, scale = normalize(value)
        act[at, :] = low(unit * line(2) + line(3))

    by_rows(64, enter_mlp)
    act_t[...] = act[...].T
    loads[0].wait()
    for m in range(sets // 2):
        i = 2 * m + y
        pltpu.make_async_copy(half_ref.at[m], down_at(across, i), down_x_sem.at[m]).wait()
        i = 2 * m + 1 - y
        down_y(m, i).wait_recv()
        down_relay(i, down_at(across, i)).start()
    steps = make_pipe(
        place, own, None, None, from_core, from_x, from_y, from_near, from_far, final, sem
    )
    finish_step = steps[-1]

    def settle(k):
        finish_step(k)
        i, side = k // 2, k % 2
        for owner in range(4):
            up_final[span(side * tall, tall), span(owner * deep + i * tall, tall)] = final[
                k, :, owner * tall : (owner + 1) * tall
            ]

    steps[-1] = settle
    count = 2 * sets

    def stage_copy(i, part):
        return pltpu.make_async_copy(
            stage.at[i % 2, part], rest.at[2 * i + part], stage_sem.at[i % 2, part]
        )

    @pl.loop(0, sets)
    def _(i):
        down_core(i).wait_recv()
        down_relay(i, down_at(across, i)).wait_recv()
        columns = [span(owner * deep + i * tall, tall) for owner in range(4)]
        w_in = jnp.concatenate([wu[:, at] for at in columns], axis=1)
        w_back = jnp.concatenate([wd[at, :] for at in columns], axis=0)
        pre[...] = matmul(act[...], w_in)

        def activate(at):
            value = pre[at, :] + bias_ref[pl.ds(i, 1), :]
            cdf = 0.5 * (1.0 + erf(value * (0.5**0.5)))
            hidden[at, :] = low(value * cdf)
            slope[at, :] = cdf + value * (jnp.exp(-0.5 * value * value) * 0.3989422804014327)

        by_rows(64, activate)
        pre[...] = lax.dot_general(slim[...], w_back, NT, preferred_element_type=jnp.float32)
        branch[...] += matmul(hidden[...], w_back)

        def descend(at):
            value = pre[at, :] * slope[at, :]
            pre[at, :] = value
            pre_grad[at, :] = low(value)

        by_rows(64, descend)
        total = jnp.sum(pre[...], axis=0, keepdims=True)
        for owner in range(4):
            small_out[owner, pl.ds(20 + i, 1), :] = total[:, owner * tall : (owner + 1) * tall]
        up_grad = low(matmul(act_t[...], pre_grad[...]))
        for side in range(2):
            for owner in range(4):
                top = owner * 2 * tall + side * tall
                own[2 * i + side, owner] = up_grad[top : top + tall]
        run_pipe(steps, count, 2 * i)
        act_grad[...] += lax.dot_general(
            pre_grad[...], w_in, NT, preferred_element_type=jnp.float32
        )

        @pl.when(i >= 2)
        def _():
            for part in range(2):
                stage_copy(i - 2, part).wait()

        down_grad = low(matmul(hidden[...].T, slim[...]))
        for part in range(2):
            for owner in range(4):
                stage[i % 2, part, owner] = down_grad[
                    owner * tall : (owner + 1) * tall, part * 4 * tall : (part + 1) * 4 * tall
                ]
            stage_copy(i, part).start()
        run_pipe(steps, count, 2 * i + 1)

    def leave_mlp(at):
        grad = high(grad_ref[at, :])
        out = branch[at, :] + line(4)
        layer_out[at, :] = low(x1[at, :] + line(5) * out)
        unit, scale = normalize(x1[at, :])
        back = act_grad[at, :]
        value = grad + norm_back(back, unit, scale, line(2))
        residual_out[at, :] = value
        scaled = line(1) * value
        proj_grad[at, :] = low(scaled)
        rows = (scaled, value * proj[at, :], back * unit, back, line(5) * grad, grad * out)
        for which, member in enumerate(rows):
            sums[which : which + 1, :] += jnp.sum(member, axis=0, keepdims=True)

    by_rows(64, leave_mlp)
    attn_grad[...] = low(
        lax.dot_general(proj_grad[...], wo[...], NT, preferred_element_type=jnp.float32)
    )
    for e in order:
        grad_copy(e).start()
    grad_out[span(lo * tok_rows, tok_rows), :] = attn_grad[:, span(lo * PAIR, PAIR)]
    for which in range(6):
        for owner in range(4):
            for row in range(2):
                at = (owner * 2 + row) * PAIR
                place_row = 8 + 2 * which + row
                small_out[owner, place_row : place_row + 1, :] = sums[
                    which : which + 1, at : at + PAIR
                ]
    for i in range(sets - 2, sets):
        for part in range(2):
            stage_copy(i, part).wait()

    def out_copy(side, part):
        return pltpu.make_async_copy(
            stage.at[side, part], rest.at[count + 2 * side + part], stage_sem.at[side, part]
        )

    act_t[...] = attn[...].T
    for owner in range(4):
        part_grad = low(matmul(act_t[owner * share : (owner + 1) * share, :], proj_grad[...]))
        for side in range(2):
            for part in range(2):
                stage[side, part, owner] = part_grad[
                    side * tall : (side + 1) * tall, part * 4 * tall : (part + 1) * 4 * tall
                ]
    for side in range(2):
        for part in range(2):
            out_copy(side, part).start()

    @pl.loop(count, count + LAG * (len(steps) - 1))
    def _(now):
        run_pipe(steps, count, now)

    for side in range(2):
        for part in range(2):
            out_copy(side, part).wait()
    for e in order:
        attn_copy(e).wait_send()
        grad_copy(e).wait()
    for m in range(sets // 2):
        down_y(m, 2 * m + y).wait_send()
    for i in range(sets):
        down_core(i).wait_send()
        down_relay(i, down_at(across, i)).wait_send()


def middle(mixed, tokens, out_grad, lines, bias, wide_out, w_out, wide_up, w_up, w_down, half):
    tok_rows = tokens.shape[0]
    rows = GROUP * tok_rows
    sets = bias.shape[0]
    count = 2 * sets
    wide = bias.shape[1]
    anywhere = pl.BlockSpec(memory_space=pl.ANY)
    vmem = pl.BlockSpec(memory_space=pltpu.VMEM)
    dma = pltpu.SemaphoreType.DMA
    shape = jax.ShapeDtypeStruct
    slight, full = jnp.bfloat16, jnp.float32
    return pl.pallas_call(
        middle_kernel,
        out_shape=(
            shape((tok_rows, D), slight),
            shape((tok_rows, D), full),
            shape((rows, PAIR), slight),
            shape((4, 28, PAIR), full),
            shape(w_up.shape, slight),
            shape((count + 4, 4, 128, wide), slight),
        ),
        in_specs=[vmem] * 5 + [anywhere] * 6,
        out_specs=(vmem,) * 5 + (anywhere,),
        scratch_shapes=[
            pltpu.VMEM(wide_out.shape, slight),
            pltpu.VMEM(wide_up.shape, slight),
            pltpu.VMEM((4 * w_down.shape[0], D), slight),
            pltpu.VMEM((tok_rows, D), slight),
            pltpu.VMEM((tok_rows, D), slight),
            pltpu.VMEM((D, tok_rows), slight),
            pltpu.VMEM((tok_rows, D), slight),
            pltpu.VMEM((tok_rows, D), full),
            pltpu.VMEM((tok_rows, D), full),
            pltpu.VMEM((tok_rows, D), full),
            pltpu.VMEM((tok_rows, D), full),
            pltpu.VMEM((tok_rows, wide), full),
            pltpu.VMEM((tok_rows, wide), slight),
            pltpu.VMEM((tok_rows, wide), full),
            pltpu.VMEM((tok_rows, wide), slight),
            pltpu.VMEM((tok_rows, D), slight),
            pltpu.VMEM((tok_rows, D), slight),
            pltpu.VMEM((8, D), full),
            pltpu.VMEM((2, 2, 4, 128, wide), slight),
        ]
        + pipe_shapes(count, 4, 128, wide, False)
        + [
            dma((9,)),
            dma((2, GROUP)),
            dma((2, GROUP)),
            dma((sets // 2,)),
            dma((2, sets // 2)),
            dma((2, sets)),
            dma((2, sets)),
            dma((2, 2)),
        ],
        compiler_params=pltpu.CompilerParams(
            collective_id=3, has_side_effects=True, vmem_limit_bytes=67043328
        ),
        cost_estimate=pl.CostEstimate(
            flops=40 * tok_rows * D * D, transcendentals=0, bytes_accessed=100 << 20
        ),
        name="middle",
    )(mixed, tokens, out_grad, lines, bias, wide_out, w_out, wide_up, w_up, w_down, half)


def finish_kernel(
    replicas,
    dq_ref,
    dk_ref,
    dv_ref,
    act_ref,
    pairs_ref,
    tokens_ref,
    residual_ref,
    gain_ref,
    small_ref,
    rest_ref,
    tokens_out,
    down_final,
    out_final,
    qkv_final,
    small_final,
    own,
    from_core,
    from_x,
    from_y,
    from_near,
    from_far,
    final,
    sem,
    load_sem,
    pair_own,
    pair_core,
    pair_x,
    pair_y,
    pair_near,
    pair_far,
    pair_final,
    pair_sem,
    halos,
    stage,
    arrived,
    w_buf,
    act_t,
    act_grad,
    small_work,
    small_own,
    small_core,
    small_x,
    small_all,
    halo_sem,
    block_sem,
    w_sem,
    small_sem,
):
    place = find_place()
    f, r, x, c, lo, base = (place[name] for name in ("f", "r", "x", "c", "lo", "base"))
    core_peer, x_peer, plane = place["core"], place["x_peer"], place["plane"]
    has_next, next_peer, has_prev, prev_peer = group_neighbours(f, r, replicas)
    total = own.shape[0]
    tok_rows = act_ref.shape[0]
    rows = GROUP * tok_rows
    halo = rows // 2
    half_group = GROUP // 2
    greet([core_peer, x_peer] + plane, [(has_next, next_peer), (has_prev, prev_peer)])

    def block(ref, source, lead=0):
        return ref.at[pl.ds(pl.multiple_of(lead + source * tok_rows, 128), tok_rows), :]

    def lanes(part):
        return pl.ds(part * PAIR, PAIR)

    def halo_copy(source, part, forward):
        ref = (dk_ref, dv_ref)[part]
        return remote(
            block(ref, source, halo + rows if forward else -halo),
            block(halos.at[part], source),
            halo_sem.at[0, source, part],
            halo_sem.at[1, source, part],
            next_peer if forward else prev_peer,
        )

    def block_copy(e, part):
        source = block(dq_ref, mixed_bits(lo, e)) if part == 0 else stage.at[e, part - 1]
        return remote(
            source,
            arrived.at[e, :, lanes(part)],
            block_sem.at[0, e, part],
            block_sem.at[1, e, part],
            (f, base + mixed_bits(lo, e)),
        )

    def nth(p):
        h = p // 2
        near = jnp.where(h == 0, 2, jnp.where(h == 1, 1, jnp.where(h == 2, 3, 0)))
        return jnp.where(p % 2 == 0, 4 + h, near)

    def w_copy(p):
        spot = p % 2
        return pltpu.make_async_copy(pairs_ref.at[nth(p)], w_buf.at[spot], w_sem.at[spot])

    for there, forward in ((has_next, True), (has_prev, False)):

        @pl.when(there)
        def _():
            for i in range(half_group):
                for part in range(2):
                    halo_copy(i if forward else i + half_group, part, forward).start()

        @pl.when(jnp.logical_not(there))
        def _():
            start = halo if forward else 0
            halos[:, start : start + halo, :] = jnp.zeros((2, halo, PAIR), jnp.bfloat16)

    order = (4, 2, 5, 1, 6, 3, 7)
    for e in order:
        block_copy(e, 0).start()
    arrived[0, :, lanes(0)] = dq_ref[pl.ds(pl.multiple_of(lo * tok_rows, 128), tok_rows), :]
    small_work[...] = small_ref[...]
    act_grad[...] = jnp.zeros_like(act_grad)
    act_t[...] = act_ref[...].T
    w_copy(0).start()

    def give(p):
        e = nth(p)
        source = mixed_bits(lo, e)
        for there, forward, fits in (
            (has_next, False, source >= half_group),
            (has_prev, True, source < half_group),
        ):

            @pl.when(there & fits)
            def _():
                for part in range(2):
                    halo_copy(source, part, forward).wait_recv()

        sums = []
        for part, ref in enumerate((dk_ref, dv_ref)):
            near = ref[pl.ds(pl.multiple_of(halo + source * tok_rows, 128), tok_rows), :]
            far = halos[part, pl.ds(pl.multiple_of(source * tok_rows, 128), tok_rows), :]
            sums.append(low(high(near) + high(far)))
            stage[e, part] = sums[part]

        @pl.when(e > 0)
        def _():
            for part in range(1, 3):
                block_copy(e, part).start()

        @pl.when(e == 0)
        def _():
            for part in range(1, 3):
                arrived[0, :, lanes(part)] = sums[part - 1]

    pair_steps = make_pipe(
        place,
        pair_own,
        None,
        None,
        pair_core,
        pair_x,
        pair_y,
        pair_near,
        pair_far,
        pair_final,
        pair_sem,
    )
    pair_enter = pair_steps.pop(0)

    def take(p):
        e = nth(p)
        j = mixed_bits(lo, e)

        @pl.when(p + 1 < GROUP)
        def _():
            w_copy(p + 1).start()

        @pl.when(e > 0)
        def _():
            for part in range(3):
                block_copy(e, part).wait_recv()

        w_copy(p).wait()
        grads = arrived[e]
        pair_own[j] = low(matmul(act_t[...], grads)).reshape(4, D // 4, 3 * PAIR)
        pair_enter(j)
        act_grad[...] += lax.dot_general(
            grads, w_buf[p % 2], NT, preferred_element_type=jnp.float32
        )
        sums = jnp.sum(high(grads), axis=0, keepdims=True)
        for line, part in ((4, 0), (6, 2)):
            small_work[j // 2, pl.ds(line + j % 2, 1), :] = sums[:, part * PAIR : (part + 1) * PAIR]

    def leave():
        unit, scale = normalize(high(tokens_ref[...]))
        grad = act_grad[...]
        back = norm_back(grad, unit, scale, gain_ref[...])
        tokens_out[...] = low(residual_ref[...] + back)
        for line, values in ((0, grad * unit), (2, grad)):
            sums = jnp.sum(values, axis=0, keepdims=True)
            for owner in range(4):
                for row in range(2):
                    at = (owner * 2 + row) * PAIR
                    small_work[owner, line + row : line + row + 1, :] = sums[:, at : at + PAIR]
        for side in range(2):
            small_enter(side).start()

    steps = make_pipe(
        place,
        own,
        lambda k, owner: rest_ref.at[k, owner],
        load_sem,
        from_core,
        from_x,
        from_y,
        from_near,
        from_far,
        final,
        sem,
    )
    finish_step = steps[-1]
    tall, wide = final.shape[1:]
    downs = down_final.shape[0] // tall * 2

    def settle(k):
        finish_step(k)

        @pl.when(k < downs)
        def _():
            down_final[span((k // 2) * tall, tall), span((k % 2) * wide, wide)] = final[k]

        @pl.when(k >= downs)
        def _():
            at = k - downs
            out_final[span((at // 2) * tall, tall), span((at % 2) * wide, wide)] = final[k]

    steps[-1] = settle

    def small_enter(side):
        return remote(
            small_work.at[side * 2 + 1 - c],
            small_core.at[side],
            small_sem.at[0, side],
            small_sem.at[1, side],
            core_peer,
        )

    small_cross = remote(
        small_own.at[1 - x], small_x, small_sem.at[0, 2], small_sem.at[1, 2], x_peer
    )

    def small_spread(step):
        return remote(
            small_own.at[2],
            small_all.at[step - 1],
            small_sem.at[0, 2 + step],
            small_sem.at[1, 2 + step],
            plane[step - 1],
        )

    def small_first():
        for side in range(2):
            small_enter(side).wait()
        for side in range(2):
            small_own[side] = small_work[side * 2 + c] + small_core[side]
        small_cross.start()

    def small_second():
        small_cross.wait()
        small_own[2] = small_own[x] + small_x[...]
        for step in range(1, GROUP):
            small_spread(step).start()

    def arrive(p):
        pair_steps[0](mixed_bits(lo, nth(p)))

    def cross(p):
        pair_steps[1](mixed_bits(lo, nth(p)))

    stop = max(total + LAG * (len(steps) - 1), LAST_TAKE + 5 + GROUP // PAIR_BY + LAG * 5)

    @pl.loop(0, stop)
    def _(now):
        @pl.when((now >= GIVE_AT) & (now < GIVE_AT + GROUP))
        def _():
            give(now - GIVE_AT)

        run_pipe(steps, total, now)

        for step, lag in ((take, 0), (arrive, 2), (cross, 4)):
            gone = now - TAKE_AT - lag

            @pl.when((gone >= 0) & (gone < TAKE_BY * GROUP) & (gone % TAKE_BY == 0))
            def _():
                step(gone // TAKE_BY)

        for event, at in (
            (leave, LAST_TAKE + 1),
            (small_first, LAST_TAKE + 5),
            (small_second, LAST_TAKE + 9),
        ):
            pl.when(now == at)(event)

        for where, step in enumerate(pair_steps[2:]):
            gone = now - LAST_TAKE - 5 - LAG * where

            @pl.when((gone >= 0) & (gone < GROUP // PAIR_BY))
            def _():
                for each in range(PAIR_BY):
                    step(PAIR_BY * gone + each)

    for step in range(1, GROUP):
        small_spread(step).wait()
    value = small_own[2]
    for step in range(1, GROUP):
        value = value + small_all[step - 1]
    small_final[...] = value
    for j in range(GROUP):
        for part in range(3):
            at = part * D + j * PAIR
            qkv_final[:, at : at + PAIR] = pair_final[j, :, part * PAIR : (part + 1) * PAIR]

    for e in order:
        for part in range(3):
            block_copy(e, part).wait_send()
    for there, forward in ((has_next, True), (has_prev, False)):

        @pl.when(there)
        def _():
            for i in range(half_group):
                for part in range(2):
                    halo_copy(i if forward else i + half_group, part, forward).wait_send()


def wrap_up(replicas, moved, act, pairs, tokens, residual, gain, small, rest, shapes):
    chunks = rest.shape[0]
    tok_rows = act.shape[0]
    tall = small.shape[1]
    anywhere = pl.BlockSpec(memory_space=pl.ANY)
    vmem = pl.BlockSpec(memory_space=pltpu.VMEM)
    dma = pltpu.SemaphoreType.DMA
    low = jnp.bfloat16
    shape = jax.ShapeDtypeStruct
    pair = 3 * PAIR
    return pl.pallas_call(
        functools.partial(finish_kernel, replicas),
        out_shape=(shape((tok_rows, D), low),)
        + tuple(shape(size, low) for size in shapes)
        + (shape((D // 4, 3 * D), low), shape((tall, PAIR), jnp.float32)),
        in_specs=[vmem] * 4 + [anywhere] + [vmem] * 4 + [anywhere],
        out_specs=(vmem,) * 5,
        scratch_shapes=pipe_shapes(chunks, 2, *rest.shape[2:], True)
        + pipe_shapes(GROUP, 4, D // 4, pair, False)
        + [
            pltpu.VMEM((2, GROUP * tok_rows, PAIR), low),
            pltpu.VMEM((GROUP, 2, tok_rows, PAIR), low),
            pltpu.VMEM((GROUP, tok_rows, pair), low),
            pltpu.VMEM((2, D, pair), low),
            pltpu.VMEM((D, tok_rows), low),
            pltpu.VMEM((tok_rows, D), jnp.float32),
            pltpu.VMEM((4, tall, PAIR), jnp.float32),
            pltpu.VMEM((3, tall, PAIR), jnp.float32),
            pltpu.VMEM((2, tall, PAIR), jnp.float32),
            pltpu.VMEM((tall, PAIR), jnp.float32),
            pltpu.VMEM((GROUP - 1, tall, PAIR), jnp.float32),
            dma((2, GROUP, 2)),
            dma((2, GROUP, 3)),
            dma((2,)),
            dma((2, GROUP + 2)),
        ],
        compiler_params=pltpu.CompilerParams(
            collective_id=1, has_side_effects=True, vmem_limit_bytes=67043328
        ),
        cost_estimate=pl.CostEstimate(
            flops=12 * tok_rows * D * D, transcendentals=0, bytes_accessed=200 << 20
        ),
        name="finish",
    )(*moved, act, pairs, tokens, residual, gain, small, rest)


def shards(
    tokens,
    out_grad,
    norm1_gain,
    norm1_bias,
    w_qkv,
    q_bias,
    v_bias,
    w_out,
    out_bias,
    attn_scale,
    norm2_gain,
    norm2_bias,
    w_up,
    up_bias,
    w_down,
    down_bias,
    mlp_scale,
    image_ids,
    pad_mask,
):
    both = ("fsdp", "rep")
    owners = lax.axis_size("fsdp")
    replicas = lax.axis_size("rep")
    tok_rows = tokens.shape[0]
    rows = GROUP * tok_rows
    groups = [list(range(g, g + GROUP)) for g in range(0, replicas, GROUP)]
    factor = HEAD_DIM ** (-0.5)

    small = (
        norm1_gain,
        norm1_bias,
        q_bias,
        v_bias,
        out_bias,
        attn_scale,
        norm2_gain,
        norm2_bias,
        down_bias,
        mlp_scale,
        up_bias,
    )
    sizes = [member.shape[0] for member in small]
    packed = jnp.concatenate(small + (jnp.zeros((-sum(sizes) % 2048,), jnp.bfloat16),))
    codes = jnp.where(pad_mask > 0, image_ids + 1, 0).astype(jnp.float32).reshape(-1, PAIR)
    code_rows = codes.shape[0]
    codes = jnp.concatenate([codes, jnp.zeros((8 - code_rows, PAIR), jnp.float32)], axis=0)
    act_one, query, key_window, value_window, codes, vectors, w_pairs, wide_out, wide_up = project(
        replicas, tokens, packed.reshape(-1, PAIR), codes, w_qkv, w_out, w_up
    )
    vectors = vectors.reshape(4, -1).astype(jnp.float32)
    parts = []
    place = 0
    for member in small:
        parts.append(vectors[:, place : place + member.shape[0]].reshape(-1))
        place += member.shape[0]
    (
        gain_first,
        shift_first,
        query_bias,
        value_bias,
        proj_bias,
        attn_gamma,
        gain_second,
        shift_second,
        final_bias,
        mlp_gamma,
        hidden_bias,
    ) = parts


    window = key_window.shape[0]
    halo = rows // 2
    seen = codes[:, :code_rows].reshape(-1).astype(jnp.int32)
    seen = jnp.concatenate([seen, jnp.zeros((KEYS,), jnp.int32)])
    spot = jnp.arange(window, dtype=jnp.int32)
    asked = seen[halo : halo + rows]
    tile_codes = asked.reshape(rows // BLOCK, BLOCK)
    first_code = jnp.min(jnp.where(tile_codes > 0, tile_codes, 1 << 30), axis=1)
    last_code = jnp.max(tile_codes, axis=1)
    begin = jnp.min(jnp.where(seen[None] == first_code[:, None], spot[None], window), axis=1)
    finish = jnp.max(jnp.where(seen[None] == last_code[:, None], spot[None] + 1, 0), axis=1)
    begin = begin // 128 * 128
    count = jnp.where(last_code > 0, (finish - begin + KEYS - 1) // KEYS, 0)
    meta = jnp.stack([begin, count], axis=1).reshape(-1)

    lane_slot = jnp.arange(PAIR, dtype=jnp.int32) % HEAD_DIM
    key_slot = jnp.where(seen > 0, 1 + (seen - 1) % SLOTS, 0)
    marks = (key_slot[:, None] == lane_slot[None]).astype(jnp.bfloat16)


    down_half = w_down.reshape(-1, 2, 128, D)
    down_half = lax.dynamic_index_in_dim(down_half, lax.axis_index("rep") % 2, 1, False)
    down_half, query = lax.optimization_barrier((down_half, query))
    down_half = lax.ppermute(down_half, "fsdp", [(f, (f + 2) % 4) for f in range(4)])
    attn_mine, attn_t, lse = attend(meta, query, key_window, value_window, marks)

    lines = jnp.stack(
        (proj_bias, attn_gamma, gain_second, shift_second, final_bias, mlp_gamma) + (gain_second,) * 2
    )
    wide_bias = hidden_bias.reshape(4, -1, PAIR).transpose(1, 0, 2).reshape(-1, 4 * PAIR)
    layer_out, residual_grad, grad_mine, packed, up_out, rest = middle(
        attn_mine,
        tokens,
        out_grad,
        lines,
        wide_bias,
        wide_out,
        w_out,
        wide_up,
        w_up,
        w_down,
        down_half,
    )
    dq, dk, dv = attend_back(
        meta, query, key_window, value_window, marks, grad_mine, attn_t, lse
    )
    tokens_grad, *grads, packed = wrap_up(
        replicas,
        (dq, dk, dv),
        act_one,
        w_pairs,
        tokens,
        residual_grad,
        gain_first.reshape(1, D),
        packed,
        rest,
        (w_down.shape, w_out.shape),
    )
    grads.insert(1, up_out)
    grads = [grad.astype(jnp.float32) for grad in grads]
    if replicas > GROUP:
        apart = [list(range(low, replicas, GROUP)) for low in range(GROUP)]
        grads = lax.psum(grads, "rep", axis_index_groups=apart)
        packed = lax.psum(packed, "rep", axis_index_groups=apart)
    packed = packed.reshape(-1)
    small_out = []
    place = 0
    for member in (norm1_gain, norm1_bias, q_bias, v_bias) + small[4:]:
        size = member.shape[0]
        small_out.append(packed[place : place + size])
        place += size

    down_out, up_out, out_out, qkv_out = grads
    return (
        layer_out,
        tokens_grad,
        small_out[0],
        small_out[1],
        qkv_out,
        small_out[2],
        small_out[3],
        out_out,
        small_out[4],
        small_out[5],
        small_out[6],
        small_out[7],
        up_out,
        small_out[10],
        down_out,
        small_out[8],
        small_out[9],
    )


def solution(mesh):
    spread = P(("fsdp", "rep"), None)
    line = P("fsdp")
    plane = P("fsdp", None)
    return jax.shard_map(
        shards,
        mesh=mesh,
        in_specs=(
            spread,
            spread,
            line,
            line,
            plane,
            line,
            line,
            plane,
            line,
            line,
            line,
            line,
            plane,
            line,
            plane,
            line,
            line,
            P(("fsdp", "rep")),
            P(("fsdp", "rep")),
        ),
        out_specs=(
            spread,
            spread,
            line,
            line,
            plane,
            line,
            line,
            plane,
            line,
            line,
            line,
            line,
            plane,
            line,
            plane,
            line,
            line,
        ),
        check_vma=False,
    )
```

```python
import functools

import jax
import jax.numpy as jnp
from jax import lax
from jax.experimental import pallas as pl
from jax.experimental.pallas import tpu as pltpu
from jax.sharding import PartitionSpec as P

D = 1024
HEADS = 16
HEAD_DIM = 64
IMG = 1370

PAIR = 2 * HEAD_DIM
GROUP = HEADS // 2
BLOCK = 256
KEYS = 1536
SLOTS = 63

EPSILON = 1e-06
NEG_BIG = -1e30
NEG_EDGE = -1e29

NT = (((1,), (1,)), ((), ()))


def from_behind(block, axis, distance):
    devices = range(lax.axis_size(axis))
    route = [(i - distance, i) for i in devices if i - distance in devices]
    return lax.ppermute(block, axis, route)


def normalize(values):
    center = jnp.mean(values, axis=-1, keepdims=True)
    centered = values - center
    spread = jnp.mean(centered * centered, axis=-1, keepdims=True)
    scale = lax.rsqrt(spread + EPSILON)
    return centered * scale, scale


def norm_back(cotangent, unit, scale, gain):
    scaled = cotangent * gain
    along = jnp.mean(scaled, axis=-1, keepdims=True)
    across = jnp.mean(scaled * unit, axis=-1, keepdims=True)
    return scale * (scaled - along - unit * across)


def matmul(left, right):
    return jnp.dot(left, right, preferred_element_type=jnp.float32)


def fold_rows(values, op):
    return op(values.reshape(values.shape[0] // 8, 8, values.shape[1]), axis=0)


def lane_marks():
    lane = lax.broadcasted_iota(jnp.int32, (BLOCK, PAIR), 1)
    return lane // HEAD_DIM, lane % HEAD_DIM > 0


def asking(query, marks, half, usable):
    wanted = jnp.where((marks.astype(jnp.float32) > 0) & usable, 0.0, NEG_BIG).astype(jnp.bfloat16)
    return [jnp.where(half == h, query, wanted) for h in range(2)]


def attend_kernel(meta, q_ref, k_ref, v_ref, m_ref, o_ref, ot_ref, lse_ref, vt, k_aug, scores):
    rows_all = o_ref.shape[0]
    tiles = rows_all // BLOCK
    window = k_ref.shape[0]
    halo = (window - KEYS - rows_all) // 2
    half, usable = lane_marks()

    @pl.loop(0, window // BLOCK)
    def _(i):
        at = pl.ds(pl.multiple_of(i * BLOCK, BLOCK), BLOCK)
        vt[:, at] = v_ref[at, :].T
        for h in range(2):
            k_aug[h, at, :] = jnp.where(half == h, k_ref[at, :], m_ref[at, :])

    @pl.loop(0, tiles)
    def _(t):
        start = meta[2 * t]
        count = meta[2 * t + 1]
        rows = pl.ds(pl.multiple_of(t * BLOCK, BLOCK), BLOCK)
        spots = pl.ds(pl.multiple_of(halo + t * BLOCK, BLOCK), BLOCK)
        query = asking(q_ref[rows, :], m_ref[spots, :], half, usable)

        def score(i, tops):
            at = pl.ds(pl.multiple_of(start + i * KEYS, 128), KEYS)
            keep = pl.ds(pl.multiple_of(i * KEYS, KEYS), KEYS)
            new = []
            for h in range(2):
                part = lax.dot_general(
                    k_aug[h, at, :], query[h], NT, preferred_element_type=jnp.float32
                )
                scores[h, keep, :] = part
                new.append(jnp.maximum(tops[h], fold_rows(part, jnp.max)))
            return tuple(new)

        low = jnp.full((8, BLOCK), NEG_BIG, jnp.float32)
        tops = lax.fori_loop(0, count, score, (low, low))
        tops = [jnp.max(top, axis=0, keepdims=True) for top in tops]
        tops = [jnp.where(top < NEG_EDGE, 0.0, top) for top in tops]

        def mix(i, carry):
            at = pl.ds(pl.multiple_of(start + i * KEYS, 128), KEYS)
            keep = pl.ds(pl.multiple_of(i * KEYS, KEYS), KEYS)
            new = []
            for h in range(2):
                total, mixed = carry[h]
                weights = jnp.exp(scores[h, keep, :] - tops[h])
                total = total + fold_rows(weights, jnp.sum)
                mixed = mixed + matmul(
                    vt[h * HEAD_DIM : (h + 1) * HEAD_DIM, at], weights.astype(jnp.bfloat16)
                )
                new.append((total, mixed))
            return tuple(new)

        zero = (jnp.zeros((8, BLOCK), jnp.float32), jnp.zeros((HEAD_DIM, BLOCK), jnp.float32))
        done = lax.fori_loop(0, count, mix, (zero, zero))
        outs = []
        for h in range(2):
            total = jnp.sum(done[h][0], axis=0, keepdims=True)
            total = jnp.where(total > 0, total, 1.0)
            lse_ref[h : h + 1, rows] = tops[h] + jnp.log(total)
            outs.append(done[h][1] / total)
        out = jnp.concatenate(outs, axis=0)
        ot_ref[:, rows] = out
        o_ref[rows, :] = out.T.astype(jnp.bfloat16)


def attend(meta, query, keys, values, marks):
    rows = query.shape[0]
    window = keys.shape[0]
    deepest = (2 * IMG + 2 * BLOCK + KEYS) // KEYS * KEYS
    vmem = pl.BlockSpec(memory_space=pltpu.VMEM)
    return pl.pallas_call(
        attend_kernel,
        out_shape=(
            jax.ShapeDtypeStruct((rows, PAIR), jnp.bfloat16),
            jax.ShapeDtypeStruct((PAIR, rows), jnp.float32),
            jax.ShapeDtypeStruct((8, rows), jnp.float32),
        ),
        in_specs=[pl.BlockSpec(memory_space=pltpu.SMEM), vmem, vmem, vmem, vmem],
        out_specs=(vmem, vmem, vmem),
        scratch_shapes=[
            pltpu.VMEM((PAIR, window), jnp.bfloat16),
            pltpu.VMEM((2, window, PAIR), jnp.bfloat16),
            pltpu.VMEM((2, deepest, BLOCK), jnp.float32),
        ],
        cost_estimate=pl.CostEstimate(
            flops=4 * rows * 2 * IMG * PAIR, transcendentals=2 * rows * IMG, bytes_accessed=9 << 20
        ),
        name="attend",
    )(meta, query, keys, values, marks)


def attend_back_kernel(
    meta, q_ref, k_ref, v_ref, m_ref, g_ref, ot_ref, lse_ref, dq_ref, dk_out, dv_out, kt, k_aug, dk_ref, dv_ref
):
    rows_all = dq_ref.shape[0]
    tiles = rows_all // BLOCK
    window = k_ref.shape[0]
    halo = (window - KEYS - rows_all) // 2
    half, usable = lane_marks()

    @pl.loop(0, window // BLOCK)
    def _(i):
        at = pl.ds(pl.multiple_of(i * BLOCK, BLOCK), BLOCK)
        kt[:, at] = k_ref[at, :].T
        for h in range(2):
            k_aug[h, at, :] = jnp.where(half == h, k_ref[at, :], m_ref[at, :])
        dk_ref[at, :] = jnp.zeros((BLOCK, PAIR), jnp.float32)
        dv_ref[at, :] = jnp.zeros((BLOCK, PAIR), jnp.float32)

    @pl.loop(0, tiles)
    def _(t):
        start = meta[2 * t]
        count = meta[2 * t + 1]
        rows = pl.ds(pl.multiple_of(t * BLOCK, BLOCK), BLOCK)
        grad = g_ref[rows, :]
        blank = jnp.zeros_like(grad)
        spots = pl.ds(pl.multiple_of(halo + t * BLOCK, BLOCK), BLOCK)
        query = asking(q_ref[rows, :], m_ref[spots, :], half, usable)
        query_only = jnp.concatenate(
            [jnp.where(half == h, query[h], blank) for h in range(2)], axis=0
        )
        grads = [jnp.where(half == h, grad, blank) for h in range(2)]
        grads_both = jnp.concatenate(grads, axis=0)
        product = grad.astype(jnp.float32).T * ot_ref[:, rows]
        delta = [
            jnp.sum(product[h * HEAD_DIM : (h + 1) * HEAD_DIM], axis=0, keepdims=True)
            for h in range(2)
        ]
        lse = [lse_ref[h : h + 1, rows] for h in range(2)]

        def step(i, carry):
            at = pl.ds(pl.multiple_of(start + i * KEYS, 128), KEYS)
            value = v_ref[at, :]
            probs, slopes, new = [], [], []
            for h in range(2):
                part = lax.dot_general(
                    k_aug[h, at, :], query[h], NT, preferred_element_type=jnp.float32
                )
                weights = jnp.exp(part - lse[h])
                pull = lax.dot_general(value, grads[h], NT, preferred_element_type=jnp.float32)
                slope = (weights * (pull - delta[h])).astype(jnp.bfloat16)
                probs.append(weights.astype(jnp.bfloat16))
                slopes.append(slope)
                new.append(carry[h] + matmul(kt[h * HEAD_DIM : (h + 1) * HEAD_DIM, at], slope))
            dv_ref[at, :] += matmul(jnp.concatenate(probs, axis=1), grads_both)
            dk_ref[at, :] += matmul(jnp.concatenate(slopes, axis=1), query_only)
            return tuple(new)

        zero = jnp.zeros((HEAD_DIM, BLOCK), jnp.float32)
        done = lax.fori_loop(0, count, step, (zero, zero))
        dq = jnp.concatenate(done, axis=0) * (HEAD_DIM**-0.5)
        dq_ref[rows, :] = dq.T.astype(jnp.bfloat16)

    @pl.loop(0, window // BLOCK)
    def _(i):
        at = pl.ds(pl.multiple_of(i * BLOCK, BLOCK), BLOCK)
        dk_out[at, :] = dk_ref[at, :].astype(jnp.bfloat16)
        dv_out[at, :] = dv_ref[at, :].astype(jnp.bfloat16)


def attend_back(meta, query, keys, values, marks, grad, out_t, lse):
    rows = query.shape[0]
    window = keys.shape[0]
    vmem = pl.BlockSpec(memory_space=pltpu.VMEM)
    return pl.pallas_call(
        attend_back_kernel,
        out_shape=(
            jax.ShapeDtypeStruct((rows, PAIR), jnp.bfloat16),
            jax.ShapeDtypeStruct((window, PAIR), jnp.bfloat16),
            jax.ShapeDtypeStruct((window, PAIR), jnp.bfloat16),
        ),
        in_specs=[pl.BlockSpec(memory_space=pltpu.SMEM)] + [vmem] * 7,
        out_specs=(vmem, vmem, vmem),
        scratch_shapes=[
            pltpu.VMEM((PAIR, window), jnp.bfloat16),
            pltpu.VMEM((2, window, PAIR), jnp.bfloat16),
            pltpu.VMEM((window, PAIR), jnp.float32),
            pltpu.VMEM((window, PAIR), jnp.float32),
        ],
        cost_estimate=pl.CostEstimate(
            flops=10 * rows * 2 * IMG * PAIR, transcendentals=2 * rows * IMG, bytes_accessed=16 << 20
        ),
        name="attend_back",
    )(meta, query, keys, values, marks, grad, out_t, lse)


CHUNK = 64
LAG = 2
GIVE_AT = 3
TAKE_AT = 16
TAKE_BY = 1
LAST_TAKE = TAKE_AT + (GROUP - 1) * TAKE_BY
PAIR_BY = 2
MESH = pl.DeviceIdType.MESH


def split_index(f, r):
    return f // 2, f % 2, (r % GROUP) // 2, r % 2


def mixed_bits(left, right):
    value = 0
    for weight in (4, 2, 1):
        value = value + weight * ((left // weight + right // weight) % 2)
    return value


def remote(source, target, send, recv, peer):
    return pltpu.make_async_remote_copy(
        src_ref=source,
        dst_ref=target,
        send_sem=send,
        recv_sem=recv,
        device_id=peer,
        device_id_type=MESH,
    )


def greet(peers, optional=()):
    barrier = pltpu.get_barrier_semaphore()
    expected = len(peers)
    for peer in peers:
        pl.semaphore_signal(barrier, inc=1, device_id=peer, device_id_type=MESH)
    for there, peer in optional:

        @pl.when(there)
        def _():
            pl.semaphore_signal(barrier, inc=1, device_id=peer, device_id_type=MESH)

        expected = expected + there.astype(jnp.int32)
    pl.semaphore_wait(barrier, expected)


def group_neighbours(f, r, replicas):
    spot = f * replicas + r
    after = lax.rem(spot + GROUP, 4 * replicas)
    before = lax.rem(spot + 3 * replicas + (replicas - GROUP), 4 * replicas)
    next_peer = (after // replicas, lax.rem(after, replicas))
    prev_peer = (before // replicas, lax.rem(before, replicas))
    return spot + GROUP < 4 * replicas, next_peer, spot >= GROUP, prev_peer


def qkv_kernel(
    replicas,
    tokens_ref,
    small_ref,
    codes_ref,
    w_ref,
    out_ref,
    up_ref,
    act_ref,
    q_out,
    k_out,
    v_out,
    codes_out,
    small_out,
    w_pairs,
    out_across,
    up_half,
    w_buf,
    stage,
    bias,
    own_sem,
    x_sem,
    y_sem,
    core_sem,
    relay_sem,
    block_sem,
    halo_sem,
    code_sem,
    edge_sem,
    small_sem,
    wide_sem,
    pair_sem,
):
    f = lax.axis_index("fsdp")
    r = lax.axis_index("rep")
    x, c, z, y = split_index(f, r)
    lo = r % GROUP
    base = r - lo
    tok_rows = tokens_ref.shape[0]
    rows = GROUP * tok_rows
    halo = (k_out.shape[0] - KEYS - rows) // 2
    half = GROUP // 2
    share = w_ref.shape[0]
    core_peer = (x * 2 + 1 - c, r)
    x_peer = ((1 - x) * 2 + c, r)
    y_peer = (f, base + z * 2 + 1 - y)
    fsdp_peers = [((f + step) % 4, r) for step in range(1, 4)]
    plane = [(f, base + (lo + step) % GROUP) for step in range(1, GROUP)]
    has_next, next_peer, has_prev, prev_peer = group_neighbours(f, r, replicas)
    greet(fsdp_peers + plane, [(has_next, next_peer), (has_prev, prev_peer)])

    def small_copy(step):
        return remote(
            small_ref,
            small_out.at[f],
            small_sem.at[0, step - 1],
            small_sem.at[1, step - 1],
            fsdp_peers[step - 1],
        )

    def lanes(part):
        return pl.ds(part * PAIR, PAIR)

    def shard_rows(owner):
        return pl.ds(pl.multiple_of(owner * share, share), share)

    def columns(part, pair):
        return w_ref.at[:, pl.ds(pl.multiple_of(part * D + pair * PAIR, PAIR), PAIR)]

    def slot(e, owner, part):
        return w_buf.at[e, shard_rows(owner), lanes(part)]

    across = (1 - x) * 2 + c
    out_copy = remote(out_ref, out_across, wide_sem.at[0, 0], wide_sem.at[1, 0], x_peer)
    up_tall = up_half.shape[0]
    up_copy = remote(
        up_ref.at[pl.ds(pl.multiple_of(y * up_tall, up_tall), up_tall)],
        up_half,
        wide_sem.at[0, 1],
        wide_sem.at[1, 1],
        x_peer,
    )

    def pair_store(e):
        return pltpu.make_async_copy(w_buf.at[e], w_pairs.at[e], pair_sem.at[e])

    def x_copy(e, part):
        pair = mixed_bits(lo, e)
        return remote(
            columns(part, pair), slot(e, f, part), x_sem.at[0, e, part], x_sem.at[1, e, part], x_peer
        )

    def y_copy(e, part):
        return remote(
            slot(e, across, part),
            slot(e + 1, across, part),
            y_sem.at[e, part],
            x_sem.at[1, e + 1, part],
            y_peer,
        )

    def arrival(e, part):
        here = slot(e, across, part)
        return remote(here, here, x_sem.at[0, e, part], x_sem.at[1, e, part], x_peer)

    def core_copy(e, part):
        pair = mixed_bits(lo, e)
        return remote(
            columns(part, pair),
            slot(e, f, part),
            core_sem.at[0, e, part],
            core_sem.at[1, e, part],
            core_peer,
        )

    def own_copy(e, part):
        pair = mixed_bits(lo, e)
        return pltpu.make_async_copy(columns(part, pair), slot(e, f, part), own_sem.at[e, part])

    def relay_copy(e, part):
        here = slot(e, across, part)
        return remote(here, here, relay_sem.at[0, e, part], relay_sem.at[1, e, part], core_peer)

    def code_copy(step):
        return remote(
            codes_ref,
            codes_out.at[half + lo],
            code_sem.at[0, step - 1],
            code_sem.at[1, step - 1],
            plane[step - 1],
        )

    order = (4, 5, 2, 3, 6, 7, 0, 1)
    for step in range(1, 4):
        small_copy(step).start()
    for e in order:
        for part in range(3):
            if e % 2 == 0:
                x_copy(e, part).start()
            core_copy(e, part).start()
            own_copy(e, part).start()
    out_copy.start()
    up_copy.start()
    for step in range(1, GROUP):
        code_copy(step).start()
    codes_out[half + lo] = codes_ref[...]

    k_out[2 * halo + rows :, :] = jnp.zeros((KEYS, PAIR), jnp.bfloat16)
    v_out[2 * halo + rows :, :] = jnp.zeros((KEYS, PAIR), jnp.bfloat16)
    for there, low, edge in ((has_prev, 0, 0), (has_next, halo + rows, half + GROUP)):

        @pl.when(jnp.logical_not(there))
        def _():
            k_out[low : low + halo, :] = jnp.zeros((halo, PAIR), jnp.bfloat16)
            v_out[low : low + halo, :] = jnp.zeros((halo, PAIR), jnp.bfloat16)
            codes_out[edge : edge + half] = jnp.zeros((half, 8, PAIR), jnp.float32)

    unit, scale = normalize(tokens_ref[...].astype(jnp.float32))
    small_out[f] = small_ref[...]
    for step in range(1, 4):
        small_copy(step).wait()
    table = [small_out[owner].astype(jnp.float32) for owner in range(4)]

    def vector(line):
        return jnp.concatenate(
            [table[owner][line + row : line + row + 1] for owner in range(4) for row in range(2)],
            axis=1,
        )

    for which, line in ((0, 4), (1, 6)):
        bias[which] = jnp.concatenate(
            [table[owner][line : line + 2] for owner in range(4)], axis=0
        )
    act_ref[...] = (unit * vector(0) + vector(2)).astype(jnp.bfloat16)

    def block_copy(e, part):
        pair = mixed_bits(lo, e)
        into = (q_out, k_out, v_out)[part]
        lead = lo * tok_rows + (0 if part == 0 else halo)
        return remote(
            stage.at[e, part],
            into.at[pl.ds(pl.multiple_of(lead, 128), tok_rows), :],
            block_sem.at[0, e, part],
            block_sem.at[1, e, part],
            (f, base + pair),
        )

    def nth(s):
        return jnp.where(s < 2, s + 4, jnp.where(s < 4, s, jnp.where(s < 6, s + 2, s - 6)))

    def halo_copy(source, part, forward):
        into = (k_out, v_out)[part]
        lead = source * tok_rows
        put = lead + halo - rows if forward else lead + halo + rows
        return remote(
            into.at[pl.ds(pl.multiple_of(halo + lead, 128), tok_rows), :],
            into.at[pl.ds(pl.multiple_of(put, 128), tok_rows), :],
            halo_sem.at[0, source, part],
            halo_sem.at[1, source, part],
            next_peer if forward else prev_peer,
        )

    def pass_on(source):
        for there, forward, fits in (
            (has_next, True, source >= half),
            (has_prev, False, source < half),
        ):

            @pl.when(there & fits)
            def _():
                for part in range(2):
                    halo_copy(source, part, forward).start()

    def pass_arrived(e):
        for part in range(3):
            block_copy(e, part).wait_recv()
        pass_on(mixed_bits(lo, e))

    @pl.loop(0, GROUP)
    def _(s):
        e = nth(s)
        pair = mixed_bits(lo, e)
        for part in range(3):
            arrival(e, part).wait_recv()
            relay_copy(e, part).start()

        @pl.when(e % 2 == 0)
        def _():
            for part in range(3):
                y_copy(e, part).start()

        for part in range(3):
            own_copy(e, part).wait()
            core_copy(e, part).wait_recv()
            relay_copy(e, part).wait_recv()
        pair_store(e).start()
        result = matmul(act_ref[...], w_buf[e])
        outs = (
            (result[:, :PAIR] + bias[0, pl.ds(pair, 1), :]) * (HEAD_DIM**-0.5),
            result[:, PAIR : 2 * PAIR],
            result[:, 2 * PAIR :] + bias[1, pl.ds(pair, 1), :],
        )
        for part in range(3):
            stage[e, part] = outs[part].astype(jnp.bfloat16)

        @pl.when(e > 0)
        def _():
            for part in range(3):
                block_copy(e, part).start()

        @pl.when(e == 0)
        def _():
            for part, into in enumerate((q_out, k_out, v_out)):
                lead = lo * tok_rows + (0 if part == 0 else halo)
                into[pl.ds(pl.multiple_of(lead, 128), tok_rows), :] = outs[part].astype(
                    jnp.bfloat16
                )
            pass_on(lo)

        @pl.when(s >= GROUP // 2)
        def _():
            pass_arrived(nth(s - GROUP // 2))

    for e in (1, 6, 7):
        pass_arrived(e)

    for step in range(1, GROUP):
        code_copy(step).wait()

    def edge_copy(forward):
        low, put = (GROUP, 0) if forward else (half, half + GROUP)
        return remote(
            codes_out.at[pl.ds(low, half)],
            codes_out.at[pl.ds(put, half)],
            edge_sem.at[0, int(forward)],
            edge_sem.at[1, int(forward)],
            next_peer if forward else prev_peer,
        )

    sides = ((has_next, has_prev, True), (has_prev, has_next, False))
    for there, here, forward in sides:

        @pl.when(there)
        def _():
            edge_copy(forward).start()

    out_copy.wait()
    up_copy.wait()
    for e in range(GROUP):
        pair_store(e).wait()
    for e in range(GROUP):
        for part in range(3):
            if e % 2 == 0:
                x_copy(e, part).wait_send()
                y_copy(e, part).wait_send()
            core_copy(e, part).wait_send()
            relay_copy(e, part).wait_send()
            if e > 0:
                block_copy(e, part).wait_send()
    for there, here, forward in sides:
        sources = range(half, GROUP) if forward else range(half)

        @pl.when(there)
        def _():
            edge_copy(forward).wait_send()
            for source in sources:
                for part in range(2):
                    halo_copy(source, part, forward).wait_send()

        @pl.when(here)
        def _():
            edge_copy(forward).wait_recv()
            for source in sources:
                for part in range(2):
                    halo_copy(source, part, forward).wait_recv()


def project(replicas, tokens, small, codes, w_qkv, w_out, w_up):
    tok_rows = tokens.shape[0]
    rows = GROUP * tok_rows
    window = 2 * rows + KEYS
    low = jnp.bfloat16
    vmem = pl.BlockSpec(memory_space=pltpu.VMEM)
    anywhere = pl.BlockSpec(memory_space=pl.ANY)
    dma = pltpu.SemaphoreType.DMA
    shape = jax.ShapeDtypeStruct
    return pl.pallas_call(
        functools.partial(qkv_kernel, replicas),
        out_shape=(
            shape((tok_rows, D), low),
            shape((rows, PAIR), low),
            shape((window, PAIR), low),
            shape((window, PAIR), low),
            shape((2 * GROUP, 8, PAIR), jnp.float32),
            shape((4,) + small.shape, low),
            shape((GROUP, D, 3 * PAIR), low),
            shape(w_out.shape, low),
            shape((w_up.shape[0] // 2, w_up.shape[1]), low),
        ),
        in_specs=[vmem] * 3 + [anywhere] * 3,
        out_specs=(vmem,) * 6 + (anywhere,) * 3,
        scratch_shapes=[
            pltpu.VMEM((GROUP, D, 3 * PAIR), low),
            pltpu.VMEM((GROUP, 3, tok_rows, PAIR), low),
            pltpu.VMEM((2, GROUP, PAIR), jnp.float32),
            dma((GROUP, 3)),
            dma((2, GROUP, 3)),
            dma((GROUP, 3)),
            dma((2, GROUP, 3)),
            dma((2, GROUP, 3)),
            dma((2, GROUP, 3)),
            dma((2, GROUP, 2)),
            dma((2, GROUP - 1)),
            dma((2, 2)),
            dma((2, 3)),
            dma((2, 2)),
            dma((GROUP,)),
        ],
        compiler_params=pltpu.CompilerParams(
            collective_id=2, has_side_effects=True, vmem_limit_bytes=40 << 20
        ),
        cost_estimate=pl.CostEstimate(
            flops=2 * tok_rows * D * 3 * D, transcendentals=0, bytes_accessed=60 << 20
        ),
        name="project",
    )(tokens, small, codes, w_qkv, w_out, w_up)


def low(value):
    return value.astype(jnp.bfloat16)


def high(value):
    return value.astype(jnp.float32)


def span(start, size):
    return pl.ds(pl.multiple_of(start, size), size)


def make_pipe(place, own, source, load, from_core, from_x, from_y, from_near, from_far, final, sem):
    x, c, y, z_near, z_far = place["x"], place["c"], place["y"], place["z_near"], place["z_far"]
    depth = final.shape[1]
    half, mid, short = depth // 2, depth // 4, depth // 8
    my_half = span(y * half, half)
    my_mid = span(y * half + z_near * mid, mid)
    my_short = span(y * half + z_near * mid + z_far * short, short)

    def spot(side):
        return side if own.shape[1] == 2 else side * 2 + c

    def link(k, which, here, there, peer):
        return remote(here, there, sem.at[0, k, which], sem.at[1, k, which], place[peer])

    def core_copy(k, side):
        owner = side * 2 + 1 - c
        here = own.at[k, owner] if source is None else source(k, owner)
        return link(k, side, here, from_core.at[k, side], "core")

    def load_copy(k, side):
        return pltpu.make_async_copy(
            source(k, side * 2 + c), own.at[k, side], load.at[k, side]
        )

    def x_copy(k):
        return link(k, 2, own.at[k, spot(1 - x)], from_x.at[k], "x_peer")

    def y_copy(k):
        return link(k, 3, own.at[k, spot(x), span((1 - y) * half, half)], from_y.at[k], "y_peer")

    def near_copy(k):
        away = span(y * half + (1 - z_near) * mid, mid)
        return link(k, 4, own.at[k, spot(x), away], from_near.at[k], "near")

    def far_copy(k):
        away = span(y * half + z_near * mid + (1 - z_far) * short, short)
        return link(k, 5, own.at[k, spot(x), away], from_far.at[k], "far")

    def far_join_copy(k):
        here = final.at[k, my_short]
        return link(k, 6, here, here, "far")

    def near_join_copy(k):
        here = final.at[k, my_mid]
        return link(k, 7, here, here, "near")

    def y_join_copy(k):
        here = final.at[k, my_half]
        return link(k, 8, here, here, "y_peer")

    def enter(k):
        for side in range(2):
            core_copy(k, side).start()
            if source is not None:
                load_copy(k, side).start()

    def core_sum(k):
        for side in range(2):
            if source is not None:
                load_copy(k, side).wait()
            core_copy(k, side).wait()
            own[k, spot(side)] = low(high(own[k, spot(side)]) + high(from_core[k, side]))
        x_copy(k).start()

    def x_sum(k):
        x_copy(k).wait()
        own[k, spot(x)] = low(high(own[k, spot(x)]) + high(from_x[k]))
        y_copy(k).start()

    def y_sum(k):
        y_copy(k).wait()
        own[k, spot(x), my_half] = low(high(own[k, spot(x), my_half]) + high(from_y[k]))
        near_copy(k).start()

    def near_sum(k):
        near_copy(k).wait()
        own[k, spot(x), my_mid] = low(high(own[k, spot(x), my_mid]) + high(from_near[k]))
        far_copy(k).start()

    def far_sum(k):
        far_copy(k).wait()
        final[k, my_short] = low(high(own[k, spot(x), my_short]) + high(from_far[k]))
        far_join_copy(k).start()

    def far_join(k):
        far_join_copy(k).wait()
        near_join_copy(k).start()

    def near_join(k):
        near_join_copy(k).wait()
        y_join_copy(k).start()

    def y_join(k):
        y_join_copy(k).wait()

    return [enter, core_sum, x_sum, y_sum, near_sum, far_sum, far_join, near_join, y_join]


def run_pipe(steps, count, now):
    for where, step in enumerate(steps):
        k = now - where * LAG

        @pl.when((k >= 0) & (k < count))
        def _():
            step(k)


def pipe_shapes(count, held, depth, width, loads):
    low_type = jnp.bfloat16
    return [
        pltpu.VMEM((count, held, depth, width), low_type),
        pltpu.VMEM((count, 2, depth, width), low_type),
        pltpu.VMEM((count, depth, width), low_type),
        pltpu.VMEM((count, depth // 2, width), low_type),
        pltpu.VMEM((count, depth // 4, width), low_type),
        pltpu.VMEM((count, depth // 8, width), low_type),
        pltpu.VMEM((count, depth, width), low_type),
        pltpu.SemaphoreType.DMA((2, count, 9)),
    ] + ([pltpu.SemaphoreType.DMA((count, 2))] if loads else [])


def find_place():
    f = lax.axis_index("fsdp")
    r = lax.axis_index("rep")
    x, c, z, y = split_index(f, r)
    lo = r % GROUP
    base = r - lo
    z_near, z_far = z % 2, z // 2
    return {
        "f": f,
        "r": r,
        "x": x,
        "c": c,
        "y": y,
        "z_near": z_near,
        "z_far": z_far,
        "lo": lo,
        "base": base,
        "core": (x * 2 + 1 - c, r),
        "x_peer": ((1 - x) * 2 + c, r),
        "y_peer": (f, base + z * 2 + 1 - y),
        "near": (f, base + (z_far * 2 + 1 - z_near) * 2 + y),
        "far": (f, base + ((1 - z_far) * 2 + z_near) * 2 + y),
        "plane": [(f, base + (lo + step) % GROUP) for step in range(1, GROUP)],
    }


def erf(value):
    return lax.erf(value)


def middle_kernel(
    o_ref,
    tokens_ref,
    grad_ref,
    lines_ref,
    bias_ref,
    wo_own,
    wo_across,
    wu_own,
    wu_half,
    wu_other,
    wd_own,
    wd_across,
    layer_out,
    residual_out,
    grad_out,
    small_out,
    up_final,
    rest,
    wo,
    wu,
    wd,
    attn,
    act,
    act_t,
    slim,
    x1,
    proj,
    branch,
    act_grad,
    pre,
    hidden,
    slope,
    pre_grad,
    attn_grad,
    proj_grad,
    sums,
    stage,
    own,
    from_core,
    from_x,
    from_y,
    from_near,
    from_far,
    final,
    sem,
    load_sem,
    attn_sem,
    grad_sem,
    core_load_sem,
    stage_sem,
):
    place = find_place()
    f, x, c, y, lo, base = (place[name] for name in ("f", "x", "c", "y", "lo", "base"))
    across = (1 - x) * 2 + c
    tok_rows = tokens_ref.shape[0]
    share = wo_own.shape[0]
    deep = wd_own.shape[0]
    sets = bias_ref.shape[0]
    tall = 128
    greet([place["core"], place["x_peer"]] + place["plane"])

    def shard_rows(owner, size):
        return span(owner * size, size)

    def attn_copy(e):
        pair = mixed_bits(lo, e)
        return remote(
            o_ref.at[span(pair * tok_rows, tok_rows), :],
            attn.at[:, span(lo * PAIR, PAIR)],
            attn_sem.at[0, e],
            attn_sem.at[1, e],
            (f, base + pair),
        )

    def grad_copy(e):
        pair = mixed_bits(lo, e)
        return remote(
            attn_grad.at[:, span(pair * PAIR, PAIR)],
            grad_out.at[span(lo * tok_rows, tok_rows), :],
            grad_sem.at[0, e],
            grad_sem.at[1, e],
            (f, base + pair),
        )

    share_half = share // 2
    lead = across * share
    moves = (
        (wo_own, wo, f * share, share),
        (wo_across, wo, lead, share),
        (wu_own, wu, f * share, share),
        (wu_half, wu, lead + y * share_half, share_half),
        (wu_other, wu, lead + (1 - y) * share_half, share_half),
        (wd_own, wd, f * deep, deep),
        (wd_across, wd, across * deep, deep),
    )

    def local_copy(which):
        source, into, top, size = moves[which]
        target = into.at[pl.ds(pl.multiple_of(top, 128), size)]
        return pltpu.make_async_copy(source, target, load_sem.at[which])

    def core_copy(which):
        source, into, top, size = moves[which]
        target = into.at[pl.ds(pl.multiple_of(top, 128), size)]
        return remote(
            source, target, core_load_sem.at[0, which], core_load_sem.at[1, which], place["core"]
        )

    order = (4, 5, 6, 7, 2, 3, 1)
    for e in order:
        attn_copy(e).start()
    for which in range(len(moves)):
        core_copy(which).start()
        local_copy(which).start()
    attn[:, span(lo * PAIR, PAIR)] = o_ref[span(lo * tok_rows, tok_rows), :]
    small_out[...] = jnp.zeros_like(small_out)
    sums[...] = jnp.zeros_like(sums)
    branch[...] = jnp.zeros_like(branch)
    act_grad[...] = jnp.zeros_like(act_grad)

    def line(which):
        return lines_ref[which : which + 1, :]

    def by_rows(step, body):
        @pl.loop(0, tok_rows // step)
        def _(b):
            body(span(b * step, step))

    def scale_grad(at):
        slim[at, :] = low(line(5) * high(grad_ref[at, :]))

    by_rows(64, scale_grad)

    for e in order:
        attn_copy(e).wait_recv()
    for which in range(2):
        local_copy(which).wait()
        core_copy(which).wait_recv()
    proj[...] = matmul(attn[...], wo[...])

    def enter_mlp(at):
        value = proj[at, :] + line(0)
        proj[at, :] = value
        value = high(tokens_ref[at, :]) + line(1) * value
        x1[at, :] = value
        unit, scale = normalize(value)
        act[at, :] = low(unit * line(2) + line(3))

    by_rows(64, enter_mlp)
    act_t[...] = act[...].T
    for which in range(2, len(moves)):
        local_copy(which).wait()
        core_copy(which).wait_recv()
    steps = make_pipe(
        place, own, None, None, from_core, from_x, from_y, from_near, from_far, final, sem
    )
    finish_step = steps[-1]

    def settle(k):
        finish_step(k)
        i, side = k // 2, k % 2
        for owner in range(4):
            up_final[span(side * tall, tall), span(owner * deep + i * tall, tall)] = final[
                k, :, owner * tall : (owner + 1) * tall
            ]

    steps[-1] = settle
    count = 2 * sets

    def stage_copy(i, part):
        return pltpu.make_async_copy(
            stage.at[i % 2, part], rest.at[2 * i + part], stage_sem.at[i % 2, part]
        )

    @pl.loop(0, sets)
    def _(i):
        columns = [span(owner * deep + i * tall, tall) for owner in range(4)]
        w_in = jnp.concatenate([wu[:, at] for at in columns], axis=1)
        w_back = jnp.concatenate([wd[at, :] for at in columns], axis=0)
        pre[...] = matmul(act[...], w_in)

        def activate(at):
            value = pre[at, :] + bias_ref[pl.ds(i, 1), :]
            cdf = 0.5 * (1.0 + erf(value * (0.5**0.5)))
            hidden[at, :] = low(value * cdf)
            slope[at, :] = cdf + value * (jnp.exp(-0.5 * value * value) * 0.3989422804014327)

        by_rows(64, activate)
        pre[...] = lax.dot_general(slim[...], w_back, NT, preferred_element_type=jnp.float32)
        branch[...] += matmul(hidden[...], w_back)

        def descend(at):
            value = pre[at, :] * slope[at, :]
            pre[at, :] = value
            pre_grad[at, :] = low(value)

        by_rows(64, descend)
        total = jnp.sum(pre[...], axis=0, keepdims=True)
        for owner in range(4):
            small_out[owner, pl.ds(20 + i, 1), :] = total[:, owner * tall : (owner + 1) * tall]
        up_grad = low(matmul(act_t[...], pre_grad[...]))
        for side in range(2):
            for owner in range(4):
                top = owner * 2 * tall + side * tall
                own[2 * i + side, owner] = up_grad[top : top + tall]
        run_pipe(steps, count, 2 * i)
        act_grad[...] += lax.dot_general(
            pre_grad[...], w_in, NT, preferred_element_type=jnp.float32
        )

        @pl.when(i >= 2)
        def _():
            for part in range(2):
                stage_copy(i - 2, part).wait()

        down_grad = low(matmul(hidden[...].T, slim[...]))
        for part in range(2):
            for owner in range(4):
                stage[i % 2, part, owner] = down_grad[
                    owner * tall : (owner + 1) * tall, part * 4 * tall : (part + 1) * 4 * tall
                ]
            stage_copy(i, part).start()
        run_pipe(steps, count, 2 * i + 1)

    def leave_mlp(at):
        grad = high(grad_ref[at, :])
        out = branch[at, :] + line(4)
        layer_out[at, :] = low(x1[at, :] + line(5) * out)
        unit, scale = normalize(x1[at, :])
        back = act_grad[at, :]
        value = grad + norm_back(back, unit, scale, line(2))
        residual_out[at, :] = value
        scaled = line(1) * value
        proj_grad[at, :] = low(scaled)
        rows = (scaled, value * proj[at, :], back * unit, back, line(5) * grad, grad * out)
        for which, member in enumerate(rows):
            sums[which : which + 1, :] += jnp.sum(member, axis=0, keepdims=True)

    by_rows(64, leave_mlp)
    attn_grad[...] = low(
        lax.dot_general(proj_grad[...], wo[...], NT, preferred_element_type=jnp.float32)
    )
    for e in order:
        grad_copy(e).start()
    grad_out[span(lo * tok_rows, tok_rows), :] = attn_grad[:, span(lo * PAIR, PAIR)]
    for which in range(6):
        for owner in range(4):
            for row in range(2):
                at = (owner * 2 + row) * PAIR
                place_row = 8 + 2 * which + row
                small_out[owner, place_row : place_row + 1, :] = sums[
                    which : which + 1, at : at + PAIR
                ]
    for i in range(sets - 2, sets):
        for part in range(2):
            stage_copy(i, part).wait()

    def out_copy(side, part):
        return pltpu.make_async_copy(
            stage.at[side, part], rest.at[count + 2 * side + part], stage_sem.at[side, part]
        )

    act_t[...] = attn[...].T
    for owner in range(4):
        part_grad = low(matmul(act_t[owner * share : (owner + 1) * share, :], proj_grad[...]))
        for side in range(2):
            for part in range(2):
                stage[side, part, owner] = part_grad[
                    side * tall : (side + 1) * tall, part * 4 * tall : (part + 1) * 4 * tall
                ]
    for side in range(2):
        for part in range(2):
            out_copy(side, part).start()

    @pl.loop(count, count + LAG * (len(steps) - 1))
    def _(now):
        run_pipe(steps, count, now)

    for side in range(2):
        for part in range(2):
            out_copy(side, part).wait()
    for e in order:
        attn_copy(e).wait_send()
        grad_copy(e).wait()
    for which in range(len(moves)):
        core_copy(which).wait_send()


def middle(mixed, tokens, out_grad, lines, bias, weights):
    w_out, w_up, w_down = weights[0], weights[2], weights[5]
    tok_rows = tokens.shape[0]
    rows = GROUP * tok_rows
    sets = bias.shape[0]
    count = 2 * sets
    wide = bias.shape[1]
    anywhere = pl.BlockSpec(memory_space=pl.ANY)
    vmem = pl.BlockSpec(memory_space=pltpu.VMEM)
    dma = pltpu.SemaphoreType.DMA
    shape = jax.ShapeDtypeStruct
    slight, full = jnp.bfloat16, jnp.float32
    return pl.pallas_call(
        middle_kernel,
        out_shape=(
            shape((tok_rows, D), slight),
            shape((tok_rows, D), full),
            shape((rows, PAIR), slight),
            shape((4, 28, PAIR), full),
            shape(w_up.shape, slight),
            shape((count + 4, 4, 128, wide), slight),
        ),
        in_specs=[vmem] * 5 + [anywhere] * 7,
        out_specs=(vmem,) * 5 + (anywhere,),
        scratch_shapes=[
            pltpu.VMEM((4 * w_out.shape[0], D), slight),
            pltpu.VMEM((4 * w_up.shape[0], w_up.shape[1]), slight),
            pltpu.VMEM((4 * w_down.shape[0], D), slight),
            pltpu.VMEM((tok_rows, D), slight),
            pltpu.VMEM((tok_rows, D), slight),
            pltpu.VMEM((D, tok_rows), slight),
            pltpu.VMEM((tok_rows, D), slight),
            pltpu.VMEM((tok_rows, D), full),
            pltpu.VMEM((tok_rows, D), full),
            pltpu.VMEM((tok_rows, D), full),
            pltpu.VMEM((tok_rows, D), full),
            pltpu.VMEM((tok_rows, wide), full),
            pltpu.VMEM((tok_rows, wide), slight),
            pltpu.VMEM((tok_rows, wide), full),
            pltpu.VMEM((tok_rows, wide), slight),
            pltpu.VMEM((tok_rows, D), slight),
            pltpu.VMEM((tok_rows, D), slight),
            pltpu.VMEM((8, D), full),
            pltpu.VMEM((2, 2, 4, 128, wide), slight),
        ]
        + pipe_shapes(count, 4, 128, wide, False)
        + [
            dma((7,)),
            dma((2, GROUP)),
            dma((2, GROUP)),
            dma((2, 7)),
            dma((2, 2)),
        ],
        compiler_params=pltpu.CompilerParams(
            collective_id=3, has_side_effects=True, vmem_limit_bytes=67043328
        ),
        cost_estimate=pl.CostEstimate(
            flops=40 * tok_rows * D * D, transcendentals=0, bytes_accessed=100 << 20
        ),
        name="middle",
    )(mixed, tokens, out_grad, lines, bias, *weights)


def finish_kernel(
    replicas,
    dq_ref,
    dk_ref,
    dv_ref,
    act_ref,
    pairs_ref,
    tokens_ref,
    residual_ref,
    gain_ref,
    small_ref,
    rest_ref,
    tokens_out,
    down_final,
    out_final,
    qkv_final,
    small_final,
    own,
    from_core,
    from_x,
    from_y,
    from_near,
    from_far,
    final,
    sem,
    load_sem,
    pair_own,
    pair_core,
    pair_x,
    pair_y,
    pair_near,
    pair_far,
    pair_final,
    pair_sem,
    halos,
    stage,
    arrived,
    w_buf,
    act_t,
    act_grad,
    small_work,
    small_own,
    small_core,
    small_x,
    small_all,
    halo_sem,
    block_sem,
    w_sem,
    small_sem,
):
    place = find_place()
    f, r, x, c, lo, base = (place[name] for name in ("f", "r", "x", "c", "lo", "base"))
    core_peer, x_peer, plane = place["core"], place["x_peer"], place["plane"]
    has_next, next_peer, has_prev, prev_peer = group_neighbours(f, r, replicas)
    total = own.shape[0]
    tok_rows = act_ref.shape[0]
    rows = GROUP * tok_rows
    halo = rows // 2
    half_group = GROUP // 2
    greet([core_peer, x_peer] + plane, [(has_next, next_peer), (has_prev, prev_peer)])

    def block(ref, source, lead=0):
        return ref.at[pl.ds(pl.multiple_of(lead + source * tok_rows, 128), tok_rows), :]

    def lanes(part):
        return pl.ds(part * PAIR, PAIR)

    def halo_copy(source, part, forward):
        ref = (dk_ref, dv_ref)[part]
        return remote(
            block(ref, source, halo + rows if forward else -halo),
            block(halos.at[part], source),
            halo_sem.at[0, source, part],
            halo_sem.at[1, source, part],
            next_peer if forward else prev_peer,
        )

    def block_copy(e, part):
        source = block(dq_ref, mixed_bits(lo, e)) if part == 0 else stage.at[e, part - 1]
        return remote(
            source,
            arrived.at[e, :, lanes(part)],
            block_sem.at[0, e, part],
            block_sem.at[1, e, part],
            (f, base + mixed_bits(lo, e)),
        )

    def nth(p):
        h = p // 2
        near = jnp.where(h == 0, 2, jnp.where(h == 1, 1, jnp.where(h == 2, 3, 0)))
        return jnp.where(p % 2 == 0, 4 + h, near)

    def w_copy(p):
        spot = p % 2
        return pltpu.make_async_copy(pairs_ref.at[nth(p)], w_buf.at[spot], w_sem.at[spot])

    for there, forward in ((has_next, True), (has_prev, False)):

        @pl.when(there)
        def _():
            for i in range(half_group):
                for part in range(2):
                    halo_copy(i if forward else i + half_group, part, forward).start()

        @pl.when(jnp.logical_not(there))
        def _():
            start = halo if forward else 0
            halos[:, start : start + halo, :] = jnp.zeros((2, halo, PAIR), jnp.bfloat16)

    order = (4, 2, 5, 1, 6, 3, 7)
    for e in order:
        block_copy(e, 0).start()
    arrived[0, :, lanes(0)] = dq_ref[pl.ds(pl.multiple_of(lo * tok_rows, 128), tok_rows), :]
    small_work[...] = small_ref[...]
    act_grad[...] = jnp.zeros_like(act_grad)
    act_t[...] = act_ref[...].T
    w_copy(0).start()

    def give(p):
        e = nth(p)
        source = mixed_bits(lo, e)
        for there, forward, fits in (
            (has_next, False, source >= half_group),
            (has_prev, True, source < half_group),
        ):

            @pl.when(there & fits)
            def _():
                for part in range(2):
                    halo_copy(source, part, forward).wait_recv()

        sums = []
        for part, ref in enumerate((dk_ref, dv_ref)):
            near = ref[pl.ds(pl.multiple_of(halo + source * tok_rows, 128), tok_rows), :]
            far = halos[part, pl.ds(pl.multiple_of(source * tok_rows, 128), tok_rows), :]
            sums.append(low(high(near) + high(far)))
            stage[e, part] = sums[part]

        @pl.when(e > 0)
        def _():
            for part in range(1, 3):
                block_copy(e, part).start()

        @pl.when(e == 0)
        def _():
            for part in range(1, 3):
                arrived[0, :, lanes(part)] = sums[part - 1]

    pair_steps = make_pipe(
        place,
        pair_own,
        None,
        None,
        pair_core,
        pair_x,
        pair_y,
        pair_near,
        pair_far,
        pair_final,
        pair_sem,
    )
    pair_enter = pair_steps.pop(0)

    def take(p):
        e = nth(p)
        j = mixed_bits(lo, e)

        @pl.when(p + 1 < GROUP)
        def _():
            w_copy(p + 1).start()

        @pl.when(e > 0)
        def _():
            for part in range(3):
                block_copy(e, part).wait_recv()

        w_copy(p).wait()
        grads = arrived[e]
        pair_own[j] = low(matmul(act_t[...], grads)).reshape(4, D // 4, 3 * PAIR)
        pair_enter(j)
        act_grad[...] += lax.dot_general(
            grads, w_buf[p % 2], NT, preferred_element_type=jnp.float32
        )
        sums = jnp.sum(high(grads), axis=0, keepdims=True)
        for line, part in ((4, 0), (6, 2)):
            small_work[j // 2, pl.ds(line + j % 2, 1), :] = sums[:, part * PAIR : (part + 1) * PAIR]

    def leave():
        unit, scale = normalize(high(tokens_ref[...]))
        grad = act_grad[...]
        back = norm_back(grad, unit, scale, gain_ref[...])
        tokens_out[...] = low(residual_ref[...] + back)
        for line, values in ((0, grad * unit), (2, grad)):
            sums = jnp.sum(values, axis=0, keepdims=True)
            for owner in range(4):
                for row in range(2):
                    at = (owner * 2 + row) * PAIR
                    small_work[owner, line + row : line + row + 1, :] = sums[:, at : at + PAIR]
        for side in range(2):
            small_enter(side).start()

    steps = make_pipe(
        place,
        own,
        lambda k, owner: rest_ref.at[k, owner],
        load_sem,
        from_core,
        from_x,
        from_y,
        from_near,
        from_far,
        final,
        sem,
    )
    finish_step = steps[-1]
    tall, wide = final.shape[1:]
    downs = down_final.shape[0] // tall * 2

    def settle(k):
        finish_step(k)

        @pl.when(k < downs)
        def _():
            down_final[span((k // 2) * tall, tall), span((k % 2) * wide, wide)] = final[k]

        @pl.when(k >= downs)
        def _():
            at = k - downs
            out_final[span((at // 2) * tall, tall), span((at % 2) * wide, wide)] = final[k]

    steps[-1] = settle

    def small_enter(side):
        return remote(
            small_work.at[side * 2 + 1 - c],
            small_core.at[side],
            small_sem.at[0, side],
            small_sem.at[1, side],
            core_peer,
        )

    small_cross = remote(
        small_own.at[1 - x], small_x, small_sem.at[0, 2], small_sem.at[1, 2], x_peer
    )

    def small_spread(step):
        return remote(
            small_own.at[2],
            small_all.at[step - 1],
            small_sem.at[0, 2 + step],
            small_sem.at[1, 2 + step],
            plane[step - 1],
        )

    def small_first():
        for side in range(2):
            small_enter(side).wait()
        for side in range(2):
            small_own[side] = small_work[side * 2 + c] + small_core[side]
        small_cross.start()

    def small_second():
        small_cross.wait()
        small_own[2] = small_own[x] + small_x[...]
        for step in range(1, GROUP):
            small_spread(step).start()

    def arrive(p):
        pair_steps[0](mixed_bits(lo, nth(p)))

    def cross(p):
        pair_steps[1](mixed_bits(lo, nth(p)))

    stop = max(total + LAG * (len(steps) - 1), LAST_TAKE + 5 + GROUP // PAIR_BY + LAG * 5)

    @pl.loop(0, stop)
    def _(now):
        @pl.when((now >= GIVE_AT) & (now < GIVE_AT + GROUP))
        def _():
            give(now - GIVE_AT)

        run_pipe(steps, total, now)

        for step, lag in ((take, 0), (arrive, 2), (cross, 4)):
            gone = now - TAKE_AT - lag

            @pl.when((gone >= 0) & (gone < TAKE_BY * GROUP) & (gone % TAKE_BY == 0))
            def _():
                step(gone // TAKE_BY)

        for event, at in (
            (leave, LAST_TAKE + 1),
            (small_first, LAST_TAKE + 5),
            (small_second, LAST_TAKE + 9),
        ):
            pl.when(now == at)(event)

        for where, step in enumerate(pair_steps[2:]):
            gone = now - LAST_TAKE - 5 - LAG * where

            @pl.when((gone >= 0) & (gone < GROUP // PAIR_BY))
            def _():
                for each in range(PAIR_BY):
                    step(PAIR_BY * gone + each)

    for step in range(1, GROUP):
        small_spread(step).wait()
    value = small_own[2]
    for step in range(1, GROUP):
        value = value + small_all[step - 1]
    small_final[...] = value
    for j in range(GROUP):
        for part in range(3):
            at = part * D + j * PAIR
            qkv_final[:, at : at + PAIR] = pair_final[j, :, part * PAIR : (part + 1) * PAIR]

    for e in order:
        for part in range(3):
            block_copy(e, part).wait_send()
    for there, forward in ((has_next, True), (has_prev, False)):

        @pl.when(there)
        def _():
            for i in range(half_group):
                for part in range(2):
                    halo_copy(i if forward else i + half_group, part, forward).wait_send()


def wrap_up(replicas, moved, act, pairs, tokens, residual, gain, small, rest, shapes):
    chunks = rest.shape[0]
    tok_rows = act.shape[0]
    tall = small.shape[1]
    anywhere = pl.BlockSpec(memory_space=pl.ANY)
    vmem = pl.BlockSpec(memory_space=pltpu.VMEM)
    dma = pltpu.SemaphoreType.DMA
    low = jnp.bfloat16
    shape = jax.ShapeDtypeStruct
    pair = 3 * PAIR
    return pl.pallas_call(
        functools.partial(finish_kernel, replicas),
        out_shape=(shape((tok_rows, D), low),)
        + tuple(shape(size, low) for size in shapes)
        + (shape((D // 4, 3 * D), low), shape((tall, PAIR), jnp.float32)),
        in_specs=[vmem] * 4 + [anywhere] + [vmem] * 4 + [anywhere],
        out_specs=(vmem,) * 5,
        scratch_shapes=pipe_shapes(chunks, 2, *rest.shape[2:], True)
        + pipe_shapes(GROUP, 4, D // 4, pair, False)
        + [
            pltpu.VMEM((2, GROUP * tok_rows, PAIR), low),
            pltpu.VMEM((GROUP, 2, tok_rows, PAIR), low),
            pltpu.VMEM((GROUP, tok_rows, pair), low),
            pltpu.VMEM((2, D, pair), low),
            pltpu.VMEM((D, tok_rows), low),
            pltpu.VMEM((tok_rows, D), jnp.float32),
            pltpu.VMEM((4, tall, PAIR), jnp.float32),
            pltpu.VMEM((3, tall, PAIR), jnp.float32),
            pltpu.VMEM((2, tall, PAIR), jnp.float32),
            pltpu.VMEM((tall, PAIR), jnp.float32),
            pltpu.VMEM((GROUP - 1, tall, PAIR), jnp.float32),
            dma((2, GROUP, 2)),
            dma((2, GROUP, 3)),
            dma((2,)),
            dma((2, GROUP + 2)),
        ],
        compiler_params=pltpu.CompilerParams(
            collective_id=1, has_side_effects=True, vmem_limit_bytes=67043328
        ),
        cost_estimate=pl.CostEstimate(
            flops=12 * tok_rows * D * D, transcendentals=0, bytes_accessed=200 << 20
        ),
        name="finish",
    )(*moved, act, pairs, tokens, residual, gain, small, rest)


def shards(
    tokens,
    out_grad,
    norm1_gain,
    norm1_bias,
    w_qkv,
    q_bias,
    v_bias,
    w_out,
    out_bias,
    attn_scale,
    norm2_gain,
    norm2_bias,
    w_up,
    up_bias,
    w_down,
    down_bias,
    mlp_scale,
    image_ids,
    pad_mask,
):
    both = ("fsdp", "rep")
    owners = lax.axis_size("fsdp")
    replicas = lax.axis_size("rep")
    tok_rows = tokens.shape[0]
    rows = GROUP * tok_rows
    groups = [list(range(g, g + GROUP)) for g in range(0, replicas, GROUP)]
    factor = HEAD_DIM ** (-0.5)

    small = (
        norm1_gain,
        norm1_bias,
        q_bias,
        v_bias,
        out_bias,
        attn_scale,
        norm2_gain,
        norm2_bias,
        down_bias,
        mlp_scale,
        up_bias,
    )
    sizes = [member.shape[0] for member in small]
    packed = jnp.concatenate(small + (jnp.zeros((-sum(sizes) % 2048,), jnp.bfloat16),))
    codes = jnp.where(pad_mask > 0, image_ids + 1, 0).astype(jnp.float32).reshape(-1, PAIR)
    code_rows = codes.shape[0]
    codes = jnp.concatenate([codes, jnp.zeros((8 - code_rows, PAIR), jnp.float32)], axis=0)
    act_one, query, key_window, value_window, codes, vectors, w_pairs, out_across, up_half = project(
        replicas, tokens, packed.reshape(-1, PAIR), codes, w_qkv, w_out, w_up
    )
    vectors = vectors.reshape(4, -1).astype(jnp.float32)
    parts = []
    place = 0
    for member in small:
        parts.append(vectors[:, place : place + member.shape[0]].reshape(-1))
        place += member.shape[0]
    (
        gain_first,
        shift_first,
        query_bias,
        value_bias,
        proj_bias,
        attn_gamma,
        gain_second,
        shift_second,
        final_bias,
        mlp_gamma,
        hidden_bias,
    ) = parts


    window = key_window.shape[0]
    halo = rows // 2
    seen = codes[:, :code_rows].reshape(-1).astype(jnp.int32)
    seen = jnp.concatenate([seen, jnp.zeros((KEYS,), jnp.int32)])
    spot = jnp.arange(window, dtype=jnp.int32)
    asked = seen[halo : halo + rows]
    tile_codes = asked.reshape(rows // BLOCK, BLOCK)
    first_code = jnp.min(jnp.where(tile_codes > 0, tile_codes, 1 << 30), axis=1)
    last_code = jnp.max(tile_codes, axis=1)
    begin = jnp.min(jnp.where(seen[None] == first_code[:, None], spot[None], window), axis=1)
    finish = jnp.max(jnp.where(seen[None] == last_code[:, None], spot[None] + 1, 0), axis=1)
    begin = begin // 128 * 128
    count = jnp.where(last_code > 0, (finish - begin + KEYS - 1) // KEYS, 0)
    meta = jnp.stack([begin, count], axis=1).reshape(-1)

    lane_slot = jnp.arange(PAIR, dtype=jnp.int32) % HEAD_DIM
    key_slot = jnp.where(seen > 0, 1 + (seen - 1) % SLOTS, 0)
    marks = (key_slot[:, None] == lane_slot[None]).astype(jnp.bfloat16)


    down_late, query = lax.optimization_barrier((w_down, query))
    down_across = lax.ppermute(down_late, "fsdp", [(f, (f + 2) % 4) for f in range(4)])
    swapped = [(r, r + 1 - 2 * (r % 2)) for r in range(replicas)]
    up_other = lax.ppermute(up_half, "rep", swapped)
    attn_mine, attn_t, lse = attend(meta, query, key_window, value_window, marks)

    lines = jnp.stack(
        (proj_bias, attn_gamma, gain_second, shift_second, final_bias, mlp_gamma) + (gain_second,) * 2
    )
    wide_bias = hidden_bias.reshape(4, -1, PAIR).transpose(1, 0, 2).reshape(-1, 4 * PAIR)
    layer_out, residual_grad, grad_mine, packed, up_out, rest = middle(
        attn_mine,
        tokens,
        out_grad,
        lines,
        wide_bias,
        (w_out, out_across, w_up, up_half, up_other, w_down, down_across),
    )
    dq, dk, dv = attend_back(
        meta, query, key_window, value_window, marks, grad_mine, attn_t, lse
    )
    tokens_grad, *grads, packed = wrap_up(
        replicas,
        (dq, dk, dv),
        act_one,
        w_pairs,
        tokens,
        residual_grad,
        gain_first.reshape(1, D),
        packed,
        rest,
        (w_down.shape, w_out.shape),
    )
    grads.insert(1, up_out)
    grads = [grad.astype(jnp.float32) for grad in grads]
    if replicas > GROUP:
        apart = [list(range(low, replicas, GROUP)) for low in range(GROUP)]
        grads = lax.psum(grads, "rep", axis_index_groups=apart)
        packed = lax.psum(packed, "rep", axis_index_groups=apart)
    packed = packed.reshape(-1)
    small_out = []
    place = 0
    for member in (norm1_gain, norm1_bias, q_bias, v_bias) + small[4:]:
        size = member.shape[0]
        small_out.append(packed[place : place + size])
        place += size

    down_out, up_out, out_out, qkv_out = grads
    return (
        layer_out,
        tokens_grad,
        small_out[0],
        small_out[1],
        qkv_out,
        small_out[2],
        small_out[3],
        out_out,
        small_out[4],
        small_out[5],
        small_out[6],
        small_out[7],
        up_out,
        small_out[10],
        down_out,
        small_out[8],
        small_out[9],
    )


def solution(mesh):
    spread = P(("fsdp", "rep"), None)
    line = P("fsdp")
    plane = P("fsdp", None)
    return jax.shard_map(
        shards,
        mesh=mesh,
        in_specs=(
            spread,
            spread,
            line,
            line,
            plane,
            line,
            line,
            plane,
            line,
            line,
            line,
            line,
            plane,
            line,
            plane,
            line,
            line,
            P(("fsdp", "rep")),
            P(("fsdp", "rep")),
        ),
        out_specs=(
            spread,
            spread,
            line,
            line,
            plane,
            line,
            line,
            plane,
            line,
            line,
            line,
            line,
            plane,
            line,
            plane,
            line,
            line,
        ),
        check_vma=False,
    )
```

```python
import functools

import jax
import jax.numpy as jnp
from jax import lax
from jax.experimental import pallas as pl
from jax.experimental.pallas import tpu as pltpu
from jax.sharding import PartitionSpec as P

D = 1024
HEADS = 16
HEAD_DIM = 64
IMG = 1370

PAIR = 2 * HEAD_DIM
GROUP = HEADS // 2
BLOCK = 256
KEYS = 1536
SLOTS = 63

EPSILON = 1e-06
NEG_BIG = -1e30
NEG_EDGE = -1e29

NT = (((1,), (1,)), ((), ()))


def from_behind(block, axis, distance):
    devices = range(lax.axis_size(axis))
    route = [(i - distance, i) for i in devices if i - distance in devices]
    return lax.ppermute(block, axis, route)


def normalize(values):
    center = jnp.mean(values, axis=-1, keepdims=True)
    centered = values - center
    spread = jnp.mean(centered * centered, axis=-1, keepdims=True)
    scale = lax.rsqrt(spread + EPSILON)
    return centered * scale, scale


def norm_back(cotangent, unit, scale, gain):
    scaled = cotangent * gain
    along = jnp.mean(scaled, axis=-1, keepdims=True)
    across = jnp.mean(scaled * unit, axis=-1, keepdims=True)
    return scale * (scaled - along - unit * across)


def matmul(left, right):
    return jnp.dot(left, right, preferred_element_type=jnp.float32)


def fold_rows(values, op):
    return op(values.reshape(values.shape[0] // 8, 8, values.shape[1]), axis=0)


def lane_marks():
    lane = lax.broadcasted_iota(jnp.int32, (BLOCK, PAIR), 1)
    return lane // HEAD_DIM, lane % HEAD_DIM > 0


def asking(query, marks, half, usable):
    wanted = jnp.where((marks.astype(jnp.float32) > 0) & usable, 0.0, NEG_BIG).astype(jnp.bfloat16)
    return [jnp.where(half == h, query, wanted) for h in range(2)]


def attend_kernel(meta, q_ref, k_ref, v_ref, m_ref, o_ref, ot_ref, lse_ref, vt, k_aug, scores):
    rows_all = o_ref.shape[0]
    tiles = rows_all // BLOCK
    window = k_ref.shape[0]
    halo = (window - KEYS - rows_all) // 2
    half, usable = lane_marks()

    @pl.loop(0, window // BLOCK)
    def _(i):
        at = pl.ds(pl.multiple_of(i * BLOCK, BLOCK), BLOCK)
        vt[:, at] = v_ref[at, :].T
        for h in range(2):
            k_aug[h, at, :] = jnp.where(half == h, k_ref[at, :], m_ref[at, :])

    @pl.loop(0, tiles)
    def _(t):
        start = meta[2 * t]
        count = meta[2 * t + 1]
        rows = pl.ds(pl.multiple_of(t * BLOCK, BLOCK), BLOCK)
        spots = pl.ds(pl.multiple_of(halo + t * BLOCK, BLOCK), BLOCK)
        query = asking(q_ref[rows, :], m_ref[spots, :], half, usable)

        def score(i, tops):
            at = pl.ds(pl.multiple_of(start + i * KEYS, 128), KEYS)
            keep = pl.ds(pl.multiple_of(i * KEYS, KEYS), KEYS)
            new = []
            for h in range(2):
                part = lax.dot_general(
                    k_aug[h, at, :], query[h], NT, preferred_element_type=jnp.float32
                )
                scores[h, keep, :] = part
                new.append(jnp.maximum(tops[h], fold_rows(part, jnp.max)))
            return tuple(new)

        low = jnp.full((8, BLOCK), NEG_BIG, jnp.float32)
        tops = lax.fori_loop(0, count, score, (low, low))
        tops = [jnp.max(top, axis=0, keepdims=True) for top in tops]
        tops = [jnp.where(top < NEG_EDGE, 0.0, top) for top in tops]

        def mix(i, carry):
            at = pl.ds(pl.multiple_of(start + i * KEYS, 128), KEYS)
            keep = pl.ds(pl.multiple_of(i * KEYS, KEYS), KEYS)
            new = []
            for h in range(2):
                total, mixed = carry[h]
                weights = jnp.exp(scores[h, keep, :] - tops[h])
                total = total + fold_rows(weights, jnp.sum)
                mixed = mixed + matmul(
                    vt[h * HEAD_DIM : (h + 1) * HEAD_DIM, at], weights.astype(jnp.bfloat16)
                )
                new.append((total, mixed))
            return tuple(new)

        zero = (jnp.zeros((8, BLOCK), jnp.float32), jnp.zeros((HEAD_DIM, BLOCK), jnp.float32))
        done = lax.fori_loop(0, count, mix, (zero, zero))
        outs = []
        for h in range(2):
            total = jnp.sum(done[h][0], axis=0, keepdims=True)
            total = jnp.where(total > 0, total, 1.0)
            lse_ref[h : h + 1, rows] = tops[h] + jnp.log(total)
            outs.append(done[h][1] / total)
        out = jnp.concatenate(outs, axis=0)
        ot_ref[:, rows] = out
        o_ref[rows, :] = out.T.astype(jnp.bfloat16)


def attend(meta, query, keys, values, marks):
    rows = query.shape[0]
    window = keys.shape[0]
    deepest = (2 * IMG + 2 * BLOCK + KEYS) // KEYS * KEYS
    vmem = pl.BlockSpec(memory_space=pltpu.VMEM)
    return pl.pallas_call(
        attend_kernel,
        out_shape=(
            jax.ShapeDtypeStruct((rows, PAIR), jnp.bfloat16),
            jax.ShapeDtypeStruct((PAIR, rows), jnp.float32),
            jax.ShapeDtypeStruct((8, rows), jnp.float32),
        ),
        in_specs=[pl.BlockSpec(memory_space=pltpu.SMEM), vmem, vmem, vmem, vmem],
        out_specs=(vmem, vmem, vmem),
        scratch_shapes=[
            pltpu.VMEM((PAIR, window), jnp.bfloat16),
            pltpu.VMEM((2, window, PAIR), jnp.bfloat16),
            pltpu.VMEM((2, deepest, BLOCK), jnp.float32),
        ],
        cost_estimate=pl.CostEstimate(
            flops=4 * rows * 2 * IMG * PAIR, transcendentals=2 * rows * IMG, bytes_accessed=9 << 20
        ),
        name="attend",
    )(meta, query, keys, values, marks)


def attend_back_kernel(
    meta, q_ref, k_ref, v_ref, m_ref, g_ref, ot_ref, lse_ref, dq_ref, dk_out, dv_out, kt, k_aug, dk_ref, dv_ref
):
    rows_all = dq_ref.shape[0]
    tiles = rows_all // BLOCK
    window = k_ref.shape[0]
    halo = (window - KEYS - rows_all) // 2
    half, usable = lane_marks()

    @pl.loop(0, window // BLOCK)
    def _(i):
        at = pl.ds(pl.multiple_of(i * BLOCK, BLOCK), BLOCK)
        kt[:, at] = k_ref[at, :].T
        for h in range(2):
            k_aug[h, at, :] = jnp.where(half == h, k_ref[at, :], m_ref[at, :])
        dk_ref[at, :] = jnp.zeros((BLOCK, PAIR), jnp.float32)
        dv_ref[at, :] = jnp.zeros((BLOCK, PAIR), jnp.float32)

    @pl.loop(0, tiles)
    def _(t):
        start = meta[2 * t]
        count = meta[2 * t + 1]
        rows = pl.ds(pl.multiple_of(t * BLOCK, BLOCK), BLOCK)
        grad = g_ref[rows, :]
        blank = jnp.zeros_like(grad)
        spots = pl.ds(pl.multiple_of(halo + t * BLOCK, BLOCK), BLOCK)
        query = asking(q_ref[rows, :], m_ref[spots, :], half, usable)
        query_only = jnp.concatenate(
            [jnp.where(half == h, query[h], blank) for h in range(2)], axis=0
        )
        grads = [jnp.where(half == h, grad, blank) for h in range(2)]
        grads_both = jnp.concatenate(grads, axis=0)
        product = grad.astype(jnp.float32).T * ot_ref[:, rows]
        delta = [
            jnp.sum(product[h * HEAD_DIM : (h + 1) * HEAD_DIM], axis=0, keepdims=True)
            for h in range(2)
        ]
        lse = [lse_ref[h : h + 1, rows] for h in range(2)]

        def step(i, carry):
            at = pl.ds(pl.multiple_of(start + i * KEYS, 128), KEYS)
            value = v_ref[at, :]
            probs, slopes, new = [], [], []
            for h in range(2):
                part = lax.dot_general(
                    k_aug[h, at, :], query[h], NT, preferred_element_type=jnp.float32
                )
                weights = jnp.exp(part - lse[h])
                pull = lax.dot_general(value, grads[h], NT, preferred_element_type=jnp.float32)
                slope = (weights * (pull - delta[h])).astype(jnp.bfloat16)
                probs.append(weights.astype(jnp.bfloat16))
                slopes.append(slope)
                new.append(carry[h] + matmul(kt[h * HEAD_DIM : (h + 1) * HEAD_DIM, at], slope))
            dv_ref[at, :] += matmul(jnp.concatenate(probs, axis=1), grads_both)
            dk_ref[at, :] += matmul(jnp.concatenate(slopes, axis=1), query_only)
            return tuple(new)

        zero = jnp.zeros((HEAD_DIM, BLOCK), jnp.float32)
        done = lax.fori_loop(0, count, step, (zero, zero))
        dq = jnp.concatenate(done, axis=0) * (HEAD_DIM**-0.5)
        dq_ref[rows, :] = dq.T.astype(jnp.bfloat16)

    @pl.loop(0, window // BLOCK)
    def _(i):
        at = pl.ds(pl.multiple_of(i * BLOCK, BLOCK), BLOCK)
        dk_out[at, :] = dk_ref[at, :].astype(jnp.bfloat16)
        dv_out[at, :] = dv_ref[at, :].astype(jnp.bfloat16)


def attend_back(meta, query, keys, values, marks, grad, out_t, lse):
    rows = query.shape[0]
    window = keys.shape[0]
    vmem = pl.BlockSpec(memory_space=pltpu.VMEM)
    return pl.pallas_call(
        attend_back_kernel,
        out_shape=(
            jax.ShapeDtypeStruct((rows, PAIR), jnp.bfloat16),
            jax.ShapeDtypeStruct((window, PAIR), jnp.bfloat16),
            jax.ShapeDtypeStruct((window, PAIR), jnp.bfloat16),
        ),
        in_specs=[pl.BlockSpec(memory_space=pltpu.SMEM)] + [vmem] * 7,
        out_specs=(vmem, vmem, vmem),
        scratch_shapes=[
            pltpu.VMEM((PAIR, window), jnp.bfloat16),
            pltpu.VMEM((2, window, PAIR), jnp.bfloat16),
            pltpu.VMEM((window, PAIR), jnp.float32),
            pltpu.VMEM((window, PAIR), jnp.float32),
        ],
        cost_estimate=pl.CostEstimate(
            flops=10 * rows * 2 * IMG * PAIR, transcendentals=2 * rows * IMG, bytes_accessed=16 << 20
        ),
        name="attend_back",
    )(meta, query, keys, values, marks, grad, out_t, lse)


CHUNK = 64
LAG = 2
GIVE_AT = 4
TAKE_AT = 20
TAKE_BY = 1
LAST_TAKE = TAKE_AT + (GROUP - 1) * TAKE_BY
PAIR_BY = 1
MESH = pl.DeviceIdType.MESH


def split_index(f, r):
    return f // 2, f % 2, (r % GROUP) // 2, r % 2


def mixed_bits(left, right):
    value = 0
    for weight in (4, 2, 1):
        value = value + weight * ((left // weight + right // weight) % 2)
    return value


def remote(source, target, send, recv, peer):
    return pltpu.make_async_remote_copy(
        src_ref=source,
        dst_ref=target,
        send_sem=send,
        recv_sem=recv,
        device_id=peer,
        device_id_type=MESH,
    )


def greet(peers, optional=()):
    barrier = pltpu.get_barrier_semaphore()
    expected = len(peers)
    for peer in peers:
        pl.semaphore_signal(barrier, inc=1, device_id=peer, device_id_type=MESH)
    for there, peer in optional:

        @pl.when(there)
        def _():
            pl.semaphore_signal(barrier, inc=1, device_id=peer, device_id_type=MESH)

        expected = expected + there.astype(jnp.int32)
    pl.semaphore_wait(barrier, expected)


def group_neighbours(f, r, replicas):
    spot = f * replicas + r
    after = lax.rem(spot + GROUP, 4 * replicas)
    before = lax.rem(spot + 3 * replicas + (replicas - GROUP), 4 * replicas)
    next_peer = (after // replicas, lax.rem(after, replicas))
    prev_peer = (before // replicas, lax.rem(before, replicas))
    return spot + GROUP < 4 * replicas, next_peer, spot >= GROUP, prev_peer


def qkv_kernel(
    replicas,
    tokens_ref,
    small_ref,
    codes_ref,
    w_ref,
    out_ref,
    up_ref,
    act_ref,
    q_out,
    k_out,
    v_out,
    codes_out,
    small_out,
    w_pairs,
    out_across,
    up_half,
    w_buf,
    stage,
    bias,
    own_sem,
    x_sem,
    y_sem,
    core_sem,
    relay_sem,
    block_sem,
    halo_sem,
    code_sem,
    edge_sem,
    small_sem,
    wide_sem,
    pair_sem,
):
    f = lax.axis_index("fsdp")
    r = lax.axis_index("rep")
    x, c, z, y = split_index(f, r)
    lo = r % GROUP
    base = r - lo
    tok_rows = tokens_ref.shape[0]
    rows = GROUP * tok_rows
    halo = (k_out.shape[0] - KEYS - rows) // 2
    half = GROUP // 2
    share = w_ref.shape[0]
    core_peer = (x * 2 + 1 - c, r)
    x_peer = ((1 - x) * 2 + c, r)
    y_peer = (f, base + z * 2 + 1 - y)
    fsdp_peers = [((f + step) % 4, r) for step in range(1, 4)]
    plane = [(f, base + (lo + step) % GROUP) for step in range(1, GROUP)]
    has_next, next_peer, has_prev, prev_peer = group_neighbours(f, r, replicas)
    greet(fsdp_peers + plane, [(has_next, next_peer), (has_prev, prev_peer)])

    def small_copy(step):
        return remote(
            small_ref,
            small_out.at[f],
            small_sem.at[0, step - 1],
            small_sem.at[1, step - 1],
            fsdp_peers[step - 1],
        )

    def lanes(part):
        return pl.ds(part * PAIR, PAIR)

    def shard_rows(owner):
        return pl.ds(pl.multiple_of(owner * share, share), share)

    def columns(part, pair):
        return w_ref.at[:, pl.ds(pl.multiple_of(part * D + pair * PAIR, PAIR), PAIR)]

    def slot(e, owner, part):
        return w_buf.at[e, shard_rows(owner), lanes(part)]

    across = (1 - x) * 2 + c
    out_copy = remote(out_ref, out_across, wide_sem.at[0, 0], wide_sem.at[1, 0], x_peer)
    up_tall = up_half.shape[0]
    up_copy = remote(
        up_ref.at[pl.ds(pl.multiple_of(y * up_tall, up_tall), up_tall)],
        up_half,
        wide_sem.at[0, 1],
        wide_sem.at[1, 1],
        x_peer,
    )

    def pair_store(e):
        return pltpu.make_async_copy(w_buf.at[e], w_pairs.at[e], pair_sem.at[e])

    def x_copy(e, part):
        pair = mixed_bits(lo, e)
        return remote(
            columns(part, pair), slot(e, f, part), x_sem.at[0, e, part], x_sem.at[1, e, part], x_peer
        )

    def y_copy(e, part):
        return remote(
            slot(e, across, part),
            slot(e + 1, across, part),
            y_sem.at[e, part],
            x_sem.at[1, e + 1, part],
            y_peer,
        )

    def arrival(e, part):
        here = slot(e, across, part)
        return remote(here, here, x_sem.at[0, e, part], x_sem.at[1, e, part], x_peer)

    def core_copy(e, part):
        pair = mixed_bits(lo, e)
        return remote(
            columns(part, pair),
            slot(e, f, part),
            core_sem.at[0, e, part],
            core_sem.at[1, e, part],
            core_peer,
        )

    def own_copy(e, part):
        pair = mixed_bits(lo, e)
        return pltpu.make_async_copy(columns(part, pair), slot(e, f, part), own_sem.at[e, part])

    def relay_copy(e, part):
        here = slot(e, across, part)
        return remote(here, here, relay_sem.at[0, e, part], relay_sem.at[1, e, part], core_peer)

    def code_copy(step):
        return remote(
            codes_ref,
            codes_out.at[half + lo],
            code_sem.at[0, step - 1],
            code_sem.at[1, step - 1],
            plane[step - 1],
        )

    order = (4, 5, 2, 3, 6, 7, 0, 1)
    for step in range(1, 4):
        small_copy(step).start()
    for e in order:
        for part in range(3):
            if e % 2 == 0:
                x_copy(e, part).start()
            core_copy(e, part).start()
            own_copy(e, part).start()
    out_copy.start()
    up_copy.start()
    for step in range(1, GROUP):
        code_copy(step).start()
    codes_out[half + lo] = codes_ref[...]

    k_out[2 * halo + rows :, :] = jnp.zeros((KEYS, PAIR), jnp.bfloat16)
    v_out[2 * halo + rows :, :] = jnp.zeros((KEYS, PAIR), jnp.bfloat16)
    for there, low, edge in ((has_prev, 0, 0), (has_next, halo + rows, half + GROUP)):

        @pl.when(jnp.logical_not(there))
        def _():
            k_out[low : low + halo, :] = jnp.zeros((halo, PAIR), jnp.bfloat16)
            v_out[low : low + halo, :] = jnp.zeros((halo, PAIR), jnp.bfloat16)
            codes_out[edge : edge + half] = jnp.zeros((half, 8, PAIR), jnp.float32)

    unit, scale = normalize(tokens_ref[...].astype(jnp.float32))
    small_out[f] = small_ref[...]
    for step in range(1, 4):
        small_copy(step).wait()
    table = [small_out[owner] for owner in range(4)]

    def vector(line):
        return jnp.concatenate([rows_of[line : line + 1] for rows_of in table], axis=1)

    for which, line in ((0, 2), (1, 3)):
        for owner in range(4):
            for side in range(2):
                bias[which, 2 * owner + side : 2 * owner + side + 1, :] = table[owner][
                    line : line + 1, side * PAIR : (side + 1) * PAIR
                ]
    act_ref[...] = (unit * vector(0) + vector(1)).astype(jnp.bfloat16)

    def block_copy(e, part):
        pair = mixed_bits(lo, e)
        into = (q_out, k_out, v_out)[part]
        lead = lo * tok_rows + (0 if part == 0 else halo)
        return remote(
            stage.at[e, part],
            into.at[pl.ds(pl.multiple_of(lead, 128), tok_rows), :],
            block_sem.at[0, e, part],
            block_sem.at[1, e, part],
            (f, base + pair),
        )

    def nth(s):
        return jnp.where(s < 2, s + 4, jnp.where(s < 4, s, jnp.where(s < 6, s + 2, s - 6)))

    def halo_copy(source, part, forward):
        into = (k_out, v_out)[part]
        lead = source * tok_rows
        put = lead + halo - rows if forward else lead + halo + rows
        return remote(
            into.at[pl.ds(pl.multiple_of(halo + lead, 128), tok_rows), :],
            into.at[pl.ds(pl.multiple_of(put, 128), tok_rows), :],
            halo_sem.at[0, source, part],
            halo_sem.at[1, source, part],
            next_peer if forward else prev_peer,
        )

    def pass_on(source):
        for there, forward, fits in (
            (has_next, True, source >= half),
            (has_prev, False, source < half),
        ):

            @pl.when(there & fits)
            def _():
                for part in range(2):
                    halo_copy(source, part, forward).start()

    def pass_arrived(e):
        for part in range(3):
            block_copy(e, part).wait_recv()
        pass_on(mixed_bits(lo, e))

    @pl.loop(0, GROUP)
    def _(s):
        e = nth(s)
        pair = mixed_bits(lo, e)
        for part in range(3):
            arrival(e, part).wait_recv()
            relay_copy(e, part).start()

        @pl.when(e % 2 == 0)
        def _():
            for part in range(3):
                y_copy(e, part).start()

        for part in range(3):
            own_copy(e, part).wait()
            core_copy(e, part).wait_recv()
            relay_copy(e, part).wait_recv()
        pair_store(e).start()
        result = matmul(act_ref[...], w_buf[e])
        outs = (
            (result[:, :PAIR] + bias[0, pl.ds(pair, 1), :]) * (HEAD_DIM**-0.5),
            result[:, PAIR : 2 * PAIR],
            result[:, 2 * PAIR :] + bias[1, pl.ds(pair, 1), :],
        )
        for part in range(3):
            stage[e, part] = outs[part].astype(jnp.bfloat16)

        @pl.when(e > 0)
        def _():
            for part in range(3):
                block_copy(e, part).start()

        @pl.when(e == 0)
        def _():
            for part, into in enumerate((q_out, k_out, v_out)):
                lead = lo * tok_rows + (0 if part == 0 else halo)
                into[pl.ds(pl.multiple_of(lead, 128), tok_rows), :] = outs[part].astype(
                    jnp.bfloat16
                )
            pass_on(lo)

        @pl.when(s >= GROUP // 2)
        def _():
            pass_arrived(nth(s - GROUP // 2))

    for e in (1, 6, 7):
        pass_arrived(e)

    for step in range(1, GROUP):
        code_copy(step).wait()

    def edge_copy(forward):
        low, put = (GROUP, 0) if forward else (half, half + GROUP)
        return remote(
            codes_out.at[pl.ds(low, half)],
            codes_out.at[pl.ds(put, half)],
            edge_sem.at[0, int(forward)],
            edge_sem.at[1, int(forward)],
            next_peer if forward else prev_peer,
        )

    sides = ((has_next, has_prev, True), (has_prev, has_next, False))
    for there, here, forward in sides:

        @pl.when(there)
        def _():
            edge_copy(forward).start()

    out_copy.wait()
    up_copy.wait()
    for e in range(GROUP):
        pair_store(e).wait()
    for e in range(GROUP):
        for part in range(3):
            if e % 2 == 0:
                x_copy(e, part).wait_send()
                y_copy(e, part).wait_send()
            core_copy(e, part).wait_send()
            relay_copy(e, part).wait_send()
            if e > 0:
                block_copy(e, part).wait_send()
    for there, here, forward in sides:
        sources = range(half, GROUP) if forward else range(half)

        @pl.when(there)
        def _():
            edge_copy(forward).wait_send()
            for source in sources:
                for part in range(2):
                    halo_copy(source, part, forward).wait_send()

        @pl.when(here)
        def _():
            edge_copy(forward).wait_recv()
            for source in sources:
                for part in range(2):
                    halo_copy(source, part, forward).wait_recv()


def project(replicas, tokens, small, codes, w_qkv, w_out, w_up):
    tok_rows = tokens.shape[0]
    rows = GROUP * tok_rows
    window = 2 * rows + KEYS
    low = jnp.bfloat16
    vmem = pl.BlockSpec(memory_space=pltpu.VMEM)
    anywhere = pl.BlockSpec(memory_space=pl.ANY)
    dma = pltpu.SemaphoreType.DMA
    shape = jax.ShapeDtypeStruct
    return pl.pallas_call(
        functools.partial(qkv_kernel, replicas),
        out_shape=(
            shape((tok_rows, D), low),
            shape((rows, PAIR), low),
            shape((window, PAIR), low),
            shape((window, PAIR), low),
            shape((2 * GROUP, 8, PAIR), jnp.float32),
            shape((4,) + small.shape, jnp.float32),
            shape((GROUP, D, 3 * PAIR), low),
            shape(w_out.shape, low),
            shape((w_up.shape[0] // 2, w_up.shape[1]), low),
        ),
        in_specs=[vmem] * 3 + [anywhere] * 3,
        out_specs=(vmem,) * 6 + (anywhere,) * 3,
        scratch_shapes=[
            pltpu.VMEM((GROUP, D, 3 * PAIR), low),
            pltpu.VMEM((GROUP, 3, tok_rows, PAIR), low),
            pltpu.VMEM((2, GROUP, PAIR), jnp.float32),
            dma((GROUP, 3)),
            dma((2, GROUP, 3)),
            dma((GROUP, 3)),
            dma((2, GROUP, 3)),
            dma((2, GROUP, 3)),
            dma((2, GROUP, 3)),
            dma((2, GROUP, 2)),
            dma((2, GROUP - 1)),
            dma((2, 2)),
            dma((2, 3)),
            dma((2, 2)),
            dma((GROUP,)),
        ],
        compiler_params=pltpu.CompilerParams(
            collective_id=2, has_side_effects=True, vmem_limit_bytes=67043328
        ),
        cost_estimate=pl.CostEstimate(
            flops=2 * tok_rows * D * 3 * D, transcendentals=0, bytes_accessed=60 << 20
        ),
        name="project",
    )(tokens, small, codes, w_qkv, w_out, w_up)


def low(value):
    return value.astype(jnp.bfloat16)


def high(value):
    return value.astype(jnp.float32)


def span(start, size):
    return pl.ds(pl.multiple_of(start, size), size)


def make_pipe(
    place, own, source, load, from_core, from_x, from_y, from_near, from_far, final, sem, spread=True
):
    x, c, y, z_near, z_far = place["x"], place["c"], place["y"], place["z_near"], place["z_far"]
    depth = final.shape[1]
    half, mid, short = depth // 2, depth // 4, depth // 8
    my_half = span(y * half, half)
    my_mid = span(y * half + z_near * mid, mid)
    my_short = span(y * half + z_near * mid + z_far * short, short)

    def spot(side):
        return side if own.shape[1] == 2 else side * 2 + c

    def link(k, which, here, there, peer):
        return remote(here, there, sem.at[0, k, which], sem.at[1, k, which], place[peer])

    def core_copy(k, side):
        owner = side * 2 + 1 - c
        here = own.at[k, owner] if source is None else source(k, owner)
        return link(k, side, here, from_core.at[k, side], "core")

    def load_copy(k, side):
        return pltpu.make_async_copy(
            source(k, side * 2 + c), own.at[k, side], load.at[k, side]
        )

    def x_copy(k):
        return link(k, 2, own.at[k, spot(1 - x)], from_x.at[k], "x_peer")

    def y_copy(k):
        return link(k, 3, own.at[k, spot(x), span((1 - y) * half, half)], from_y.at[k], "y_peer")

    def near_copy(k):
        away = span(y * half + (1 - z_near) * mid, mid)
        return link(k, 4, own.at[k, spot(x), away], from_near.at[k], "near")

    def far_copy(k):
        away = span(y * half + z_near * mid + (1 - z_far) * short, short)
        return link(k, 5, own.at[k, spot(x), away], from_far.at[k], "far")

    def far_join_copy(k):
        here = final.at[k, my_short]
        return link(k, 6, here, here, "far")

    def near_join_copy(k):
        here = final.at[k, my_mid]
        return link(k, 7, here, here, "near")

    def y_join_copy(k):
        here = final.at[k, my_half]
        return link(k, 8, here, here, "y_peer")

    def enter(k):
        for side in range(2):
            core_copy(k, side).start()
            if source is not None:
                load_copy(k, side).start()

    def core_sum(k):
        for side in range(2):
            if source is not None:
                load_copy(k, side).wait()
            core_copy(k, side).wait()
            own[k, spot(side)] = low(high(own[k, spot(side)]) + high(from_core[k, side]))
        x_copy(k).start()

    def x_sum(k):
        x_copy(k).wait()
        own[k, spot(x)] = low(high(own[k, spot(x)]) + high(from_x[k]))
        y_copy(k).start()

    def y_sum(k):
        y_copy(k).wait()
        own[k, spot(x), my_half] = low(high(own[k, spot(x), my_half]) + high(from_y[k]))
        near_copy(k).start()

    def near_sum(k):
        near_copy(k).wait()
        own[k, spot(x), my_mid] = low(high(own[k, spot(x), my_mid]) + high(from_near[k]))
        far_copy(k).start()

    def far_sum(k):
        far_copy(k).wait()
        final[k, my_short] = low(high(own[k, spot(x), my_short]) + high(from_far[k]))
        far_join_copy(k).start()

    def far_join(k):
        far_join_copy(k).wait()
        near_join_copy(k).start()

    def near_join(k):
        near_join_copy(k).wait()
        if spread:
            y_join_copy(k).start()

    def y_join(k):
        y_join_copy(k).wait()

    return [enter, core_sum, x_sum, y_sum, near_sum, far_sum, far_join, near_join, y_join]


def run_pipe(steps, count, now):
    for where, step in enumerate(steps):
        k = now - where * LAG

        @pl.when((k >= 0) & (k < count))
        def _():
            step(k)


def pipe_shapes(count, held, depth, width, loads):
    low_type = jnp.bfloat16
    return [
        pltpu.VMEM((count, held, depth, width), low_type),
        pltpu.VMEM((count, 2, depth, width), low_type),
        pltpu.VMEM((count, depth, width), low_type),
        pltpu.VMEM((count, depth // 2, width), low_type),
        pltpu.VMEM((count, depth // 4, width), low_type),
        pltpu.VMEM((count, depth // 8, width), low_type),
        pltpu.VMEM((count, depth, width), low_type),
        pltpu.SemaphoreType.DMA((2, count, 9)),
    ] + ([pltpu.SemaphoreType.DMA((count, 2))] if loads else [])


def find_place():
    f = lax.axis_index("fsdp")
    r = lax.axis_index("rep")
    x, c, z, y = split_index(f, r)
    lo = r % GROUP
    base = r - lo
    z_near, z_far = z % 2, z // 2
    return {
        "f": f,
        "r": r,
        "x": x,
        "c": c,
        "y": y,
        "z_near": z_near,
        "z_far": z_far,
        "lo": lo,
        "base": base,
        "core": (x * 2 + 1 - c, r),
        "x_peer": ((1 - x) * 2 + c, r),
        "y_peer": (f, base + z * 2 + 1 - y),
        "near": (f, base + (z_far * 2 + 1 - z_near) * 2 + y),
        "far": (f, base + ((1 - z_far) * 2 + z_near) * 2 + y),
        "plane": [(f, base + (lo + step) % GROUP) for step in range(1, GROUP)],
    }


def erf(value):
    return lax.erf(value)


def middle_kernel(
    o_ref,
    tokens_ref,
    grad_ref,
    vectors_ref,
    wo_own,
    wo_across,
    wu_own,
    wu_half,
    wu_other,
    wd_own,
    wd_across,
    layer_out,
    residual_out,
    grad_out,
    small_out,
    up_final,
    rest,
    wo,
    wu,
    wd,
    attn,
    act,
    act_t,
    slim,
    x1,
    proj,
    branch,
    act_grad,
    pre,
    hidden,
    slope,
    pre_grad,
    attn_grad,
    proj_grad,
    lines_ref,
    bias_ref,
    sums,
    stage,
    own,
    from_core,
    from_x,
    from_y,
    from_near,
    from_far,
    final,
    sem,
    load_sem,
    attn_sem,
    grad_sem,
    core_load_sem,
    down_sem,
    stage_sem,
):
    place = find_place()
    f, x, c, y, lo, base = (place[name] for name in ("f", "x", "c", "y", "lo", "base"))
    across = (1 - x) * 2 + c
    tok_rows = tokens_ref.shape[0]
    share = wo_own.shape[0]
    deep = wd_own.shape[0]
    sets = bias_ref.shape[0]
    tall = 128
    greet([place["core"], place["x_peer"]] + place["plane"])

    def shard_rows(owner, size):
        return span(owner * size, size)

    def attn_copy(e):
        pair = mixed_bits(lo, e)
        return remote(
            o_ref.at[span(pair * tok_rows, tok_rows), :],
            attn.at[:, span(lo * PAIR, PAIR)],
            attn_sem.at[0, e],
            attn_sem.at[1, e],
            (f, base + pair),
        )

    def grad_copy(e):
        pair = mixed_bits(lo, e)
        return remote(
            attn_grad.at[:, span(pair * PAIR, PAIR)],
            grad_out.at[span(lo * tok_rows, tok_rows), :],
            grad_sem.at[0, e],
            grad_sem.at[1, e],
            (f, base + pair),
        )

    share_half = share // 2
    lead = across * share
    moves = (
        (wo_own, wo, f * share, share),
        (wo_across, wo, lead, share),
        (wu_own, wu, f * share, share),
        (wu_half, wu, lead + y * share_half, share_half),
        (wu_other, wu, lead + (1 - y) * share_half, share_half),
        (wd_own, wd, f * deep, deep),
        (wd_across.at[: deep // 2], wd, across * deep, deep // 2),
        (wd_across.at[deep // 2 :], wd, across * deep + deep // 2 + y * (deep // 4), deep // 4),
    )

    def down_at(side):
        top = across * deep + deep // 2 + side * (deep // 4)
        return wd.at[span(top, deep // 4)]

    y_copy = remote(
        wd_across.at[deep // 2 :], down_at(y), down_sem.at[0], down_sem.at[1], place["y_peer"]
    )
    y_relay = remote(
        down_at(1 - y), down_at(1 - y), down_sem.at[2], down_sem.at[3], place["core"]
    )

    def local_copy(which):
        source, into, top, size = moves[which]
        target = into.at[pl.ds(pl.multiple_of(top, 128), size)]
        return pltpu.make_async_copy(source, target, load_sem.at[which])

    def core_copy(which):
        source, into, top, size = moves[which]
        target = into.at[pl.ds(pl.multiple_of(top, 128), size)]
        return remote(
            source, target, core_load_sem.at[0, which], core_load_sem.at[1, which], place["core"]
        )

    order = (4, 5, 6, 7, 2, 3, 1)
    for e in order:
        attn_copy(e).start()
    y_copy.start()
    for which in range(len(moves)):
        core_copy(which).start()
        local_copy(which).start()
    attn[:, span(lo * PAIR, PAIR)] = o_ref[span(lo * tok_rows, tok_rows), :]
    table = [vectors_ref[owner] for owner in range(4)]
    for which in range(6):
        lines_ref[which : which + 1, :] = jnp.concatenate(
            [rows_of[4 + which : 5 + which] for rows_of in table], axis=1
        )
    for i in range(sets):
        at, side = 10 + i // 2, i % 2 * tall
        bias_ref[i : i + 1, :] = jnp.concatenate(
            [rows_of[at : at + 1, side : side + tall] for rows_of in table], axis=1
        )
    small_out[...] = jnp.zeros_like(small_out)
    sums[...] = jnp.zeros_like(sums)
    branch[...] = jnp.zeros_like(branch)
    act_grad[...] = jnp.zeros_like(act_grad)

    def line(which):
        return lines_ref[which : which + 1, :]

    def by_rows(step, body):
        @pl.loop(0, tok_rows // step)
        def _(b):
            body(span(b * step, step))

    def scale_grad(at):
        slim[at, :] = low(line(5) * high(grad_ref[at, :]))

    by_rows(64, scale_grad)

    for e in order:
        attn_copy(e).wait_recv()
    for which in range(2):
        local_copy(which).wait()
        core_copy(which).wait_recv()
    proj[...] = matmul(attn[...], wo[...])

    def enter_mlp(at):
        value = proj[at, :] + line(0)
        proj[at, :] = value
        value = high(tokens_ref[at, :]) + line(1) * value
        x1[at, :] = value
        unit, scale = normalize(value)
        act[at, :] = low(unit * line(2) + line(3))

    by_rows(64, enter_mlp)
    act_t[...] = act[...].T
    y_copy.wait_recv()
    y_relay.start()
    for which in range(2, len(moves)):
        local_copy(which).wait()
        core_copy(which).wait_recv()
    y_relay.wait_recv()
    steps = make_pipe(
        place, own, None, None, from_core, from_x, from_y, from_near, from_far, final, sem, False
    )
    steps.pop()
    wait_near = steps.pop()

    def settle(k):
        wait_near(k)
        i, side = k // 2, k % 2
        mine = span(y * (tall // 2), tall // 2)
        for owner in range(4):
            up_final[side, :, span(owner * deep + i * tall, tall)] = final[
                k, mine, owner * tall : (owner + 1) * tall
            ]

    steps.append(settle)
    count = 2 * sets

    def stage_copy(i, part):
        return pltpu.make_async_copy(
            stage.at[i % 2, part], rest.at[2 * i + part], stage_sem.at[i % 2, part]
        )

    @pl.loop(0, sets)
    def _(i):
        columns = [span(owner * deep + i * tall, tall) for owner in range(4)]
        w_in = jnp.concatenate([wu[:, at] for at in columns], axis=1)
        w_back = jnp.concatenate([wd[at, :] for at in columns], axis=0)
        pre[...] = matmul(act[...], w_in)

        def activate(at):
            value = pre[at, :] + bias_ref[pl.ds(i, 1), :]
            cdf = 0.5 * (1.0 + erf(value * (0.5**0.5)))
            hidden[at, :] = low(value * cdf)
            slope[at, :] = cdf + value * (jnp.exp(-0.5 * value * value) * 0.3989422804014327)

        by_rows(64, activate)
        pre[...] = lax.dot_general(slim[...], w_back, NT, preferred_element_type=jnp.float32)
        branch[...] += matmul(hidden[...], w_back)

        def descend(at):
            value = pre[at, :] * slope[at, :]
            pre[at, :] = value
            pre_grad[at, :] = low(value)

        by_rows(64, descend)
        total = jnp.sum(pre[...], axis=0, keepdims=True)
        for owner in range(4):
            small_out[owner, pl.ds(20 + i, 1), :] = total[:, owner * tall : (owner + 1) * tall]
        up_grad = low(matmul(act_t[...], pre_grad[...]))
        for side in range(2):
            for owner in range(4):
                top = owner * 2 * tall + side * tall
                own[2 * i + side, owner] = up_grad[top : top + tall]
        run_pipe(steps, count, 2 * i)
        act_grad[...] += lax.dot_general(
            pre_grad[...], w_in, NT, preferred_element_type=jnp.float32
        )

        @pl.when(i >= 2)
        def _():
            for part in range(2):
                stage_copy(i - 2, part).wait()

        down_grad = low(matmul(hidden[...].T, slim[...]))
        for part in range(2):
            for owner in range(4):
                stage[i % 2, part, owner] = down_grad[
                    owner * tall : (owner + 1) * tall, part * 4 * tall : (part + 1) * 4 * tall
                ]
            stage_copy(i, part).start()
        run_pipe(steps, count, 2 * i + 1)

    def leave_mlp(at):
        grad = high(grad_ref[at, :])
        out = branch[at, :] + line(4)
        layer_out[at, :] = low(x1[at, :] + line(5) * out)
        unit, scale = normalize(x1[at, :])
        back = act_grad[at, :]
        value = grad + norm_back(back, unit, scale, line(2))
        residual_out[at, :] = value
        scaled = line(1) * value
        proj_grad[at, :] = low(scaled)
        rows = (scaled, value * proj[at, :], back * unit, back, line(5) * grad, grad * out)
        for which, member in enumerate(rows):
            sums[which : which + 1, :] += jnp.sum(member, axis=0, keepdims=True)

    by_rows(64, leave_mlp)
    attn_grad[...] = low(
        lax.dot_general(proj_grad[...], wo[...], NT, preferred_element_type=jnp.float32)
    )
    for e in order:
        grad_copy(e).start()
    grad_out[span(lo * tok_rows, tok_rows), :] = attn_grad[:, span(lo * PAIR, PAIR)]
    for which in range(6):
        for owner in range(4):
            for row in range(2):
                at = (owner * 2 + row) * PAIR
                place_row = 8 + 2 * which + row
                small_out[owner, place_row : place_row + 1, :] = sums[
                    which : which + 1, at : at + PAIR
                ]
    for i in range(sets - 2, sets):
        for part in range(2):
            stage_copy(i, part).wait()

    def out_copy(side, part):
        return pltpu.make_async_copy(
            stage.at[side, part], rest.at[count + 2 * side + part], stage_sem.at[side, part]
        )

    act_t[...] = attn[...].T
    for owner in range(4):
        part_grad = low(matmul(act_t[owner * share : (owner + 1) * share, :], proj_grad[...]))
        for side in range(2):
            for part in range(2):
                stage[side, part, owner] = part_grad[
                    side * tall : (side + 1) * tall, part * 4 * tall : (part + 1) * 4 * tall
                ]
    for side in range(2):
        for part in range(2):
            out_copy(side, part).start()

    @pl.loop(count, count + LAG * (len(steps) - 1))
    def _(now):
        run_pipe(steps, count, now)

    for side in range(2):
        for part in range(2):
            out_copy(side, part).wait()
    for e in order:
        attn_copy(e).wait_send()
        grad_copy(e).wait()
    y_copy.wait_send()
    y_relay.wait_send()
    for which in range(len(moves)):
        core_copy(which).wait_send()


def middle(mixed, tokens, out_grad, vectors, weights):
    w_out, w_up, w_down = weights[0], weights[2], weights[5]
    tok_rows = tokens.shape[0]
    rows = GROUP * tok_rows
    sets = w_down.shape[0] // 128
    count = 2 * sets
    wide = 4 * 128
    anywhere = pl.BlockSpec(memory_space=pl.ANY)
    vmem = pl.BlockSpec(memory_space=pltpu.VMEM)
    dma = pltpu.SemaphoreType.DMA
    shape = jax.ShapeDtypeStruct
    slight, full = jnp.bfloat16, jnp.float32
    return pl.pallas_call(
        middle_kernel,
        out_shape=(
            shape((tok_rows, D), slight),
            shape((tok_rows, D), full),
            shape((rows, PAIR), slight),
            shape((4, 28, PAIR), full),
            shape((2, w_up.shape[0] // 4, w_up.shape[1]), slight),
            shape((count + 4, 4, 128, wide), slight),
        ),
        in_specs=[vmem] * 4 + [anywhere] * 7,
        out_specs=(vmem,) * 5 + (anywhere,),
        scratch_shapes=[
            pltpu.VMEM((4 * w_out.shape[0], D), slight),
            pltpu.VMEM((4 * w_up.shape[0], w_up.shape[1]), slight),
            pltpu.VMEM((4 * w_down.shape[0], D), slight),
            pltpu.VMEM((tok_rows, D), slight),
            pltpu.VMEM((tok_rows, D), slight),
            pltpu.VMEM((D, tok_rows), slight),
            pltpu.VMEM((tok_rows, D), slight),
            pltpu.VMEM((tok_rows, D), full),
            pltpu.VMEM((tok_rows, D), full),
            pltpu.VMEM((tok_rows, D), full),
            pltpu.VMEM((tok_rows, D), full),
            pltpu.VMEM((tok_rows, wide), full),
            pltpu.VMEM((tok_rows, wide), slight),
            pltpu.VMEM((tok_rows, wide), full),
            pltpu.VMEM((tok_rows, wide), slight),
            pltpu.VMEM((tok_rows, D), slight),
            pltpu.VMEM((tok_rows, D), slight),
            pltpu.VMEM((8, D), full),
            pltpu.VMEM((sets, wide), full),
            pltpu.VMEM((8, D), full),
            pltpu.VMEM((2, 2, 4, 128, wide), slight),
        ]
        + pipe_shapes(count, 4, 128, wide, False)
        + [
            dma((8,)),
            dma((2, GROUP)),
            dma((2, GROUP)),
            dma((2, 8)),
            dma((4,)),
            dma((2, 2)),
        ],
        compiler_params=pltpu.CompilerParams(
            collective_id=3, has_side_effects=True, vmem_limit_bytes=67043328
        ),
        cost_estimate=pl.CostEstimate(
            flops=40 * tok_rows * D * D, transcendentals=0, bytes_accessed=100 << 20
        ),
        name="middle",
    )(mixed, tokens, out_grad, vectors, *weights)


def finish_kernel(
    replicas,
    dq_ref,
    dk_ref,
    dv_ref,
    act_ref,
    pairs_ref,
    tokens_ref,
    residual_ref,
    gain_ref,
    small_ref,
    rest_ref,
    tokens_out,
    down_final,
    out_final,
    qkv_final,
    small_final,
    own,
    from_core,
    from_x,
    from_y,
    from_near,
    from_far,
    final,
    sem,
    load_sem,
    pair_own,
    pair_core,
    pair_x,
    pair_y,
    pair_near,
    pair_far,
    pair_final,
    pair_sem,
    halos,
    stage,
    arrived,
    w_buf,
    act_t,
    act_grad,
    small_work,
    small_own,
    small_core,
    small_x,
    small_all,
    halo_sem,
    block_sem,
    w_sem,
    small_sem,
):
    place = find_place()
    f, r, x, c, lo, base = (place[name] for name in ("f", "r", "x", "c", "lo", "base"))
    core_peer, x_peer, plane = place["core"], place["x_peer"], place["plane"]
    has_next, next_peer, has_prev, prev_peer = group_neighbours(f, r, replicas)
    total = own.shape[0]
    tok_rows = act_ref.shape[0]
    rows = GROUP * tok_rows
    halo = rows // 2
    half_group = GROUP // 2
    greet([core_peer, x_peer] + plane, [(has_next, next_peer), (has_prev, prev_peer)])

    def block(ref, source, lead=0):
        return ref.at[pl.ds(pl.multiple_of(lead + source * tok_rows, 128), tok_rows), :]

    def lanes(part):
        return pl.ds(part * PAIR, PAIR)

    def halo_copy(source, part, forward):
        ref = (dk_ref, dv_ref)[part]
        return remote(
            block(ref, source, halo + rows if forward else -halo),
            block(halos.at[part], source),
            halo_sem.at[0, source, part],
            halo_sem.at[1, source, part],
            next_peer if forward else prev_peer,
        )

    def block_copy(e, part):
        source = block(dq_ref, mixed_bits(lo, e)) if part == 0 else stage.at[e, part - 1]
        return remote(
            source,
            arrived.at[e, :, lanes(part)],
            block_sem.at[0, e, part],
            block_sem.at[1, e, part],
            (f, base + mixed_bits(lo, e)),
        )

    def nth(p):
        h = p // 2
        near = jnp.where(h == 0, 2, jnp.where(h == 1, 1, jnp.where(h == 2, 3, 0)))
        return jnp.where(p % 2 == 0, 4 + h, near)

    def w_copy(p):
        spot = p % 2
        return pltpu.make_async_copy(pairs_ref.at[nth(p)], w_buf.at[spot], w_sem.at[spot])

    for there, forward in ((has_next, True), (has_prev, False)):

        @pl.when(there)
        def _():
            for i in range(half_group):
                for part in range(2):
                    halo_copy(i if forward else i + half_group, part, forward).start()

        @pl.when(jnp.logical_not(there))
        def _():
            start = halo if forward else 0
            halos[:, start : start + halo, :] = jnp.zeros((2, halo, PAIR), jnp.bfloat16)

    order = (4, 2, 5, 1, 6, 3, 7)
    for e in order:
        block_copy(e, 0).start()
    arrived[0, :, lanes(0)] = dq_ref[pl.ds(pl.multiple_of(lo * tok_rows, 128), tok_rows), :]
    small_work[...] = small_ref[...]
    act_grad[...] = jnp.zeros_like(act_grad)
    act_t[...] = act_ref[...].T
    w_copy(0).start()

    def give(p):
        e = nth(p)
        source = mixed_bits(lo, e)
        for there, forward, fits in (
            (has_next, False, source >= half_group),
            (has_prev, True, source < half_group),
        ):

            @pl.when(there & fits)
            def _():
                for part in range(2):
                    halo_copy(source, part, forward).wait_recv()

        sums = []
        for part, ref in enumerate((dk_ref, dv_ref)):
            near = ref[pl.ds(pl.multiple_of(halo + source * tok_rows, 128), tok_rows), :]
            far = halos[part, pl.ds(pl.multiple_of(source * tok_rows, 128), tok_rows), :]
            sums.append(low(high(near) + high(far)))
            stage[e, part] = sums[part]

        @pl.when(e > 0)
        def _():
            for part in range(1, 3):
                block_copy(e, part).start()

        @pl.when(e == 0)
        def _():
            for part in range(1, 3):
                arrived[0, :, lanes(part)] = sums[part - 1]

    pair_steps = make_pipe(
        place,
        pair_own,
        None,
        None,
        pair_core,
        pair_x,
        pair_y,
        pair_near,
        pair_far,
        pair_final,
        pair_sem,
    )
    pair_enter = pair_steps.pop(0)

    def take(p):
        e = nth(p)
        j = mixed_bits(lo, e)

        @pl.when(p + 1 < GROUP)
        def _():
            w_copy(p + 1).start()

        @pl.when(e > 0)
        def _():
            for part in range(3):
                block_copy(e, part).wait_recv()

        w_copy(p).wait()
        grads = arrived[e]
        pair_own[j] = low(matmul(act_t[...], grads)).reshape(4, D // 4, 3 * PAIR)
        pair_enter(j)
        act_grad[...] += lax.dot_general(
            grads, w_buf[p % 2], NT, preferred_element_type=jnp.float32
        )
        sums = jnp.sum(high(grads), axis=0, keepdims=True)
        for line, part in ((4, 0), (6, 2)):
            small_work[j // 2, pl.ds(line + j % 2, 1), :] = sums[:, part * PAIR : (part + 1) * PAIR]

    def leave():
        unit, scale = normalize(high(tokens_ref[...]))
        grad = act_grad[...]
        back = norm_back(
            grad, unit, scale, jnp.concatenate([gain_ref[owner, :1] for owner in range(4)], axis=1)
        )
        tokens_out[...] = low(residual_ref[...] + back)
        for line, values in ((0, grad * unit), (2, grad)):
            sums = jnp.sum(values, axis=0, keepdims=True)
            for owner in range(4):
                for row in range(2):
                    at = (owner * 2 + row) * PAIR
                    small_work[owner, line + row : line + row + 1, :] = sums[:, at : at + PAIR]
        for side in range(2):
            small_enter(side).start()

    steps = make_pipe(
        place,
        own,
        lambda k, owner: rest_ref.at[k, owner],
        load_sem,
        from_core,
        from_x,
        from_y,
        from_near,
        from_far,
        final,
        sem,
    )
    finish_step = steps[-1]
    tall, wide = final.shape[1:]
    downs = down_final.shape[0] // tall * 2

    def settle(k):
        finish_step(k)

        @pl.when(k < downs)
        def _():
            down_final[span((k // 2) * tall, tall), span((k % 2) * wide, wide)] = final[k]

        @pl.when(k >= downs)
        def _():
            at = k - downs
            out_final[span((at // 2) * tall, tall), span((at % 2) * wide, wide)] = final[k]

    steps[-1] = settle

    def small_enter(side):
        return remote(
            small_work.at[side * 2 + 1 - c],
            small_core.at[side],
            small_sem.at[0, side],
            small_sem.at[1, side],
            core_peer,
        )

    small_cross = remote(
        small_own.at[1 - x], small_x, small_sem.at[0, 2], small_sem.at[1, 2], x_peer
    )

    def small_spread(step):
        return remote(
            small_own.at[2],
            small_all.at[step - 1],
            small_sem.at[0, 2 + step],
            small_sem.at[1, 2 + step],
            plane[step - 1],
        )

    def small_first():
        for side in range(2):
            small_enter(side).wait()
        for side in range(2):
            small_own[side] = small_work[side * 2 + c] + small_core[side]
        small_cross.start()

    def small_second():
        small_cross.wait()
        small_own[2] = small_own[x] + small_x[...]
        for step in range(1, GROUP):
            small_spread(step).start()

    def arrive(p):
        pair_steps[0](mixed_bits(lo, nth(p)))

    def cross(p):
        pair_steps[1](mixed_bits(lo, nth(p)))

    stop = max(total + LAG * (len(steps) - 1), LAST_TAKE + 5 + GROUP // PAIR_BY + LAG * 5)

    @pl.loop(0, stop)
    def _(now):
        @pl.when((now >= GIVE_AT) & (now < GIVE_AT + GROUP))
        def _():
            give(now - GIVE_AT)

        run_pipe(steps, total, now)

        for step, lag in ((take, 0), (arrive, 2), (cross, 4)):
            gone = now - TAKE_AT - lag

            @pl.when((gone >= 0) & (gone < TAKE_BY * GROUP) & (gone % TAKE_BY == 0))
            def _():
                step(gone // TAKE_BY)

        for event, at in (
            (leave, LAST_TAKE + 1),
            (small_first, LAST_TAKE + 5),
            (small_second, LAST_TAKE + 9),
        ):
            pl.when(now == at)(event)

        for where, step in enumerate(pair_steps[2:]):
            gone = now - LAST_TAKE - 5 - LAG * where

            @pl.when((gone >= 0) & (gone < GROUP // PAIR_BY))
            def _():
                for each in range(PAIR_BY):
                    step(PAIR_BY * gone + each)

    for step in range(1, GROUP):
        small_spread(step).wait()
    value = small_own[2]
    for step in range(1, GROUP):
        value = value + small_all[step - 1]
    small_final[...] = value
    for j in range(GROUP):
        for part in range(3):
            at = part * D + j * PAIR
            qkv_final[:, at : at + PAIR] = pair_final[j, :, part * PAIR : (part + 1) * PAIR]

    for e in order:
        for part in range(3):
            block_copy(e, part).wait_send()
    for there, forward in ((has_next, True), (has_prev, False)):

        @pl.when(there)
        def _():
            for i in range(half_group):
                for part in range(2):
                    halo_copy(i if forward else i + half_group, part, forward).wait_send()


def wrap_up(replicas, moved, act, pairs, tokens, residual, gain, small, rest, shapes):
    chunks = rest.shape[0]
    tok_rows = act.shape[0]
    tall = small.shape[1]
    anywhere = pl.BlockSpec(memory_space=pl.ANY)
    vmem = pl.BlockSpec(memory_space=pltpu.VMEM)
    dma = pltpu.SemaphoreType.DMA
    low = jnp.bfloat16
    shape = jax.ShapeDtypeStruct
    pair = 3 * PAIR
    return pl.pallas_call(
        functools.partial(finish_kernel, replicas),
        out_shape=(shape((tok_rows, D), low),)
        + tuple(shape(size, low) for size in shapes)
        + (shape((D // 4, 3 * D), low), shape((tall, PAIR), jnp.float32)),
        in_specs=[vmem] * 4 + [anywhere] + [vmem] * 4 + [anywhere],
        out_specs=(vmem,) * 5,
        scratch_shapes=pipe_shapes(chunks, 2, *rest.shape[2:], True)
        + pipe_shapes(GROUP, 4, D // 4, pair, False)
        + [
            pltpu.VMEM((2, GROUP * tok_rows, PAIR), low),
            pltpu.VMEM((GROUP, 2, tok_rows, PAIR), low),
            pltpu.VMEM((GROUP, tok_rows, pair), low),
            pltpu.VMEM((2, D, pair), low),
            pltpu.VMEM((D, tok_rows), low),
            pltpu.VMEM((tok_rows, D), jnp.float32),
            pltpu.VMEM((4, tall, PAIR), jnp.float32),
            pltpu.VMEM((3, tall, PAIR), jnp.float32),
            pltpu.VMEM((2, tall, PAIR), jnp.float32),
            pltpu.VMEM((tall, PAIR), jnp.float32),
            pltpu.VMEM((GROUP - 1, tall, PAIR), jnp.float32),
            dma((2, GROUP, 2)),
            dma((2, GROUP, 3)),
            dma((2,)),
            dma((2, GROUP + 2)),
        ],
        compiler_params=pltpu.CompilerParams(
            collective_id=1, has_side_effects=True, vmem_limit_bytes=67043328
        ),
        cost_estimate=pl.CostEstimate(
            flops=12 * tok_rows * D * D, transcendentals=0, bytes_accessed=200 << 20
        ),
        name="finish",
    )(*moved, act, pairs, tokens, residual, gain, small, rest)


def shards(
    tokens,
    out_grad,
    norm1_gain,
    norm1_bias,
    w_qkv,
    q_bias,
    v_bias,
    w_out,
    out_bias,
    attn_scale,
    norm2_gain,
    norm2_bias,
    w_up,
    up_bias,
    w_down,
    down_bias,
    mlp_scale,
    image_ids,
    pad_mask,
):
    both = ("fsdp", "rep")
    owners = lax.axis_size("fsdp")
    replicas = lax.axis_size("rep")
    tok_rows = tokens.shape[0]
    rows = GROUP * tok_rows
    groups = [list(range(g, g + GROUP)) for g in range(0, replicas, GROUP)]
    factor = HEAD_DIM ** (-0.5)

    small = (
        norm1_gain,
        norm1_bias,
        q_bias,
        v_bias,
        out_bias,
        attn_scale,
        norm2_gain,
        norm2_bias,
        down_bias,
        mlp_scale,
        up_bias,
    )
    share = norm1_gain.shape[0]
    lines = list(small[:-1]) + list(up_bias.reshape(-1, share))
    line_at = lax.broadcasted_iota(jnp.int32, (-(-len(lines) // 8) * 8, share), 0)
    packed = jnp.zeros(line_at.shape, jnp.float32)
    for at, member in enumerate(lines):
        packed = jnp.where(line_at == at, member.astype(jnp.float32)[None], packed)
    codes = jnp.where(pad_mask > 0, image_ids + 1, 0).astype(jnp.float32).reshape(-1, PAIR)
    code_rows = codes.shape[0]
    codes = jnp.concatenate([codes, jnp.zeros((8 - code_rows, PAIR), jnp.float32)], axis=0)
    act_one, query, key_window, value_window, codes, vectors, w_pairs, out_across, up_half = project(
        replicas, tokens, packed, codes, w_qkv, w_out, w_up
    )
    window = key_window.shape[0]
    halo = rows // 2
    seen = codes[:, :code_rows].reshape(-1).astype(jnp.int32)
    seen = jnp.concatenate([seen, jnp.zeros((KEYS,), jnp.int32)])
    spot = jnp.arange(window, dtype=jnp.int32)
    asked = seen[halo : halo + rows]
    tile_codes = asked.reshape(rows // BLOCK, BLOCK)
    first_code = jnp.min(jnp.where(tile_codes > 0, tile_codes, 1 << 30), axis=1)
    last_code = jnp.max(tile_codes, axis=1)
    begin = jnp.min(jnp.where(seen[None] == first_code[:, None], spot[None], window), axis=1)
    finish = jnp.max(jnp.where(seen[None] == last_code[:, None], spot[None] + 1, 0), axis=1)
    begin = begin // 128 * 128
    count = jnp.where(last_code > 0, (finish - begin + KEYS - 1) // KEYS, 0)
    meta = jnp.stack([begin, count], axis=1).reshape(-1)

    lane_slot = jnp.arange(PAIR, dtype=jnp.int32) % HEAD_DIM
    key_slot = jnp.where(seen > 0, 1 + (seen - 1) % SLOTS, 0)
    marks = (key_slot[:, None] == lane_slot[None]).astype(jnp.bfloat16)


    deep = w_down.shape[0]
    side = deep // 2 + lax.axis_index("rep") % 2 * (deep // 4)
    down_most = jnp.concatenate(
        [w_down[: deep // 2], lax.dynamic_slice_in_dim(w_down, side, deep // 4, 0)], axis=0
    )
    down_late, query = lax.optimization_barrier((down_most, query))
    down_across = lax.ppermute(down_late, "fsdp", [(f, (f + 2) % 4) for f in range(4)])
    swapped = [(r, r + 1 - 2 * (r % 2)) for r in range(replicas)]
    up_other = lax.ppermute(up_half, "rep", swapped)
    attn_mine, attn_t, lse = attend(meta, query, key_window, value_window, marks)

    layer_out, residual_grad, grad_mine, packed, up_out, rest = middle(
        attn_mine,
        tokens,
        out_grad,
        vectors,
        (w_out, out_across, w_up, up_half, up_other, w_down, down_across),
    )
    up_theirs = lax.ppermute(up_out, "rep", swapped)
    dq, dk, dv = attend_back(
        meta, query, key_window, value_window, marks, grad_mine, attn_t, lse
    )
    tokens_grad, *grads, packed = wrap_up(
        replicas,
        (dq, dk, dv),
        act_one,
        w_pairs,
        tokens,
        residual_grad,
        vectors,
        packed,
        rest,
        (w_down.shape, w_out.shape),
    )
    half = jnp.arange(2).reshape(1, 2, 1, 1) == lax.axis_index("rep") % 2
    up_out = jnp.where(half, up_out[:, None], up_theirs[:, None]).reshape(w_up.shape)
    grads.insert(1, up_out)
    grads = [grad.astype(jnp.float32) for grad in grads]
    if replicas > GROUP:
        apart = [list(range(low, replicas, GROUP)) for low in range(GROUP)]
        grads = lax.psum(grads, "rep", axis_index_groups=apart)
        packed = lax.psum(packed, "rep", axis_index_groups=apart)
    packed = packed.reshape(-1)
    small_out = []
    place = 0
    for member in (norm1_gain, norm1_bias, q_bias, v_bias) + small[4:]:
        size = member.shape[0]
        small_out.append(packed[place : place + size])
        place += size

    down_out, up_out, out_out, qkv_out = grads
    return (
        layer_out,
        tokens_grad,
        small_out[0],
        small_out[1],
        qkv_out,
        small_out[2],
        small_out[3],
        out_out,
        small_out[4],
        small_out[5],
        small_out[6],
        small_out[7],
        up_out,
        small_out[10],
        down_out,
        small_out[8],
        small_out[9],
    )


def solution(mesh):
    spread = P(("fsdp", "rep"), None)
    line = P("fsdp")
    plane = P("fsdp", None)
    return jax.shard_map(
        shards,
        mesh=mesh,
        in_specs=(
            spread,
            spread,
            line,
            line,
            plane,
            line,
            line,
            plane,
            line,
            line,
            line,
            line,
            plane,
            line,
            plane,
            line,
            line,
            P(("fsdp", "rep")),
            P(("fsdp", "rep")),
        ),
        out_specs=(
            spread,
            spread,
            line,
            line,
            plane,
            line,
            line,
            plane,
            line,
            line,
            line,
            line,
            plane,
            line,
            plane,
            line,
            line,
        ),
        check_vma=False,
    )
```

```python
import functools

import jax
import jax.numpy as jnp
from jax import lax
from jax.experimental import pallas as pl
from jax.experimental.pallas import tpu as pltpu
from jax.sharding import PartitionSpec as P

D = 1024
HEADS = 16
HEAD_DIM = 64
IMG = 1370

PAIR = 2 * HEAD_DIM
GROUP = HEADS // 2
BLOCK = 256
KEYS = 1536
SLOTS = 63

EPSILON = 1e-06
NEG_BIG = -1e30
NEG_EDGE = -1e29

NT = (((1,), (1,)), ((), ()))


def from_behind(block, axis, distance):
    devices = range(lax.axis_size(axis))
    route = [(i - distance, i) for i in devices if i - distance in devices]
    return lax.ppermute(block, axis, route)


def normalize(values):
    center = jnp.mean(values, axis=-1, keepdims=True)
    centered = values - center
    spread = jnp.mean(centered * centered, axis=-1, keepdims=True)
    scale = lax.rsqrt(spread + EPSILON)
    return centered * scale, scale


def norm_back(cotangent, unit, scale, gain):
    scaled = cotangent * gain
    along = jnp.mean(scaled, axis=-1, keepdims=True)
    across = jnp.mean(scaled * unit, axis=-1, keepdims=True)
    return scale * (scaled - along - unit * across)


def matmul(left, right):
    return jnp.dot(left, right, preferred_element_type=jnp.float32)


def fold_rows(values, op):
    return op(values.reshape(values.shape[0] // 8, 8, values.shape[1]), axis=0)


def lane_marks():
    lane = lax.broadcasted_iota(jnp.int32, (BLOCK, PAIR), 1)
    return lane // HEAD_DIM, lane % HEAD_DIM > 0


def asking(query, marks, half, usable):
    wanted = jnp.where((marks.astype(jnp.float32) > 0) & usable, 0.0, NEG_BIG).astype(jnp.bfloat16)
    return [jnp.where(half == h, query, wanted) for h in range(2)]


def attend_kernel(meta, q_ref, k_ref, v_ref, m_ref, o_ref, ot_ref, lse_ref, vt, k_aug, scores):
    rows_all = o_ref.shape[0]
    tiles = rows_all // BLOCK
    window = k_ref.shape[0]
    halo = (window - KEYS - rows_all) // 2
    half, usable = lane_marks()

    @pl.loop(0, window // BLOCK)
    def _(i):
        at = pl.ds(pl.multiple_of(i * BLOCK, BLOCK), BLOCK)
        vt[:, at] = v_ref[at, :].T
        for h in range(2):
            k_aug[h, at, :] = jnp.where(half == h, k_ref[at, :], m_ref[at, :])

    @pl.loop(0, tiles)
    def _(t):
        start = meta[2 * t]
        count = meta[2 * t + 1]
        rows = pl.ds(pl.multiple_of(t * BLOCK, BLOCK), BLOCK)
        spots = pl.ds(pl.multiple_of(halo + t * BLOCK, BLOCK), BLOCK)
        query = asking(q_ref[rows, :], m_ref[spots, :], half, usable)

        def score(i, tops):
            at = pl.ds(pl.multiple_of(start + i * KEYS, 128), KEYS)
            keep = pl.ds(pl.multiple_of(i * KEYS, KEYS), KEYS)
            new = []
            for h in range(2):
                part = lax.dot_general(
                    k_aug[h, at, :], query[h], NT, preferred_element_type=jnp.float32
                )
                scores[h, keep, :] = part
                new.append(jnp.maximum(tops[h], fold_rows(part, jnp.max)))
            return tuple(new)

        low = jnp.full((8, BLOCK), NEG_BIG, jnp.float32)
        tops = lax.fori_loop(0, count, score, (low, low))
        tops = [jnp.max(top, axis=0, keepdims=True) for top in tops]
        tops = [jnp.where(top < NEG_EDGE, 0.0, top) for top in tops]

        def mix(i, carry):
            at = pl.ds(pl.multiple_of(start + i * KEYS, 128), KEYS)
            keep = pl.ds(pl.multiple_of(i * KEYS, KEYS), KEYS)
            new = []
            for h in range(2):
                total, mixed = carry[h]
                weights = jnp.exp(scores[h, keep, :] - tops[h])
                total = total + fold_rows(weights, jnp.sum)
                mixed = mixed + matmul(
                    vt[h * HEAD_DIM : (h + 1) * HEAD_DIM, at], weights.astype(jnp.bfloat16)
                )
                new.append((total, mixed))
            return tuple(new)

        zero = (jnp.zeros((8, BLOCK), jnp.float32), jnp.zeros((HEAD_DIM, BLOCK), jnp.float32))
        done = lax.fori_loop(0, count, mix, (zero, zero))
        outs = []
        for h in range(2):
            total = jnp.sum(done[h][0], axis=0, keepdims=True)
            total = jnp.where(total > 0, total, 1.0)
            lse_ref[h : h + 1, rows] = tops[h] + jnp.log(total)
            outs.append(done[h][1] / total)
        out = jnp.concatenate(outs, axis=0)
        ot_ref[:, rows] = out
        o_ref[rows, :] = out.T.astype(jnp.bfloat16)


def attend(meta, query, keys, values, marks):
    rows = query.shape[0]
    window = keys.shape[0]
    deepest = (2 * IMG + 2 * BLOCK + KEYS) // KEYS * KEYS
    vmem = pl.BlockSpec(memory_space=pltpu.VMEM)
    return pl.pallas_call(
        attend_kernel,
        out_shape=(
            jax.ShapeDtypeStruct((rows, PAIR), jnp.bfloat16),
            jax.ShapeDtypeStruct((PAIR, rows), jnp.float32),
            jax.ShapeDtypeStruct((8, rows), jnp.float32),
        ),
        in_specs=[pl.BlockSpec(memory_space=pltpu.SMEM), vmem, vmem, vmem, vmem],
        out_specs=(vmem, vmem, vmem),
        scratch_shapes=[
            pltpu.VMEM((PAIR, window), jnp.bfloat16),
            pltpu.VMEM((2, window, PAIR), jnp.bfloat16),
            pltpu.VMEM((2, deepest, BLOCK), jnp.float32),
        ],
        cost_estimate=pl.CostEstimate(
            flops=4 * rows * 2 * IMG * PAIR, transcendentals=2 * rows * IMG, bytes_accessed=9 << 20
        ),
        name="attend",
    )(meta, query, keys, values, marks)


def attend_back_kernel(
    meta, q_ref, k_ref, v_ref, m_ref, g_ref, ot_ref, lse_ref, dq_ref, dk_out, dv_out, kt, k_aug, dk_ref, dv_ref
):
    rows_all = dq_ref.shape[0]
    tiles = rows_all // BLOCK
    window = k_ref.shape[0]
    halo = (window - KEYS - rows_all) // 2
    half, usable = lane_marks()

    @pl.loop(0, window // BLOCK)
    def _(i):
        at = pl.ds(pl.multiple_of(i * BLOCK, BLOCK), BLOCK)
        kt[:, at] = k_ref[at, :].T
        for h in range(2):
            k_aug[h, at, :] = jnp.where(half == h, k_ref[at, :], m_ref[at, :])
        dk_ref[at, :] = jnp.zeros((BLOCK, PAIR), jnp.float32)
        dv_ref[at, :] = jnp.zeros((BLOCK, PAIR), jnp.float32)

    @pl.loop(0, tiles)
    def _(t):
        start = meta[2 * t]
        count = meta[2 * t + 1]
        rows = pl.ds(pl.multiple_of(t * BLOCK, BLOCK), BLOCK)
        grad = g_ref[rows, :]
        blank = jnp.zeros_like(grad)
        spots = pl.ds(pl.multiple_of(halo + t * BLOCK, BLOCK), BLOCK)
        query = asking(q_ref[rows, :], m_ref[spots, :], half, usable)
        query_only = jnp.concatenate(
            [jnp.where(half == h, query[h], blank) for h in range(2)], axis=0
        )
        grads = [jnp.where(half == h, grad, blank) for h in range(2)]
        grads_both = jnp.concatenate(grads, axis=0)
        product = grad.astype(jnp.float32).T * ot_ref[:, rows]
        delta = [
            jnp.sum(product[h * HEAD_DIM : (h + 1) * HEAD_DIM], axis=0, keepdims=True)
            for h in range(2)
        ]
        lse = [lse_ref[h : h + 1, rows] for h in range(2)]

        def step(i, carry):
            at = pl.ds(pl.multiple_of(start + i * KEYS, 128), KEYS)
            value = v_ref[at, :]
            probs, slopes, new = [], [], []
            for h in range(2):
                part = lax.dot_general(
                    k_aug[h, at, :], query[h], NT, preferred_element_type=jnp.float32
                )
                weights = jnp.exp(part - lse[h])
                pull = lax.dot_general(value, grads[h], NT, preferred_element_type=jnp.float32)
                slope = (weights * (pull - delta[h])).astype(jnp.bfloat16)
                probs.append(weights.astype(jnp.bfloat16))
                slopes.append(slope)
                new.append(carry[h] + matmul(kt[h * HEAD_DIM : (h + 1) * HEAD_DIM, at], slope))
            dv_ref[at, :] += matmul(jnp.concatenate(probs, axis=1), grads_both)
            dk_ref[at, :] += matmul(jnp.concatenate(slopes, axis=1), query_only)
            return tuple(new)

        zero = jnp.zeros((HEAD_DIM, BLOCK), jnp.float32)
        done = lax.fori_loop(0, count, step, (zero, zero))
        dq = jnp.concatenate(done, axis=0) * (HEAD_DIM**-0.5)
        dq_ref[rows, :] = dq.T.astype(jnp.bfloat16)

    @pl.loop(0, window // BLOCK)
    def _(i):
        at = pl.ds(pl.multiple_of(i * BLOCK, BLOCK), BLOCK)
        dk_out[at, :] = dk_ref[at, :].astype(jnp.bfloat16)
        dv_out[at, :] = dv_ref[at, :].astype(jnp.bfloat16)


def attend_back(meta, query, keys, values, marks, grad, out_t, lse):
    rows = query.shape[0]
    window = keys.shape[0]
    vmem = pl.BlockSpec(memory_space=pltpu.VMEM)
    return pl.pallas_call(
        attend_back_kernel,
        out_shape=(
            jax.ShapeDtypeStruct((rows, PAIR), jnp.bfloat16),
            jax.ShapeDtypeStruct((window, PAIR), jnp.bfloat16),
            jax.ShapeDtypeStruct((window, PAIR), jnp.bfloat16),
        ),
        in_specs=[pl.BlockSpec(memory_space=pltpu.SMEM)] + [vmem] * 7,
        out_specs=(vmem, vmem, vmem),
        scratch_shapes=[
            pltpu.VMEM((PAIR, window), jnp.bfloat16),
            pltpu.VMEM((2, window, PAIR), jnp.bfloat16),
            pltpu.VMEM((window, PAIR), jnp.float32),
            pltpu.VMEM((window, PAIR), jnp.float32),
        ],
        cost_estimate=pl.CostEstimate(
            flops=10 * rows * 2 * IMG * PAIR, transcendentals=2 * rows * IMG, bytes_accessed=16 << 20
        ),
        name="attend_back",
    )(meta, query, keys, values, marks, grad, out_t, lse)


CHUNK = 64
LAG = 2
GIVE_AT = 4
TAKE_AT = 20
TAKE_BY = 1
LAST_TAKE = TAKE_AT + (GROUP - 1) * TAKE_BY
PAIR_BY = 1
MESH = pl.DeviceIdType.MESH


def split_index(f, r):
    return f // 2, f % 2, (r % GROUP) // 2, r % 2


def mixed_bits(left, right):
    value = 0
    for weight in (4, 2, 1):
        value = value + weight * ((left // weight + right // weight) % 2)
    return value


def remote(source, target, send, recv, peer):
    return pltpu.make_async_remote_copy(
        src_ref=source,
        dst_ref=target,
        send_sem=send,
        recv_sem=recv,
        device_id=peer,
        device_id_type=MESH,
    )


def greet(peers, optional=()):
    barrier = pltpu.get_barrier_semaphore()
    expected = len(peers)
    for peer in peers:
        pl.semaphore_signal(barrier, inc=1, device_id=peer, device_id_type=MESH)
    for there, peer in optional:

        @pl.when(there)
        def _():
            pl.semaphore_signal(barrier, inc=1, device_id=peer, device_id_type=MESH)

        expected = expected + there.astype(jnp.int32)
    pl.semaphore_wait(barrier, expected)


def group_neighbours(f, r, replicas):
    spot = f * replicas + r
    after = lax.rem(spot + GROUP, 4 * replicas)
    before = lax.rem(spot + 3 * replicas + (replicas - GROUP), 4 * replicas)
    next_peer = (after // replicas, lax.rem(after, replicas))
    prev_peer = (before // replicas, lax.rem(before, replicas))
    return spot + GROUP < 4 * replicas, next_peer, spot >= GROUP, prev_peer


def qkv_kernel(
    replicas,
    tokens_ref,
    small_ref,
    codes_ref,
    w_ref,
    out_ref,
    up_ref,
    act_ref,
    q_out,
    k_out,
    v_out,
    codes_out,
    small_out,
    w_pairs,
    out_across,
    up_half,
    w_buf,
    stage,
    bias,
    own_sem,
    x_sem,
    y_sem,
    core_sem,
    relay_sem,
    block_sem,
    halo_sem,
    code_sem,
    edge_sem,
    small_sem,
    wide_sem,
    pair_sem,
):
    f = lax.axis_index("fsdp")
    r = lax.axis_index("rep")
    x, c, z, y = split_index(f, r)
    lo = r % GROUP
    base = r - lo
    tok_rows = tokens_ref.shape[0]
    rows = GROUP * tok_rows
    halo = (k_out.shape[0] - KEYS - rows) // 2
    half = GROUP // 2
    share = w_ref.shape[0]
    core_peer = (x * 2 + 1 - c, r)
    x_peer = ((1 - x) * 2 + c, r)
    y_peer = (f, base + z * 2 + 1 - y)
    fsdp_peers = [((f + step) % 4, r) for step in range(1, 4)]
    plane = [(f, base + (lo + step) % GROUP) for step in range(1, GROUP)]
    has_next, next_peer, has_prev, prev_peer = group_neighbours(f, r, replicas)
    greet(fsdp_peers + plane, [(has_next, next_peer), (has_prev, prev_peer)])

    def small_copy(step):
        return remote(
            small_ref,
            small_out.at[f],
            small_sem.at[0, step - 1],
            small_sem.at[1, step - 1],
            fsdp_peers[step - 1],
        )

    def lanes(part):
        return pl.ds(part * PAIR, PAIR)

    def shard_rows(owner):
        return pl.ds(pl.multiple_of(owner * share, share), share)

    def columns(part, pair):
        return w_ref.at[:, pl.ds(pl.multiple_of(part * D + pair * PAIR, PAIR), PAIR)]

    def slot(e, owner, part):
        return w_buf.at[e, shard_rows(owner), lanes(part)]

    across = (1 - x) * 2 + c
    out_copy = remote(out_ref, out_across, wide_sem.at[0, 0], wide_sem.at[1, 0], x_peer)
    up_tall = up_half.shape[0]
    up_copy = remote(
        up_ref.at[pl.ds(pl.multiple_of(y * up_tall, up_tall), up_tall)],
        up_half,
        wide_sem.at[0, 1],
        wide_sem.at[1, 1],
        x_peer,
    )

    def pair_store(e):
        return pltpu.make_async_copy(w_buf.at[e], w_pairs.at[e], pair_sem.at[e])

    def x_copy(e, part):
        pair = mixed_bits(lo, e)
        return remote(
            columns(part, pair), slot(e, f, part), x_sem.at[0, e, part], x_sem.at[1, e, part], x_peer
        )

    def y_copy(e, part):
        return remote(
            slot(e, across, part),
            slot(e + 1, across, part),
            y_sem.at[e, part],
            x_sem.at[1, e + 1, part],
            y_peer,
        )

    def arrival(e, part):
        here = slot(e, across, part)
        return remote(here, here, x_sem.at[0, e, part], x_sem.at[1, e, part], x_peer)

    def core_copy(e, part):
        pair = mixed_bits(lo, e)
        return remote(
            columns(part, pair),
            slot(e, f, part),
            core_sem.at[0, e, part],
            core_sem.at[1, e, part],
            core_peer,
        )

    def own_copy(e, part):
        pair = mixed_bits(lo, e)
        return pltpu.make_async_copy(columns(part, pair), slot(e, f, part), own_sem.at[e, part])

    def relay_copy(e, part):
        here = slot(e, across, part)
        return remote(here, here, relay_sem.at[0, e, part], relay_sem.at[1, e, part], core_peer)

    def code_copy(step):
        return remote(
            codes_ref,
            codes_out.at[half + lo],
            code_sem.at[0, step - 1],
            code_sem.at[1, step - 1],
            plane[step - 1],
        )

    order = (4, 5, 2, 3, 6, 7, 0, 1)
    for step in range(1, 4):
        small_copy(step).start()
    for e in order:
        for part in range(3):
            if e % 2 == 0:
                x_copy(e, part).start()
            core_copy(e, part).start()
            own_copy(e, part).start()
    out_copy.start()
    up_copy.start()
    for step in range(1, GROUP):
        code_copy(step).start()
    codes_out[half + lo] = codes_ref[...]

    k_out[2 * halo + rows :, :] = jnp.zeros((KEYS, PAIR), jnp.bfloat16)
    v_out[2 * halo + rows :, :] = jnp.zeros((KEYS, PAIR), jnp.bfloat16)
    for there, low, edge in ((has_prev, 0, 0), (has_next, halo + rows, half + GROUP)):

        @pl.when(jnp.logical_not(there))
        def _():
            k_out[low : low + halo, :] = jnp.zeros((halo, PAIR), jnp.bfloat16)
            v_out[low : low + halo, :] = jnp.zeros((halo, PAIR), jnp.bfloat16)
            codes_out[edge : edge + half] = jnp.zeros((half, 8, PAIR), jnp.float32)

    unit, scale = normalize(tokens_ref[...].astype(jnp.float32))
    small_out[f] = small_ref[...]
    for step in range(1, 4):
        small_copy(step).wait()
    table = [small_out[owner] for owner in range(4)]

    def vector(line):
        return jnp.concatenate([rows_of[line : line + 1] for rows_of in table], axis=1)

    for which, line in ((0, 2), (1, 3)):
        for owner in range(4):
            for side in range(2):
                bias[which, 2 * owner + side : 2 * owner + side + 1, :] = table[owner][
                    line : line + 1, side * PAIR : (side + 1) * PAIR
                ]
    act_ref[...] = (unit * vector(0) + vector(1)).astype(jnp.bfloat16)

    def block_copy(e, part):
        pair = mixed_bits(lo, e)
        into = (q_out, k_out, v_out)[part]
        lead = lo * tok_rows + (0 if part == 0 else halo)
        return remote(
            stage.at[e, part],
            into.at[pl.ds(pl.multiple_of(lead, 128), tok_rows), :],
            block_sem.at[0, e, part],
            block_sem.at[1, e, part],
            (f, base + pair),
        )

    def nth(s):
        return jnp.where(s < 2, s + 4, jnp.where(s < 4, s, jnp.where(s < 6, s + 2, s - 6)))

    def halo_copy(source, part, forward):
        into = (k_out, v_out)[part]
        lead = source * tok_rows
        put = lead + halo - rows if forward else lead + halo + rows
        return remote(
            into.at[pl.ds(pl.multiple_of(halo + lead, 128), tok_rows), :],
            into.at[pl.ds(pl.multiple_of(put, 128), tok_rows), :],
            halo_sem.at[0, source, part],
            halo_sem.at[1, source, part],
            next_peer if forward else prev_peer,
        )

    def pass_on(source):
        for there, forward, fits in (
            (has_next, True, source >= half),
            (has_prev, False, source < half),
        ):

            @pl.when(there & fits)
            def _():
                for part in range(2):
                    halo_copy(source, part, forward).start()

    def pass_arrived(e):
        for part in range(3):
            block_copy(e, part).wait_recv()
        pass_on(mixed_bits(lo, e))

    @pl.loop(0, GROUP)
    def _(s):
        e = nth(s)
        pair = mixed_bits(lo, e)
        for part in range(3):
            arrival(e, part).wait_recv()
            relay_copy(e, part).start()

        @pl.when(e % 2 == 0)
        def _():
            for part in range(3):
                y_copy(e, part).start()

        for part in range(3):
            own_copy(e, part).wait()
            core_copy(e, part).wait_recv()
            relay_copy(e, part).wait_recv()
        pair_store(e).start()
        result = matmul(act_ref[...], w_buf[e])
        outs = (
            (result[:, :PAIR] + bias[0, pl.ds(pair, 1), :]) * (HEAD_DIM**-0.5),
            result[:, PAIR : 2 * PAIR],
            result[:, 2 * PAIR :] + bias[1, pl.ds(pair, 1), :],
        )
        for part in range(3):
            stage[e, part] = outs[part].astype(jnp.bfloat16)

        @pl.when(e > 0)
        def _():
            for part in range(3):
                block_copy(e, part).start()

        @pl.when(e == 0)
        def _():
            for part, into in enumerate((q_out, k_out, v_out)):
                lead = lo * tok_rows + (0 if part == 0 else halo)
                into[pl.ds(pl.multiple_of(lead, 128), tok_rows), :] = outs[part].astype(
                    jnp.bfloat16
                )
            pass_on(lo)

        @pl.when(s >= GROUP // 2)
        def _():
            pass_arrived(nth(s - GROUP // 2))

    for e in (1, 6, 7):
        pass_arrived(e)

    for step in range(1, GROUP):
        code_copy(step).wait()

    def edge_copy(forward):
        low, put = (GROUP, 0) if forward else (half, half + GROUP)
        return remote(
            codes_out.at[pl.ds(low, half)],
            codes_out.at[pl.ds(put, half)],
            edge_sem.at[0, int(forward)],
            edge_sem.at[1, int(forward)],
            next_peer if forward else prev_peer,
        )

    sides = ((has_next, has_prev, True), (has_prev, has_next, False))
    for there, here, forward in sides:

        @pl.when(there)
        def _():
            edge_copy(forward).start()

    out_copy.wait()
    up_copy.wait()
    for e in range(GROUP):
        pair_store(e).wait()
    for e in range(GROUP):
        for part in range(3):
            if e % 2 == 0:
                x_copy(e, part).wait_send()
                y_copy(e, part).wait_send()
            core_copy(e, part).wait_send()
            relay_copy(e, part).wait_send()
            if e > 0:
                block_copy(e, part).wait_send()
    for there, here, forward in sides:
        sources = range(half, GROUP) if forward else range(half)

        @pl.when(there)
        def _():
            edge_copy(forward).wait_send()
            for source in sources:
                for part in range(2):
                    halo_copy(source, part, forward).wait_send()

        @pl.when(here)
        def _():
            edge_copy(forward).wait_recv()
            for source in sources:
                for part in range(2):
                    halo_copy(source, part, forward).wait_recv()


def project(replicas, tokens, small, codes, w_qkv, w_out, w_up):
    tok_rows = tokens.shape[0]
    rows = GROUP * tok_rows
    window = 2 * rows + KEYS
    low = jnp.bfloat16
    vmem = pl.BlockSpec(memory_space=pltpu.VMEM)
    anywhere = pl.BlockSpec(memory_space=pl.ANY)
    dma = pltpu.SemaphoreType.DMA
    shape = jax.ShapeDtypeStruct
    return pl.pallas_call(
        functools.partial(qkv_kernel, replicas),
        out_shape=(
            shape((tok_rows, D), low),
            shape((rows, PAIR), low),
            shape((window, PAIR), low),
            shape((window, PAIR), low),
            shape((2 * GROUP, 8, PAIR), jnp.float32),
            shape((4,) + small.shape, jnp.float32),
            shape((GROUP, D, 3 * PAIR), low),
            shape(w_out.shape, low),
            shape((w_up.shape[0] // 2, w_up.shape[1]), low),
        ),
        in_specs=[vmem] * 3 + [anywhere] * 3,
        out_specs=(vmem,) * 6 + (anywhere,) * 3,
        scratch_shapes=[
            pltpu.VMEM((GROUP, D, 3 * PAIR), low),
            pltpu.VMEM((GROUP, 3, tok_rows, PAIR), low),
            pltpu.VMEM((2, GROUP, PAIR), jnp.float32),
            dma((GROUP, 3)),
            dma((2, GROUP, 3)),
            dma((GROUP, 3)),
            dma((2, GROUP, 3)),
            dma((2, GROUP, 3)),
            dma((2, GROUP, 3)),
            dma((2, GROUP, 2)),
            dma((2, GROUP - 1)),
            dma((2, 2)),
            dma((2, 3)),
            dma((2, 2)),
            dma((GROUP,)),
        ],
        compiler_params=pltpu.CompilerParams(
            collective_id=2, has_side_effects=True, vmem_limit_bytes=67043328
        ),
        cost_estimate=pl.CostEstimate(
            flops=2 * tok_rows * D * 3 * D, transcendentals=0, bytes_accessed=60 << 20
        ),
        name="project",
    )(tokens, small, codes, w_qkv, w_out, w_up)


def low(value):
    return value.astype(jnp.bfloat16)


def high(value):
    return value.astype(jnp.float32)


def span(start, size):
    return pl.ds(pl.multiple_of(start, size), size)


def make_pipe(
    place, own, source, load, from_core, from_x, from_y, from_near, from_far, final, sem, spread=True
):
    x, c, y, z_near, z_far = place["x"], place["c"], place["y"], place["z_near"], place["z_far"]
    depth = final.shape[1]
    half, mid, short = depth // 2, depth // 4, depth // 8
    my_half = span(y * half, half)
    my_mid = span(y * half + z_near * mid, mid)
    my_short = span(y * half + z_near * mid + z_far * short, short)

    def spot(side):
        return side if own.shape[1] == 2 else side * 2 + c

    def link(k, which, here, there, peer):
        return remote(here, there, sem.at[0, k, which], sem.at[1, k, which], place[peer])

    def core_copy(k, side):
        owner = side * 2 + 1 - c
        here = own.at[k, owner] if source is None else source(k, owner)
        return link(k, side, here, from_core.at[k, side], "core")

    def load_copy(k, side):
        return pltpu.make_async_copy(
            source(k, side * 2 + c), own.at[k, side], load.at[k, side]
        )

    def x_copy(k):
        return link(k, 2, own.at[k, spot(1 - x)], from_x.at[k], "x_peer")

    def y_copy(k):
        return link(k, 3, own.at[k, spot(x), span((1 - y) * half, half)], from_y.at[k], "y_peer")

    def near_copy(k):
        away = span(y * half + (1 - z_near) * mid, mid)
        return link(k, 4, own.at[k, spot(x), away], from_near.at[k], "near")

    def far_copy(k):
        away = span(y * half + z_near * mid + (1 - z_far) * short, short)
        return link(k, 5, own.at[k, spot(x), away], from_far.at[k], "far")

    def far_join_copy(k):
        here = final.at[k, my_short]
        return link(k, 6, here, here, "far")

    def near_join_copy(k):
        here = final.at[k, my_mid]
        return link(k, 7, here, here, "near")

    def y_join_copy(k):
        here = final.at[k, my_half]
        return link(k, 8, here, here, "y_peer")

    def enter(k):
        for side in range(2):
            core_copy(k, side).start()
            if source is not None:
                load_copy(k, side).start()

    def core_sum(k):
        for side in range(2):
            if source is not None:
                load_copy(k, side).wait()
            core_copy(k, side).wait()
            own[k, spot(side)] = low(high(own[k, spot(side)]) + high(from_core[k, side]))
        x_copy(k).start()

    def x_sum(k):
        x_copy(k).wait()
        own[k, spot(x)] = low(high(own[k, spot(x)]) + high(from_x[k]))
        y_copy(k).start()

    def y_sum(k):
        y_copy(k).wait()
        own[k, spot(x), my_half] = low(high(own[k, spot(x), my_half]) + high(from_y[k]))
        near_copy(k).start()

    def near_sum(k):
        near_copy(k).wait()
        own[k, spot(x), my_mid] = low(high(own[k, spot(x), my_mid]) + high(from_near[k]))
        far_copy(k).start()

    def far_sum(k):
        far_copy(k).wait()
        final[k, my_short] = low(high(own[k, spot(x), my_short]) + high(from_far[k]))
        far_join_copy(k).start()

    def far_join(k):
        far_join_copy(k).wait()
        near_join_copy(k).start()

    def near_join(k):
        near_join_copy(k).wait()
        if spread:
            y_join_copy(k).start()

    def y_join(k):
        y_join_copy(k).wait()

    return [enter, core_sum, x_sum, y_sum, near_sum, far_sum, far_join, near_join, y_join]


def run_pipe(steps, count, now):
    for where, step in enumerate(steps):
        k = now - where * LAG

        @pl.when((k >= 0) & (k < count))
        def _():
            step(k)


def pipe_shapes(count, held, depth, width, loads):
    low_type = jnp.bfloat16
    return [
        pltpu.VMEM((count, held, depth, width), low_type),
        pltpu.VMEM((count, 2, depth, width), low_type),
        pltpu.VMEM((count, depth, width), low_type),
        pltpu.VMEM((count, depth // 2, width), low_type),
        pltpu.VMEM((count, depth // 4, width), low_type),
        pltpu.VMEM((count, depth // 8, width), low_type),
        pltpu.VMEM((count, depth, width), low_type),
        pltpu.SemaphoreType.DMA((2, count, 9)),
    ] + ([pltpu.SemaphoreType.DMA((count, 2))] if loads else [])


def find_place():
    f = lax.axis_index("fsdp")
    r = lax.axis_index("rep")
    x, c, z, y = split_index(f, r)
    lo = r % GROUP
    base = r - lo
    z_near, z_far = z % 2, z // 2
    return {
        "f": f,
        "r": r,
        "x": x,
        "c": c,
        "y": y,
        "z_near": z_near,
        "z_far": z_far,
        "lo": lo,
        "base": base,
        "core": (x * 2 + 1 - c, r),
        "x_peer": ((1 - x) * 2 + c, r),
        "y_peer": (f, base + z * 2 + 1 - y),
        "near": (f, base + (z_far * 2 + 1 - z_near) * 2 + y),
        "far": (f, base + ((1 - z_far) * 2 + z_near) * 2 + y),
        "plane": [(f, base + (lo + step) % GROUP) for step in range(1, GROUP)],
    }


def erf(value):
    return lax.erf(value)


def middle_kernel(
    o_ref,
    tokens_ref,
    grad_ref,
    vectors_ref,
    wo_own,
    wo_across,
    wu_own,
    wu_half,
    wu_other,
    wd_own,
    wd_across,
    layer_out,
    residual_out,
    grad_out,
    small_out,
    up_final,
    rest,
    wo,
    wu,
    wd,
    attn,
    act,
    act_t,
    slim,
    x1,
    proj,
    branch,
    act_grad,
    pre,
    hidden,
    slope,
    pre_grad,
    attn_grad,
    proj_grad,
    lines_ref,
    bias_ref,
    sums,
    stage,
    own,
    from_core,
    from_x,
    from_y,
    from_near,
    from_far,
    final,
    sem,
    load_sem,
    attn_sem,
    grad_sem,
    core_load_sem,
    down_sem,
    stage_sem,
):
    place = find_place()
    f, x, c, y, lo, base = (place[name] for name in ("f", "x", "c", "y", "lo", "base"))
    across = (1 - x) * 2 + c
    tok_rows = tokens_ref.shape[0]
    share = wo_own.shape[0]
    deep = wd_own.shape[0]
    sets = bias_ref.shape[0]
    tall = 128
    greet([place["core"], place["x_peer"]] + place["plane"])

    def shard_rows(owner, size):
        return span(owner * size, size)

    def attn_copy(e):
        pair = mixed_bits(lo, e)
        return remote(
            o_ref.at[span(pair * tok_rows, tok_rows), :],
            attn.at[:, span(lo * PAIR, PAIR)],
            attn_sem.at[0, e],
            attn_sem.at[1, e],
            (f, base + pair),
        )

    def grad_copy(e):
        pair = mixed_bits(lo, e)
        return remote(
            attn_grad.at[:, span(pair * PAIR, PAIR)],
            grad_out.at[span(lo * tok_rows, tok_rows), :],
            grad_sem.at[0, e],
            grad_sem.at[1, e],
            (f, base + pair),
        )

    share_half = share // 2
    lead = across * share
    moves = (
        (wo_own, wo, f * share, share),
        (wo_across, wo, lead, share),
        (wu_own, wu, f * share, share),
        (wu_half, wu, lead + y * share_half, share_half),
        (wu_other, wu, lead + (1 - y) * share_half, share_half),
        (wd_own, wd, f * deep, deep),
        (wd_across.at[: deep // 2], wd, across * deep, deep // 2),
        (wd_across.at[deep // 2 :], wd, across * deep + deep // 2 + y * (deep // 4), deep // 4),
    )

    def down_at(side):
        top = across * deep + deep // 2 + side * (deep // 4)
        return wd.at[span(top, deep // 4)]

    y_copy = remote(
        wd_across.at[deep // 2 :], down_at(y), down_sem.at[0], down_sem.at[1], place["y_peer"]
    )
    y_relay = remote(
        down_at(1 - y), down_at(1 - y), down_sem.at[2], down_sem.at[3], place["core"]
    )

    def local_copy(which):
        source, into, top, size = moves[which]
        target = into.at[pl.ds(pl.multiple_of(top, 128), size)]
        return pltpu.make_async_copy(source, target, load_sem.at[which])

    def core_copy(which):
        source, into, top, size = moves[which]
        target = into.at[pl.ds(pl.multiple_of(top, 128), size)]
        return remote(
            source, target, core_load_sem.at[0, which], core_load_sem.at[1, which], place["core"]
        )

    order = (4, 5, 6, 7, 2, 3, 1)
    for e in order:
        attn_copy(e).start()
    y_copy.start()
    for which in range(len(moves)):
        core_copy(which).start()
        local_copy(which).start()
    attn[:, span(lo * PAIR, PAIR)] = o_ref[span(lo * tok_rows, tok_rows), :]
    table = [vectors_ref[owner] for owner in range(4)]
    for which in range(6):
        lines_ref[which : which + 1, :] = jnp.concatenate(
            [rows_of[4 + which : 5 + which] for rows_of in table], axis=1
        )
    for i in range(sets):
        at, side = 10 + i // 2, i % 2 * tall
        bias_ref[i : i + 1, :] = jnp.concatenate(
            [rows_of[at : at + 1, side : side + tall] for rows_of in table], axis=1
        )
    small_out[...] = jnp.zeros_like(small_out)
    sums[...] = jnp.zeros_like(sums)
    branch[...] = jnp.zeros_like(branch)
    act_grad[...] = jnp.zeros_like(act_grad)

    def line(which):
        return lines_ref[which : which + 1, :]

    def by_rows(step, body):
        @pl.loop(0, tok_rows // step)
        def _(b):
            body(span(b * step, step))

    def scale_grad(at):
        slim[at, :] = low(line(5) * high(grad_ref[at, :]))

    by_rows(64, scale_grad)

    for e in order:
        attn_copy(e).wait_recv()
    for which in range(2):
        local_copy(which).wait()
        core_copy(which).wait_recv()
    proj[...] = matmul(attn[...], wo[...])

    def enter_mlp(at):
        value = proj[at, :] + line(0)
        proj[at, :] = value
        value = high(tokens_ref[at, :]) + line(1) * value
        x1[at, :] = value
        unit, scale = normalize(value)
        act[at, :] = low(unit * line(2) + line(3))

    by_rows(64, enter_mlp)
    act_t[...] = act[...].T
    y_copy.wait_recv()
    y_relay.start()
    for which in range(2, len(moves)):
        local_copy(which).wait()
        core_copy(which).wait_recv()
    y_relay.wait_recv()
    steps = make_pipe(
        place, own, None, None, from_core, from_x, from_y, from_near, from_far, final, sem, False
    )
    steps.pop()
    wait_near = steps.pop()

    def settle(k):
        wait_near(k)
        i, side = k // 2, k % 2
        mine = span(y * (tall // 2), tall // 2)
        for owner in range(4):
            up_final[side, :, span(owner * deep + i * tall, tall)] = final[
                k, mine, owner * tall : (owner + 1) * tall
            ]

    steps.append(settle)
    count = 2 * sets

    def stage_copy(i, part):
        return pltpu.make_async_copy(
            stage.at[i % 2, part], rest.at[2 * i + part], stage_sem.at[i % 2, part]
        )

    @pl.loop(0, sets)
    def _(i):
        columns = [span(owner * deep + i * tall, tall) for owner in range(4)]
        w_in = jnp.concatenate([wu[:, at] for at in columns], axis=1)
        w_back = jnp.concatenate([wd[at, :] for at in columns], axis=0)
        pre[...] = matmul(act[...], w_in)

        def activate(at):
            value = pre[at, :] + bias_ref[pl.ds(i, 1), :]
            cdf = 0.5 * (1.0 + erf(value * (0.5**0.5)))
            hidden[at, :] = low(value * cdf)
            slope[at, :] = cdf + value * (jnp.exp(-0.5 * value * value) * 0.3989422804014327)

        by_rows(64, activate)
        pre[...] = lax.dot_general(slim[...], w_back, NT, preferred_element_type=jnp.float32)
        branch[...] += matmul(hidden[...], w_back)

        def descend(at):
            value = pre[at, :] * slope[at, :]
            pre[at, :] = value
            pre_grad[at, :] = low(value)

        by_rows(64, descend)
        total = jnp.sum(pre[...], axis=0, keepdims=True)
        for owner in range(4):
            small_out[owner, pl.ds(20 + i, 1), :] = total[:, owner * tall : (owner + 1) * tall]
        up_grad = low(matmul(act_t[...], pre_grad[...]))
        for side in range(2):
            for owner in range(4):
                top = owner * 2 * tall + side * tall
                own[2 * i + side, owner] = up_grad[top : top + tall]
        run_pipe(steps, count, 2 * i)
        act_grad[...] += lax.dot_general(
            pre_grad[...], w_in, NT, preferred_element_type=jnp.float32
        )

        @pl.when(i >= 2)
        def _():
            for part in range(2):
                stage_copy(i - 2, part).wait()

        down_grad = low(matmul(hidden[...].T, slim[...]))
        for part in range(2):
            for owner in range(4):
                stage[i % 2, part, owner] = down_grad[
                    owner * tall : (owner + 1) * tall, part * 4 * tall : (part + 1) * 4 * tall
                ]
            stage_copy(i, part).start()
        run_pipe(steps, count, 2 * i + 1)

    def leave_mlp(at):
        grad = high(grad_ref[at, :])
        out = branch[at, :] + line(4)
        layer_out[at, :] = low(x1[at, :] + line(5) * out)
        unit, scale = normalize(x1[at, :])
        back = act_grad[at, :]
        value = grad + norm_back(back, unit, scale, line(2))
        residual_out[at, :] = value
        scaled = line(1) * value
        proj_grad[at, :] = low(scaled)
        rows = (scaled, value * proj[at, :], back * unit, back, line(5) * grad, grad * out)
        for which, member in enumerate(rows):
            sums[which : which + 1, :] += jnp.sum(member, axis=0, keepdims=True)

    by_rows(64, leave_mlp)
    attn_grad[...] = low(
        lax.dot_general(proj_grad[...], wo[...], NT, preferred_element_type=jnp.float32)
    )
    for e in order:
        grad_copy(e).start()
    grad_out[span(lo * tok_rows, tok_rows), :] = attn_grad[:, span(lo * PAIR, PAIR)]
    for which in range(6):
        for owner in range(4):
            for row in range(2):
                at = (owner * 2 + row) * PAIR
                place_row = 8 + 2 * which + row
                small_out[owner, place_row : place_row + 1, :] = sums[
                    which : which + 1, at : at + PAIR
                ]
    for i in range(sets - 2, sets):
        for part in range(2):
            stage_copy(i, part).wait()

    def out_copy(side, part):
        return pltpu.make_async_copy(
            stage.at[side, part], rest.at[count + 2 * side + part], stage_sem.at[side, part]
        )

    act_t[...] = attn[...].T
    for owner in range(4):
        part_grad = low(matmul(act_t[owner * share : (owner + 1) * share, :], proj_grad[...]))
        for side in range(2):
            for part in range(2):
                stage[side, part, owner] = part_grad[
                    side * tall : (side + 1) * tall, part * 4 * tall : (part + 1) * 4 * tall
                ]
    for side in range(2):
        for part in range(2):
            out_copy(side, part).start()

    @pl.loop(count, count + LAG * (len(steps) - 1))
    def _(now):
        run_pipe(steps, count, now)

    for side in range(2):
        for part in range(2):
            out_copy(side, part).wait()
    for e in order:
        attn_copy(e).wait_send()
        grad_copy(e).wait()
    y_copy.wait_send()
    y_relay.wait_send()
    for which in range(len(moves)):
        core_copy(which).wait_send()


def middle(mixed, tokens, out_grad, vectors, weights):
    w_out, w_up, w_down = weights[0], weights[2], weights[5]
    tok_rows = tokens.shape[0]
    rows = GROUP * tok_rows
    sets = w_down.shape[0] // 128
    count = 2 * sets
    wide = 4 * 128
    anywhere = pl.BlockSpec(memory_space=pl.ANY)
    vmem = pl.BlockSpec(memory_space=pltpu.VMEM)
    dma = pltpu.SemaphoreType.DMA
    shape = jax.ShapeDtypeStruct
    slight, full = jnp.bfloat16, jnp.float32
    return pl.pallas_call(
        middle_kernel,
        out_shape=(
            shape((tok_rows, D), slight),
            shape((tok_rows, D), full),
            shape((rows, PAIR), slight),
            shape((4, 28, PAIR), full),
            shape((2, w_up.shape[0] // 4, w_up.shape[1]), slight),
            shape((count + 4, 4, 128, wide), slight),
        ),
        in_specs=[vmem] * 4 + [anywhere] * 7,
        out_specs=(vmem,) * 5 + (anywhere,),
        scratch_shapes=[
            pltpu.VMEM((4 * w_out.shape[0], D), slight),
            pltpu.VMEM((4 * w_up.shape[0], w_up.shape[1]), slight),
            pltpu.VMEM((4 * w_down.shape[0], D), slight),
            pltpu.VMEM((tok_rows, D), slight),
            pltpu.VMEM((tok_rows, D), slight),
            pltpu.VMEM((D, tok_rows), slight),
            pltpu.VMEM((tok_rows, D), slight),
            pltpu.VMEM((tok_rows, D), full),
            pltpu.VMEM((tok_rows, D), full),
            pltpu.VMEM((tok_rows, D), full),
            pltpu.VMEM((tok_rows, D), full),
            pltpu.VMEM((tok_rows, wide), full),
            pltpu.VMEM((tok_rows, wide), slight),
            pltpu.VMEM((tok_rows, wide), full),
            pltpu.VMEM((tok_rows, wide), slight),
            pltpu.VMEM((tok_rows, D), slight),
            pltpu.VMEM((tok_rows, D), slight),
            pltpu.VMEM((8, D), full),
            pltpu.VMEM((sets, wide), full),
            pltpu.VMEM((8, D), full),
            pltpu.VMEM((2, 2, 4, 128, wide), slight),
        ]
        + pipe_shapes(count, 4, 128, wide, False)
        + [
            dma((8,)),
            dma((2, GROUP)),
            dma((2, GROUP)),
            dma((2, 8)),
            dma((4,)),
            dma((2, 2)),
        ],
        compiler_params=pltpu.CompilerParams(
            collective_id=3, has_side_effects=True, vmem_limit_bytes=67043328
        ),
        cost_estimate=pl.CostEstimate(
            flops=40 * tok_rows * D * D, transcendentals=0, bytes_accessed=100 << 20
        ),
        name="middle",
    )(mixed, tokens, out_grad, vectors, *weights)


def finish_kernel(
    replicas,
    dq_ref,
    dk_ref,
    dv_ref,
    act_ref,
    pairs_ref,
    tokens_ref,
    residual_ref,
    gain_ref,
    small_ref,
    rest_ref,
    tokens_out,
    down_final,
    out_final,
    qkv_final,
    small_final,
    own,
    from_core,
    from_x,
    from_y,
    from_near,
    from_far,
    final,
    sem,
    load_sem,
    pair_own,
    pair_core,
    pair_x,
    pair_y,
    pair_near,
    pair_far,
    pair_final,
    pair_sem,
    halos,
    stage,
    arrived,
    w_buf,
    act_t,
    act_grad,
    small_work,
    small_own,
    small_core,
    small_x,
    small_all,
    halo_sem,
    block_sem,
    w_sem,
    small_sem,
):
    place = find_place()
    f, r, x, c, lo, base = (place[name] for name in ("f", "r", "x", "c", "lo", "base"))
    core_peer, x_peer, plane = place["core"], place["x_peer"], place["plane"]
    has_next, next_peer, has_prev, prev_peer = group_neighbours(f, r, replicas)
    total = own.shape[0]
    tok_rows = act_ref.shape[0]
    rows = GROUP * tok_rows
    halo = rows // 2
    half_group = GROUP // 2
    greet([core_peer, x_peer] + plane, [(has_next, next_peer), (has_prev, prev_peer)])

    def block(ref, source, lead=0):
        return ref.at[pl.ds(pl.multiple_of(lead + source * tok_rows, 128), tok_rows), :]

    def lanes(part):
        return pl.ds(part * PAIR, PAIR)

    def halo_copy(source, part, forward):
        ref = (dk_ref, dv_ref)[part]
        return remote(
            block(ref, source, halo + rows if forward else -halo),
            block(halos.at[part], source),
            halo_sem.at[0, source, part],
            halo_sem.at[1, source, part],
            next_peer if forward else prev_peer,
        )

    def block_copy(e, part):
        source = block(dq_ref, mixed_bits(lo, e)) if part == 0 else stage.at[e, part - 1]
        return remote(
            source,
            arrived.at[e, :, lanes(part)],
            block_sem.at[0, e, part],
            block_sem.at[1, e, part],
            (f, base + mixed_bits(lo, e)),
        )

    def nth(p):
        h = p // 2
        near = jnp.where(h == 0, 2, jnp.where(h == 1, 1, jnp.where(h == 2, 3, 0)))
        return jnp.where(p % 2 == 0, 4 + h, near)

    def w_copy(p):
        spot = p % 2
        return pltpu.make_async_copy(pairs_ref.at[nth(p)], w_buf.at[spot], w_sem.at[spot])

    for there, forward in ((has_next, True), (has_prev, False)):

        @pl.when(there)
        def _():
            for i in range(half_group):
                for part in range(2):
                    halo_copy(i if forward else i + half_group, part, forward).start()

        @pl.when(jnp.logical_not(there))
        def _():
            start = halo if forward else 0
            halos[:, start : start + halo, :] = jnp.zeros((2, halo, PAIR), jnp.bfloat16)

    order = (4, 2, 5, 1, 6, 3, 7)
    for e in order:
        block_copy(e, 0).start()
    arrived[0, :, lanes(0)] = dq_ref[pl.ds(pl.multiple_of(lo * tok_rows, 128), tok_rows), :]
    small_work[...] = small_ref[...]
    act_grad[...] = jnp.zeros_like(act_grad)
    act_t[...] = act_ref[...].T
    w_copy(0).start()

    def give(p):
        e = nth(p)
        source = mixed_bits(lo, e)
        for there, forward, fits in (
            (has_next, False, source >= half_group),
            (has_prev, True, source < half_group),
        ):

            @pl.when(there & fits)
            def _():
                for part in range(2):
                    halo_copy(source, part, forward).wait_recv()

        sums = []
        for part, ref in enumerate((dk_ref, dv_ref)):
            near = ref[pl.ds(pl.multiple_of(halo + source * tok_rows, 128), tok_rows), :]
            far = halos[part, pl.ds(pl.multiple_of(source * tok_rows, 128), tok_rows), :]
            sums.append(low(high(near) + high(far)))
            stage[e, part] = sums[part]

        @pl.when(e > 0)
        def _():
            for part in range(1, 3):
                block_copy(e, part).start()

        @pl.when(e == 0)
        def _():
            for part in range(1, 3):
                arrived[0, :, lanes(part)] = sums[part - 1]

    pair_steps = make_pipe(
        place,
        pair_own,
        None,
        None,
        pair_core,
        pair_x,
        pair_y,
        pair_near,
        pair_far,
        pair_final,
        pair_sem,
    )
    pair_enter = pair_steps.pop(0)

    def take(p):
        e = nth(p)
        j = mixed_bits(lo, e)

        @pl.when(p + 1 < GROUP)
        def _():
            w_copy(p + 1).start()

        @pl.when(e > 0)
        def _():
            for part in range(3):
                block_copy(e, part).wait_recv()

        w_copy(p).wait()
        grads = arrived[e]
        pair_own[j] = low(matmul(act_t[...], grads)).reshape(4, D // 4, 3 * PAIR)
        pair_enter(j)
        act_grad[...] += lax.dot_general(
            grads, w_buf[p % 2], NT, preferred_element_type=jnp.float32
        )
        sums = jnp.sum(high(grads), axis=0, keepdims=True)
        for line, part in ((4, 0), (6, 2)):
            small_work[j // 2, pl.ds(line + j % 2, 1), :] = sums[:, part * PAIR : (part + 1) * PAIR]

    def leave():
        unit, scale = normalize(high(tokens_ref[...]))
        grad = act_grad[...]
        back = norm_back(
            grad, unit, scale, jnp.concatenate([gain_ref[owner, :1] for owner in range(4)], axis=1)
        )
        tokens_out[...] = low(residual_ref[...] + back)
        for line, values in ((0, grad * unit), (2, grad)):
            sums = jnp.sum(values, axis=0, keepdims=True)
            for owner in range(4):
                for row in range(2):
                    at = (owner * 2 + row) * PAIR
                    small_work[owner, line + row : line + row + 1, :] = sums[:, at : at + PAIR]
        for side in range(2):
            small_enter(side).start()

    steps = make_pipe(
        place,
        own,
        lambda k, owner: rest_ref.at[k, owner],
        load_sem,
        from_core,
        from_x,
        from_y,
        from_near,
        from_far,
        final,
        sem,
    )
    finish_step = steps[-1]
    tall, wide = final.shape[1:]
    downs = down_final.shape[0] // tall * 2

    def settle(k):
        finish_step(k)

        @pl.when(k < downs)
        def _():
            down_final[span((k // 2) * tall, tall), span((k % 2) * wide, wide)] = final[k]

        @pl.when(k >= downs)
        def _():
            at = k - downs
            out_final[span((at // 2) * tall, tall), span((at % 2) * wide, wide)] = final[k]

    steps[-1] = settle

    def small_enter(side):
        return remote(
            small_work.at[side * 2 + 1 - c],
            small_core.at[side],
            small_sem.at[0, side],
            small_sem.at[1, side],
            core_peer,
        )

    small_cross = remote(
        small_own.at[1 - x], small_x, small_sem.at[0, 2], small_sem.at[1, 2], x_peer
    )

    def small_spread(step):
        return remote(
            small_own.at[2],
            small_all.at[step - 1],
            small_sem.at[0, 2 + step],
            small_sem.at[1, 2 + step],
            plane[step - 1],
        )

    def small_first():
        for side in range(2):
            small_enter(side).wait()
        for side in range(2):
            small_own[side] = small_work[side * 2 + c] + small_core[side]
        small_cross.start()

    def small_second():
        small_cross.wait()
        small_own[2] = small_own[x] + small_x[...]
        for step in range(1, GROUP):
            small_spread(step).start()

    def arrive(p):
        pair_steps[0](mixed_bits(lo, nth(p)))

    def cross(p):
        pair_steps[1](mixed_bits(lo, nth(p)))

    stop = max(total + LAG * (len(steps) - 1), LAST_TAKE + 5 + GROUP // PAIR_BY + LAG * 5)

    @pl.loop(0, stop)
    def _(now):
        @pl.when((now >= GIVE_AT) & (now < GIVE_AT + GROUP))
        def _():
            give(now - GIVE_AT)

        run_pipe(steps, total, now)

        for step, lag in ((take, 0), (arrive, 2), (cross, 4)):
            gone = now - TAKE_AT - lag

            @pl.when((gone >= 0) & (gone < TAKE_BY * GROUP) & (gone % TAKE_BY == 0))
            def _():
                step(gone // TAKE_BY)

        for event, at in (
            (leave, LAST_TAKE + 1),
            (small_first, LAST_TAKE + 5),
            (small_second, LAST_TAKE + 9),
        ):
            pl.when(now == at)(event)

        for where, step in enumerate(pair_steps[2:]):
            gone = now - LAST_TAKE - 5 - LAG * where

            @pl.when((gone >= 0) & (gone < GROUP // PAIR_BY))
            def _():
                for each in range(PAIR_BY):
                    step(PAIR_BY * gone + each)

    for step in range(1, GROUP):
        small_spread(step).wait()
    value = small_own[2]
    for step in range(1, GROUP):
        value = value + small_all[step - 1]
    small_final[...] = value
    for j in range(GROUP):
        for part in range(3):
            at = part * D + j * PAIR
            qkv_final[:, at : at + PAIR] = pair_final[j, :, part * PAIR : (part + 1) * PAIR]

    for e in order:
        for part in range(3):
            block_copy(e, part).wait_send()
    for there, forward in ((has_next, True), (has_prev, False)):

        @pl.when(there)
        def _():
            for i in range(half_group):
                for part in range(2):
                    halo_copy(i if forward else i + half_group, part, forward).wait_send()


def wrap_up(replicas, moved, act, pairs, tokens, residual, gain, small, rest, shapes):
    chunks = rest.shape[0]
    tok_rows = act.shape[0]
    tall = small.shape[1]
    anywhere = pl.BlockSpec(memory_space=pl.ANY)
    vmem = pl.BlockSpec(memory_space=pltpu.VMEM)
    dma = pltpu.SemaphoreType.DMA
    low = jnp.bfloat16
    shape = jax.ShapeDtypeStruct
    pair = 3 * PAIR
    return pl.pallas_call(
        functools.partial(finish_kernel, replicas),
        out_shape=(shape((tok_rows, D), low),)
        + tuple(shape(size, low) for size in shapes)
        + (shape((D // 4, 3 * D), low), shape((tall, PAIR), jnp.float32)),
        in_specs=[vmem] * 4 + [anywhere] + [vmem] * 4 + [anywhere],
        out_specs=(vmem,) * 5,
        scratch_shapes=pipe_shapes(chunks, 2, *rest.shape[2:], True)
        + pipe_shapes(GROUP, 4, D // 4, pair, False)
        + [
            pltpu.VMEM((2, GROUP * tok_rows, PAIR), low),
            pltpu.VMEM((GROUP, 2, tok_rows, PAIR), low),
            pltpu.VMEM((GROUP, tok_rows, pair), low),
            pltpu.VMEM((2, D, pair), low),
            pltpu.VMEM((D, tok_rows), low),
            pltpu.VMEM((tok_rows, D), jnp.float32),
            pltpu.VMEM((4, tall, PAIR), jnp.float32),
            pltpu.VMEM((3, tall, PAIR), jnp.float32),
            pltpu.VMEM((2, tall, PAIR), jnp.float32),
            pltpu.VMEM((tall, PAIR), jnp.float32),
            pltpu.VMEM((GROUP - 1, tall, PAIR), jnp.float32),
            dma((2, GROUP, 2)),
            dma((2, GROUP, 3)),
            dma((2,)),
            dma((2, GROUP + 2)),
        ],
        compiler_params=pltpu.CompilerParams(
            collective_id=1, has_side_effects=True, vmem_limit_bytes=67043328
        ),
        cost_estimate=pl.CostEstimate(
            flops=12 * tok_rows * D * D, transcendentals=0, bytes_accessed=200 << 20
        ),
        name="finish",
    )(*moved, act, pairs, tokens, residual, gain, small, rest)


def shards(
    tokens,
    out_grad,
    norm1_gain,
    norm1_bias,
    w_qkv,
    q_bias,
    v_bias,
    w_out,
    out_bias,
    attn_scale,
    norm2_gain,
    norm2_bias,
    w_up,
    up_bias,
    w_down,
    down_bias,
    mlp_scale,
    image_ids,
    pad_mask,
):
    both = ("fsdp", "rep")
    owners = lax.axis_size("fsdp")
    replicas = lax.axis_size("rep")
    tok_rows = tokens.shape[0]
    rows = GROUP * tok_rows
    groups = [list(range(g, g + GROUP)) for g in range(0, replicas, GROUP)]
    factor = HEAD_DIM ** (-0.5)

    small = (
        norm1_gain,
        norm1_bias,
        q_bias,
        v_bias,
        out_bias,
        attn_scale,
        norm2_gain,
        norm2_bias,
        down_bias,
        mlp_scale,
        up_bias,
    )
    share = norm1_gain.shape[0]
    lines = list(small[:-1]) + list(up_bias.reshape(-1, share))
    line_at = lax.broadcasted_iota(jnp.int32, (-(-len(lines) // 8) * 8, share), 0)
    packed = jnp.zeros(line_at.shape, jnp.bfloat16)
    for at, member in enumerate(lines):
        packed = jnp.where(line_at == at, member[None], packed)
    packed = packed.astype(jnp.float32)
    codes = jnp.where(pad_mask > 0, image_ids + 1, 0).astype(jnp.float32).reshape(-1, PAIR)
    code_rows = codes.shape[0]
    codes = jnp.pad(codes, ((0, 8 - code_rows), (0, 0)))
    act_one, query, key_window, value_window, codes, vectors, w_pairs, out_across, up_half = project(
        replicas, tokens, packed, codes, w_qkv, w_out, w_up
    )
    window = key_window.shape[0]
    halo = rows // 2
    seen = codes[:, :code_rows].reshape(-1).astype(jnp.int32)
    seen = jnp.concatenate([seen, jnp.zeros((KEYS,), jnp.int32)])
    spot = jnp.arange(window, dtype=jnp.int32)
    asked = seen[halo : halo + rows]
    tile_codes = asked.reshape(rows // BLOCK, BLOCK)
    first_code = jnp.min(jnp.where(tile_codes > 0, tile_codes, 1 << 30), axis=1)
    last_code = jnp.max(tile_codes, axis=1)
    begin = jnp.min(jnp.where(seen[None] == first_code[:, None], spot[None], window), axis=1)
    finish = jnp.max(jnp.where(seen[None] == last_code[:, None], spot[None] + 1, 0), axis=1)
    begin = begin // 128 * 128
    count = jnp.where(last_code > 0, (finish - begin + KEYS - 1) // KEYS, 0)
    meta = jnp.stack([begin, count], axis=1).reshape(-1)

    lane_slot = jnp.arange(PAIR, dtype=jnp.int32) % HEAD_DIM
    key_slot = jnp.where(seen > 0, 1 + (seen - 1) % SLOTS, 0)
    marks = (key_slot[:, None] == lane_slot[None]).astype(jnp.bfloat16)


    deep = w_down.shape[0]
    side = deep // 2 + lax.axis_index("rep") % 2 * (deep // 4)
    down_most = jnp.concatenate(
        [w_down[: deep // 2], lax.dynamic_slice_in_dim(w_down, side, deep // 4, 0)], axis=0
    )
    down_late, query = lax.optimization_barrier((down_most, query))
    down_across = lax.ppermute(down_late, "fsdp", [(f, (f + 2) % 4) for f in range(4)])
    swapped = [(r, r + 1 - 2 * (r % 2)) for r in range(replicas)]
    up_other = lax.ppermute(up_half, "rep", swapped)
    attn_mine, attn_t, lse = attend(meta, query, key_window, value_window, marks)

    layer_out, residual_grad, grad_mine, packed, up_out, rest = middle(
        attn_mine,
        tokens,
        out_grad,
        vectors,
        (w_out, out_across, w_up, up_half, up_other, w_down, down_across),
    )
    up_theirs = lax.ppermute(up_out, "rep", swapped)
    dq, dk, dv = attend_back(
        meta, query, key_window, value_window, marks, grad_mine, attn_t, lse
    )
    tokens_grad, *grads, packed = wrap_up(
        replicas,
        (dq, dk, dv),
        act_one,
        w_pairs,
        tokens,
        residual_grad,
        vectors,
        packed,
        rest,
        (w_down.shape, w_out.shape),
    )
    half = jnp.arange(2).reshape(1, 2, 1, 1) == lax.axis_index("rep") % 2
    up_out = jnp.where(half, up_out[:, None], up_theirs[:, None]).reshape(w_up.shape)
    grads.insert(1, up_out)
    grads = [grad.astype(jnp.float32) for grad in grads]
    if replicas > GROUP:
        apart = [list(range(low, replicas, GROUP)) for low in range(GROUP)]
        grads = lax.psum(grads, "rep", axis_index_groups=apart)
        packed = lax.psum(packed, "rep", axis_index_groups=apart)
    packed = packed.reshape(-1)
    small_out = []
    place = 0
    for member in (norm1_gain, norm1_bias, q_bias, v_bias) + small[4:]:
        size = member.shape[0]
        small_out.append(packed[place : place + size])
        place += size

    down_out, up_out, out_out, qkv_out = grads
    return (
        layer_out,
        tokens_grad,
        small_out[0],
        small_out[1],
        qkv_out,
        small_out[2],
        small_out[3],
        out_out,
        small_out[4],
        small_out[5],
        small_out[6],
        small_out[7],
        up_out,
        small_out[10],
        down_out,
        small_out[8],
        small_out[9],
    )


def solution(mesh):
    spread = P(("fsdp", "rep"), None)
    line = P("fsdp")
    plane = P("fsdp", None)
    return jax.shard_map(
        shards,
        mesh=mesh,
        in_specs=(
            spread,
            spread,
            line,
            line,
            plane,
            line,
            line,
            plane,
            line,
            line,
            line,
            line,
            plane,
            line,
            plane,
            line,
            line,
            P(("fsdp", "rep")),
            P(("fsdp", "rep")),
        ),
        out_specs=(
            spread,
            spread,
            line,
            line,
            plane,
            line,
            line,
            plane,
            line,
            line,
            line,
            line,
            plane,
            line,
            plane,
            line,
            line,
        ),
        check_vma=False,
    )
```

```python
import functools

import jax
import jax.numpy as jnp
from jax import lax
from jax.experimental import pallas as pl
from jax.experimental.pallas import tpu as pltpu
from jax.sharding import PartitionSpec as P

D = 1024
HEADS = 16
HEAD_DIM = 64
IMG = 1370

PAIR = 2 * HEAD_DIM
GROUP = HEADS // 2
BLOCK = 256
KEYS = 1536
SLOTS = 63

EPSILON = 1e-06
NEG_BIG = -1e30
NEG_EDGE = -1e29

NT = (((1,), (1,)), ((), ()))


def from_behind(block, axis, distance):
    devices = range(lax.axis_size(axis))
    route = [(i - distance, i) for i in devices if i - distance in devices]
    return lax.ppermute(block, axis, route)


def normalize(values):
    center = jnp.mean(values, axis=-1, keepdims=True)
    centered = values - center
    spread = jnp.mean(centered * centered, axis=-1, keepdims=True)
    scale = lax.rsqrt(spread + EPSILON)
    return centered * scale, scale


def norm_back(cotangent, unit, scale, gain):
    scaled = cotangent * gain
    along = jnp.mean(scaled, axis=-1, keepdims=True)
    across = jnp.mean(scaled * unit, axis=-1, keepdims=True)
    return scale * (scaled - along - unit * across)


def matmul(left, right):
    return jnp.dot(left, right, preferred_element_type=jnp.float32)


def fold_rows(values, op):
    return op(values.reshape(values.shape[0] // 8, 8, values.shape[1]), axis=0)


def lane_marks():
    lane = lax.broadcasted_iota(jnp.int32, (BLOCK, PAIR), 1)
    return lane // HEAD_DIM, lane % HEAD_DIM > 0


def asking(query, marks, half, usable):
    wanted = jnp.where((marks.astype(jnp.float32) > 0) & usable, 0.0, NEG_BIG).astype(jnp.bfloat16)
    return [jnp.where(half == h, query, wanted) for h in range(2)]


def attend_kernel(meta, q_ref, k_ref, v_ref, m_ref, o_ref, ot_ref, lse_ref, vt, k_aug, scores):
    rows_all = o_ref.shape[0]
    tiles = rows_all // BLOCK
    window = k_ref.shape[0]
    halo = (window - KEYS - rows_all) // 2
    half, usable = lane_marks()

    @pl.loop(0, window // BLOCK)
    def _(i):
        at = pl.ds(pl.multiple_of(i * BLOCK, BLOCK), BLOCK)
        vt[:, at] = v_ref[at, :].T
        for h in range(2):
            k_aug[h, at, :] = jnp.where(half == h, k_ref[at, :], m_ref[at, :])

    @pl.loop(0, tiles)
    def _(t):
        start = meta[2 * t]
        count = meta[2 * t + 1]
        rows = pl.ds(pl.multiple_of(t * BLOCK, BLOCK), BLOCK)
        spots = pl.ds(pl.multiple_of(halo + t * BLOCK, BLOCK), BLOCK)
        query = asking(q_ref[rows, :], m_ref[spots, :], half, usable)

        def score(i, tops):
            at = pl.ds(pl.multiple_of(start + i * KEYS, 128), KEYS)
            keep = pl.ds(pl.multiple_of(i * KEYS, KEYS), KEYS)
            new = []
            for h in range(2):
                part = lax.dot_general(
                    k_aug[h, at, :], query[h], NT, preferred_element_type=jnp.float32
                )
                scores[h, keep, :] = part
                new.append(jnp.maximum(tops[h], fold_rows(part, jnp.max)))
            return tuple(new)

        low = jnp.full((8, BLOCK), NEG_BIG, jnp.float32)
        tops = lax.fori_loop(0, count, score, (low, low))
        tops = [jnp.max(top, axis=0, keepdims=True) for top in tops]
        tops = [jnp.where(top < NEG_EDGE, 0.0, top) for top in tops]

        def mix(i, carry):
            at = pl.ds(pl.multiple_of(start + i * KEYS, 128), KEYS)
            keep = pl.ds(pl.multiple_of(i * KEYS, KEYS), KEYS)
            new = []
            for h in range(2):
                total, mixed = carry[h]
                weights = jnp.exp(scores[h, keep, :] - tops[h])
                total = total + fold_rows(weights, jnp.sum)
                mixed = mixed + matmul(
                    vt[h * HEAD_DIM : (h + 1) * HEAD_DIM, at], weights.astype(jnp.bfloat16)
                )
                new.append((total, mixed))
            return tuple(new)

        zero = (jnp.zeros((8, BLOCK), jnp.float32), jnp.zeros((HEAD_DIM, BLOCK), jnp.float32))
        done = lax.fori_loop(0, count, mix, (zero, zero))
        outs = []
        for h in range(2):
            total = jnp.sum(done[h][0], axis=0, keepdims=True)
            total = jnp.where(total > 0, total, 1.0)
            lse_ref[h : h + 1, rows] = tops[h] + jnp.log(total)
            outs.append(done[h][1] / total)
        out = jnp.concatenate(outs, axis=0)
        ot_ref[:, rows] = out
        o_ref[rows, :] = out.T.astype(jnp.bfloat16)


def attend(meta, query, keys, values, marks):
    rows = query.shape[0]
    window = keys.shape[0]
    deepest = (2 * IMG + 2 * BLOCK + KEYS) // KEYS * KEYS
    vmem = pl.BlockSpec(memory_space=pltpu.VMEM)
    return pl.pallas_call(
        attend_kernel,
        out_shape=(
            jax.ShapeDtypeStruct((rows, PAIR), jnp.bfloat16),
            jax.ShapeDtypeStruct((PAIR, rows), jnp.float32),
            jax.ShapeDtypeStruct((8, rows), jnp.float32),
        ),
        in_specs=[pl.BlockSpec(memory_space=pltpu.SMEM), vmem, vmem, vmem, vmem],
        out_specs=(vmem, vmem, vmem),
        scratch_shapes=[
            pltpu.VMEM((PAIR, window), jnp.bfloat16),
            pltpu.VMEM((2, window, PAIR), jnp.bfloat16),
            pltpu.VMEM((2, deepest, BLOCK), jnp.float32),
        ],
        cost_estimate=pl.CostEstimate(
            flops=4 * rows * 2 * IMG * PAIR, transcendentals=2 * rows * IMG, bytes_accessed=9 << 20
        ),
        name="attend",
    )(meta, query, keys, values, marks)


def attend_back_kernel(
    meta, q_ref, k_ref, v_ref, m_ref, g_ref, ot_ref, lse_ref, dq_ref, dk_out, dv_out, kt, k_aug, dk_ref, dv_ref
):
    rows_all = dq_ref.shape[0]
    tiles = rows_all // BLOCK
    window = k_ref.shape[0]
    halo = (window - KEYS - rows_all) // 2
    half, usable = lane_marks()

    @pl.loop(0, window // BLOCK)
    def _(i):
        at = pl.ds(pl.multiple_of(i * BLOCK, BLOCK), BLOCK)
        kt[:, at] = k_ref[at, :].T
        for h in range(2):
            k_aug[h, at, :] = jnp.where(half == h, k_ref[at, :], m_ref[at, :])
        dk_ref[at, :] = jnp.zeros((BLOCK, PAIR), jnp.float32)
        dv_ref[at, :] = jnp.zeros((BLOCK, PAIR), jnp.float32)

    @pl.loop(0, tiles)
    def _(t):
        start = meta[2 * t]
        count = meta[2 * t + 1]
        rows = pl.ds(pl.multiple_of(t * BLOCK, BLOCK), BLOCK)
        grad = g_ref[rows, :]
        blank = jnp.zeros_like(grad)
        spots = pl.ds(pl.multiple_of(halo + t * BLOCK, BLOCK), BLOCK)
        query = asking(q_ref[rows, :], m_ref[spots, :], half, usable)
        query_only = jnp.concatenate(
            [jnp.where(half == h, query[h], blank) for h in range(2)], axis=0
        )
        grads = [jnp.where(half == h, grad, blank) for h in range(2)]
        grads_both = jnp.concatenate(grads, axis=0)
        product = grad.astype(jnp.float32).T * ot_ref[:, rows]
        delta = [
            jnp.sum(product[h * HEAD_DIM : (h + 1) * HEAD_DIM], axis=0, keepdims=True)
            for h in range(2)
        ]
        lse = [lse_ref[h : h + 1, rows] for h in range(2)]

        def step(i, carry):
            at = pl.ds(pl.multiple_of(start + i * KEYS, 128), KEYS)
            value = v_ref[at, :]
            probs, slopes, new = [], [], []
            for h in range(2):
                part = lax.dot_general(
                    k_aug[h, at, :], query[h], NT, preferred_element_type=jnp.float32
                )
                weights = jnp.exp(part - lse[h])
                pull = lax.dot_general(value, grads[h], NT, preferred_element_type=jnp.float32)
                slope = (weights * (pull - delta[h])).astype(jnp.bfloat16)
                probs.append(weights.astype(jnp.bfloat16))
                slopes.append(slope)
                new.append(carry[h] + matmul(kt[h * HEAD_DIM : (h + 1) * HEAD_DIM, at], slope))
            dv_ref[at, :] += matmul(jnp.concatenate(probs, axis=1), grads_both)
            dk_ref[at, :] += matmul(jnp.concatenate(slopes, axis=1), query_only)
            return tuple(new)

        zero = jnp.zeros((HEAD_DIM, BLOCK), jnp.float32)
        done = lax.fori_loop(0, count, step, (zero, zero))
        dq = jnp.concatenate(done, axis=0) * (HEAD_DIM**-0.5)
        dq_ref[rows, :] = dq.T.astype(jnp.bfloat16)

    @pl.loop(0, window // BLOCK)
    def _(i):
        at = pl.ds(pl.multiple_of(i * BLOCK, BLOCK), BLOCK)
        dk_out[at, :] = dk_ref[at, :].astype(jnp.bfloat16)
        dv_out[at, :] = dv_ref[at, :].astype(jnp.bfloat16)


def attend_back(meta, query, keys, values, marks, grad, out_t, lse):
    rows = query.shape[0]
    window = keys.shape[0]
    vmem = pl.BlockSpec(memory_space=pltpu.VMEM)
    return pl.pallas_call(
        attend_back_kernel,
        out_shape=(
            jax.ShapeDtypeStruct((rows, PAIR), jnp.bfloat16),
            jax.ShapeDtypeStruct((window, PAIR), jnp.bfloat16),
            jax.ShapeDtypeStruct((window, PAIR), jnp.bfloat16),
        ),
        in_specs=[pl.BlockSpec(memory_space=pltpu.SMEM)] + [vmem] * 7,
        out_specs=(vmem, vmem, vmem),
        scratch_shapes=[
            pltpu.VMEM((PAIR, window), jnp.bfloat16),
            pltpu.VMEM((2, window, PAIR), jnp.bfloat16),
            pltpu.VMEM((window, PAIR), jnp.float32),
            pltpu.VMEM((window, PAIR), jnp.float32),
        ],
        cost_estimate=pl.CostEstimate(
            flops=10 * rows * 2 * IMG * PAIR, transcendentals=2 * rows * IMG, bytes_accessed=16 << 20
        ),
        name="attend_back",
    )(meta, query, keys, values, marks, grad, out_t, lse)


CHUNK = 64
LAG = 2
GIVE_AT = 5
TAKE_AT = 19
TAKE_BY = 1
LAST_TAKE = TAKE_AT + (GROUP - 1) * TAKE_BY
PAIR_BY = 1
MESH = pl.DeviceIdType.MESH


def split_index(f, r):
    return f // 2, f % 2, (r % GROUP) // 2, r % 2


def mixed_bits(left, right):
    value = 0
    for weight in (4, 2, 1):
        value = value + weight * ((left // weight + right // weight) % 2)
    return value


def remote(source, target, send, recv, peer):
    return pltpu.make_async_remote_copy(
        src_ref=source,
        dst_ref=target,
        send_sem=send,
        recv_sem=recv,
        device_id=peer,
        device_id_type=MESH,
    )


def greet(peers, optional=()):
    barrier = pltpu.get_barrier_semaphore()
    expected = len(peers)
    for peer in peers:
        pl.semaphore_signal(barrier, inc=1, device_id=peer, device_id_type=MESH)
    for there, peer in optional:

        @pl.when(there)
        def _():
            pl.semaphore_signal(barrier, inc=1, device_id=peer, device_id_type=MESH)

        expected = expected + there.astype(jnp.int32)
    pl.semaphore_wait(barrier, expected)


def group_neighbours(f, r, replicas):
    spot = f * replicas + r
    after = lax.rem(spot + GROUP, 4 * replicas)
    before = lax.rem(spot + 3 * replicas + (replicas - GROUP), 4 * replicas)
    next_peer = (after // replicas, lax.rem(after, replicas))
    prev_peer = (before // replicas, lax.rem(before, replicas))
    return spot + GROUP < 4 * replicas, next_peer, spot >= GROUP, prev_peer


def qkv_kernel(
    replicas,
    tokens_ref,
    small_ref,
    codes_ref,
    w_ref,
    out_ref,
    up_ref,
    act_ref,
    q_out,
    k_out,
    v_out,
    codes_out,
    small_out,
    w_pairs,
    out_across,
    up_half,
    w_buf,
    stage,
    bias,
    own_sem,
    x_sem,
    y_sem,
    core_sem,
    relay_sem,
    block_sem,
    halo_sem,
    code_sem,
    edge_sem,
    small_sem,
    wide_sem,
    pair_sem,
):
    f = lax.axis_index("fsdp")
    r = lax.axis_index("rep")
    x, c, z, y = split_index(f, r)
    lo = r % GROUP
    base = r - lo
    tok_rows = tokens_ref.shape[0]
    rows = GROUP * tok_rows
    halo = (k_out.shape[0] - KEYS - rows) // 2
    half = GROUP // 2
    share = w_ref.shape[0]
    core_peer = (x * 2 + 1 - c, r)
    x_peer = ((1 - x) * 2 + c, r)
    y_peer = (f, base + z * 2 + 1 - y)
    fsdp_peers = [((f + step) % 4, r) for step in range(1, 4)]
    plane = [(f, base + (lo + step) % GROUP) for step in range(1, GROUP)]
    has_next, next_peer, has_prev, prev_peer = group_neighbours(f, r, replicas)
    greet(fsdp_peers + plane, [(has_next, next_peer), (has_prev, prev_peer)])

    def small_copy(step):
        return remote(
            small_ref,
            small_out.at[f],
            small_sem.at[0, step - 1],
            small_sem.at[1, step - 1],
            fsdp_peers[step - 1],
        )

    def lanes(part):
        return pl.ds(part * PAIR, PAIR)

    def shard_rows(owner):
        return pl.ds(pl.multiple_of(owner * share, share), share)

    def columns(part, pair):
        return w_ref.at[:, pl.ds(pl.multiple_of(part * D + pair * PAIR, PAIR), PAIR)]

    def slot(e, owner, part):
        return w_buf.at[e, shard_rows(owner), lanes(part)]

    across = (1 - x) * 2 + c
    out_copy = remote(out_ref, out_across, wide_sem.at[0, 0], wide_sem.at[1, 0], x_peer)
    up_tall = up_half.shape[0]
    up_copy = remote(
        up_ref.at[pl.ds(pl.multiple_of(y * up_tall, up_tall), up_tall)],
        up_half,
        wide_sem.at[0, 1],
        wide_sem.at[1, 1],
        x_peer,
    )

    def pair_store(e):
        return pltpu.make_async_copy(w_buf.at[e], w_pairs.at[e], pair_sem.at[e])

    def x_copy(e, part):
        pair = mixed_bits(lo, e)
        return remote(
            columns(part, pair), slot(e, f, part), x_sem.at[0, e, part], x_sem.at[1, e, part], x_peer
        )

    def y_copy(e, part):
        return remote(
            slot(e, across, part),
            slot(e + 1, across, part),
            y_sem.at[e, part],
            x_sem.at[1, e + 1, part],
            y_peer,
        )

    def arrival(e, part):
        here = slot(e, across, part)
        return remote(here, here, x_sem.at[0, e, part], x_sem.at[1, e, part], x_peer)

    def core_copy(e, part):
        pair = mixed_bits(lo, e)
        return remote(
            columns(part, pair),
            slot(e, f, part),
            core_sem.at[0, e, part],
            core_sem.at[1, e, part],
            core_peer,
        )

    def own_copy(e, part):
        pair = mixed_bits(lo, e)
        return pltpu.make_async_copy(columns(part, pair), slot(e, f, part), own_sem.at[e, part])

    def relay_copy(e, part):
        here = slot(e, across, part)
        return remote(here, here, relay_sem.at[0, e, part], relay_sem.at[1, e, part], core_peer)

    def code_copy(step):
        return remote(
            codes_ref,
            codes_out.at[half + lo],
            code_sem.at[0, step - 1],
            code_sem.at[1, step - 1],
            plane[step - 1],
        )

    order = (4, 5, 2, 3, 6, 7, 0, 1)
    for step in range(1, 4):
        small_copy(step).start()
    for e in order:
        for part in range(3):
            if e % 2 == 0:
                x_copy(e, part).start()
            core_copy(e, part).start()
            own_copy(e, part).start()
    out_copy.start()
    up_copy.start()
    for step in range(1, GROUP):
        code_copy(step).start()
    codes_out[half + lo] = codes_ref[...]

    k_out[2 * halo + rows :, :] = jnp.zeros((KEYS, PAIR), jnp.bfloat16)
    v_out[2 * halo + rows :, :] = jnp.zeros((KEYS, PAIR), jnp.bfloat16)
    for there, low, edge in ((has_prev, 0, 0), (has_next, halo + rows, half + GROUP)):

        @pl.when(jnp.logical_not(there))
        def _():
            k_out[low : low + halo, :] = jnp.zeros((halo, PAIR), jnp.bfloat16)
            v_out[low : low + halo, :] = jnp.zeros((halo, PAIR), jnp.bfloat16)
            codes_out[edge : edge + half] = jnp.zeros((half, 8, PAIR), jnp.float32)

    unit, scale = normalize(tokens_ref[...].astype(jnp.float32))
    small_out[f] = small_ref[...]
    for step in range(1, 4):
        small_copy(step).wait()
    table = [small_out[owner] for owner in range(4)]

    def vector(line):
        return jnp.concatenate([rows_of[line : line + 1] for rows_of in table], axis=1)

    for which, line in ((0, 2), (1, 3)):
        for owner in range(4):
            for side in range(2):
                bias[which, 2 * owner + side : 2 * owner + side + 1, :] = table[owner][
                    line : line + 1, side * PAIR : (side + 1) * PAIR
                ]
    act_ref[...] = (unit * vector(0) + vector(1)).astype(jnp.bfloat16)

    def block_copy(e, part):
        pair = mixed_bits(lo, e)
        into = (q_out, k_out, v_out)[part]
        lead = lo * tok_rows + (0 if part == 0 else halo)
        return remote(
            stage.at[e, part],
            into.at[pl.ds(pl.multiple_of(lead, 128), tok_rows), :],
            block_sem.at[0, e, part],
            block_sem.at[1, e, part],
            (f, base + pair),
        )

    def nth(s):
        return jnp.where(s < 2, s + 4, jnp.where(s < 4, s, jnp.where(s < 6, s + 2, s - 6)))

    def halo_copy(source, part, forward):
        into = (k_out, v_out)[part]
        lead = source * tok_rows
        put = lead + halo - rows if forward else lead + halo + rows
        return remote(
            into.at[pl.ds(pl.multiple_of(halo + lead, 128), tok_rows), :],
            into.at[pl.ds(pl.multiple_of(put, 128), tok_rows), :],
            halo_sem.at[0, source, part],
            halo_sem.at[1, source, part],
            next_peer if forward else prev_peer,
        )

    def pass_on(source):
        for there, forward, fits in (
            (has_next, True, source >= half),
            (has_prev, False, source < half),
        ):

            @pl.when(there & fits)
            def _():
                for part in range(2):
                    halo_copy(source, part, forward).start()

    def pass_arrived(e):
        for part in range(3):
            block_copy(e, part).wait_recv()
        pass_on(mixed_bits(lo, e))

    @pl.loop(0, GROUP)
    def _(s):
        e = nth(s)
        pair = mixed_bits(lo, e)
        for part in range(3):
            arrival(e, part).wait_recv()
            relay_copy(e, part).start()

        @pl.when(e % 2 == 0)
        def _():
            for part in range(3):
                y_copy(e, part).start()

        for part in range(3):
            own_copy(e, part).wait()
            core_copy(e, part).wait_recv()
            relay_copy(e, part).wait_recv()
        pair_store(e).start()
        result = matmul(act_ref[...], w_buf[e])
        outs = (
            (result[:, :PAIR] + bias[0, pl.ds(pair, 1), :]) * (HEAD_DIM**-0.5),
            result[:, PAIR : 2 * PAIR],
            result[:, 2 * PAIR :] + bias[1, pl.ds(pair, 1), :],
        )
        for part in range(3):
            stage[e, part] = outs[part].astype(jnp.bfloat16)

        @pl.when(e > 0)
        def _():
            for part in range(3):
                block_copy(e, part).start()

        @pl.when(e == 0)
        def _():
            for part, into in enumerate((q_out, k_out, v_out)):
                lead = lo * tok_rows + (0 if part == 0 else halo)
                into[pl.ds(pl.multiple_of(lead, 128), tok_rows), :] = outs[part].astype(
                    jnp.bfloat16
                )
            pass_on(lo)

        @pl.when(s >= GROUP // 2)
        def _():
            pass_arrived(nth(s - GROUP // 2))

    for e in (1, 6, 7):
        pass_arrived(e)

    for step in range(1, GROUP):
        code_copy(step).wait()

    def edge_copy(forward):
        low, put = (GROUP, 0) if forward else (half, half + GROUP)
        return remote(
            codes_out.at[pl.ds(low, half)],
            codes_out.at[pl.ds(put, half)],
            edge_sem.at[0, int(forward)],
            edge_sem.at[1, int(forward)],
            next_peer if forward else prev_peer,
        )

    sides = ((has_next, has_prev, True), (has_prev, has_next, False))
    for there, here, forward in sides:

        @pl.when(there)
        def _():
            edge_copy(forward).start()

    out_copy.wait()
    up_copy.wait()
    for e in range(GROUP):
        pair_store(e).wait()
    for e in range(GROUP):
        for part in range(3):
            if e % 2 == 0:
                x_copy(e, part).wait_send()
                y_copy(e, part).wait_send()
            core_copy(e, part).wait_send()
            relay_copy(e, part).wait_send()
            if e > 0:
                block_copy(e, part).wait_send()
    for there, here, forward in sides:
        sources = range(half, GROUP) if forward else range(half)

        @pl.when(there)
        def _():
            edge_copy(forward).wait_send()
            for source in sources:
                for part in range(2):
                    halo_copy(source, part, forward).wait_send()

        @pl.when(here)
        def _():
            edge_copy(forward).wait_recv()
            for source in sources:
                for part in range(2):
                    halo_copy(source, part, forward).wait_recv()


def project(replicas, tokens, small, codes, w_qkv, w_out, w_up):
    tok_rows = tokens.shape[0]
    rows = GROUP * tok_rows
    window = 2 * rows + KEYS
    low = jnp.bfloat16
    vmem = pl.BlockSpec(memory_space=pltpu.VMEM)
    anywhere = pl.BlockSpec(memory_space=pl.ANY)
    dma = pltpu.SemaphoreType.DMA
    shape = jax.ShapeDtypeStruct
    return pl.pallas_call(
        functools.partial(qkv_kernel, replicas),
        out_shape=(
            shape((tok_rows, D), low),
            shape((rows, PAIR), low),
            shape((window, PAIR), low),
            shape((window, PAIR), low),
            shape((2 * GROUP, 8, PAIR), jnp.float32),
            shape((4,) + small.shape, jnp.float32),
            shape((GROUP, D, 3 * PAIR), low),
            shape(w_out.shape, low),
            shape((w_up.shape[0] // 2, w_up.shape[1]), low),
        ),
        in_specs=[vmem] * 3 + [anywhere] * 3,
        out_specs=(vmem,) * 6 + (anywhere,) * 3,
        scratch_shapes=[
            pltpu.VMEM((GROUP, D, 3 * PAIR), low),
            pltpu.VMEM((GROUP, 3, tok_rows, PAIR), low),
            pltpu.VMEM((2, GROUP, PAIR), jnp.float32),
            dma((GROUP, 3)),
            dma((2, GROUP, 3)),
            dma((GROUP, 3)),
            dma((2, GROUP, 3)),
            dma((2, GROUP, 3)),
            dma((2, GROUP, 3)),
            dma((2, GROUP, 2)),
            dma((2, GROUP - 1)),
            dma((2, 2)),
            dma((2, 3)),
            dma((2, 2)),
            dma((GROUP,)),
        ],
        compiler_params=pltpu.CompilerParams(
            collective_id=2, has_side_effects=True, vmem_limit_bytes=67043328
        ),
        cost_estimate=pl.CostEstimate(
            flops=2 * tok_rows * D * 3 * D, transcendentals=0, bytes_accessed=60 << 20
        ),
        name="project",
    )(tokens, small, codes, w_qkv, w_out, w_up)


def low(value):
    return value.astype(jnp.bfloat16)


def high(value):
    return value.astype(jnp.float32)


def span(start, size):
    return pl.ds(pl.multiple_of(start, size), size)


def make_pipe(
    place, own, source, load, from_core, from_x, from_y, from_near, from_far, final, sem, spread=True
):
    x, c, y, z_near, z_far = place["x"], place["c"], place["y"], place["z_near"], place["z_far"]
    depth = final.shape[1]
    half, mid, short = depth // 2, depth // 4, depth // 8
    my_half = span(y * half, half)
    my_mid = span(y * half + z_near * mid, mid)
    my_short = span(y * half + z_near * mid + z_far * short, short)

    def spot(side):
        return side if own.shape[1] == 2 else side * 2 + c

    def link(k, which, here, there, peer):
        return remote(here, there, sem.at[0, k, which], sem.at[1, k, which], place[peer])

    def core_copy(k, side):
        owner = side * 2 + 1 - c
        here = own.at[k, owner] if source is None else source(k, owner)
        return link(k, side, here, from_core.at[k, side], "core")

    def load_copy(k, side):
        return pltpu.make_async_copy(
            source(k, side * 2 + c), own.at[k, side], load.at[k, side]
        )

    def x_copy(k):
        return link(k, 2, own.at[k, spot(1 - x)], from_x.at[k], "x_peer")

    def y_copy(k):
        return link(k, 3, own.at[k, spot(x), span((1 - y) * half, half)], from_y.at[k], "y_peer")

    def near_copy(k):
        away = span(y * half + (1 - z_near) * mid, mid)
        return link(k, 4, own.at[k, spot(x), away], from_near.at[k], "near")

    def far_copy(k):
        away = span(y * half + z_near * mid + (1 - z_far) * short, short)
        return link(k, 5, own.at[k, spot(x), away], from_far.at[k], "far")

    def far_join_copy(k):
        here = final.at[k, my_short]
        return link(k, 6, here, here, "far")

    def near_join_copy(k):
        here = final.at[k, my_mid]
        return link(k, 7, here, here, "near")

    def y_join_copy(k):
        here = final.at[k, my_half]
        return link(k, 8, here, here, "y_peer")

    def enter(k):
        for side in range(2):
            core_copy(k, side).start()
            if source is not None:
                load_copy(k, side).start()

    def core_sum(k):
        for side in range(2):
            if source is not None:
                load_copy(k, side).wait()
            core_copy(k, side).wait()
            own[k, spot(side)] = low(high(own[k, spot(side)]) + high(from_core[k, side]))
        x_copy(k).start()

    def x_sum(k):
        x_copy(k).wait()
        own[k, spot(x)] = low(high(own[k, spot(x)]) + high(from_x[k]))
        y_copy(k).start()

    def y_sum(k):
        y_copy(k).wait()
        own[k, spot(x), my_half] = low(high(own[k, spot(x), my_half]) + high(from_y[k]))
        near_copy(k).start()

    def near_sum(k):
        near_copy(k).wait()
        own[k, spot(x), my_mid] = low(high(own[k, spot(x), my_mid]) + high(from_near[k]))
        far_copy(k).start()

    def far_sum(k):
        far_copy(k).wait()
        final[k, my_short] = low(high(own[k, spot(x), my_short]) + high(from_far[k]))
        far_join_copy(k).start()

    def far_join(k):
        far_join_copy(k).wait()
        near_join_copy(k).start()

    def near_join(k):
        near_join_copy(k).wait()
        if spread:
            y_join_copy(k).start()

    def y_join(k):
        y_join_copy(k).wait()

    return [enter, core_sum, x_sum, y_sum, near_sum, far_sum, far_join, near_join, y_join]


def run_pipe(steps, count, now):
    for where, step in enumerate(steps):
        k = now - where * LAG

        @pl.when((k >= 0) & (k < count))
        def _():
            step(k)


def pipe_shapes(count, held, depth, width, loads):
    low_type = jnp.bfloat16
    return [
        pltpu.VMEM((count, held, depth, width), low_type),
        pltpu.VMEM((count, 2, depth, width), low_type),
        pltpu.VMEM((count, depth, width), low_type),
        pltpu.VMEM((count, depth // 2, width), low_type),
        pltpu.VMEM((count, depth // 4, width), low_type),
        pltpu.VMEM((count, depth // 8, width), low_type),
        pltpu.VMEM((count, depth, width), low_type),
        pltpu.SemaphoreType.DMA((2, count, 9)),
    ] + ([pltpu.SemaphoreType.DMA((count, 2))] if loads else [])


def find_place():
    f = lax.axis_index("fsdp")
    r = lax.axis_index("rep")
    x, c, z, y = split_index(f, r)
    lo = r % GROUP
    base = r - lo
    z_near, z_far = z % 2, z // 2
    return {
        "f": f,
        "r": r,
        "x": x,
        "c": c,
        "y": y,
        "z_near": z_near,
        "z_far": z_far,
        "lo": lo,
        "base": base,
        "core": (x * 2 + 1 - c, r),
        "x_peer": ((1 - x) * 2 + c, r),
        "y_peer": (f, base + z * 2 + 1 - y),
        "near": (f, base + (z_far * 2 + 1 - z_near) * 2 + y),
        "far": (f, base + ((1 - z_far) * 2 + z_near) * 2 + y),
        "plane": [(f, base + (lo + step) % GROUP) for step in range(1, GROUP)],
    }


def erf(value):
    return lax.erf(value)


def middle_kernel(
    o_ref,
    tokens_ref,
    grad_ref,
    vectors_ref,
    wo_own,
    wo_across,
    wu_own,
    wu_half,
    wu_other,
    wd_own,
    wd_across,
    layer_out,
    residual_out,
    grad_out,
    small_out,
    up_final,
    rest,
    wo,
    wu,
    wd,
    attn,
    act,
    act_t,
    slim,
    x1,
    proj,
    branch,
    act_grad,
    pre,
    hidden,
    slope,
    pre_grad,
    attn_grad,
    proj_grad,
    lines_ref,
    bias_ref,
    sums,
    stage,
    own,
    from_core,
    from_x,
    from_y,
    from_near,
    from_far,
    final,
    sem,
    load_sem,
    attn_sem,
    grad_sem,
    core_load_sem,
    down_sem,
    stage_sem,
):
    place = find_place()
    f, x, c, y, lo, base = (place[name] for name in ("f", "x", "c", "y", "lo", "base"))
    across = (1 - x) * 2 + c
    tok_rows = tokens_ref.shape[0]
    share = wo_own.shape[0]
    deep = wd_own.shape[0]
    sets = bias_ref.shape[0]
    tall = 128
    greet([place["core"], place["x_peer"]] + place["plane"])

    def shard_rows(owner, size):
        return span(owner * size, size)

    def attn_copy(e):
        pair = mixed_bits(lo, e)
        return remote(
            o_ref.at[span(pair * tok_rows, tok_rows), :],
            attn.at[:, span(lo * PAIR, PAIR)],
            attn_sem.at[0, e],
            attn_sem.at[1, e],
            (f, base + pair),
        )

    def grad_copy(e):
        pair = mixed_bits(lo, e)
        return remote(
            attn_grad.at[:, span(pair * PAIR, PAIR)],
            grad_out.at[span(lo * tok_rows, tok_rows), :],
            grad_sem.at[0, e],
            grad_sem.at[1, e],
            (f, base + pair),
        )

    share_half = share // 2
    lead = across * share
    moves = (
        (wo_own, wo, f * share, share),
        (wo_across, wo, lead, share),
        (wu_own, wu, f * share, share),
        (wu_half, wu, lead + y * share_half, share_half),
        (wu_other, wu, lead + (1 - y) * share_half, share_half),
        (wd_own, wd, f * deep, deep),
        (wd_across.at[: deep // 2], wd, across * deep, deep // 2),
        (wd_across.at[deep // 2 :], wd, across * deep + deep // 2 + y * (deep // 4), deep // 4),
    )

    def down_at(side):
        top = across * deep + deep // 2 + side * (deep // 4)
        return wd.at[span(top, deep // 4)]

    y_copy = remote(
        wd_across.at[deep // 2 :], down_at(y), down_sem.at[0], down_sem.at[1], place["y_peer"]
    )
    y_relay = remote(
        down_at(1 - y), down_at(1 - y), down_sem.at[2], down_sem.at[3], place["core"]
    )

    def local_copy(which):
        source, into, top, size = moves[which]
        target = into.at[pl.ds(pl.multiple_of(top, 128), size)]
        return pltpu.make_async_copy(source, target, load_sem.at[which])

    def core_copy(which):
        source, into, top, size = moves[which]
        target = into.at[pl.ds(pl.multiple_of(top, 128), size)]
        return remote(
            source, target, core_load_sem.at[0, which], core_load_sem.at[1, which], place["core"]
        )

    order = (4, 5, 6, 7, 2, 3, 1)
    for e in order:
        attn_copy(e).start()
    y_copy.start()
    for which in range(len(moves)):
        core_copy(which).start()
        local_copy(which).start()
    attn[:, span(lo * PAIR, PAIR)] = o_ref[span(lo * tok_rows, tok_rows), :]
    table = [vectors_ref[owner] for owner in range(4)]
    for which in range(6):
        lines_ref[which : which + 1, :] = jnp.concatenate(
            [rows_of[4 + which : 5 + which] for rows_of in table], axis=1
        )
    for i in range(sets):
        at, side = 10 + i // 2, i % 2 * tall
        bias_ref[i : i + 1, :] = jnp.concatenate(
            [rows_of[at : at + 1, side : side + tall] for rows_of in table], axis=1
        )
    small_out[...] = jnp.zeros_like(small_out)
    sums[...] = jnp.zeros_like(sums)
    branch[...] = jnp.zeros_like(branch)
    act_grad[...] = jnp.zeros_like(act_grad)

    def line(which):
        return lines_ref[which : which + 1, :]

    def by_rows(step, body):
        @pl.loop(0, tok_rows // step)
        def _(b):
            body(span(b * step, step))

    def scale_grad(at):
        slim[at, :] = low(line(5) * high(grad_ref[at, :]))

    by_rows(128, scale_grad)

    for e in order:
        attn_copy(e).wait_recv()
    for which in range(2):
        local_copy(which).wait()
        core_copy(which).wait_recv()
    proj[...] = matmul(attn[...], wo[...])

    def enter_mlp(at):
        value = proj[at, :] + line(0)
        proj[at, :] = value
        value = high(tokens_ref[at, :]) + line(1) * value
        x1[at, :] = value
        unit, scale = normalize(value)
        act[at, :] = low(unit * line(2) + line(3))

    by_rows(128, enter_mlp)
    act_t[...] = act[...].T
    y_copy.wait_recv()
    y_relay.start()
    for which in range(2, len(moves)):
        local_copy(which).wait()
        core_copy(which).wait_recv()
    y_relay.wait_recv()
    steps = make_pipe(
        place, own, None, None, from_core, from_x, from_y, from_near, from_far, final, sem, False
    )
    steps.pop()
    wait_near = steps.pop()

    def settle(k):
        wait_near(k)
        i, side = k // 2, k % 2
        mine = span(y * (tall // 2), tall // 2)
        for owner in range(4):
            up_final[side, :, span(owner * deep + i * tall, tall)] = final[
                k, mine, owner * tall : (owner + 1) * tall
            ]

    steps.append(settle)
    count = 2 * sets

    def stage_copy(i, part):
        return pltpu.make_async_copy(
            stage.at[i % 2, part], rest.at[2 * i + part], stage_sem.at[i % 2, part]
        )

    @pl.loop(0, sets)
    def _(i):
        columns = [span(owner * deep + i * tall, tall) for owner in range(4)]
        w_in = jnp.concatenate([wu[:, at] for at in columns], axis=1)
        w_back = jnp.concatenate([wd[at, :] for at in columns], axis=0)
        pre[...] = matmul(act[...], w_in)

        def activate(at):
            value = pre[at, :] + bias_ref[pl.ds(i, 1), :]
            cdf = 0.5 * (1.0 + erf(value * (0.5**0.5)))
            hidden[at, :] = low(value * cdf)
            slope[at, :] = cdf + value * (jnp.exp(-0.5 * value * value) * 0.3989422804014327)

        by_rows(128, activate)
        pre[...] = lax.dot_general(slim[...], w_back, NT, preferred_element_type=jnp.float32)
        branch[...] += matmul(hidden[...], w_back)

        def descend(at):
            value = pre[at, :] * slope[at, :]
            pre[at, :] = value
            pre_grad[at, :] = low(value)

        by_rows(128, descend)
        total = jnp.sum(pre[...], axis=0, keepdims=True)
        for owner in range(4):
            small_out[owner, pl.ds(20 + i, 1), :] = total[:, owner * tall : (owner + 1) * tall]
        up_grad = low(matmul(act_t[...], pre_grad[...]))
        for side in range(2):
            for owner in range(4):
                top = owner * 2 * tall + side * tall
                own[2 * i + side, owner] = up_grad[top : top + tall]
        run_pipe(steps, count, 2 * i)
        act_grad[...] += lax.dot_general(
            pre_grad[...], w_in, NT, preferred_element_type=jnp.float32
        )

        @pl.when(i >= 2)
        def _():
            for part in range(2):
                stage_copy(i - 2, part).wait()

        down_grad = low(matmul(hidden[...].T, slim[...]))
        for part in range(2):
            for owner in range(4):
                stage[i % 2, part, owner] = down_grad[
                    owner * tall : (owner + 1) * tall, part * 4 * tall : (part + 1) * 4 * tall
                ]
            stage_copy(i, part).start()
        run_pipe(steps, count, 2 * i + 1)

    def leave_mlp(at):
        grad = high(grad_ref[at, :])
        out = branch[at, :] + line(4)
        layer_out[at, :] = low(x1[at, :] + line(5) * out)
        unit, scale = normalize(x1[at, :])
        back = act_grad[at, :]
        value = grad + norm_back(back, unit, scale, line(2))
        residual_out[at, :] = value
        scaled = line(1) * value
        proj_grad[at, :] = low(scaled)
        rows = (scaled, value * proj[at, :], back * unit, back, line(5) * grad, grad * out)
        for which, member in enumerate(rows):
            sums[which : which + 1, :] += jnp.sum(member, axis=0, keepdims=True)

    by_rows(128, leave_mlp)
    attn_grad[...] = low(
        lax.dot_general(proj_grad[...], wo[...], NT, preferred_element_type=jnp.float32)
    )
    for e in order:
        grad_copy(e).start()
    grad_out[span(lo * tok_rows, tok_rows), :] = attn_grad[:, span(lo * PAIR, PAIR)]
    for which in range(6):
        for owner in range(4):
            for row in range(2):
                at = (owner * 2 + row) * PAIR
                place_row = 8 + 2 * which + row
                small_out[owner, place_row : place_row + 1, :] = sums[
                    which : which + 1, at : at + PAIR
                ]
    for i in range(sets - 2, sets):
        for part in range(2):
            stage_copy(i, part).wait()

    def out_copy(side, part):
        return pltpu.make_async_copy(
            stage.at[side, part], rest.at[count + 2 * side + part], stage_sem.at[side, part]
        )

    act_t[...] = attn[...].T
    for owner in range(4):
        part_grad = low(matmul(act_t[owner * share : (owner + 1) * share, :], proj_grad[...]))
        for side in range(2):
            for part in range(2):
                stage[side, part, owner] = part_grad[
                    side * tall : (side + 1) * tall, part * 4 * tall : (part + 1) * 4 * tall
                ]
    for side in range(2):
        for part in range(2):
            out_copy(side, part).start()

    @pl.loop(count, count + LAG * (len(steps) - 1))
    def _(now):
        run_pipe(steps, count, now)

    for side in range(2):
        for part in range(2):
            out_copy(side, part).wait()
    for e in order:
        attn_copy(e).wait_send()
        grad_copy(e).wait()
    y_copy.wait_send()
    y_relay.wait_send()
    for which in range(len(moves)):
        core_copy(which).wait_send()


def middle(mixed, tokens, out_grad, vectors, weights):
    w_out, w_up, w_down = weights[0], weights[2], weights[5]
    tok_rows = tokens.shape[0]
    rows = GROUP * tok_rows
    sets = w_down.shape[0] // 128
    count = 2 * sets
    wide = 4 * 128
    anywhere = pl.BlockSpec(memory_space=pl.ANY)
    vmem = pl.BlockSpec(memory_space=pltpu.VMEM)
    dma = pltpu.SemaphoreType.DMA
    shape = jax.ShapeDtypeStruct
    slight, full = jnp.bfloat16, jnp.float32
    return pl.pallas_call(
        middle_kernel,
        out_shape=(
            shape((tok_rows, D), slight),
            shape((tok_rows, D), full),
            shape((rows, PAIR), slight),
            shape((4, 28, PAIR), full),
            shape((2, w_up.shape[0] // 4, w_up.shape[1]), slight),
            shape((count + 4, 4, 128, wide), slight),
        ),
        in_specs=[vmem] * 4 + [anywhere] * 7,
        out_specs=(vmem,) * 5 + (anywhere,),
        scratch_shapes=[
            pltpu.VMEM((4 * w_out.shape[0], D), slight),
            pltpu.VMEM((4 * w_up.shape[0], w_up.shape[1]), slight),
            pltpu.VMEM((4 * w_down.shape[0], D), slight),
            pltpu.VMEM((tok_rows, D), slight),
            pltpu.VMEM((tok_rows, D), slight),
            pltpu.VMEM((D, tok_rows), slight),
            pltpu.VMEM((tok_rows, D), slight),
            pltpu.VMEM((tok_rows, D), full),
            pltpu.VMEM((tok_rows, D), full),
            pltpu.VMEM((tok_rows, D), full),
            pltpu.VMEM((tok_rows, D), full),
            pltpu.VMEM((tok_rows, wide), full),
            pltpu.VMEM((tok_rows, wide), slight),
            pltpu.VMEM((tok_rows, wide), full),
            pltpu.VMEM((tok_rows, wide), slight),
            pltpu.VMEM((tok_rows, D), slight),
            pltpu.VMEM((tok_rows, D), slight),
            pltpu.VMEM((8, D), full),
            pltpu.VMEM((sets, wide), full),
            pltpu.VMEM((8, D), full),
            pltpu.VMEM((2, 2, 4, 128, wide), slight),
        ]
        + pipe_shapes(count, 4, 128, wide, False)
        + [
            dma((8,)),
            dma((2, GROUP)),
            dma((2, GROUP)),
            dma((2, 8)),
            dma((4,)),
            dma((2, 2)),
        ],
        compiler_params=pltpu.CompilerParams(
            collective_id=3, has_side_effects=True, vmem_limit_bytes=67043328
        ),
        cost_estimate=pl.CostEstimate(
            flops=40 * tok_rows * D * D, transcendentals=0, bytes_accessed=100 << 20
        ),
        name="middle",
    )(mixed, tokens, out_grad, vectors, *weights)


def finish_kernel(
    replicas,
    dq_ref,
    dk_ref,
    dv_ref,
    act_ref,
    pairs_ref,
    tokens_ref,
    residual_ref,
    gain_ref,
    small_ref,
    rest_ref,
    tokens_out,
    down_final,
    out_final,
    qkv_final,
    small_final,
    own,
    from_core,
    from_x,
    from_y,
    from_near,
    from_far,
    final,
    sem,
    load_sem,
    pair_own,
    pair_core,
    pair_x,
    pair_y,
    pair_near,
    pair_far,
    pair_final,
    pair_sem,
    halos,
    stage,
    arrived,
    w_buf,
    act_t,
    act_grad,
    small_work,
    small_own,
    small_core,
    small_x,
    small_all,
    halo_sem,
    block_sem,
    w_sem,
    small_sem,
):
    place = find_place()
    f, r, x, c, lo, base = (place[name] for name in ("f", "r", "x", "c", "lo", "base"))
    core_peer, x_peer, plane = place["core"], place["x_peer"], place["plane"]
    has_next, next_peer, has_prev, prev_peer = group_neighbours(f, r, replicas)
    total = own.shape[0]
    tok_rows = act_ref.shape[0]
    rows = GROUP * tok_rows
    halo = rows // 2
    half_group = GROUP // 2
    greet([core_peer, x_peer] + plane, [(has_next, next_peer), (has_prev, prev_peer)])

    def block(ref, source, lead=0):
        return ref.at[pl.ds(pl.multiple_of(lead + source * tok_rows, 128), tok_rows), :]

    def lanes(part):
        return pl.ds(part * PAIR, PAIR)

    def halo_copy(source, part, forward):
        ref = (dk_ref, dv_ref)[part]
        return remote(
            block(ref, source, halo + rows if forward else -halo),
            block(halos.at[part], source),
            halo_sem.at[0, source, part],
            halo_sem.at[1, source, part],
            next_peer if forward else prev_peer,
        )

    def block_copy(e, part):
        source = block(dq_ref, mixed_bits(lo, e)) if part == 0 else stage.at[e, part - 1]
        return remote(
            source,
            arrived.at[e, :, lanes(part)],
            block_sem.at[0, e, part],
            block_sem.at[1, e, part],
            (f, base + mixed_bits(lo, e)),
        )

    def nth(p):
        h = p // 2
        near = jnp.where(h == 0, 2, jnp.where(h == 1, 1, jnp.where(h == 2, 3, 0)))
        return jnp.where(p % 2 == 0, 4 + h, near)

    def w_copy(p):
        spot = p % 2
        return pltpu.make_async_copy(pairs_ref.at[nth(p)], w_buf.at[spot], w_sem.at[spot])

    for there, forward in ((has_next, True), (has_prev, False)):

        @pl.when(there)
        def _():
            for i in range(half_group):
                for part in range(2):
                    halo_copy(i if forward else i + half_group, part, forward).start()

        @pl.when(jnp.logical_not(there))
        def _():
            start = halo if forward else 0
            halos[:, start : start + halo, :] = jnp.zeros((2, halo, PAIR), jnp.bfloat16)

    order = (4, 2, 5, 1, 6, 3, 7)
    for e in order:
        block_copy(e, 0).start()
    arrived[0, :, lanes(0)] = dq_ref[pl.ds(pl.multiple_of(lo * tok_rows, 128), tok_rows), :]
    small_work[...] = small_ref[...]
    act_grad[...] = jnp.zeros_like(act_grad)
    act_t[...] = act_ref[...].T
    w_copy(0).start()

    def give(p):
        e = nth(p)
        source = mixed_bits(lo, e)
        for there, forward, fits in (
            (has_next, False, source >= half_group),
            (has_prev, True, source < half_group),
        ):

            @pl.when(there & fits)
            def _():
                for part in range(2):
                    halo_copy(source, part, forward).wait_recv()

        sums = []
        for part, ref in enumerate((dk_ref, dv_ref)):
            near = ref[pl.ds(pl.multiple_of(halo + source * tok_rows, 128), tok_rows), :]
            far = halos[part, pl.ds(pl.multiple_of(source * tok_rows, 128), tok_rows), :]
            sums.append(low(high(near) + high(far)))
            stage[e, part] = sums[part]

        @pl.when(e > 0)
        def _():
            for part in range(1, 3):
                block_copy(e, part).start()

        @pl.when(e == 0)
        def _():
            for part in range(1, 3):
                arrived[0, :, lanes(part)] = sums[part - 1]

    pair_steps = make_pipe(
        place,
        pair_own,
        None,
        None,
        pair_core,
        pair_x,
        pair_y,
        pair_near,
        pair_far,
        pair_final,
        pair_sem,
    )
    pair_enter = pair_steps.pop(0)

    def take(p):
        e = nth(p)
        j = mixed_bits(lo, e)

        @pl.when(p + 1 < GROUP)
        def _():
            w_copy(p + 1).start()

        @pl.when(e > 0)
        def _():
            for part in range(3):
                block_copy(e, part).wait_recv()

        w_copy(p).wait()
        grads = arrived[e]
        pair_own[j] = low(matmul(act_t[...], grads)).reshape(4, D // 4, 3 * PAIR)
        pair_enter(j)
        act_grad[...] += lax.dot_general(
            grads, w_buf[p % 2], NT, preferred_element_type=jnp.float32
        )
        sums = jnp.sum(high(grads), axis=0, keepdims=True)
        for line, part in ((4, 0), (6, 2)):
            small_work[j // 2, pl.ds(line + j % 2, 1), :] = sums[:, part * PAIR : (part + 1) * PAIR]

    def leave():
        unit, scale = normalize(high(tokens_ref[...]))
        grad = act_grad[...]
        back = norm_back(
            grad, unit, scale, jnp.concatenate([gain_ref[owner, :1] for owner in range(4)], axis=1)
        )
        tokens_out[...] = low(residual_ref[...] + back)
        for line, values in ((0, grad * unit), (2, grad)):
            sums = jnp.sum(values, axis=0, keepdims=True)
            for owner in range(4):
                for row in range(2):
                    at = (owner * 2 + row) * PAIR
                    small_work[owner, line + row : line + row + 1, :] = sums[:, at : at + PAIR]
        for side in range(2):
            small_enter(side).start()

    steps = make_pipe(
        place,
        own,
        lambda k, owner: rest_ref.at[k, owner],
        load_sem,
        from_core,
        from_x,
        from_y,
        from_near,
        from_far,
        final,
        sem,
    )
    finish_step = steps[-1]
    tall, wide = final.shape[1:]
    downs = down_final.shape[0] // tall * 2

    def settle(k):
        finish_step(k)

        @pl.when(k < downs)
        def _():
            down_final[span((k // 2) * tall, tall), span((k % 2) * wide, wide)] = final[k]

        @pl.when(k >= downs)
        def _():
            at = k - downs
            out_final[span((at // 2) * tall, tall), span((at % 2) * wide, wide)] = final[k]

    steps[-1] = settle

    def small_enter(side):
        return remote(
            small_work.at[side * 2 + 1 - c],
            small_core.at[side],
            small_sem.at[0, side],
            small_sem.at[1, side],
            core_peer,
        )

    small_cross = remote(
        small_own.at[1 - x], small_x, small_sem.at[0, 2], small_sem.at[1, 2], x_peer
    )

    def small_spread(step):
        return remote(
            small_own.at[2],
            small_all.at[step - 1],
            small_sem.at[0, 2 + step],
            small_sem.at[1, 2 + step],
            plane[step - 1],
        )

    def small_first():
        for side in range(2):
            small_enter(side).wait()
        for side in range(2):
            small_own[side] = small_work[side * 2 + c] + small_core[side]
        small_cross.start()

    def small_second():
        small_cross.wait()
        small_own[2] = small_own[x] + small_x[...]
        for step in range(1, GROUP):
            small_spread(step).start()

    def arrive(p):
        pair_steps[0](mixed_bits(lo, nth(p)))

    def cross(p):
        pair_steps[1](mixed_bits(lo, nth(p)))

    stop = max(total + LAG * (len(steps) - 1), LAST_TAKE + 5 + GROUP // PAIR_BY + LAG * 5)

    @pl.loop(0, stop)
    def _(now):
        @pl.when((now >= GIVE_AT) & (now < GIVE_AT + GROUP))
        def _():
            give(now - GIVE_AT)

        run_pipe(steps, total, now)

        for step, lag in ((take, 0), (arrive, 2), (cross, 4)):
            gone = now - TAKE_AT - lag

            @pl.when((gone >= 0) & (gone < TAKE_BY * GROUP) & (gone % TAKE_BY == 0))
            def _():
                step(gone // TAKE_BY)

        for event, at in (
            (leave, LAST_TAKE + 1),
            (small_first, LAST_TAKE + 5),
            (small_second, LAST_TAKE + 9),
        ):
            pl.when(now == at)(event)

        for where, step in enumerate(pair_steps[2:]):
            gone = now - LAST_TAKE - 5 - LAG * where

            @pl.when((gone >= 0) & (gone < GROUP // PAIR_BY))
            def _():
                for each in range(PAIR_BY):
                    step(PAIR_BY * gone + each)

    for step in range(1, GROUP):
        small_spread(step).wait()
    value = small_own[2]
    for step in range(1, GROUP):
        value = value + small_all[step - 1]
    small_final[...] = value
    for j in range(GROUP):
        for part in range(3):
            at = part * D + j * PAIR
            qkv_final[:, at : at + PAIR] = pair_final[j, :, part * PAIR : (part + 1) * PAIR]

    for e in order:
        for part in range(3):
            block_copy(e, part).wait_send()
    for there, forward in ((has_next, True), (has_prev, False)):

        @pl.when(there)
        def _():
            for i in range(half_group):
                for part in range(2):
                    halo_copy(i if forward else i + half_group, part, forward).wait_send()


def wrap_up(replicas, moved, act, pairs, tokens, residual, gain, small, rest, shapes):
    chunks = rest.shape[0]
    tok_rows = act.shape[0]
    tall = small.shape[1]
    anywhere = pl.BlockSpec(memory_space=pl.ANY)
    vmem = pl.BlockSpec(memory_space=pltpu.VMEM)
    dma = pltpu.SemaphoreType.DMA
    low = jnp.bfloat16
    shape = jax.ShapeDtypeStruct
    pair = 3 * PAIR
    return pl.pallas_call(
        functools.partial(finish_kernel, replicas),
        out_shape=(shape((tok_rows, D), low),)
        + tuple(shape(size, low) for size in shapes)
        + (shape((D // 4, 3 * D), low), shape((tall, PAIR), jnp.float32)),
        in_specs=[vmem] * 4 + [anywhere] + [vmem] * 4 + [anywhere],
        out_specs=(vmem,) * 5,
        scratch_shapes=pipe_shapes(chunks, 2, *rest.shape[2:], True)
        + pipe_shapes(GROUP, 4, D // 4, pair, False)
        + [
            pltpu.VMEM((2, GROUP * tok_rows, PAIR), low),
            pltpu.VMEM((GROUP, 2, tok_rows, PAIR), low),
            pltpu.VMEM((GROUP, tok_rows, pair), low),
            pltpu.VMEM((2, D, pair), low),
            pltpu.VMEM((D, tok_rows), low),
            pltpu.VMEM((tok_rows, D), jnp.float32),
            pltpu.VMEM((4, tall, PAIR), jnp.float32),
            pltpu.VMEM((3, tall, PAIR), jnp.float32),
            pltpu.VMEM((2, tall, PAIR), jnp.float32),
            pltpu.VMEM((tall, PAIR), jnp.float32),
            pltpu.VMEM((GROUP - 1, tall, PAIR), jnp.float32),
            dma((2, GROUP, 2)),
            dma((2, GROUP, 3)),
            dma((2,)),
            dma((2, GROUP + 2)),
        ],
        compiler_params=pltpu.CompilerParams(
            collective_id=1, has_side_effects=True, vmem_limit_bytes=67043328
        ),
        cost_estimate=pl.CostEstimate(
            flops=12 * tok_rows * D * D, transcendentals=0, bytes_accessed=200 << 20
        ),
        name="finish",
    )(*moved, act, pairs, tokens, residual, gain, small, rest)


def shards(
    tokens,
    out_grad,
    norm1_gain,
    norm1_bias,
    w_qkv,
    q_bias,
    v_bias,
    w_out,
    out_bias,
    attn_scale,
    norm2_gain,
    norm2_bias,
    w_up,
    up_bias,
    w_down,
    down_bias,
    mlp_scale,
    image_ids,
    pad_mask,
):
    both = ("fsdp", "rep")
    owners = lax.axis_size("fsdp")
    replicas = lax.axis_size("rep")
    tok_rows = tokens.shape[0]
    rows = GROUP * tok_rows
    groups = [list(range(g, g + GROUP)) for g in range(0, replicas, GROUP)]
    factor = HEAD_DIM ** (-0.5)

    small = (
        norm1_gain,
        norm1_bias,
        q_bias,
        v_bias,
        out_bias,
        attn_scale,
        norm2_gain,
        norm2_bias,
        down_bias,
        mlp_scale,
        up_bias,
    )
    share = norm1_gain.shape[0]
    lines = list(small[:-1]) + list(up_bias.reshape(-1, share))
    line_at = lax.broadcasted_iota(jnp.int32, (-(-len(lines) // 8) * 8, share), 0)
    packed = jnp.zeros(line_at.shape, jnp.bfloat16)
    for at, member in enumerate(lines):
        packed = jnp.where(line_at == at, member[None], packed)
    packed = packed.astype(jnp.float32)
    codes = jnp.where(pad_mask > 0, image_ids + 1, 0).astype(jnp.float32).reshape(-1, PAIR)
    code_rows = codes.shape[0]
    codes = jnp.pad(codes, ((0, 8 - code_rows), (0, 0)))
    act_one, query, key_window, value_window, codes, vectors, w_pairs, out_across, up_half = project(
        replicas, tokens, packed, codes, w_qkv, w_out, w_up
    )
    window = key_window.shape[0]
    halo = rows // 2
    seen = codes[:, :code_rows].reshape(-1).astype(jnp.int32)
    seen = jnp.concatenate([seen, jnp.zeros((KEYS,), jnp.int32)])
    spot = jnp.arange(window, dtype=jnp.int32)
    asked = seen[halo : halo + rows]
    tile_codes = asked.reshape(rows // BLOCK, BLOCK)
    first_code = jnp.min(jnp.where(tile_codes > 0, tile_codes, 1 << 30), axis=1)
    last_code = jnp.max(tile_codes, axis=1)
    begin = jnp.min(jnp.where(seen[None] == first_code[:, None], spot[None], window), axis=1)
    finish = jnp.max(jnp.where(seen[None] == last_code[:, None], spot[None] + 1, 0), axis=1)
    begin = begin // 128 * 128
    count = jnp.where(last_code > 0, (finish - begin + KEYS - 1) // KEYS, 0)
    meta = jnp.stack([begin, count], axis=1).reshape(-1)

    lane_slot = jnp.arange(PAIR, dtype=jnp.int32) % HEAD_DIM
    key_slot = jnp.where(seen > 0, 1 + (seen - 1) % SLOTS, 0)
    marks = (key_slot[:, None] == lane_slot[None]).astype(jnp.bfloat16)


    deep = w_down.shape[0]
    side = deep // 2 + lax.axis_index("rep") % 2 * (deep // 4)
    down_most = jnp.concatenate(
        [w_down[: deep // 2], lax.dynamic_slice_in_dim(w_down, side, deep // 4, 0)], axis=0
    )
    down_late, query = lax.optimization_barrier((down_most, query))
    down_across = lax.ppermute(down_late, "fsdp", [(f, (f + 2) % 4) for f in range(4)])
    swapped = [(r, r + 1 - 2 * (r % 2)) for r in range(replicas)]
    up_other = lax.ppermute(up_half, "rep", swapped)
    attn_mine, attn_t, lse = attend(meta, query, key_window, value_window, marks)

    layer_out, residual_grad, grad_mine, packed, up_out, rest = middle(
        attn_mine,
        tokens,
        out_grad,
        vectors,
        (w_out, out_across, w_up, up_half, up_other, w_down, down_across),
    )
    up_theirs = lax.ppermute(up_out, "rep", swapped)
    dq, dk, dv = attend_back(
        meta, query, key_window, value_window, marks, grad_mine, attn_t, lse
    )
    tokens_grad, *grads, packed = wrap_up(
        replicas,
        (dq, dk, dv),
        act_one,
        w_pairs,
        tokens,
        residual_grad,
        vectors,
        packed,
        rest,
        (w_down.shape, w_out.shape),
    )
    half = jnp.arange(2).reshape(1, 2, 1, 1) == lax.axis_index("rep") % 2
    up_out = jnp.where(half, up_out[:, None], up_theirs[:, None]).reshape(w_up.shape)
    grads.insert(1, up_out)
    grads = [grad.astype(jnp.float32) for grad in grads]
    if replicas > GROUP:
        apart = [list(range(low, replicas, GROUP)) for low in range(GROUP)]
        grads = lax.psum(grads, "rep", axis_index_groups=apart)
        packed = lax.psum(packed, "rep", axis_index_groups=apart)
    packed = packed.reshape(-1)
    small_out = []
    place = 0
    for member in (norm1_gain, norm1_bias, q_bias, v_bias) + small[4:]:
        size = member.shape[0]
        small_out.append(packed[place : place + size])
        place += size

    down_out, up_out, out_out, qkv_out = grads
    return (
        layer_out,
        tokens_grad,
        small_out[0],
        small_out[1],
        qkv_out,
        small_out[2],
        small_out[3],
        out_out,
        small_out[4],
        small_out[5],
        small_out[6],
        small_out[7],
        up_out,
        small_out[10],
        down_out,
        small_out[8],
        small_out[9],
    )


def solution(mesh):
    spread = P(("fsdp", "rep"), None)
    line = P("fsdp")
    plane = P("fsdp", None)
    return jax.shard_map(
        shards,
        mesh=mesh,
        in_specs=(
            spread,
            spread,
            line,
            line,
            plane,
            line,
            line,
            plane,
            line,
            line,
            line,
            line,
            plane,
            line,
            plane,
            line,
            line,
            P(("fsdp", "rep")),
            P(("fsdp", "rep")),
        ),
        out_specs=(
            spread,
            spread,
            line,
            line,
            plane,
            line,
            line,
            plane,
            line,
            line,
            line,
            line,
            plane,
            line,
            plane,
            line,
            line,
        ),
        check_vma=False,
    )
```
